32 devices in a mesh: section: 2 (over y), gx: 4 (over z), gy: 4 (over x, core).
Axes of the slice: x: 2, y: 2, z: 4, core: 2. Of those that a mesh axis runs over, the one named last changes fastest.
Arguments:
- load_index: int32 [2], P('section'), may hold values from 0 to 63
- load_table: float32 [64, 3], replicated, may hold values from -4 to 4
- toughness: float32 [2, 64, 64, 128], P('section', 'gx', 'gy'), may hold values from 0.3 to 3
- clamp_mask: int32 [64, 64, 128], P('gx', 'gy'), may hold values 0 or 1
- load_mask: int32 [64, 64, 128], P('gx', 'gy'), may hold values 0 or 1
- crack_mask: int32 [64, 64, 128], P('gx', 'gy'), may hold values 0 or 1
Outputs:
- displacement: float32 [2, 3, 64, 64, 128], P('section', None, 'gx', 'gy')
- damage: float32 [2, 64, 64, 128], P('section', 'gx', 'gy')
- section_residuals: float32 [2, 2], P('section')
The draws below stay inside these ranges and needn't reach their ends.
All inputs are finite; a program needn't handle non-finite values. No bound on the sum of `clamp_mask` or of `load_mask` or of `crack_mask` on one device may be relied on, other than what follows from the above.
Results may differ from the reference program's by a relative error of at most 0.0003.
Values sent between devices are 32-bit elements; how exact they have to be, the bound alone decides.
A program may use at most 64 MiB of HBM per device.

```python
import math
import jax
import jax.numpy as jnp
from jax import lax

CASE_DEV = 1
LOADS = 64
CASES = 2
SECTIONS = 2
NX = 64
NY = 64
NZ = 128
N_SECTION = 2


def with_ends(array, rng, low, high):
    dims = array.shape
    spot = [jax.random.randint(jax.random.fold_in(rng, axis), (), 0, dims[axis]) for axis in range(len(dims))]
    array = array.at[tuple(spot)].set(low)
    longest = dims.index(max(dims))
    spot[longest] = (spot[longest] + 1) % dims[longest]
    return array.at[tuple(spot)].set(high)


def steps_of(key, dims, cuts, least, high):
    def one(position, blocks):
        heights = jax.random.uniform(jax.random.fold_in(jax.random.fold_in(key, 6), position), (blocks,), jnp.float32, least / len(cuts), high / len(cuts))
        return jnp.repeat(jnp.exp(heights), dims[position] // blocks).reshape((-1,) + (1,) * (len(dims) - position - 1))

    level = one(*cuts[0])
    for cut in cuts[1:]:
        level = level * one(*cut)
    return level


def centred(stream_key, dims, scale, most, kind=jnp.bfloat16):
    values = jax.random.normal(stream_key, dims, jnp.float32) * scale
    return jnp.minimum(jnp.maximum(values, -most), most).astype(kind)


def setup_inputs(seed: int = 0) -> dict:
    keys = jax.random.split(jax.random.key(seed), 7)
    return {
        "load_index": jax.random.randint(keys[0], (CASES,), 0, LOADS).astype(jnp.int32),
        "load_table": centred(keys[1], (LOADS, 3), 1.0, 4.0, jnp.float32),
        "toughness": jnp.clip(jnp.exp(math.log(3.0) - 2.3025851 * jax.random.uniform(keys[2], (SECTIONS, NX, NY, NZ), jnp.float32) ** steps_of(keys[2], (SECTIONS, NX, NY, NZ), ((0, 2), (1, 4), (2, 4)), -0.2, 0.2)), 0.3, 3.0),
        "clamp_mask": with_ends((jax.random.randint(keys[3], (NX, NY, NZ), 0, 8) < 1).astype(jnp.int32), jax.random.fold_in(keys[3], 1), 0, 1),
        "load_mask": with_ends((jax.random.randint(keys[4], (NX, NY, NZ), 0, 8) < 1).astype(jnp.int32), jax.random.fold_in(keys[4], 1), 0, 1),
        "crack_mask": with_ends((jax.random.randint(keys[5], (NX, NY, NZ), 0, 32) < 1).astype(jnp.int32), jax.random.fold_in(keys[5], 1), 0, 1),
    }


lame_lambda = 1.0
shear_modulus = 1.0
relax_weight = 0.6
stiff_floor = 0.001
eigen_guard = 1e-08
neighbour_offsets = ((1, 0, 0), (-1, 0, 0), (0, 1, 0), (0, -1, 0), (0, 0, 1), (0, 0, -1))

def unit_offset(axis_index, sign):
    return tuple((sign if other == axis_index else 0 for other in range(3)))

def shifted(padded, offset):
    span_first = padded.shape[-3] - 2
    span_second = padded.shape[-2] - 2
    span_third = padded.shape[-1] - 2
    return padded[..., 1 + offset[0]:1 + offset[0] + span_first, 1 + offset[1]:1 + offset[1] + span_second, 1 + offset[2]:1 + offset[2] + span_third]

def component(field, index):
    return field[..., index, :, :, :]

def elastic_parts(moved_pad, damage_pad):
    stiff_pad = jnp.square(1.0 - damage_pad) + stiff_floor
    centre = shifted(stiff_pad, (0, 0, 0))
    current = shifted(moved_pad, (0, 0, 0))
    laplace = jnp.zeros_like(current)
    weights = jnp.zeros_like(centre)
    for offset in neighbour_offsets:
        face = 0.5 * (centre + shifted(stiff_pad, offset))
        weights = weights + face
        laplace = laplace + jnp.expand_dims(face, -4) * (shifted(moved_pad, offset) - current)
    divergence = jnp.zeros_like(centre)
    pairs = []
    for axis_index in range(3):
        forward = unit_offset(axis_index, 1)
        backward = unit_offset(axis_index, -1)
        part = component(moved_pad, axis_index)
        divergence = divergence + 0.5 * (shifted(part, forward) - shifted(part, backward))
        pairs.append(shifted(stiff_pad, forward) + shifted(stiff_pad, backward))
    flow = centre * divergence
    diagonal = shear_modulus * jnp.expand_dims(weights, -4) + 0.25 * (lame_lambda + shear_modulus) * jnp.stack(pairs, axis=-4)
    return (current, laplace, flow, diagonal)

def flow_gradient(flow_pad):
    parts = [0.5 * (shifted(flow_pad, unit_offset(axis_index, 1)) - shifted(flow_pad, unit_offset(axis_index, -1))) for axis_index in range(3)]
    return jnp.stack(parts, axis=-4)

def spectral_energy(strain_xx, strain_yy, strain_zz, strain_xy, strain_xz, strain_yz):
    middle_value = (strain_xx + strain_yy + strain_zz) / 3.0
    dev_xx = strain_xx - middle_value
    dev_yy = strain_yy - middle_value
    dev_zz = strain_zz - middle_value
    shear_sum = jnp.square(strain_xy) + jnp.square(strain_xz) + jnp.square(strain_yz)
    spread = jnp.square(dev_xx) + jnp.square(dev_yy) + jnp.square(dev_zz) + 2.0 * shear_sum
    radius = jnp.sqrt(spread / 6.0)
    guarded = spread / 6.0 + eigen_guard
    determinant = dev_xx * (dev_yy * dev_zz - jnp.square(strain_yz)) - strain_xy * (strain_xy * dev_zz - strain_yz * strain_xz) + strain_xz * (strain_xy * strain_yz - dev_yy * strain_xz)
    ratio = jnp.clip(determinant / (2.0 * guarded * jnp.sqrt(guarded)), -1.0, 1.0)
    angle = jnp.arccos(ratio) / 3.0
    largest = middle_value + 2.0 * radius * jnp.cos(angle)
    smallest = middle_value + 2.0 * radius * jnp.cos(angle + 2.0 * jnp.pi / 3.0)
    between = 3.0 * middle_value - largest - smallest
    positive = jnp.square(jax.nn.relu(largest)) + jnp.square(jax.nn.relu(between)) + jnp.square(jax.nn.relu(smallest))
    return 0.5 * lame_lambda * jnp.square(jax.nn.relu(3.0 * middle_value)) + shear_modulus * positive

def damage_update(moved_pad, damage_pad, toughness_cell, crack_cell):
    grads = [[0.5 * (shifted(component(moved_pad, first), unit_offset(second, 1)) - shifted(component(moved_pad, first), unit_offset(second, -1))) for second in range(3)] for first in range(3)]
    energy = spectral_energy(grads[0][0], grads[1][1], grads[2][2], 0.5 * (grads[0][1] + grads[1][0]), 0.5 * (grads[0][2] + grads[2][0]), 0.5 * (grads[1][2] + grads[2][1]))
    beside_all = jnp.zeros_like(energy)
    for offset in neighbour_offsets:
        beside_all = beside_all + shifted(damage_pad, offset)
    updated = (2.0 * energy + toughness_cell * beside_all) / (toughness_cell + 2.0 * energy + 6.0 * toughness_cell)
    return jnp.where(crack_cell > 0.5, 1.0, updated)

def pad_all(field):
    return jnp.pad(field, [(0, 0)] * (field.ndim - 3) + [(1, 1), (1, 1), (1, 1)])

def sweep(moved, damage, load_vector, toughness_cell, fixed, load, crack):
    damage_pad = pad_all(damage)
    current, laplace, flow, diagonal = elastic_parts(pad_all(moved), damage_pad)
    gradient = flow_gradient(pad_all(flow))
    residual = shear_modulus * laplace + (lame_lambda + shear_modulus) * gradient
    prescribed = load[None] * load_vector[:, None, None, None]
    relaxed = current + relax_weight * residual / diagonal
    new_moved = jnp.where(fixed[None] > 0.5, prescribed, relaxed)
    squares = jnp.sum((1.0 - fixed)[None] * jnp.square(residual))
    new_damage = damage_update(pad_all(new_moved), damage_pad, toughness_cell, crack)
    return (new_moved, new_damage, squares)

def reference(load_index, load_table, toughness, clamp_mask, load_mask, crack_mask):
    clamp = clamp_mask.astype(jnp.float32)
    load = load_mask.astype(jnp.float32)
    crack = crack_mask.astype(jnp.float32)
    fixed = jnp.maximum(clamp, load)
    cells = float(NX * NY * NZ)
    columns = jnp.arange(N_SECTION, dtype=jnp.int32)

    def one_case(item):
        case_index, table_row = item
        load_vector = load_table[table_row]
        home = (case_index // CASE_DEV).astype(jnp.int32)
        moved = load[None] * load_vector[:, None, None, None]
        norms = jnp.zeros((N_SECTION,), jnp.float32)

        def advance(round_index, carry):
            moved_now, damage_now, norms_now = carry
            section_index = ((home + round_index) % N_SECTION).astype(jnp.int32)
            field = lax.dynamic_index_in_dim(toughness, section_index, 0, keepdims=False)
            moved_next, damage_next, squares = sweep(moved_now, damage_now, load_vector, field, fixed, load, crack)
            entry = jnp.sqrt(squares / (3.0 * cells))
            norms_next = norms_now + (columns == section_index).astype(jnp.float32) * entry
            return (moved_next, damage_next, norms_next)
        return lax.fori_loop(0, N_SECTION, advance, (moved, crack, norms))
    moved, damage, norms = lax.map(one_case, (jnp.arange(CASES, dtype=jnp.int32), load_index))
    return (moved, damage, norms)
```

```python
import functools
import math

import jax
import jax.numpy as jnp
from jax import lax
from jax.experimental import pallas as pl
from jax.experimental.pallas import tpu as pltpu
from jax.sharding import PartitionSpec as P

relax_weight = 0.6
stiff_floor = 0.001
eigen_guard = 1e-08
MESH = pl.DeviceIdType.MESH

HX = 3
OY = 8

ACOS = (
    1.5707963050,
    -0.2145988016,
    0.0889789874,
    -0.0501743046,
    0.0308918810,
    -0.0170881256,
    0.0066700901,
    -0.0012624911,
)


def up8(n):
    return -(-n // 8) * 8


def part(n, most):
    return max(k for k in range(1, most + 1) if n % k == 0)


def spectral_energy(xx, yy, zz, xy, xz, yz):
    trace = xx + yy + zz
    mid = trace * (1.0 / 3.0)
    dx = xx - mid
    dy = yy - mid
    dz = zz - mid
    xy2 = xy * xy
    xz2 = xz * xz
    yz2 = yz * yz
    sixth = (dx * dx + dy * dy + dz * dz + 2.0 * (xy2 + xz2 + yz2)) * (1.0 / 6.0)
    twice_radius = 2.0 * jnp.sqrt(sixth)
    guarded = sixth + eigen_guard
    det = dx * (dy * dz - yz2) - dz * xy2 - dy * xz2 + 2.0 * (xy * xz * yz)
    ratio = det / (2.0 * guarded * jnp.sqrt(guarded))
    size = jnp.minimum(jnp.abs(ratio), 1.0)
    poly = jnp.full_like(size, ACOS[-1] / 3.0)
    for c in ACOS[-2::-1]:
        poly = poly * size + c / 3.0
    t = jnp.sqrt(1.0 - size) * poly
    t2 = t * t
    cos_t = 1.0 + t2 * (-0.5 + t2 * (1.0 / 24.0 + t2 * (-1.0 / 720.0 + t2 * (1.0 / 40320.0))))
    sin_t = t * (1.0 + t2 * (-1.0 / 6.0 + t2 * (1.0 / 120.0 + t2 * (-1.0 / 5040.0))))
    other = 0.5 * cos_t + math.sqrt(0.75) * sin_t
    upper = ratio >= 0.0
    first = jnp.where(upper, cos_t, other)
    last = jnp.where(upper, other, cos_t)
    largest = mid + twice_radius * first
    smallest = mid - twice_radius * last
    between = trace - largest - smallest
    relu = lambda v: jnp.maximum(v, 0.0)
    return (
        0.5 * jnp.square(relu(trace))
        + jnp.square(relu(largest))
        + jnp.square(relu(between))
        + jnp.square(relu(smallest))
    )


def kernel(
    sizes,
    index_hbm,
    table_hbm,
    tough_hbm,
    clamp_hbm,
    load_hbm,
    crack_hbm,
    first_ref,
    second_ref,
    third_ref,
    dam_ref,
    norm_ref,
    index_ref,
    table_ref,
    tough_ref,
    clamp_ref,
    load_ref,
    crack_ref,
    local,
    state,
    stiff,
    flow,
    held,
    pinned,
    free,
    tough_in,
    pack_mask,
    pack_u,
    pack_d,
    in_mask_x,
    in_mask_y,
    in_mask_c,
    in_u_x,
    in_u_x3,
    in_u_y,
    in_u_c,
    in_d_x,
    in_d_y,
    in_d_c,
    sums,
    mask_send,
    mask_recv,
    u_send,
    u_recv,
    d_send,
    d_recv,
    tough_send,
    tough_recv,
    sum_send,
    sum_recv,
):
    sections, ngx, ngy, nx, ny, nz = sizes
    disp_refs = (first_ref, second_ref, third_ref)
    sec = lax.axis_index("section")
    gx = lax.axis_index("gx")
    gy = lax.axis_index("gy")
    group = ngx * ngy
    me = gx * ngy + gy
    peers = []
    for k in range(1, group):
        other = lax.rem(me + k, group)
        peers.append({"gx": other // ngy, "gy": lax.rem(other, ngy)})

    fetch = [
        pltpu.make_async_copy(src, dst, local.at[n])
        for n, (src, dst) in enumerate(
            (
                (load_hbm, load_ref),
                (crack_hbm, crack_ref),
                (clamp_hbm, clamp_ref),
                (tough_hbm, tough_ref),
                (index_hbm, index_ref),
                (table_hbm, table_ref),
            )
        )
    ]
    for copy in fetch:
        copy.start()

    barrier = pltpu.get_barrier_semaphore()
    for peer in peers:
        pl.semaphore_signal(barrier, inc=1, device_id=peer, device_id_type=MESH)
    for k in range(1, sections):
        pl.semaphore_signal(
            barrier,
            inc=1,
            device_id={"section": lax.rem(sec + k, sections)},
            device_id_type=MESH,
        )

    there = {
        "gx": (gx > 0, gx < ngx - 1),
        "gy": (gy > 0, gy < ngy - 1),
    }
    step = (-1, 1)

    def x_dev(s):
        return there["gx"][s], {"gx": gx + step[s]}

    def y_dev(s):
        return there["gy"][s], {"gy": gy + step[s]}

    def c_dev(sx, sy):
        return (
            jnp.logical_and(there["gx"][sx], there["gy"][sy]),
            {"gx": gx + step[sx], "gy": gy + step[sy]},
        )

    class Exchange:
        def __init__(self, send, recv):
            self.items = []
            self.send = send
            self.recv = recv

        def add(self, where, src, dst, mine, out_slot, in_slot):
            cond, dev = where
            n = len(self.items)
            copy = pltpu.make_async_remote_copy(
                src_ref=src,
                dst_ref=dst,
                send_sem=self.send.at[n],
                recv_sem=self.recv.at[out_slot],
                device_id=dev,
                device_id_type=MESH,
            )
            back = pltpu.make_async_remote_copy(
                src_ref=src,
                dst_ref=mine,
                send_sem=self.send.at[n],
                recv_sem=self.recv.at[in_slot],
                device_id=dev,
                device_id_type=MESH,
            )
            self.items.append((cond, copy, back))

        def start(self):
            for cond, copy, _ in self.items:
                pl.when(cond)(copy.start)

        def finish(self):
            for cond, copy, back in self.items:

                @pl.when(cond)
                def _():
                    back.wait_recv()
                    copy.wait_send()

    rows = ny + 2 * OY

    def clear(xp, carry):
        zero = jnp.zeros((rows, nz), jnp.float32)
        for f in range(4):
            state[1, f, xp] = zero
        state[0, 3, xp] = zero
        held[xp] = zero
        pinned[xp] = zero + 1.0
        free[xp] = zero
        return carry

    lax.fori_loop(0, nx + 2 * HX, clear, 0)

    for copy in fetch:
        copy.wait()

    pack_mask[0, :, 0:3, :] = load_ref[:, 0:3, :]
    pack_mask[0, :, 3:5, :] = crack_ref[:, 0:2, :]
    pack_mask[0, :, 5:6, :] = clamp_ref[:, 0:1, :]
    pack_mask[1, :, 0:3, :] = load_ref[:, ny - 3 : ny, :]
    pack_mask[1, :, 3:5, :] = crack_ref[:, ny - 2 : ny, :]
    pack_mask[1, :, 5:6, :] = clamp_ref[:, ny - 1 : ny, :]

    pl.semaphore_wait(barrier, group - 1 + sections - 1)

    masks = Exchange(mask_send, mask_recv)
    for s in range(2):
        for j, (ref, width, at) in enumerate(
            ((load_ref, 3, 0), (crack_ref, 2, 3), (clamp_ref, 1, 5))
        ):
            first = 0 if s == 0 else nx - width
            masks.add(
                x_dev(s),
                ref.at[pl.ds(first, width)],
                in_mask_x.at[1 - s, pl.ds(at, width)],
                in_mask_x.at[s, pl.ds(at, width)],
                (1 - s) * 3 + j,
                s * 3 + j,
            )
    for s in range(2):
        masks.add(
            y_dev(s), pack_mask.at[s], in_mask_y.at[1 - s], in_mask_y.at[s], 6 + 1 - s, 6 + s
        )
    for sx in range(2):
        for sy in range(2):
            masks.add(
                c_dev(sx, sy),
                pack_mask.at[sy, pl.ds(0 if sx == 0 else nx - 2, 2)],
                in_mask_c.at[(1 - sx) * 2 + 1 - sy],
                in_mask_c.at[sx * 2 + sy],
                8 + (1 - sx) * 2 + 1 - sy,
                8 + sx * 2 + sy,
            )
    masks.start()

    tough_copies = []
    for k in range(1, sections):
        copy = pltpu.make_async_remote_copy(
            src_ref=tough_ref.at[0],
            dst_ref=tough_in.at[k - 1],
            send_sem=tough_send.at[k - 1],
            recv_sem=tough_recv.at[k - 1],
            device_id={"section": lax.rem(sec + sections - k, sections)},
            device_id_type=MESH,
        )
        copy.start()
        tough_copies.append(copy)

    inner = slice(OY, OY + ny)

    def fill(x, carry):
        load = load_ref[x].astype(jnp.float32)
        fixed = jnp.maximum(clamp_ref[x].astype(jnp.float32), load)
        held[x + HX, inner] = load
        pinned[x + HX, inner] = fixed
        free[x + HX, inner] = 1.0 - fixed
        state[0, 3, x + HX, inner] = crack_ref[x].astype(jnp.float32)
        return carry

    lax.fori_loop(0, nx, fill, 0)

    case = index_ref[0]
    vector = [table_ref[f, case] for f in range(3)]

    masks.finish()
    as_float = lambda v: v.astype(jnp.float32)
    planes = slice(HX, HX + nx)
    x_far = (slice(HX - 3, HX), slice(HX + nx, HX + nx + 3))
    x_two = (slice(HX - 2, HX), slice(HX + nx, HX + nx + 2))
    x_one = (slice(HX - 1, HX), slice(HX + nx, HX + nx + 1))
    y_far = (slice(OY - 3, OY), slice(OY + ny, OY + ny + 3))
    y_two = (slice(OY - 2, OY), slice(OY + ny, OY + ny + 2))
    y_one = (slice(OY - 1, OY), slice(OY + ny, OY + ny + 1))
    for s in range(2):

        @pl.when(there["gx"][s])
        def _(s=s):
            load = as_float(in_mask_x[s, 0:3])
            near = slice(2, 3) if s == 0 else slice(0, 1)
            held[x_far[s], inner] = load
            state[0, 3, x_two[s], inner] = as_float(in_mask_x[s, 3:5])
            pinned[x_one[s], inner] = jnp.maximum(load[near], as_float(in_mask_x[s, 5:6]))

        @pl.when(there["gy"][s])
        def _(s=s):
            held[planes, y_far[s]] = as_float(in_mask_y[s, :, 0:3])
            state[0, 3, planes, y_two[s]] = as_float(in_mask_y[s, :, 3:5])
            near = slice(2, 3) if s == 0 else slice(0, 1)
            pinned[planes, y_one[s]] = jnp.maximum(
                as_float(in_mask_y[s, :, near]), as_float(in_mask_y[s, :, 5:6])
            )

    for sx in range(2):
        for sy in range(2):

            @pl.when(c_dev(sx, sy)[0])
            def _(sx=sx, sy=sy):
                near = slice(1, 3) if sy == 0 else slice(0, 2)
                held[x_two[sx], y_two[sy]] = as_float(in_mask_c[sx * 2 + sy, :, near])
                state[0, 3, x_two[sx], y_two[sy]] = as_float(in_mask_c[sx * 2 + sy, :, 3:5])

    def begin(xp, carry):
        load = held[xp]
        for f in range(3):
            state[0, f, xp] = load * vector[f]
        return carry

    lax.fori_loop(0, nx + 2 * HX, begin, 0)

    wide = up8(ny + 4)
    near = up8(ny + 2)

    def lanes(shape, lane):
        return lax.broadcasted_iota(jnp.int32, shape, 1) == lane

    def beside(v, edge, first, last):
        up = jnp.where(last, edge, pltpu.roll(v, nz - 1, 1))
        down = jnp.where(first, edge, pltpu.roll(v, 1, 1))
        return up, down

    def sweep(rnd):
        p = rnd % 2
        q = 1 - p
        done = rnd == sections - 1
        tough = tough_ref.at[0] if rnd == 0 else tough_in.at[rnd - 1]

        shape = (wide, nz)
        first, last = lanes(shape, 0), lanes(shape, nz - 1)
        row = lax.broadcasted_iota(jnp.int32, shape, 0) + (gy * ny - 2)
        row_inside = jnp.logical_and(row >= 0, row < ny * ngy)
        a = OY - 2

        def stiffen(xp, carry):
            d = state[p, 3, xp, a : a + wide]
            half = 0.5 * (jnp.square(1.0 - d) + stiff_floor)
            stiff[xp, a : a + wide] = half
            up, down = beside(state[p, 2, xp, a : a + wide], 0.0, first, last)
            div = (
                (state[p, 0, xp + 1, a : a + wide] - state[p, 0, xp - 1, a : a + wide])
                + (state[p, 1, xp, a + 1 : a + 1 + wide] - state[p, 1, xp, a - 1 : a - 1 + wide])
                + (up - down)
            )
            plane = xp - HX + gx * nx
            ok = jnp.logical_and(plane >= 0, plane < nx * ngx)
            flow[xp, a : a + wide] = jnp.where(
                jnp.logical_and(row_inside, ok), half * div, 0.0
            )
            return carry

        lax.fori_loop(HX - 2, HX + nx + 2, stiffen, 0, unroll=part(nx + 4, 10))

        shape = (near, nz)
        first, last = lanes(shape, 0), lanes(shape, nz - 1)
        b = OY - 1

        def move(xp, total):
            at = lambda ref, dx, dy: ref[xp + dx, b + dy : b + dy + near]
            k = at(stiff, 0, 0)
            edge = 0.5 * (1.0 + stiff_floor)
            kz = beside(k, edge, first, last)
            kx = (at(stiff, 1, 0), at(stiff, -1, 0))
            ky = (at(stiff, 0, 1), at(stiff, 0, -1))
            sides = (kx, ky, kz)
            pairs = [s[0] + s[1] for s in sides]
            weights = pairs[0] + pairs[1] + pairs[2] + 6.0 * k
            faces = [(k + s[0], k + s[1]) for s in sides]
            grads = (
                at(flow, 1, 0) - at(flow, -1, 0),
                at(flow, 0, 1) - at(flow, 0, -1),
                None,
            )
            fz = beside(at(flow, 0, 0), 0.0, first, last)
            grads = (grads[0], grads[1], fz[0] - fz[1])
            pin = at(pinned, 0, 0) > 0.5
            load = at(held, 0, 0)
            squares = None
            for f in range(3):
                u = state.at[p, f]
                here = at(u, 0, 0)
                uz = beside(here, 0.0, first, last)
                res = (
                    faces[0][0] * at(u, 1, 0)
                    + faces[0][1] * at(u, -1, 0)
                    + faces[1][0] * at(u, 0, 1)
                    + faces[1][1] * at(u, 0, -1)
                    + faces[2][0] * uz[0]
                    + faces[2][1] * uz[1]
                    - weights * here
                    + grads[f]
                )
                moved = here + relax_weight * res / (weights + pairs[f])
                state[q, f, xp, b : b + near] = jnp.where(pin, load * vector[f], moved)
                square = res * res
                squares = square if squares is None else squares + square
            return total + jnp.where(at(free, 0, 0) > 0.5, squares, 0.0)

        total = lax.fori_loop(
            HX - 1, HX + nx + 1, move, jnp.zeros(shape, jnp.float32), unroll=part(nx + 2, 6)
        )
        sums[rnd, me] = jnp.sum(total, axis=0, keepdims=True)
        par = rnd % 2
        if not done:
            for f in range(3):
                pack_u[0, :, 2 * f : 2 * f + 2] = state[q, f, planes, OY : OY + 2]
                pack_u[1, :, 2 * f : 2 * f + 2] = state[q, f, planes, OY + ny - 2 : OY + ny]
            pack_u[0, :, 6:7] = state[q, 1, planes, OY + 2 : OY + 3]
            pack_u[1, :, 6:7] = state[q, 1, planes, OY + ny - 3 : OY + ny - 2]
            shift = Exchange(u_send, u_recv.at[par])
            mid = pl.ds(OY, ny)
            for s in range(2):
                shift.add(
                    x_dev(s),
                    state.at[q, pl.ds(0, 3), pl.ds(HX if s == 0 else HX + nx - 2, 2), mid],
                    in_u_x.at[par, 1 - s],
                    in_u_x.at[par, s],
                    (1 - s),
                    s,
                )
                shift.add(
                    x_dev(s),
                    state.at[q, 0, HX + 2 if s == 0 else HX + nx - 3, mid],
                    in_u_x3.at[par, 1 - s],
                    in_u_x3.at[par, s],
                    2 + (1 - s),
                    2 + s,
                )
            for s in range(2):
                shift.add(
                    y_dev(s),
                    pack_u.at[s],
                    in_u_y.at[par, 1 - s],
                    in_u_y.at[par, s],
                    4 + (1 - s),
                    4 + s,
                )
            for sx in range(2):
                for sy in range(2):
                    shift.add(
                        c_dev(sx, sy),
                        pack_u.at[sy, pl.ds(0 if sx == 0 else nx - 2, 2)],
                        in_u_c.at[par, (1 - sx) * 2 + 1 - sy],
                        in_u_c.at[par, sx * 2 + sy],
                        6 + (1 - sx) * 2 + 1 - sy,
                        6 + sx * 2 + sy,
                    )
            shift.start()

        for k, peer in enumerate(peers):
            pltpu.make_async_remote_copy(
                src_ref=sums.at[rnd, me],
                dst_ref=sums.at[rnd, me],
                send_sem=sum_send.at[rnd, k],
                recv_sem=sum_recv.at[rnd, me],
                device_id=peer,
                device_id_type=MESH,
            ).start()

        if rnd > 0:
            tough_copies[rnd - 1].wait_recv()

        shape = (ny, nz)
        first, last = lanes(shape, 0), lanes(shape, nz - 1)

        def damage(x, carry):
            xp = x + HX
            at = lambda ref, dx, dy: ref[xp + dx, OY + dy : OY + dy + ny]
            grad = []
            for f in range(3):
                u = state.at[q, f]
                here = at(u, 0, 0)
                uz = beside(here, 0.0, first, last)
                grad.append(
                    (at(u, 1, 0) - at(u, -1, 0), at(u, 0, 1) - at(u, 0, -1), uz[0] - uz[1])
                )
                if done:
                    disp_refs[f][x] = here
            energy = 2.0 * spectral_energy(
                0.5 * grad[0][0],
                0.5 * grad[1][1],
                0.5 * grad[2][2],
                0.25 * (grad[0][1] + grad[1][0]),
                0.25 * (grad[0][2] + grad[2][0]),
                0.25 * (grad[1][2] + grad[2][1]),
            )
            d = state.at[p, 3]
            dz = beside(at(d, 0, 0), 0.0, first, last)
            around = (
                at(d, 1, 0) + at(d, -1, 0) + at(d, 0, 1) + at(d, 0, -1) + dz[0] + dz[1]
            )
            g = tough[x]
            renewed = (energy + g * around) / (7.0 * g + energy)
            renewed = jnp.where(crack_ref[x] > 0, 1.0, renewed)
            if done:
                dam_ref[x] = renewed
            else:
                state[q, 3, xp, inner] = renewed
            return carry

        lax.fori_loop(0, nx, damage, 0, unroll=part(nx, 8))
        if done:
            return

        pack_d[0] = state[q, 3, planes, OY : OY + 2]
        pack_d[1] = state[q, 3, planes, OY + ny - 2 : OY + ny]
        crack = Exchange(d_send, d_recv.at[par])
        for s in range(2):
            crack.add(
                x_dev(s),
                state.at[q, 3, pl.ds(HX if s == 0 else HX + nx - 2, 2), mid],
                in_d_x.at[par, 1 - s],
                in_d_x.at[par, s],
                1 - s,
                s,
            )
        for s in range(2):
            crack.add(
                y_dev(s),
                pack_d.at[s],
                in_d_y.at[par, 1 - s],
                in_d_y.at[par, s],
                2 + 1 - s,
                2 + s,
            )
        for sx in range(2):
            for sy in range(2):
                crack.add(
                    c_dev(sx, sy),
                    pack_d.at[sy, pl.ds(0 if sx == 0 else nx - 1, 1)],
                    in_d_c.at[par, (1 - sx) * 2 + 1 - sy],
                    in_d_c.at[par, sx * 2 + sy],
                    4 + (1 - sx) * 2 + 1 - sy,
                    4 + sx * 2 + sy,
                )
        crack.start()
        shift.finish()
        third_x = (HX - 3, HX + nx + 2)
        third_y = (slice(OY - 3, OY - 2), slice(OY + ny + 2, OY + ny + 3))
        for s in range(2):

            @pl.when(there["gx"][s])
            def _(s=s):
                state[q, 0:3, x_two[s], inner] = in_u_x[par, s]
                state[q, 0, third_x[s], inner] = in_u_x3[par, s]

            @pl.when(there["gy"][s])
            def _(s=s):
                for f in range(3):
                    state[q, f, planes, y_two[s]] = in_u_y[par, s, :, 2 * f : 2 * f + 2]
                state[q, 1, planes, third_y[s]] = in_u_y[par, s, :, 6:7]

        for sx in range(2):
            for sy in range(2):

                @pl.when(c_dev(sx, sy)[0])
                def _(sx=sx, sy=sy):
                    for f in range(3):
                        state[q, f, x_two[sx], y_two[sy]] = in_u_c[
                            par, sx * 2 + sy, :, 2 * f : 2 * f + 2
                        ]

        crack.finish()
        for s in range(2):

            @pl.when(there["gx"][s])
            def _(s=s):
                state[q, 3, x_two[s], inner] = in_d_x[par, s]

            @pl.when(there["gy"][s])
            def _(s=s):
                state[q, 3, planes, y_two[s]] = in_d_y[par, s]

        for sx in range(2):
            for sy in range(2):

                @pl.when(c_dev(sx, sy)[0])
                def _(sx=sx, sy=sy):
                    state[q, 3, x_one[sx], y_two[sy]] = in_d_c[par, sx * 2 + sy]

    for rnd in range(sections):
        sweep(rnd)

    cells = 3.0 * nx * ngx * ny * ngy * nz
    column = lax.broadcasted_iota(jnp.int32, (1, sections), 1)
    norms = jnp.zeros((1, sections), jnp.float32)
    for rnd in range(sections):
        for k in range(1, group):
            other = lax.rem(me + k, group)
            pltpu.make_async_remote_copy(
                src_ref=sums.at[rnd, me],
                dst_ref=sums.at[rnd, other],
                send_sem=sum_send.at[rnd, k - 1],
                recv_sem=sum_recv.at[rnd, other],
                device_id=peers[k - 1],
                device_id_type=MESH,
            ).wait()
        total = sums[rnd, 0]
        for k in range(1, group):
            total = total + sums[rnd, k]
        entry = jnp.sqrt(jnp.sum(total, axis=1, keepdims=True) / cells)
        norms = jnp.where(column == lax.rem(sec + rnd, sections), entry, norms)
    norm_ref[...] = norms
    for copy in tough_copies:
        copy.wait_send()


def put_out(
    first_ref, second_ref, third_ref, dam_ref, norm_ref, disp_hbm, dam_hbm, norm_out, sems
):
    copies = [
        pltpu.make_async_copy(ref, disp_hbm.at[0, f], sems.at[f])
        for f, ref in enumerate((first_ref, second_ref, third_ref))
    ]
    copies.append(pltpu.make_async_copy(dam_ref, dam_hbm.at[0], sems.at[3]))
    for copy in copies:
        copy.start()
    norm_out[...] = norm_ref[...]
    for copy in copies:
        copy.wait()


def on_device(sizes, load_index, load_table, toughness, clamp_mask, load_mask, crack_mask):
    sections, ngx, ngy = sizes
    nx, ny, nz = clamp_mask.shape
    assert load_index.shape == (1,)
    group = ngx * ngy
    f32 = jnp.float32
    padded = (nx + 2 * HX, ny + 2 * OY, nz)
    vmem = pltpu.VMEM
    dma = pltpu.SemaphoreType.DMA
    later = max(sections - 1, 1)
    scratch = [
        pltpu.SMEM(load_index.shape, jnp.int32),
        pltpu.SMEM(load_table.shape[::-1], f32),
        vmem((1, nx, ny, nz), f32),
        vmem((nx, ny, nz), jnp.int32),
        vmem((nx, ny, nz), jnp.int32),
        vmem((nx, ny, nz), jnp.int32),
        dma((6,)),
        vmem((2, 4) + padded, f32),
        vmem(padded, f32),
        vmem(padded, f32),
        vmem(padded, f32),
        vmem(padded, f32),
        vmem(padded, f32),
        vmem((later, nx, ny, nz), f32),
        vmem((2, nx, 8, nz), jnp.int32),
        vmem((2, nx, 8, nz), f32),
        vmem((2, nx, 2, nz), f32),
        vmem((2, 6, ny, nz), jnp.int32),
        vmem((2, nx, 8, nz), jnp.int32),
        vmem((4, 2, 8, nz), jnp.int32),
        vmem((2, 2, 3, 2, ny, nz), f32),
        vmem((2, 2, ny, nz), f32),
        vmem((2, 2, nx, 8, nz), f32),
        vmem((2, 4, 2, 8, nz), f32),
        vmem((2, 2, 2, ny, nz), f32),
        vmem((2, 2, nx, 2, nz), f32),
        vmem((2, 4, 1, 2, nz), f32),
        vmem((sections, group, 1, nz), f32),
        dma((12,)),
        dma((12,)),
        dma((10,)),
        dma((2, 10)),
        dma((8,)),
        dma((2, 8)),
        dma((later,)),
        dma((later,)),
        dma((sections, max(group - 1, 1))),
        dma((sections, group)),
    ]
    block = pl.BlockSpec(memory_space=pltpu.VMEM)
    away = pl.BlockSpec(memory_space=pltpu.HBM)
    results = pl.pallas_call(
        functools.partial(kernel, (sections, ngx, ngy, nx, ny, nz)),
        out_shape=(
            *[jax.ShapeDtypeStruct((nx, ny, nz), f32)] * 4,
            jax.ShapeDtypeStruct((1, sections), f32),
        ),
        in_specs=[away] * 6,
        out_specs=(block,) * 5,
        scratch_shapes=scratch,
        compiler_params=pltpu.CompilerParams(
            collective_id=0, has_side_effects=True, vmem_limit_bytes=56_020_000
        ),
    )(load_index, load_table.T, toughness, clamp_mask, load_mask, crack_mask)
    return pl.pallas_call(
        put_out,
        out_shape=(
            jax.ShapeDtypeStruct((1, 3, nx, ny, nz), f32),
            jax.ShapeDtypeStruct((1, nx, ny, nz), f32),
            jax.ShapeDtypeStruct((1, sections), f32),
        ),
        in_specs=[block] * 5,
        out_specs=(away, away, block),
        scratch_shapes=[dma((4,))],
        compiler_params=pltpu.CompilerParams(vmem_limit_bytes=1024 * 1024),
    )(*results)


def solution(mesh):
    in_specs = (
        P("section"),
        P(),
        P("section", "gx", "gy", None),
        P("gx", "gy", None),
        P("gx", "gy", None),
        P("gx", "gy", None),
    )
    out_specs = (
        P("section", None, "gx", "gy", None),
        P("section", "gx", "gy", None),
        P("section", None),
    )
    sizes = tuple(mesh.shape[name] for name in ("section", "gx", "gy"))
    return jax.shard_map(
        functools.partial(on_device, sizes),
        mesh=mesh,
        in_specs=in_specs,
        out_specs=out_specs,
        check_vma=False,
    )
```

```python
import functools
import math
import types

import jax
import jax.numpy as jnp
from jax import lax
from jax.experimental import pallas as pl
from jax.experimental.pallas import tpu as pltpu
from jax.sharding import PartitionSpec as P

relax_weight = 0.6
stiff_floor = 0.001
eigen_guard = 1e-08
MESH = pl.DeviceIdType.MESH

HX = 5
OY = 8

ACOS = (
    1.5707963050,
    -0.2145988016,
    0.0889789874,
    -0.0501743046,
    0.0308918810,
    -0.0170881256,
    0.0066700901,
    -0.0012624911,
)


def up8(n):
    return -(-n // 8) * 8


def part(n, most):
    return max(k for k in range(1, most + 1) if n % k == 0)


def root(v):
    return v * lax.rsqrt(jnp.maximum(v, 1.2e-38))


def spectral_energy(xx, yy, zz, xy, xz, yz):
    trace = xx + yy + zz
    mid = trace * (1.0 / 3.0)
    dx = xx - mid
    dy = yy - mid
    dz = zz - mid
    xy2 = xy * xy
    xz2 = xz * xz
    yz2 = yz * yz
    sixth = (dx * dx + dy * dy + dz * dz + 2.0 * (xy2 + xz2 + yz2)) * (1.0 / 6.0)
    twice_radius = 2.0 * root(sixth)
    scale = lax.rsqrt(sixth + eigen_guard)
    det = dx * (dy * dz - yz2) - dz * xy2 - dy * xz2 + 2.0 * (xy * xz * yz)
    ratio = (0.5 * det * scale) * (scale * scale)
    size = jnp.minimum(jnp.abs(ratio), 1.0)
    poly = jnp.full_like(size, ACOS[-1] / 3.0)
    for c in ACOS[-2::-1]:
        poly = poly * size + c / 3.0
    t = root(1.0 - size) * poly
    t2 = t * t
    cos_t = 1.0 + t2 * (-0.5 + t2 * (1.0 / 24.0 + t2 * (-1.0 / 720.0 + t2 * (1.0 / 40320.0))))
    sin_t = t * (1.0 + t2 * (-1.0 / 6.0 + t2 * (1.0 / 120.0 + t2 * (-1.0 / 5040.0))))
    other = 0.5 * cos_t + math.sqrt(0.75) * sin_t
    upper = ratio >= 0.0
    first = jnp.where(upper, cos_t, other)
    last = jnp.where(upper, other, cos_t)
    largest = mid + twice_radius * first
    smallest = mid - twice_radius * last
    between = trace - largest - smallest
    relu = lambda v: jnp.maximum(v, 0.0)
    return (
        0.5 * jnp.square(relu(trace))
        + jnp.square(relu(largest))
        + jnp.square(relu(between))
        + jnp.square(relu(smallest))
    )


def kernel(sizes, names, *refs):
    sections, ngx, ngy, nx, ny, nz = sizes
    r = types.SimpleNamespace(**dict(zip(names, refs)))
    local, state, stiff, flow = r.local, r.state, r.stiff, r.flow
    held, clamped, free, tough_pad, crack_pad = r.held, r.clamped, r.free, r.tough_pad, r.crack_pad
    load_ref, crack_ref, clamp_ref, tough_ref = r.load_ref, r.crack_ref, r.clamp_ref, r.tough_ref
    disp_refs = (r.first_ref, r.second_ref, r.third_ref)
    sec = lax.axis_index("section")
    gx = lax.axis_index("gx")
    gy = lax.axis_index("gy")
    group = ngx * ngy
    me = gx * ngy + gy
    peers = []
    for k in range(1, group):
        other = lax.rem(me + k, group)
        peers.append({"gx": other // ngy, "gy": lax.rem(other, ngy)})

    fetch = [
        pltpu.make_async_copy(src, dst, local.at[n])
        for n, (src, dst) in enumerate(
            (
                (r.load_hbm, load_ref),
                (r.crack_hbm, crack_ref),
                (r.clamp_hbm, clamp_ref),
                (r.tough_hbm, tough_ref),
                (r.index_hbm, r.index_ref),
                (r.table_hbm, r.table_ref),
            )
        )
    ]
    for copy in fetch:
        copy.start()

    barrier = pltpu.get_barrier_semaphore()
    for peer in peers:
        pl.semaphore_signal(barrier, inc=1, device_id=peer, device_id_type=MESH)
    for k in range(1, sections):
        pl.semaphore_signal(
            barrier,
            inc=1,
            device_id={"section": lax.rem(sec + k, sections)},
            device_id_type=MESH,
        )

    there = {
        "gx": (gx > 0, gx < ngx - 1),
        "gy": (gy > 0, gy < ngy - 1),
    }
    step = (-1, 1)

    def x_dev(s):
        return there["gx"][s], {"gx": gx + step[s]}

    def y_dev(s):
        return there["gy"][s], {"gy": gy + step[s]}

    def c_dev(sx, sy):
        return (
            jnp.logical_and(there["gx"][sx], there["gy"][sy]),
            {"gx": gx + step[sx], "gy": gy + step[sy]},
        )

    class Exchange:
        def __init__(self, send, recv):
            self.items = []
            self.send = send
            self.recv = recv

        def add(self, where, src, dst, mine, out_slot, in_slot):
            cond, dev = where
            n = len(self.items)
            copy = pltpu.make_async_remote_copy(
                src_ref=src,
                dst_ref=dst,
                send_sem=self.send.at[n],
                recv_sem=self.recv.at[out_slot],
                device_id=dev,
                device_id_type=MESH,
            )
            back = pltpu.make_async_remote_copy(
                src_ref=src,
                dst_ref=mine,
                send_sem=self.send.at[n],
                recv_sem=self.recv.at[in_slot],
                device_id=dev,
                device_id_type=MESH,
            )
            self.items.append((cond, copy, back))

        def start(self):
            for cond, copy, _ in self.items:
                pl.when(cond)(copy.start)

        def finish(self):
            for cond, copy, back in self.items:

                @pl.when(cond)
                def _():
                    back.wait_recv()
                    copy.wait_send()

        def received(self):
            for cond, _, back in self.items:
                pl.when(cond)(back.wait_recv)

        def sent(self):
            for cond, copy, _ in self.items:
                pl.when(cond)(copy.wait_send)

    rows = ny + 2 * OY

    def clear(xp, carry):
        zero = jnp.zeros((rows, nz), jnp.float32)
        held[xp] = zero
        crack_pad[xp] = zero
        clamped[xp] = zero + 1.0
        tough_pad[xp] = zero + 1.0
        free[xp] = zero
        if sections > 2:
            for p in range(2):
                for f in range(4):
                    state[p, f, xp] = zero
        return carry

    lax.fori_loop(0, nx + 2 * HX, clear, 0)

    for copy in fetch[:3]:
        copy.wait()

    for s in range(2):
        side = lambda n, s=s: slice(0, n) if s == 0 else slice(ny - n, ny)
        r.pack_l[s, :, 0:5] = load_ref[:, side(5)]
        r.pack_l[s, :, 5:8] = clamp_ref[:, side(3)]
        r.pack_c[s] = crack_ref[:, side(4)]
    corner = (
        (load_ref, held, 1, 4, 0),
        (load_ref, held, 2, 3, 4),
        (load_ref, held, 4, 1, 7),
        (load_ref, held, 3, 2, 8),
        (crack_ref, crack_pad, 1, 3, 10),
        (crack_ref, crack_pad, 2, 2, 13),
        (crack_ref, crack_pad, 3, 1, 15),
        (clamp_ref, clamped, 1, 2, 16),
        (clamp_ref, clamped, 2, 1, 18),
    )
    for sx in range(2):
        for sy in range(2):
            for ref, _, deep, n, at in corner:
                plane = deep - 1 if sx == 0 else nx - deep
                first = 0 if sy == 0 else ny - n
                r.pack_k[sx * 2 + sy, at // 8, at % 8 : at % 8 + n] = ref[plane, first : first + n]

    pl.semaphore_wait(barrier, group - 1 + sections - 1)

    early = Exchange(r.early_send, r.early_recv)
    later = Exchange(r.later_send, r.later_recv)
    last_one = Exchange(r.last_send, r.last_recv)
    for s in range(2):
        for ex, ref, buf, width, at, slot in (
            (early, load_ref, r.in_x, 5, 0, 0),
            (early, crack_ref, r.in_x, 4, 5, 2),
            (later, clamp_ref, r.in_x, 3, 9, 0),
            (last_one, tough_ref.at[0], r.in_tx, 2, 0, 0),
        ):
            ex.add(
                x_dev(s),
                ref.at[pl.ds(0 if s == 0 else nx - width, width)],
                buf.at[1 - s, pl.ds(at, width)],
                buf.at[s, pl.ds(at, width)],
                slot + 1 - s,
                slot + s,
            )
    for s in range(2):
        for ex, pack, buf, slot in (
            (early, r.pack_l, r.in_l, 4),
            (early, r.pack_c, r.in_c, 6),
            (last_one, r.pack_t, r.in_ty, 2),
        ):
            ex.add(
                y_dev(s), pack.at[s], buf.at[1 - s], buf.at[s], slot + 1 - s, slot + s
            )
    for sx in range(2):
        for sy in range(2):
            here, away = sx * 2 + sy, (1 - sx) * 2 + 1 - sy
            early.add(
                c_dev(sx, sy), r.pack_k.at[here], r.in_k.at[away], r.in_k.at[here],
                8 + away, 8 + here,
            )
            last_one.add(
                c_dev(sx, sy), r.pack_tk.at[here], r.in_tk.at[away], r.in_tk.at[here],
                4 + away, 4 + here,
            )
    early.start()
    later.start()

    fetch[3].wait()
    for s in range(2):
        r.pack_t[s] = tough_ref[0, :, 0:2] if s == 0 else tough_ref[0, :, ny - 2 : ny]
    for sx in range(2):
        for sy in range(2):
            row = 0 if sy == 0 else ny - 1
            r.pack_tk[sx * 2 + sy] = tough_ref[0, 0 if sx == 0 else nx - 1, row : row + 1]
    last_one.start()

    tough_copies = []
    for k in range(1, sections):
        copy = pltpu.make_async_remote_copy(
            src_ref=tough_ref.at[0],
            dst_ref=r.tough_in.at[k - 1],
            send_sem=r.tough_send.at[k - 1],
            recv_sem=r.tough_recv.at[k - 1],
            device_id={"section": lax.rem(sec + sections - k, sections)},
            device_id_type=MESH,
        )
        copy.start()
        tough_copies.append(copy)

    inner = slice(OY, OY + ny)
    as_float = lambda v: v.astype(jnp.float32)

    def fill(x, carry):
        load = as_float(load_ref[x])
        clamp = as_float(clamp_ref[x])
        held[x + HX, inner] = load
        clamped[x + HX, inner] = clamp
        free[x + HX, inner] = 1.0 - jnp.maximum(clamp, load)
        crack_pad[x + HX, inner] = as_float(crack_ref[x])
        tough_pad[x + HX, inner] = tough_ref[0, x]
        return carry

    lax.fori_loop(0, nx, fill, 0, unroll=part(nx, 4))

    for copy in fetch[4:]:
        copy.wait()
    case = r.index_ref[0]
    vector = [r.table_ref[f, case] for f in range(3)]

    planes = slice(HX, HX + nx)

    def x_out(s, n):
        return slice(HX - n, HX) if s == 0 else slice(HX + nx, HX + nx + n)

    def y_out(s, n):
        return slice(OY - n, OY) if s == 0 else slice(OY + ny, OY + ny + n)

    early.received()
    for s in range(2):

        @pl.when(there["gx"][s])
        def _(s=s):
            held[x_out(s, 5), inner] = as_float(r.in_x[s, 0:5])
            crack_pad[x_out(s, 4), inner] = as_float(r.in_x[s, 5:9])

        @pl.when(there["gy"][s])
        def _(s=s):
            held[planes, y_out(s, 5)] = as_float(r.in_l[s, :, 0:5])
            clamped[planes, y_out(s, 3)] = as_float(r.in_l[s, :, 5:8])
            crack_pad[planes, y_out(s, 4)] = as_float(r.in_c[s])

    for sx in range(2):
        for sy in range(2):

            @pl.when(c_dev(sx, sy)[0])
            def _(sx=sx, sy=sy):
                for _, pad, deep, n, at in corner:
                    plane = HX - deep if sx == 0 else HX + nx - 1 + deep
                    pad[plane, y_out(sy, n)] = as_float(
                        r.in_k[sx * 2 + sy, at // 8, at % 8 : at % 8 + n]
                    )

    wide = up8(ny + 4)
    near = up8(ny + 2)
    deep = up8(ny + 8)

    def lanes(shape, lane):
        return lax.broadcasted_iota(jnp.int32, shape, 1) == lane

    def beside(v, edge, first, last):
        up = jnp.where(last, edge, pltpu.roll(v, nz - 1, 1))
        down = jnp.where(first, edge, pltpu.roll(v, 1, 1))
        return up, down

    def inside_rows(shape, above):
        row = lax.broadcasted_iota(jnp.int32, shape, 0) + (gy * ny - above)
        return jnp.logical_and(row >= 0, row < ny * ngy)

    def inside_plane(xp):
        plane = xp - HX + gx * nx
        return jnp.logical_and(plane >= 0, plane < nx * ngx)

    edge_stiff = 0.5 * (1.0 + stiff_floor)

    def elastic(at, first, last):
        k = at(stiff, 0, 0)
        sides = (
            (at(stiff, 1, 0), at(stiff, -1, 0)),
            (at(stiff, 0, 1), at(stiff, 0, -1)),
            beside(k, edge_stiff, first, last),
        )
        pairs = [s[0] + s[1] for s in sides]
        weights = pairs[0] + pairs[1] + pairs[2] + 6.0 * k
        faces = [(k + s[0], k + s[1]) for s in sides]
        fz = beside(at(flow, 0, 0), 0.0, first, last)
        grads = (
            at(flow, 1, 0) - at(flow, -1, 0),
            at(flow, 0, 1) - at(flow, 0, -1),
            fz[0] - fz[1],
        )
        return pairs, weights, faces, grads

    def laplace(at, ref, faces, weights, first, last):
        here = at(ref, 0, 0)
        uz = beside(here, 0.0, first, last)
        return here, (
            faces[0][0] * at(ref, 1, 0)
            + faces[0][1] * at(ref, -1, 0)
            + faces[1][0] * at(ref, 0, 1)
            + faces[1][1] * at(ref, 0, -1)
            + faces[2][0] * uz[0]
            + faces[2][1] * uz[1]
            - weights * here
        )

    def strain_energy(at, u, keep, first, last):
        grad = []
        for f in range(3):
            here = at(u.at[f], 0, 0)
            uz = beside(here, 0.0, first, last)
            grad.append(
                (
                    at(u.at[f], 1, 0) - at(u.at[f], -1, 0),
                    at(u.at[f], 0, 1) - at(u.at[f], 0, -1),
                    uz[0] - uz[1],
                )
            )
            keep(f, here)
        return 2.0 * spectral_energy(
            0.5 * grad[0][0],
            0.5 * grad[1][1],
            0.5 * grad[2][2],
            0.25 * (grad[0][1] + grad[1][0]),
            0.25 * (grad[0][2] + grad[2][0]),
            0.25 * (grad[1][2] + grad[2][1]),
        )

    def renew(at, d, energy, g, cracked, first, last):
        dz = beside(at(d, 0, 0), 0.0, first, last)
        around = at(d, 1, 0) + at(d, -1, 0) + at(d, 0, 1) + at(d, 0, -1) + dz[0] + dz[1]
        renewed = (energy + g * around) / (7.0 * g + energy)
        return jnp.where(cracked, 1.0, renewed)

    def add_up(rnd, total):
        r.sums[me, rnd : rnd + 1] = jnp.sum(total, axis=0, keepdims=True)

    def open_sweep():
        shape = (deep, nz)
        first, last = lanes(shape, 0), lanes(shape, nz - 1)
        row_inside = inside_rows(shape, 4)
        a = OY - 4

        def stiffen(xp, carry):
            half = 0.5 * (jnp.square(1.0 - crack_pad[xp, a : a + deep]) + stiff_floor)
            stiff[xp, a : a + deep] = half
            up, down = beside(held[xp, a : a + deep], 0.0, first, last)
            div = (
                vector[0] * (held[xp + 1, a : a + deep] - held[xp - 1, a : a + deep])
                + vector[1] * (held[xp, a + 1 : a + 1 + deep] - held[xp, a - 1 : a - 1 + deep])
                + vector[2] * (up - down)
            )
            flow[xp, a : a + deep] = jnp.where(
                jnp.logical_and(row_inside, inside_plane(xp)), half * div, 0.0
            )
            return carry

        lax.fori_loop(HX - 4, HX + nx + 4, stiffen, 0, unroll=part(nx + 8, 8))

        later.received()
        for s in range(2):

            @pl.when(there["gx"][s])
            def _(s=s):
                clamped[x_out(s, 3), inner] = as_float(r.in_x[s, 9:12])

        def move(xp, total):
            at = lambda ref, dx, dy: ref[xp + dx, a + dy : a + dy + deep]
            pairs, weights, faces, grads = elastic(at, first, last)
            load, spread = laplace(at, held, faces, weights, first, last)
            pin = at(clamped, 0, 0) + load > 0.5
            squares = None
            for f in range(3):
                res = vector[f] * spread + grads[f]
                moved = jnp.where(pin, 0.0, relax_weight * res / (weights + pairs[f]))
                state[1, f, xp, a : a + deep] = vector[f] * load + moved
                square = res * res
                squares = square if squares is None else squares + square
            return total + jnp.where(at(free, 0, 0) > 0.5, squares, 0.0)

        total = lax.fori_loop(
            HX - 3,
            HX + nx + 3,
            move,
            jnp.zeros(shape, jnp.float32),
            unroll=part(nx + 6, 11),
        )
        add_up(0, total)

        last_one.received()
        for s in range(2):

            @pl.when(there["gx"][s])
            def _(s=s):
                tough_pad[x_out(s, 2), inner] = r.in_tx[s]

            @pl.when(there["gy"][s])
            def _(s=s):
                tough_pad[planes, y_out(s, 2)] = r.in_ty[s]

        for sx in range(2):
            for sy in range(2):

                @pl.when(c_dev(sx, sy)[0])
                def _(sx=sx, sy=sy):
                    plane = HX - 1 if sx == 0 else HX + nx
                    tough_pad[plane, y_out(sy, 1)] = r.in_tk[sx * 2 + sy]

        def damage(xp, carry):
            at = lambda ref, dx, dy: ref[xp + dx, a + dy : a + dy + deep]
            energy = strain_energy(at, state.at[1], lambda f, v: None, first, last)
            renewed = renew(
                at,
                crack_pad,
                energy,
                at(tough_pad, 0, 0),
                at(crack_pad, 0, 0) > 0.5,
                first,
                last,
            )
            state[1, 3, xp, a : a + deep] = jnp.where(
                jnp.logical_and(row_inside, inside_plane(xp)), renewed, 0.0
            )
            return carry

        lax.fori_loop(HX - 2, HX + nx + 2, damage, 0, unroll=part(nx + 4, 5))

    def send_sums():
        for k, peer in enumerate(peers):
            pltpu.make_async_remote_copy(
                src_ref=r.sums.at[me],
                dst_ref=r.sums.at[me],
                send_sem=r.sum_send.at[k],
                recv_sem=r.sum_recv.at[me],
                device_id=peer,
                device_id_type=MESH,
            ).start()

    def sweep(rnd):
        p = rnd % 2
        q = 1 - p
        done = rnd == sections - 1
        tough = r.tough_in.at[rnd - 1]

        shape = (wide, nz)
        first, last = lanes(shape, 0), lanes(shape, nz - 1)
        row_inside = inside_rows(shape, 2)
        a = OY - 2

        def stiffen(xp, carry):
            half = 0.5 * (jnp.square(1.0 - state[p, 3, xp, a : a + wide]) + stiff_floor)
            stiff[xp, a : a + wide] = half
            up, down = beside(state[p, 2, xp, a : a + wide], 0.0, first, last)
            div = (
                (state[p, 0, xp + 1, a : a + wide] - state[p, 0, xp - 1, a : a + wide])
                + (state[p, 1, xp, a + 1 : a + 1 + wide] - state[p, 1, xp, a - 1 : a - 1 + wide])
                + (up - down)
            )
            flow[xp, a : a + wide] = jnp.where(
                jnp.logical_and(row_inside, inside_plane(xp)), half * div, 0.0
            )
            return carry

        lax.fori_loop(HX - 2, HX + nx + 2, stiffen, 0, unroll=part(nx + 4, 10))

        shape = (near, nz)
        first, last = lanes(shape, 0), lanes(shape, nz - 1)
        b = OY - 1

        def move(xp, total):
            at = lambda ref, dx, dy: ref[xp + dx, b + dy : b + dy + near]
            pairs, weights, faces, grads = elastic(at, first, last)
            load = at(held, 0, 0)
            pin = at(clamped, 0, 0) + load > 0.5
            squares = None
            for f in range(3):
                here, spread = laplace(at, state.at[p, f], faces, weights, first, last)
                res = spread + grads[f]
                moved = here + relax_weight * res / (weights + pairs[f])
                state[q, f, xp, b : b + near] = jnp.where(pin, load * vector[f], moved)
                square = res * res
                squares = square if squares is None else squares + square
            return total + jnp.where(at(free, 0, 0) > 0.5, squares, 0.0)

        total = lax.fori_loop(
            HX - 1, HX + nx + 1, move, jnp.zeros(shape, jnp.float32), unroll=part(nx + 2, 6)
        )
        add_up(rnd, total)
        par = rnd % 2
        mid = pl.ds(OY, ny)
        if done:
            send_sums()
        else:
            for f in range(3):
                r.pack_u[0, :, 2 * f : 2 * f + 2] = state[q, f, planes, OY : OY + 2]
                r.pack_u[1, :, 2 * f : 2 * f + 2] = state[q, f, planes, OY + ny - 2 : OY + ny]
            r.pack_u[0, :, 6:7] = state[q, 1, planes, OY + 2 : OY + 3]
            r.pack_u[1, :, 6:7] = state[q, 1, planes, OY + ny - 3 : OY + ny - 2]
            shift = Exchange(r.u_send, r.u_recv.at[par])
            for s in range(2):
                shift.add(
                    x_dev(s),
                    state.at[q, pl.ds(0, 3), pl.ds(HX if s == 0 else HX + nx - 2, 2), mid],
                    r.in_u_x.at[par, 1 - s],
                    r.in_u_x.at[par, s],
                    (1 - s),
                    s,
                )
                shift.add(
                    x_dev(s),
                    state.at[q, 0, HX + 2 if s == 0 else HX + nx - 3, mid],
                    r.in_u_x3.at[par, 1 - s],
                    r.in_u_x3.at[par, s],
                    2 + (1 - s),
                    2 + s,
                )
            for s in range(2):
                shift.add(
                    y_dev(s),
                    r.pack_u.at[s],
                    r.in_u_y.at[par, 1 - s],
                    r.in_u_y.at[par, s],
                    4 + (1 - s),
                    4 + s,
                )
            for sx in range(2):
                for sy in range(2):
                    shift.add(
                        c_dev(sx, sy),
                        r.pack_u.at[sy, pl.ds(0 if sx == 0 else nx - 2, 2)],
                        r.in_u_c.at[par, (1 - sx) * 2 + 1 - sy],
                        r.in_u_c.at[par, sx * 2 + sy],
                        6 + (1 - sx) * 2 + 1 - sy,
                        6 + sx * 2 + sy,
                    )
            shift.start()

        tough_copies[rnd - 1].wait_recv()

        shape = (ny, nz)
        first, last = lanes(shape, 0), lanes(shape, nz - 1)

        def damage(x, carry):
            xp = x + HX
            at = lambda ref, dx, dy: ref[xp + dx, OY + dy : OY + dy + ny]

            def keep(f, here):
                if done:
                    disp_refs[f][x] = here

            energy = strain_energy(at, state.at[q], keep, first, last)
            renewed = renew(
                at, state.at[p, 3], energy, tough[x], crack_ref[x] > 0, first, last
            )
            if done:
                r.dam_ref[x] = renewed
            else:
                state[q, 3, xp, inner] = renewed
            return carry

        lax.fori_loop(0, nx, damage, 0, unroll=part(nx, 8))
        if done:
            return

        r.pack_d[0] = state[q, 3, planes, OY : OY + 2]
        r.pack_d[1] = state[q, 3, planes, OY + ny - 2 : OY + ny]
        crack = Exchange(r.d_send, r.d_recv.at[par])
        for s in range(2):
            crack.add(
                x_dev(s),
                state.at[q, 3, pl.ds(HX if s == 0 else HX + nx - 2, 2), mid],
                r.in_d_x.at[par, 1 - s],
                r.in_d_x.at[par, s],
                1 - s,
                s,
            )
        for s in range(2):
            crack.add(
                y_dev(s),
                r.pack_d.at[s],
                r.in_d_y.at[par, 1 - s],
                r.in_d_y.at[par, s],
                2 + 1 - s,
                2 + s,
            )
        for sx in range(2):
            for sy in range(2):
                crack.add(
                    c_dev(sx, sy),
                    r.pack_d.at[sy, pl.ds(0 if sx == 0 else nx - 1, 1)],
                    r.in_d_c.at[par, (1 - sx) * 2 + 1 - sy],
                    r.in_d_c.at[par, sx * 2 + sy],
                    4 + (1 - sx) * 2 + 1 - sy,
                    4 + sx * 2 + sy,
                )
        crack.start()
        shift.finish()
        third_x = (HX - 3, HX + nx + 2)
        third_y = (slice(OY - 3, OY - 2), slice(OY + ny + 2, OY + ny + 3))
        for s in range(2):

            @pl.when(there["gx"][s])
            def _(s=s):
                state[q, 0:3, x_out(s, 2), inner] = r.in_u_x[par, s]
                state[q, 0, third_x[s], inner] = r.in_u_x3[par, s]

            @pl.when(there["gy"][s])
            def _(s=s):
                for f in range(3):
                    state[q, f, planes, y_out(s, 2)] = r.in_u_y[par, s, :, 2 * f : 2 * f + 2]
                state[q, 1, planes, third_y[s]] = r.in_u_y[par, s, :, 6:7]

        for sx in range(2):
            for sy in range(2):

                @pl.when(c_dev(sx, sy)[0])
                def _(sx=sx, sy=sy):
                    for f in range(3):
                        state[q, f, x_out(sx, 2), y_out(sy, 2)] = r.in_u_c[
                            par, sx * 2 + sy, :, 2 * f : 2 * f + 2
                        ]

        crack.finish()
        for s in range(2):

            @pl.when(there["gx"][s])
            def _(s=s):
                state[q, 3, x_out(s, 2), inner] = r.in_d_x[par, s]

            @pl.when(there["gy"][s])
            def _(s=s):
                state[q, 3, planes, y_out(s, 2)] = r.in_d_y[par, s]

        for sx in range(2):
            for sy in range(2):

                @pl.when(c_dev(sx, sy)[0])
                def _(sx=sx, sy=sy):
                    state[q, 3, x_out(sx, 1), y_out(sy, 2)] = r.in_d_c[par, sx * 2 + sy]

    open_sweep()
    if sections == 1:
        send_sums()
    for rnd in range(1, sections):
        sweep(rnd)

    cells = 3.0 * nx * ngx * ny * ngy * nz
    early.sent()
    later.sent()
    last_one.sent()
    for copy in tough_copies:
        copy.wait_send()
    for k in range(1, group):
        other = lax.rem(me + k, group)
        pltpu.make_async_remote_copy(
            src_ref=r.sums.at[me],
            dst_ref=r.sums.at[other],
            send_sem=r.sum_send.at[k - 1],
            recv_sem=r.sum_recv.at[other],
            device_id=peers[k - 1],
            device_id_type=MESH,
        ).wait()
    total = r.sums[0]
    for k in range(1, group):
        total = total + r.sums[k]
    entries = jnp.sqrt(jnp.sum(total, axis=1, keepdims=True) / cells)
    column = lax.broadcasted_iota(jnp.int32, (1, sections), 1)
    norms = jnp.zeros((1, sections), jnp.float32)
    for rnd in range(sections):
        norms = jnp.where(
            column == lax.rem(sec + rnd, sections), entries[rnd : rnd + 1], norms
        )
    r.norm_ref[...] = norms


def put_out(
    first_ref, second_ref, third_ref, dam_ref, norm_ref, disp_hbm, dam_hbm, norm_out, sems
):
    copies = [
        pltpu.make_async_copy(ref, disp_hbm.at[0, f], sems.at[f])
        for f, ref in enumerate((first_ref, second_ref, third_ref))
    ]
    copies.append(pltpu.make_async_copy(dam_ref, dam_hbm.at[0], sems.at[3]))
    for copy in copies:
        copy.start()
    norm_out[...] = norm_ref[...]
    for copy in copies:
        copy.wait()


def on_device(sizes, load_index, load_table, toughness, clamp_mask, load_mask, crack_mask):
    sections, ngx, ngy = sizes
    nx, ny, nz = clamp_mask.shape
    assert load_index.shape == (1,)
    group = ngx * ngy
    f32 = jnp.float32
    padded = (nx + 2 * HX, ny + 2 * OY, nz)
    vmem = pltpu.VMEM
    dma = pltpu.SemaphoreType.DMA
    later = max(sections - 1, 1)
    more = sections > 2
    scratch = {
        "index_ref": pltpu.SMEM(load_index.shape, jnp.int32),
        "table_ref": pltpu.SMEM(load_table.shape[::-1], f32),
        "tough_ref": vmem((1, nx, ny, nz), f32),
        "clamp_ref": vmem((nx, ny, nz), jnp.int32),
        "load_ref": vmem((nx, ny, nz), jnp.int32),
        "crack_ref": vmem((nx, ny, nz), jnp.int32),
        "local": dma((6,)),
        "state": vmem((2, 4) + padded, f32),
        "stiff": vmem(padded, f32),
        "flow": vmem(padded, f32),
        "held": vmem(padded, f32),
        "clamped": vmem(padded, f32),
        "free": vmem(padded, f32),
        "tough_pad": vmem(padded, f32),
        "crack_pad": vmem(padded, f32),
        "tough_in": vmem((later, nx, ny, nz), f32),
        "pack_l": vmem((2, nx, 8, nz), jnp.int32),
        "pack_c": vmem((2, nx, 4, nz), jnp.int32),
        "pack_t": vmem((2, nx, 2, nz), f32),
        "pack_k": vmem((4, 3, 8, nz), jnp.int32),
        "pack_tk": vmem((4, 1, nz), f32),
        "in_x": vmem((2, 12, ny, nz), jnp.int32),
        "in_tx": vmem((2, 2, ny, nz), f32),
        "in_l": vmem((2, nx, 8, nz), jnp.int32),
        "in_c": vmem((2, nx, 4, nz), jnp.int32),
        "in_ty": vmem((2, nx, 2, nz), f32),
        "in_k": vmem((4, 3, 8, nz), jnp.int32),
        "in_tk": vmem((4, 1, nz), f32),
        "sums": vmem((group, sections, nz), f32),
        "early_send": dma((12,)),
        "early_recv": dma((12,)),
        "later_send": dma((2,)),
        "later_recv": dma((2,)),
        "last_send": dma((8,)),
        "last_recv": dma((8,)),
        "tough_send": dma((later,)),
        "tough_recv": dma((later,)),
        "sum_send": dma((max(group - 1, 1),)),
        "sum_recv": dma((group,)),
    }
    if more:
        scratch |= {
            "pack_u": vmem((2, nx, 8, nz), f32),
            "pack_d": vmem((2, nx, 2, nz), f32),
            "in_u_x": vmem((2, 2, 3, 2, ny, nz), f32),
            "in_u_x3": vmem((2, 2, ny, nz), f32),
            "in_u_y": vmem((2, 2, nx, 8, nz), f32),
            "in_u_c": vmem((2, 4, 2, 8, nz), f32),
            "in_d_x": vmem((2, 2, 2, ny, nz), f32),
            "in_d_y": vmem((2, 2, nx, 2, nz), f32),
            "in_d_c": vmem((2, 4, 1, 2, nz), f32),
            "u_send": dma((10,)),
            "u_recv": dma((2, 10)),
            "d_send": dma((8,)),
            "d_recv": dma((2, 8)),
        }
    ins = ("index_hbm", "table_hbm", "tough_hbm", "clamp_hbm", "load_hbm", "crack_hbm")
    outs = ("first_ref", "second_ref", "third_ref", "dam_ref", "norm_ref")
    names = (*ins, *outs, *scratch)
    block = pl.BlockSpec(memory_space=pltpu.VMEM)
    away = pl.BlockSpec(memory_space=pltpu.HBM)
    results = pl.pallas_call(
        functools.partial(kernel, (sections, ngx, ngy, nx, ny, nz), names),
        out_shape=(
            *[jax.ShapeDtypeStruct((nx, ny, nz), f32)] * 4,
            jax.ShapeDtypeStruct((1, sections), f32),
        ),
        in_specs=[away] * 6,
        out_specs=(block,) * 5,
        scratch_shapes=list(scratch.values()),
        compiler_params=pltpu.CompilerParams(
            collective_id=0, has_side_effects=True, vmem_limit_bytes=56_020_000
        ),
    )(load_index, load_table.T, toughness, clamp_mask, load_mask, crack_mask)
    return pl.pallas_call(
        put_out,
        out_shape=(
            jax.ShapeDtypeStruct((1, 3, nx, ny, nz), f32),
            jax.ShapeDtypeStruct((1, nx, ny, nz), f32),
            jax.ShapeDtypeStruct((1, sections), f32),
        ),
        in_specs=[block] * 5,
        out_specs=(away, away, block),
        scratch_shapes=[dma((4,))],
        compiler_params=pltpu.CompilerParams(vmem_limit_bytes=1024 * 1024),
    )(*results)


def solution(mesh):
    in_specs = (
        P("section"),
        P(),
        P("section", "gx", "gy", None),
        P("gx", "gy", None),
        P("gx", "gy", None),
        P("gx", "gy", None),
    )
    out_specs = (
        P("section", None, "gx", "gy", None),
        P("section", "gx", "gy", None),
        P("section", None),
    )
    sizes = tuple(mesh.shape[name] for name in ("section", "gx", "gy"))
    return jax.shard_map(
        functools.partial(on_device, sizes),
        mesh=mesh,
        in_specs=in_specs,
        out_specs=out_specs,
        check_vma=False,
    )
```

```python
import functools
import math
import types

import jax
import jax.numpy as jnp
from jax import lax
from jax.experimental import pallas as pl
from jax.experimental.pallas import tpu as pltpu
from jax.sharding import PartitionSpec as P

relax_weight = 0.6
stiff_floor = 0.001
eigen_guard = 1e-08
MESH = pl.DeviceIdType.MESH

HX = 5
OY = 8

ACOS = (
    1.5707963050,
    -0.2145988016,
    0.0889789874,
    -0.0501743046,
    0.0308918810,
    -0.0170881256,
    0.0066700901,
    -0.0012624911,
)


def up8(n):
    return -(-n // 8) * 8


def part(n, most):
    return max(k for k in range(1, most + 1) if n % k == 0)


def root(v):
    return v * lax.rsqrt(jnp.maximum(v, 1.2e-38))


def spectral_energy(xx, yy, zz, xy, xz, yz):
    trace = xx + yy + zz
    mid = trace * (1.0 / 3.0)
    dx = xx - mid
    dy = yy - mid
    dz = zz - mid
    xy2 = xy * xy
    xz2 = xz * xz
    yz2 = yz * yz
    sixth = (dx * dx + dy * dy + dz * dz + 2.0 * (xy2 + xz2 + yz2)) * (1.0 / 6.0)
    twice_radius = 2.0 * root(sixth)
    scale = lax.rsqrt(sixth + eigen_guard)
    det = dx * (dy * dz - yz2) - dz * xy2 - dy * xz2 + 2.0 * (xy * xz * yz)
    ratio = (0.5 * det * scale) * (scale * scale)
    size = jnp.minimum(jnp.abs(ratio), 1.0)
    poly = jnp.full_like(size, ACOS[-1] / 3.0)
    for c in ACOS[-2::-1]:
        poly = poly * size + c / 3.0
    t = root(1.0 - size) * poly
    t2 = t * t
    cos_t = 1.0 + t2 * (-0.5 + t2 * (1.0 / 24.0 + t2 * (-1.0 / 720.0 + t2 * (1.0 / 40320.0))))
    sin_t = t * (1.0 + t2 * (-1.0 / 6.0 + t2 * (1.0 / 120.0 + t2 * (-1.0 / 5040.0))))
    other = 0.5 * cos_t + math.sqrt(0.75) * sin_t
    upper = ratio >= 0.0
    first = jnp.where(upper, cos_t, other)
    last = jnp.where(upper, other, cos_t)
    largest = mid + twice_radius * first
    smallest = mid - twice_radius * last
    between = trace - largest - smallest
    relu = lambda v: jnp.maximum(v, 0.0)
    return (
        0.5 * jnp.square(relu(trace))
        + jnp.square(relu(largest))
        + jnp.square(relu(between))
        + jnp.square(relu(smallest))
    )


def kernel(sizes, names, *refs):
    sections, ngx, ngy, nx, ny, nz = sizes
    r = types.SimpleNamespace(**dict(zip(names, refs)))
    local, state, stiff, flow = r.local, r.state, r.stiff, r.flow
    held, clamped, free, tough_pad, crack_pad = r.held, r.clamped, r.free, r.tough_pad, r.crack_pad
    load_ref, crack_ref, clamp_ref, tough_ref = r.load_ref, r.crack_ref, r.clamp_ref, r.tough_ref
    disp_refs = (r.first_ref, r.second_ref, r.third_ref)
    sec = lax.axis_index("section")
    gx = lax.axis_index("gx")
    gy = lax.axis_index("gy")
    group = ngx * ngy
    me = gx * ngy + gy
    peers = []
    for k in range(1, group):
        other = lax.rem(me + k, group)
        peers.append({"gx": other // ngy, "gy": lax.rem(other, ngy)})

    fetch = [
        pltpu.make_async_copy(src, dst, local.at[n])
        for n, (src, dst) in enumerate(
            (
                (r.load_hbm, load_ref),
                (r.crack_hbm, crack_ref),
                (r.clamp_hbm, clamp_ref),
                (r.tough_hbm, tough_ref),
                (r.index_hbm, r.index_ref),
                (r.table_hbm, r.table_ref),
            )
        )
    ]
    for copy in fetch:
        copy.start()

    barrier = pltpu.get_barrier_semaphore()
    for peer in peers:
        pl.semaphore_signal(barrier, inc=1, device_id=peer, device_id_type=MESH)
    for k in range(1, sections):
        pl.semaphore_signal(
            barrier,
            inc=1,
            device_id={"section": lax.rem(sec + k, sections)},
            device_id_type=MESH,
        )

    there = {
        "gx": (gx > 0, gx < ngx - 1),
        "gy": (gy > 0, gy < ngy - 1),
    }
    step = (-1, 1)

    def x_dev(s):
        return there["gx"][s], {"gx": gx + step[s]}

    def y_dev(s):
        return there["gy"][s], {"gy": gy + step[s]}

    def c_dev(sx, sy):
        return (
            jnp.logical_and(there["gx"][sx], there["gy"][sy]),
            {"gx": gx + step[sx], "gy": gy + step[sy]},
        )

    class Exchange:
        def __init__(self, send, recv):
            self.items = []
            self.send = send
            self.recv = recv

        def add(self, where, src, dst, mine, out_slot, in_slot):
            cond, dev = where
            n = len(self.items)
            copy = pltpu.make_async_remote_copy(
                src_ref=src,
                dst_ref=dst,
                send_sem=self.send.at[n],
                recv_sem=self.recv.at[out_slot],
                device_id=dev,
                device_id_type=MESH,
            )
            back = pltpu.make_async_remote_copy(
                src_ref=src,
                dst_ref=mine,
                send_sem=self.send.at[n],
                recv_sem=self.recv.at[in_slot],
                device_id=dev,
                device_id_type=MESH,
            )
            self.items.append((cond, copy, back))

        def start(self, begin=0, end=None):
            for cond, copy, _ in self.items[begin:end]:
                pl.when(cond)(copy.start)

        def finish(self):
            for cond, copy, back in self.items:

                @pl.when(cond)
                def _():
                    back.wait_recv()
                    copy.wait_send()

        def received(self):
            for cond, _, back in self.items:
                pl.when(cond)(back.wait_recv)

        def sent(self):
            for cond, copy, _ in self.items:
                pl.when(cond)(copy.wait_send)

    rows = ny + 2 * OY

    def clear(xp, carry):
        zero = jnp.zeros((rows, nz), jnp.float32)
        held[xp] = zero
        crack_pad[xp] = zero
        clamped[xp] = zero + 1.0
        tough_pad[xp] = zero + 1.0
        free[xp] = zero
        if sections > 2:
            for p in range(2):
                for f in range(4):
                    state[p, f, xp] = zero
        return carry

    lax.fori_loop(0, nx + 2 * HX, clear, 0)

    for copy in fetch[:3]:
        copy.wait()

    for s in range(2):
        side = lambda n, s=s: slice(0, n) if s == 0 else slice(ny - n, ny)
        r.pack_l[s, :, 0:5] = load_ref[:, side(5)]
        r.pack_l[s, :, 5:8] = clamp_ref[:, side(3)]
        r.pack_c[s] = crack_ref[:, side(4)]
    corner = (
        (load_ref, held, 1, 4, 0),
        (load_ref, held, 2, 3, 4),
        (load_ref, held, 4, 1, 7),
        (load_ref, held, 3, 2, 8),
        (crack_ref, crack_pad, 1, 3, 10),
        (crack_ref, crack_pad, 2, 2, 13),
        (crack_ref, crack_pad, 3, 1, 15),
        (clamp_ref, clamped, 1, 2, 16),
        (clamp_ref, clamped, 2, 1, 18),
    )
    for sx in range(2):
        for sy in range(2):
            for ref, _, deep, n, at in corner:
                plane = deep - 1 if sx == 0 else nx - deep
                first = 0 if sy == 0 else ny - n
                r.pack_k[sx * 2 + sy, at // 8, at % 8 : at % 8 + n] = ref[plane, first : first + n]

    pl.semaphore_wait(barrier, group - 1 + sections - 1)

    beside_y = Exchange(r.y_send, r.y_recv)
    early = Exchange(r.early_send, r.early_recv)
    later = Exchange(r.later_send, r.later_recv)
    last_one = Exchange(r.last_send, r.last_recv)
    for s in range(2):
        for ex, ref, buf, width, at, slot in (
            (early, load_ref, r.in_x, 5, 0, 0),
            (early, crack_ref, r.in_x, 4, 5, 2),
            (later, clamp_ref, r.in_x, 3, 9, 0),
            (last_one, tough_ref.at[0], r.in_tx, 2, 0, 0),
        ):
            ex.add(
                x_dev(s),
                ref.at[pl.ds(0 if s == 0 else nx - width, width)],
                buf.at[1 - s, pl.ds(at, width)],
                buf.at[s, pl.ds(at, width)],
                slot + 1 - s,
                slot + s,
            )
    for s in range(2):
        for pack, buf, slot in (
            (r.pack_l, r.in_l, 0),
            (r.pack_c, r.in_c, 2),
            (r.pack_t, r.in_ty, 4),
        ):
            beside_y.add(
                y_dev(s), pack.at[s], buf.at[1 - s], buf.at[s], slot + 1 - s, slot + s
            )
    for sx in range(2):
        for sy in range(2):
            here, away = sx * 2 + sy, (1 - sx) * 2 + 1 - sy
            early.add(
                c_dev(sx, sy), r.pack_k.at[here], r.in_k.at[away], r.in_k.at[here],
                4 + away, 4 + here,
            )
            last_one.add(
                c_dev(sx, sy), r.pack_tk.at[here], r.in_tk.at[away], r.in_tk.at[here],
                2 + away, 2 + here,
            )
    early.start(0, 4)
    fetch[3].wait()
    for s in range(2):
        r.pack_t[s] = tough_ref[0, :, 0:2] if s == 0 else tough_ref[0, :, ny - 2 : ny]
    for sx in range(2):
        for sy in range(2):
            row = 0 if sy == 0 else ny - 1
            r.pack_tk[sx * 2 + sy] = tough_ref[0, 0 if sx == 0 else nx - 1, row : row + 1]
    beside_y.start()
    early.start(4)
    later.start()
    last_one.start()

    tough_copies = []
    for k in range(1, sections):
        copy = pltpu.make_async_remote_copy(
            src_ref=tough_ref.at[0],
            dst_ref=r.tough_in.at[k - 1],
            send_sem=r.tough_send.at[k - 1],
            recv_sem=r.tough_recv.at[k - 1],
            device_id={"section": lax.rem(sec + sections - k, sections)},
            device_id_type=MESH,
        )
        copy.start()
        tough_copies.append(copy)

    inner = slice(OY, OY + ny)
    as_float = lambda v: v.astype(jnp.float32)

    def fill(x, carry):
        load = as_float(load_ref[x])
        clamp = as_float(clamp_ref[x])
        held[x + HX, inner] = load
        clamped[x + HX, inner] = clamp
        free[x + HX, inner] = 1.0 - jnp.maximum(clamp, load)
        crack_pad[x + HX, inner] = as_float(crack_ref[x])
        tough_pad[x + HX, inner] = tough_ref[0, x]
        return carry

    lax.fori_loop(0, nx, fill, 0, unroll=part(nx, 4))

    for copy in fetch[4:]:
        copy.wait()
    case = r.index_ref[0]
    vector = [r.table_ref[f, case] for f in range(3)]

    planes = slice(HX, HX + nx)

    def x_out(s, n):
        return slice(HX - n, HX) if s == 0 else slice(HX + nx, HX + nx + n)

    def y_out(s, n):
        return slice(OY - n, OY) if s == 0 else slice(OY + ny, OY + ny + n)

    def unpack_y():
        beside_y.received()
        for s in range(2):

            @pl.when(there["gy"][s])
            def _(s=s):
                held[planes, y_out(s, 5)] = as_float(r.in_l[s, :, 0:5])
                clamped[planes, y_out(s, 3)] = as_float(r.in_l[s, :, 5:8])
                crack_pad[planes, y_out(s, 4)] = as_float(r.in_c[s])
                tough_pad[planes, y_out(s, 2)] = r.in_ty[s]

    def unpack_x():
        early.received()
        for s in range(2):

            @pl.when(there["gx"][s])
            def _(s=s):
                held[x_out(s, 5), inner] = as_float(r.in_x[s, 0:5])
                crack_pad[x_out(s, 4), inner] = as_float(r.in_x[s, 5:9])

        for sx in range(2):
            for sy in range(2):

                @pl.when(c_dev(sx, sy)[0])
                def _(sx=sx, sy=sy):
                    for _, pad, deep, n, at in corner:
                        plane = HX - deep if sx == 0 else HX + nx - 1 + deep
                        pad[plane, y_out(sy, n)] = as_float(
                            r.in_k[sx * 2 + sy, at // 8, at % 8 : at % 8 + n]
                        )

    def unpack_clamp():
        later.received()
        for s in range(2):

            @pl.when(there["gx"][s])
            def _(s=s):
                clamped[x_out(s, 3), inner] = as_float(r.in_x[s, 9:12])

    def unpack_tough():
        last_one.received()
        for s in range(2):

            @pl.when(there["gx"][s])
            def _(s=s):
                tough_pad[x_out(s, 2), inner] = r.in_tx[s]

        for sx in range(2):
            for sy in range(2):

                @pl.when(c_dev(sx, sy)[0])
                def _(sx=sx, sy=sy):
                    plane = HX - 1 if sx == 0 else HX + nx
                    tough_pad[plane, y_out(sy, 1)] = r.in_tk[sx * 2 + sy]

    wide = up8(ny + 4)
    deep = up8(ny + 8)

    def lanes(shape, lane):
        return lax.broadcasted_iota(jnp.int32, shape, 1) == lane

    def beside(v, edge, first, last):
        up = jnp.where(last, edge, pltpu.roll(v, nz - 1, 1))
        down = jnp.where(first, edge, pltpu.roll(v, 1, 1))
        return up, down

    def inside_rows(shape, above):
        row = lax.broadcasted_iota(jnp.int32, shape, 0) + (gy * ny - above)
        return jnp.logical_and(row >= 0, row < ny * ngy)

    def inside_plane(xp):
        plane = xp - HX + gx * nx
        return jnp.logical_and(plane >= 0, plane < nx * ngx)

    edge_stiff = 0.5 * (1.0 + stiff_floor)

    def elastic(at, first, last):
        k = at(stiff, 0, 0)
        sides = (
            (at(stiff, 1, 0), at(stiff, -1, 0)),
            (at(stiff, 0, 1), at(stiff, 0, -1)),
            beside(k, edge_stiff, first, last),
        )
        pairs = [s[0] + s[1] for s in sides]
        weights = pairs[0] + pairs[1] + pairs[2] + 6.0 * k
        faces = [(k + s[0], k + s[1]) for s in sides]
        fz = beside(at(flow, 0, 0), 0.0, first, last)
        grads = (
            at(flow, 1, 0) - at(flow, -1, 0),
            at(flow, 0, 1) - at(flow, 0, -1),
            fz[0] - fz[1],
        )
        return pairs, weights, faces, grads

    def laplace(at, ref, faces, weights, first, last):
        here = at(ref, 0, 0)
        uz = beside(here, 0.0, first, last)
        return here, (
            faces[0][0] * at(ref, 1, 0)
            + faces[0][1] * at(ref, -1, 0)
            + faces[1][0] * at(ref, 0, 1)
            + faces[1][1] * at(ref, 0, -1)
            + faces[2][0] * uz[0]
            + faces[2][1] * uz[1]
            - weights * here
        )

    def strain_energy(at, u, keep, first, last):
        grad = []
        for f in range(3):
            here = at(u.at[f], 0, 0)
            uz = beside(here, 0.0, first, last)
            grad.append(
                (
                    at(u.at[f], 1, 0) - at(u.at[f], -1, 0),
                    at(u.at[f], 0, 1) - at(u.at[f], 0, -1),
                    uz[0] - uz[1],
                )
            )
            keep(f, here)
        return 2.0 * spectral_energy(
            0.5 * grad[0][0],
            0.5 * grad[1][1],
            0.5 * grad[2][2],
            0.25 * (grad[0][1] + grad[1][0]),
            0.25 * (grad[0][2] + grad[2][0]),
            0.25 * (grad[1][2] + grad[2][1]),
        )

    def renew(at, d, energy, g, cracked, first, last):
        dz = beside(at(d, 0, 0), 0.0, first, last)
        around = at(d, 1, 0) + at(d, -1, 0) + at(d, 0, 1) + at(d, 0, -1) + dz[0] + dz[1]
        renewed = (energy + g * around) / (7.0 * g + energy)
        return jnp.where(cracked, 1.0, renewed)

    def add_up(rnd, total):
        r.sums[me, rnd : rnd + 1] = jnp.sum(total, axis=0, keepdims=True)

    def open_sweep():
        shape = (deep, nz)
        first, last = lanes(shape, 0), lanes(shape, nz - 1)
        row_inside = inside_rows(shape, 4)
        a = OY - 4

        def stiffen(xp, carry):
            half = 0.5 * (jnp.square(1.0 - crack_pad[xp, a : a + deep]) + stiff_floor)
            stiff[xp, a : a + deep] = half
            up, down = beside(held[xp, a : a + deep], 0.0, first, last)
            div = (
                vector[0] * (held[xp + 1, a : a + deep] - held[xp - 1, a : a + deep])
                + vector[1] * (held[xp, a + 1 : a + 1 + deep] - held[xp, a - 1 : a - 1 + deep])
                + vector[2] * (up - down)
            )
            flow[xp, a : a + deep] = jnp.where(
                jnp.logical_and(row_inside, inside_plane(xp)), half * div, 0.0
            )
            return carry

        def move(xp, total):
            at = lambda ref, dx, dy: ref[xp + dx, a + dy : a + dy + deep]
            pairs, weights, faces, grads = elastic(at, first, last)
            load, spread = laplace(at, held, faces, weights, first, last)
            pin = at(clamped, 0, 0) + load > 0.5
            squares = None
            for f in range(3):
                res = vector[f] * spread + grads[f]
                moved = jnp.where(pin, 0.0, relax_weight * res / (weights + pairs[f]))
                state[1, f, xp, a : a + deep] = vector[f] * load + moved
                square = res * res
                squares = square if squares is None else squares + square
            return total + jnp.where(at(free, 0, 0) > 0.5, squares, 0.0)

        def damage(xp, carry):
            at = lambda ref, dx, dy: ref[xp + dx, a + dy : a + dy + deep]
            energy = strain_energy(at, state.at[1], lambda f, v: None, first, last)
            renewed = renew(
                at,
                crack_pad,
                energy,
                at(tough_pad, 0, 0),
                at(crack_pad, 0, 0) > 0.5,
                first,
                last,
            )
            state[1, 3, xp, a : a + deep] = jnp.where(
                jnp.logical_and(row_inside, inside_plane(xp)), renewed, 0.0
            )
            return carry

        def inward(skip, body, carry, most):
            n = nx - 2 * skip
            return lax.fori_loop(HX + skip, HX + nx - skip, body, carry, unroll=part(n, most))

        def outward(far, body, carry):
            def both(i, carry):
                carry = body(HX - far + i, carry)
                return body(HX + nx + far - 5 + i, carry)

            return lax.fori_loop(0, 5, both, carry, unroll=True)

        unpack_y()
        inward(1, stiffen, 0, 14)
        total = inward(2, move, jnp.zeros(shape, jnp.float32), 12)
        inward(3, damage, 0, 5)
        unpack_x()
        outward(4, stiffen, 0)
        unpack_clamp()
        total = outward(3, move, total)
        add_up(0, total)
        unpack_tough()
        outward(2, damage, 0)

    def send_sums():
        for k, peer in enumerate(peers):
            pltpu.make_async_remote_copy(
                src_ref=r.sums.at[me],
                dst_ref=r.sums.at[me],
                send_sem=r.sum_send.at[k],
                recv_sem=r.sum_recv.at[me],
                device_id=peer,
                device_id_type=MESH,
            ).start()

    def sweep(rnd):
        p = rnd % 2
        q = 1 - p
        done = rnd == sections - 1
        tough = r.tough_in.at[rnd - 1]

        shape = (wide, nz)
        first, last = lanes(shape, 0), lanes(shape, nz - 1)
        row_inside = inside_rows(shape, 2)
        a = OY - 2

        def stiffen(xp, carry):
            half = 0.5 * (jnp.square(1.0 - state[p, 3, xp, a : a + wide]) + stiff_floor)
            stiff[xp, a : a + wide] = half
            up, down = beside(state[p, 2, xp, a : a + wide], 0.0, first, last)
            div = (
                (state[p, 0, xp + 1, a : a + wide] - state[p, 0, xp - 1, a : a + wide])
                + (state[p, 1, xp, a + 1 : a + 1 + wide] - state[p, 1, xp, a - 1 : a - 1 + wide])
                + (up - down)
            )
            flow[xp, a : a + wide] = jnp.where(
                jnp.logical_and(row_inside, inside_plane(xp)), half * div, 0.0
            )
            return carry

        lax.fori_loop(HX - 2, HX + nx + 2, stiffen, 0, unroll=part(nx + 4, 10))

        def mover(b, n):
            shape = (n, nz)
            first, last = lanes(shape, 0), lanes(shape, nz - 1)

            def move(xp, total):
                at = lambda ref, dx, dy: ref[xp + dx, b + dy : b + dy + n]
                pairs, weights, faces, grads = elastic(at, first, last)
                load = at(held, 0, 0)
                pin = at(clamped, 0, 0) + load > 0.5
                squares = None
                for f in range(3):
                    here, spread = laplace(at, state.at[p, f], faces, weights, first, last)
                    res = spread + grads[f]
                    moved = here + relax_weight * res / (weights + pairs[f])
                    state[q, f, xp, b : b + n] = jnp.where(pin, load * vector[f], moved)
                    square = res * res
                    squares = square if squares is None else squares + square
                return total + jnp.where(pin, 0.0, squares)

            return move

        total = lax.fori_loop(
            HX, HX + nx, mover(OY, ny), jnp.zeros((ny, nz), jnp.float32), unroll=part(nx, 8)
        )
        add_up(rnd, total)
        if done:
            send_sums()
        none = jnp.zeros((8, nz), jnp.float32)

        def edges(xp, carry):
            mover(OY - 4, 8)(xp, none)
            mover(OY + ny - 3, 8)(xp, none)
            return carry

        lax.fori_loop(HX, HX + nx, edges, 0, unroll=part(nx, 8))
        ends = mover(OY, ny)
        ends(HX - 1, jnp.zeros((ny, nz), jnp.float32))
        ends(HX + nx, jnp.zeros((ny, nz), jnp.float32))
        par = rnd % 2
        mid = pl.ds(OY, ny)
        if not done:
            for f in range(3):
                r.pack_u[0, :, 2 * f : 2 * f + 2] = state[q, f, planes, OY : OY + 2]
                r.pack_u[1, :, 2 * f : 2 * f + 2] = state[q, f, planes, OY + ny - 2 : OY + ny]
            r.pack_u[0, :, 6:7] = state[q, 1, planes, OY + 2 : OY + 3]
            r.pack_u[1, :, 6:7] = state[q, 1, planes, OY + ny - 3 : OY + ny - 2]
            shift = Exchange(r.u_send, r.u_recv.at[par])
            for s in range(2):
                shift.add(
                    x_dev(s),
                    state.at[q, pl.ds(0, 3), pl.ds(HX if s == 0 else HX + nx - 2, 2), mid],
                    r.in_u_x.at[par, 1 - s],
                    r.in_u_x.at[par, s],
                    (1 - s),
                    s,
                )
                shift.add(
                    x_dev(s),
                    state.at[q, 0, HX + 2 if s == 0 else HX + nx - 3, mid],
                    r.in_u_x3.at[par, 1 - s],
                    r.in_u_x3.at[par, s],
                    2 + (1 - s),
                    2 + s,
                )
            for s in range(2):
                shift.add(
                    y_dev(s),
                    r.pack_u.at[s],
                    r.in_u_y.at[par, 1 - s],
                    r.in_u_y.at[par, s],
                    4 + (1 - s),
                    4 + s,
                )
            for sx in range(2):
                for sy in range(2):
                    shift.add(
                        c_dev(sx, sy),
                        r.pack_u.at[sy, pl.ds(0 if sx == 0 else nx - 2, 2)],
                        r.in_u_c.at[par, (1 - sx) * 2 + 1 - sy],
                        r.in_u_c.at[par, sx * 2 + sy],
                        6 + (1 - sx) * 2 + 1 - sy,
                        6 + sx * 2 + sy,
                    )
            shift.start()

        tough_copies[rnd - 1].wait_recv()

        shape = (ny, nz)
        first, last = lanes(shape, 0), lanes(shape, nz - 1)

        def damage(x, carry):
            xp = x + HX
            at = lambda ref, dx, dy: ref[xp + dx, OY + dy : OY + dy + ny]

            def keep(f, here):
                if done:
                    disp_refs[f][x] = here

            energy = strain_energy(at, state.at[q], keep, first, last)
            renewed = renew(
                at, state.at[p, 3], energy, tough[x], crack_ref[x] > 0, first, last
            )
            if done:
                r.dam_ref[x] = renewed
            else:
                state[q, 3, xp, inner] = renewed
            return carry

        lax.fori_loop(0, nx, damage, 0, unroll=part(nx, 8))
        if done:
            return

        r.pack_d[0] = state[q, 3, planes, OY : OY + 2]
        r.pack_d[1] = state[q, 3, planes, OY + ny - 2 : OY + ny]
        crack = Exchange(r.d_send, r.d_recv.at[par])
        for s in range(2):
            crack.add(
                x_dev(s),
                state.at[q, 3, pl.ds(HX if s == 0 else HX + nx - 2, 2), mid],
                r.in_d_x.at[par, 1 - s],
                r.in_d_x.at[par, s],
                1 - s,
                s,
            )
        for s in range(2):
            crack.add(
                y_dev(s),
                r.pack_d.at[s],
                r.in_d_y.at[par, 1 - s],
                r.in_d_y.at[par, s],
                2 + 1 - s,
                2 + s,
            )
        for sx in range(2):
            for sy in range(2):
                crack.add(
                    c_dev(sx, sy),
                    r.pack_d.at[sy, pl.ds(0 if sx == 0 else nx - 1, 1)],
                    r.in_d_c.at[par, (1 - sx) * 2 + 1 - sy],
                    r.in_d_c.at[par, sx * 2 + sy],
                    4 + (1 - sx) * 2 + 1 - sy,
                    4 + sx * 2 + sy,
                )
        crack.start()
        shift.finish()
        third_x = (HX - 3, HX + nx + 2)
        third_y = (slice(OY - 3, OY - 2), slice(OY + ny + 2, OY + ny + 3))
        for s in range(2):

            @pl.when(there["gx"][s])
            def _(s=s):
                state[q, 0:3, x_out(s, 2), inner] = r.in_u_x[par, s]
                state[q, 0, third_x[s], inner] = r.in_u_x3[par, s]

            @pl.when(there["gy"][s])
            def _(s=s):
                for f in range(3):
                    state[q, f, planes, y_out(s, 2)] = r.in_u_y[par, s, :, 2 * f : 2 * f + 2]
                state[q, 1, planes, third_y[s]] = r.in_u_y[par, s, :, 6:7]

        for sx in range(2):
            for sy in range(2):

                @pl.when(c_dev(sx, sy)[0])
                def _(sx=sx, sy=sy):
                    for f in range(3):
                        state[q, f, x_out(sx, 2), y_out(sy, 2)] = r.in_u_c[
                            par, sx * 2 + sy, :, 2 * f : 2 * f + 2
                        ]

        crack.finish()
        for s in range(2):

            @pl.when(there["gx"][s])
            def _(s=s):
                state[q, 3, x_out(s, 2), inner] = r.in_d_x[par, s]

            @pl.when(there["gy"][s])
            def _(s=s):
                state[q, 3, planes, y_out(s, 2)] = r.in_d_y[par, s]

        for sx in range(2):
            for sy in range(2):

                @pl.when(c_dev(sx, sy)[0])
                def _(sx=sx, sy=sy):
                    state[q, 3, x_out(sx, 1), y_out(sy, 2)] = r.in_d_c[par, sx * 2 + sy]

    open_sweep()
    if sections == 1:
        send_sums()
    for rnd in range(1, sections):
        sweep(rnd)

    cells = 3.0 * nx * ngx * ny * ngy * nz
    beside_y.sent()
    early.sent()
    later.sent()
    last_one.sent()
    for copy in tough_copies:
        copy.wait_send()
    for k in range(1, group):
        other = lax.rem(me + k, group)
        pltpu.make_async_remote_copy(
            src_ref=r.sums.at[me],
            dst_ref=r.sums.at[other],
            send_sem=r.sum_send.at[k - 1],
            recv_sem=r.sum_recv.at[other],
            device_id=peers[k - 1],
            device_id_type=MESH,
        ).wait()
    total = r.sums[0]
    for k in range(1, group):
        total = total + r.sums[k]
    entries = jnp.sqrt(jnp.sum(total, axis=1, keepdims=True) / cells)
    column = lax.broadcasted_iota(jnp.int32, (1, sections), 1)
    norms = jnp.zeros((1, sections), jnp.float32)
    for rnd in range(sections):
        norms = jnp.where(
            column == lax.rem(sec + rnd, sections), entries[rnd : rnd + 1], norms
        )
    r.norm_ref[...] = norms


def put_out(
    first_ref, second_ref, third_ref, dam_ref, norm_ref, disp_hbm, dam_hbm, norm_out, sems
):
    copies = [
        pltpu.make_async_copy(ref, disp_hbm.at[0, f], sems.at[f])
        for f, ref in enumerate((first_ref, second_ref, third_ref))
    ]
    copies.append(pltpu.make_async_copy(dam_ref, dam_hbm.at[0], sems.at[3]))
    for copy in copies:
        copy.start()
    norm_out[...] = norm_ref[...]
    for copy in copies:
        copy.wait()


def on_device(sizes, load_index, load_table, toughness, clamp_mask, load_mask, crack_mask):
    sections, ngx, ngy = sizes
    nx, ny, nz = clamp_mask.shape
    assert load_index.shape == (1,)
    group = ngx * ngy
    f32 = jnp.float32
    padded = (nx + 2 * HX, ny + 2 * OY, nz)
    vmem = pltpu.VMEM
    dma = pltpu.SemaphoreType.DMA
    later = max(sections - 1, 1)
    more = sections > 2
    scratch = {
        "index_ref": pltpu.SMEM(load_index.shape, jnp.int32),
        "table_ref": pltpu.SMEM(load_table.shape[::-1], f32),
        "tough_ref": vmem((1, nx, ny, nz), f32),
        "clamp_ref": vmem((nx, ny, nz), jnp.int32),
        "load_ref": vmem((nx, ny, nz), jnp.int32),
        "crack_ref": vmem((nx, ny, nz), jnp.int32),
        "local": dma((6,)),
        "state": vmem((2, 4) + padded, f32),
        "stiff": vmem(padded, f32),
        "flow": vmem(padded, f32),
        "held": vmem(padded, f32),
        "clamped": vmem(padded, f32),
        "free": vmem(padded, f32),
        "tough_pad": vmem(padded, f32),
        "crack_pad": vmem(padded, f32),
        "tough_in": vmem((later, nx, ny, nz), f32),
        "pack_l": vmem((2, nx, 8, nz), jnp.int32),
        "pack_c": vmem((2, nx, 4, nz), jnp.int32),
        "pack_t": vmem((2, nx, 2, nz), f32),
        "pack_k": vmem((4, 3, 8, nz), jnp.int32),
        "pack_tk": vmem((4, 1, nz), f32),
        "in_x": vmem((2, 12, ny, nz), jnp.int32),
        "in_tx": vmem((2, 2, ny, nz), f32),
        "in_l": vmem((2, nx, 8, nz), jnp.int32),
        "in_c": vmem((2, nx, 4, nz), jnp.int32),
        "in_ty": vmem((2, nx, 2, nz), f32),
        "in_k": vmem((4, 3, 8, nz), jnp.int32),
        "in_tk": vmem((4, 1, nz), f32),
        "sums": vmem((group, sections, nz), f32),
        "y_send": dma((6,)),
        "y_recv": dma((6,)),
        "early_send": dma((8,)),
        "early_recv": dma((8,)),
        "later_send": dma((2,)),
        "later_recv": dma((2,)),
        "last_send": dma((6,)),
        "last_recv": dma((6,)),
        "tough_send": dma((later,)),
        "tough_recv": dma((later,)),
        "sum_send": dma((max(group - 1, 1),)),
        "sum_recv": dma((group,)),
    }
    if more:
        scratch |= {
            "pack_u": vmem((2, nx, 8, nz), f32),
            "pack_d": vmem((2, nx, 2, nz), f32),
            "in_u_x": vmem((2, 2, 3, 2, ny, nz), f32),
            "in_u_x3": vmem((2, 2, ny, nz), f32),
            "in_u_y": vmem((2, 2, nx, 8, nz), f32),
            "in_u_c": vmem((2, 4, 2, 8, nz), f32),
            "in_d_x": vmem((2, 2, 2, ny, nz), f32),
            "in_d_y": vmem((2, 2, nx, 2, nz), f32),
            "in_d_c": vmem((2, 4, 1, 2, nz), f32),
            "u_send": dma((10,)),
            "u_recv": dma((2, 10)),
            "d_send": dma((8,)),
            "d_recv": dma((2, 8)),
        }
    ins = ("index_hbm", "table_hbm", "tough_hbm", "clamp_hbm", "load_hbm", "crack_hbm")
    outs = ("first_ref", "second_ref", "third_ref", "dam_ref", "norm_ref")
    names = (*ins, *outs, *scratch)
    block = pl.BlockSpec(memory_space=pltpu.VMEM)
    away = pl.BlockSpec(memory_space=pltpu.HBM)
    results = pl.pallas_call(
        functools.partial(kernel, (sections, ngx, ngy, nx, ny, nz), names),
        out_shape=(
            *[jax.ShapeDtypeStruct((nx, ny, nz), f32)] * 4,
            jax.ShapeDtypeStruct((1, sections), f32),
        ),
        in_specs=[away] * 6,
        out_specs=(block,) * 5,
        scratch_shapes=list(scratch.values()),
        compiler_params=pltpu.CompilerParams(
            collective_id=0, has_side_effects=True, vmem_limit_bytes=56_020_000
        ),
    )(load_index, pltpu.with_memory_space_constraint(load_table.T, pltpu.HBM), toughness, clamp_mask, load_mask, crack_mask)
    return pl.pallas_call(
        put_out,
        out_shape=(
            jax.ShapeDtypeStruct((1, 3, nx, ny, nz), f32),
            jax.ShapeDtypeStruct((1, nx, ny, nz), f32),
            jax.ShapeDtypeStruct((1, sections), f32),
        ),
        in_specs=[block] * 5,
        out_specs=(away, away, block),
        scratch_shapes=[dma((4,))],
        compiler_params=pltpu.CompilerParams(vmem_limit_bytes=1024 * 1024),
    )(*results)


def solution(mesh):
    in_specs = (
        P("section"),
        P(),
        P("section", "gx", "gy", None),
        P("gx", "gy", None),
        P("gx", "gy", None),
        P("gx", "gy", None),
    )
    out_specs = (
        P("section", None, "gx", "gy", None),
        P("section", "gx", "gy", None),
        P("section", None),
    )
    sizes = tuple(mesh.shape[name] for name in ("section", "gx", "gy"))
    return jax.shard_map(
        functools.partial(on_device, sizes),
        mesh=mesh,
        in_specs=in_specs,
        out_specs=out_specs,
        check_vma=False,
    )
```

```python
import functools
import math
import types

import jax
import jax.numpy as jnp
from jax import lax
from jax.experimental import pallas as pl
from jax.experimental.pallas import tpu as pltpu
from jax.sharding import PartitionSpec as P

relax_weight = 0.6
stiff_floor = 0.001
eigen_guard = 1e-08
MESH = pl.DeviceIdType.MESH

HX = 5
OY = 8

ACOS = (
    1.5707963050,
    -0.2145988016,
    0.0889789874,
    -0.0501743046,
    0.0308918810,
    -0.0170881256,
    0.0066700901,
    -0.0012624911,
)


def up8(n):
    return -(-n // 8) * 8


def part(n, most):
    return max(k for k in range(1, most + 1) if n % k == 0)


def root(v):
    return v * lax.rsqrt(jnp.maximum(v, 1.2e-38))


def spectral_energy(xx, yy, zz, xy, xz, yz):
    trace = xx + yy + zz
    mid = trace * (1.0 / 3.0)
    dx = xx - mid
    dy = yy - mid
    dz = zz - mid
    xy2 = xy * xy
    xz2 = xz * xz
    yz2 = yz * yz
    sixth = (dx * dx + dy * dy + dz * dz + 2.0 * (xy2 + xz2 + yz2)) * (1.0 / 6.0)
    twice_radius = 2.0 * root(sixth)
    scale = lax.rsqrt(sixth + eigen_guard)
    det = dx * (dy * dz - yz2) - dz * xy2 - dy * xz2 + 2.0 * (xy * xz * yz)
    ratio = (0.5 * det * scale) * (scale * scale)
    size = jnp.minimum(jnp.abs(ratio), 1.0)
    poly = jnp.full_like(size, ACOS[-1] / 3.0)
    for c in ACOS[-2::-1]:
        poly = poly * size + c / 3.0
    t = root(1.0 - size) * poly
    t2 = t * t
    cos_t = 1.0 + t2 * (-0.5 + t2 * (1.0 / 24.0 + t2 * (-1.0 / 720.0 + t2 * (1.0 / 40320.0))))
    sin_t = t * (1.0 + t2 * (-1.0 / 6.0 + t2 * (1.0 / 120.0 + t2 * (-1.0 / 5040.0))))
    other = 0.5 * cos_t + math.sqrt(0.75) * sin_t
    upper = ratio >= 0.0
    first = jnp.where(upper, cos_t, other)
    last = jnp.where(upper, other, cos_t)
    largest = mid + twice_radius * first
    smallest = mid - twice_radius * last
    between = trace - largest - smallest
    relu = lambda v: jnp.maximum(v, 0.0)
    return (
        0.5 * jnp.square(relu(trace))
        + jnp.square(relu(largest))
        + jnp.square(relu(between))
        + jnp.square(relu(smallest))
    )


def kernel(sizes, names, *refs):
    sections, ngx, ngy, nx, ny, nz = sizes
    r = types.SimpleNamespace(**dict(zip(names, refs)))
    local, state, stiff, flow = r.local, r.state, r.stiff, r.flow
    held, clamped, free, tough_pad, crack_pad = r.held, r.clamped, r.free, r.tough_pad, r.crack_pad
    load_ref, crack_ref, clamp_ref, tough_ref = r.load_ref, r.crack_ref, r.clamp_ref, r.tough_ref
    disp_refs = (r.first_ref, r.second_ref, r.third_ref)
    sec = lax.axis_index("section")
    gx = lax.axis_index("gx")
    gy = lax.axis_index("gy")
    group = ngx * ngy
    me = gx * ngy + gy
    ring = lambda k, n: min(k, n - k)
    offsets = [(i, j) for i in range(ngx) for j in range(ngy) if i or j]
    offsets.sort(key=lambda o: (ring(o[0], ngx) + ring(o[1], ngy), o))
    peers = []
    for i, j in offsets:
        peers.append({"gx": lax.rem(gx + i, ngx), "gy": lax.rem(gy + j, ngy)})

    barrier = pltpu.get_barrier_semaphore()
    for peer in peers:
        pl.semaphore_signal(barrier, inc=1, device_id=peer, device_id_type=MESH)
    for k in range(1, sections):
        pl.semaphore_signal(
            barrier,
            inc=1,
            device_id={"section": lax.rem(sec + k, sections)},
            device_id_type=MESH,
        )

    fetch = [
        pltpu.make_async_copy(src, dst, local.at[n])
        for n, (src, dst) in enumerate(
            (
                (r.load_hbm, load_ref),
                (r.crack_hbm, crack_ref),
                (r.clamp_hbm, clamp_ref),
                (r.tough_hbm, tough_ref),
                (r.index_hbm, r.index_ref),
                (r.table_hbm, r.table_ref),
            )
        )
    ]
    for copy in fetch:
        copy.start()

    there = {
        "gx": (gx > 0, gx < ngx - 1),
        "gy": (gy > 0, gy < ngy - 1),
    }
    step = (-1, 1)

    def x_dev(s):
        return there["gx"][s], {"gx": gx + step[s]}

    def y_dev(s):
        return there["gy"][s], {"gy": gy + step[s]}

    def c_dev(sx, sy):
        return (
            jnp.logical_and(there["gx"][sx], there["gy"][sy]),
            {"gx": gx + step[sx], "gy": gy + step[sy]},
        )

    class Exchange:
        def __init__(self, send, recv):
            self.items = []
            self.send = send
            self.recv = recv

        def add(self, where, src, dst, mine, out_slot, in_slot):
            cond, dev = where
            n = len(self.items)
            copy = pltpu.make_async_remote_copy(
                src_ref=src,
                dst_ref=dst,
                send_sem=self.send.at[n],
                recv_sem=self.recv.at[out_slot],
                device_id=dev,
                device_id_type=MESH,
            )
            back = pltpu.make_async_remote_copy(
                src_ref=src,
                dst_ref=mine,
                send_sem=self.send.at[n],
                recv_sem=self.recv.at[in_slot],
                device_id=dev,
                device_id_type=MESH,
            )
            self.items.append((cond, copy, back))

        def start(self, begin=0, end=None):
            for cond, copy, _ in self.items[begin:end]:
                pl.when(cond)(copy.start)

        def finish(self):
            for cond, copy, back in self.items:

                @pl.when(cond)
                def _():
                    back.wait_recv()
                    copy.wait_send()

        def received(self, begin=0, end=None):
            for cond, _, back in self.items[begin:end]:
                pl.when(cond)(back.wait_recv)

        def sent(self):
            for cond, copy, _ in self.items:
                pl.when(cond)(copy.wait_send)

    rows = ny + 2 * OY

    def clear(xp, carry):
        zero = jnp.zeros((rows, nz), jnp.float32)
        held[xp] = zero
        crack_pad[xp] = zero
        clamped[xp] = zero + 1.0
        tough_pad[xp] = zero + 1.0
        free[xp] = zero
        if sections > 2:
            for p in range(2):
                for f in range(4):
                    state[p, f, xp] = zero
        return carry

    lax.fori_loop(0, nx + 2 * HX, clear, 0)

    for copy in fetch[:3]:
        copy.wait()

    for s in range(2):
        side = lambda n, s=s: slice(0, n) if s == 0 else slice(ny - n, ny)
        r.pack_c[s] = crack_ref[:, side(4)]
        for x in range(nx):
            r.pack_l[s, 5 * x : 5 * x + 5] = load_ref[x, side(5)]
            r.pack_f[s, 3 * x : 3 * x + 3] = clamp_ref[x, side(3)]
    corner = (
        (load_ref, held, 1, 4, 0),
        (load_ref, held, 2, 3, 4),
        (load_ref, held, 4, 1, 7),
        (load_ref, held, 3, 2, 8),
        (crack_ref, crack_pad, 1, 3, 10),
        (crack_ref, crack_pad, 2, 2, 13),
        (crack_ref, crack_pad, 3, 1, 15),
        (clamp_ref, clamped, 1, 2, 16),
        (clamp_ref, clamped, 2, 1, 18),
    )
    for sx in range(2):
        for sy in range(2):
            for ref, _, deep, n, at in corner:
                plane = deep - 1 if sx == 0 else nx - deep
                first = 0 if sy == 0 else ny - n
                pack, at = (r.pack_k, at) if at < 16 else (r.pack_kf, at - 16)
                pack[sx * 2 + sy, at : at + n] = ref[plane, first : first + n]

    pl.semaphore_wait(barrier, group - 1 + sections - 1)

    beside_y = Exchange(r.y_send, r.y_recv)
    early = Exchange(r.early_send, r.early_recv)
    later = Exchange(r.later_send, r.later_recv)
    last_one = Exchange(r.last_send, r.last_recv)
    for s in range(2):
        for ex, ref, buf, width, at, slot in (
            (early, load_ref, r.in_x, 5, 0, 0),
            (early, crack_ref, r.in_x, 4, 5, 2),
            (later, clamp_ref, r.in_x, 3, 9, 0),
            (last_one, tough_ref.at[0], r.in_tx, 2, 0, 0),
        ):
            ex.add(
                x_dev(s),
                ref.at[pl.ds(0 if s == 0 else nx - width, width)],
                buf.at[1 - s, pl.ds(at, width)],
                buf.at[s, pl.ds(at, width)],
                slot + 1 - s,
                slot + s,
            )
    for n in range(8):
        s = n % 2
        for pack, buf, slot in (
            (r.pack_c, r.in_c, 0),
            (r.pack_l, r.in_l, 2),
            (r.pack_f, r.in_f, 4),
            (r.pack_t, r.in_ty, 6),
        )[n // 2 : n // 2 + 1]:
            beside_y.add(
                y_dev(s), pack.at[s], buf.at[1 - s], buf.at[s], slot + 1 - s, slot + s
            )
    for sx in range(2):
        for sy in range(2):
            here, away = sx * 2 + sy, (1 - sx) * 2 + 1 - sy
            early.add(
                c_dev(sx, sy), r.pack_k.at[here], r.in_k.at[away], r.in_k.at[here],
                4 + away, 4 + here,
            )
            later.add(
                c_dev(sx, sy), r.pack_kf.at[here], r.in_kf.at[away], r.in_kf.at[here],
                2 + away, 2 + here,
            )
            last_one.add(
                c_dev(sx, sy), r.pack_tk.at[here], r.in_tk.at[away], r.in_tk.at[here],
                2 + away, 2 + here,
            )
    early.start(0, 4)
    beside_y.start(0, 6)
    fetch[3].wait()
    for s in range(2):
        r.pack_t[s] = tough_ref[0, :, 0:2] if s == 0 else tough_ref[0, :, ny - 2 : ny]
    for sx in range(2):
        for sy in range(2):
            row = 0 if sy == 0 else ny - 1
            r.pack_tk[sx * 2 + sy] = tough_ref[0, 0 if sx == 0 else nx - 1, row : row + 1]
    beside_y.start(6)
    early.start(4)
    later.start()
    last_one.start()

    tough_copies = []
    for k in range(1, sections):
        copy = pltpu.make_async_remote_copy(
            src_ref=tough_ref.at[0],
            dst_ref=r.tough_in.at[k - 1],
            send_sem=r.tough_send.at[k - 1],
            recv_sem=r.tough_recv.at[k - 1],
            device_id={"section": lax.rem(sec + sections - k, sections)},
            device_id_type=MESH,
        )
        copy.start()
        tough_copies.append(copy)

    inner = slice(OY, OY + ny)
    as_float = lambda v: v.astype(jnp.float32)

    def fill(x, carry):
        load = as_float(load_ref[x])
        clamp = as_float(clamp_ref[x])
        held[x + HX, inner] = load
        clamped[x + HX, inner] = clamp
        free[x + HX, inner] = 1.0 - jnp.maximum(clamp, load)
        crack_pad[x + HX, inner] = as_float(crack_ref[x])
        tough_pad[x + HX, inner] = tough_ref[0, x]
        return carry

    lax.fori_loop(0, nx, fill, 0, unroll=part(nx, 4))

    for copy in fetch[4:]:
        copy.wait()
    case = r.index_ref[0]
    vector = [r.table_ref[f, case] for f in range(3)]

    planes = slice(HX, HX + nx)

    def x_out(s, n):
        return slice(HX - n, HX) if s == 0 else slice(HX + nx, HX + nx + n)

    def y_out(s, n):
        return slice(OY - n, OY) if s == 0 else slice(OY + ny, OY + ny + n)

    def unpack_y():
        beside_y.received(0, 4)
        for s in range(2):

            @pl.when(there["gy"][s])
            def _(s=s):
                crack_pad[planes, y_out(s, 4)] = as_float(r.in_c[s])
                for x in range(nx):
                    held[HX + x, y_out(s, 5)] = as_float(r.in_l[s, 5 * x : 5 * x + 5])

    def unpack_y_clamp():
        beside_y.received(4, 6)
        for s in range(2):

            @pl.when(there["gy"][s])
            def _(s=s):
                for x in range(nx):
                    clamped[HX + x, y_out(s, 3)] = as_float(r.in_f[s, 3 * x : 3 * x + 3])

    def unpack_y_tough():
        beside_y.received(6)
        for s in range(2):

            @pl.when(there["gy"][s])
            def _(s=s):
                tough_pad[planes, y_out(s, 2)] = r.in_ty[s]

    def unpack_x():
        early.received()
        for s in range(2):

            @pl.when(there["gx"][s])
            def _(s=s):
                held[x_out(s, 5), inner] = as_float(r.in_x[s, 0:5])
                crack_pad[x_out(s, 4), inner] = as_float(r.in_x[s, 5:9])

        for sx in range(2):
            for sy in range(2):

                @pl.when(c_dev(sx, sy)[0])
                def _(sx=sx, sy=sy):
                    for _, pad, deep, n, at in corner[:-2]:
                        plane = HX - deep if sx == 0 else HX + nx - 1 + deep
                        pad[plane, y_out(sy, n)] = as_float(r.in_k[sx * 2 + sy, at : at + n])

    def unpack_clamp():
        later.received()
        for s in range(2):

            @pl.when(there["gx"][s])
            def _(s=s):
                clamped[x_out(s, 3), inner] = as_float(r.in_x[s, 9:12])

        for sx in range(2):
            for sy in range(2):

                @pl.when(c_dev(sx, sy)[0])
                def _(sx=sx, sy=sy):
                    for _, pad, deep, n, at in corner[-2:]:
                        plane = HX - deep if sx == 0 else HX + nx - 1 + deep
                        at = at - 16
                        pad[plane, y_out(sy, n)] = as_float(r.in_kf[sx * 2 + sy, at : at + n])

    def unpack_tough():
        last_one.received()
        for s in range(2):

            @pl.when(there["gx"][s])
            def _(s=s):
                tough_pad[x_out(s, 2), inner] = r.in_tx[s]

        for sx in range(2):
            for sy in range(2):

                @pl.when(c_dev(sx, sy)[0])
                def _(sx=sx, sy=sy):
                    plane = HX - 1 if sx == 0 else HX + nx
                    tough_pad[plane, y_out(sy, 1)] = r.in_tk[sx * 2 + sy]

    wide = up8(ny + 4)
    deep = up8(ny + 8)

    def lanes(shape, lane):
        return lax.broadcasted_iota(jnp.int32, shape, 1) == lane

    def beside(v, edge, first, last):
        up = jnp.where(last, edge, pltpu.roll(v, nz - 1, 1))
        down = jnp.where(first, edge, pltpu.roll(v, 1, 1))
        return up, down

    def inside_rows(shape, above):
        row = lax.broadcasted_iota(jnp.int32, shape, 0) + (gy * ny - above)
        return jnp.logical_and(row >= 0, row < ny * ngy)

    def inside_plane(xp):
        plane = xp - HX + gx * nx
        return jnp.logical_and(plane >= 0, plane < nx * ngx)

    edge_stiff = 0.5 * (1.0 + stiff_floor)

    def elastic(at, first, last):
        k = at(stiff, 0, 0)
        sides = (
            (at(stiff, 1, 0), at(stiff, -1, 0)),
            (at(stiff, 0, 1), at(stiff, 0, -1)),
            beside(k, edge_stiff, first, last),
        )
        pairs = [s[0] + s[1] for s in sides]
        weights = pairs[0] + pairs[1] + pairs[2] + 6.0 * k
        faces = [(k + s[0], k + s[1]) for s in sides]
        fz = beside(at(flow, 0, 0), 0.0, first, last)
        grads = (
            at(flow, 1, 0) - at(flow, -1, 0),
            at(flow, 0, 1) - at(flow, 0, -1),
            fz[0] - fz[1],
        )
        return pairs, weights, faces, grads

    def laplace(at, ref, faces, weights, first, last):
        here = at(ref, 0, 0)
        uz = beside(here, 0.0, first, last)
        return here, (
            faces[0][0] * at(ref, 1, 0)
            + faces[0][1] * at(ref, -1, 0)
            + faces[1][0] * at(ref, 0, 1)
            + faces[1][1] * at(ref, 0, -1)
            + faces[2][0] * uz[0]
            + faces[2][1] * uz[1]
            - weights * here
        )

    def strain_energy(at, u, keep, first, last):
        grad = []
        for f in range(3):
            here = at(u.at[f], 0, 0)
            uz = beside(here, 0.0, first, last)
            grad.append(
                (
                    at(u.at[f], 1, 0) - at(u.at[f], -1, 0),
                    at(u.at[f], 0, 1) - at(u.at[f], 0, -1),
                    uz[0] - uz[1],
                )
            )
            keep(f, here)
        return 2.0 * spectral_energy(
            0.5 * grad[0][0],
            0.5 * grad[1][1],
            0.5 * grad[2][2],
            0.25 * (grad[0][1] + grad[1][0]),
            0.25 * (grad[0][2] + grad[2][0]),
            0.25 * (grad[1][2] + grad[2][1]),
        )

    def renew(at, d, energy, g, cracked, first, last):
        dz = beside(at(d, 0, 0), 0.0, first, last)
        around = at(d, 1, 0) + at(d, -1, 0) + at(d, 0, 1) + at(d, 0, -1) + dz[0] + dz[1]
        renewed = (energy + g * around) / (7.0 * g + energy)
        return jnp.where(cracked, 1.0, renewed)

    def add_up(rnd, total):
        r.sums[me, rnd : rnd + 1] = jnp.sum(total, axis=0, keepdims=True)

    def open_sweep():
        shape = (deep, nz)
        first, last = lanes(shape, 0), lanes(shape, nz - 1)
        row_inside = inside_rows(shape, 4)
        a = OY - 4

        def stiffen(xp, carry):
            half = 0.5 * (jnp.square(1.0 - crack_pad[xp, a : a + deep]) + stiff_floor)
            stiff[xp, a : a + deep] = half
            up, down = beside(held[xp, a : a + deep], 0.0, first, last)
            div = (
                vector[0] * (held[xp + 1, a : a + deep] - held[xp - 1, a : a + deep])
                + vector[1] * (held[xp, a + 1 : a + 1 + deep] - held[xp, a - 1 : a - 1 + deep])
                + vector[2] * (up - down)
            )
            flow[xp, a : a + deep] = jnp.where(
                jnp.logical_and(row_inside, inside_plane(xp)), half * div, 0.0
            )
            return carry

        def move(xp, total):
            at = lambda ref, dx, dy: ref[xp + dx, a + dy : a + dy + deep]
            pairs, weights, faces, grads = elastic(at, first, last)
            load, spread = laplace(at, held, faces, weights, first, last)
            pin = at(clamped, 0, 0) + load > 0.5
            squares = None
            for f in range(3):
                res = vector[f] * spread + grads[f]
                moved = jnp.where(pin, 0.0, relax_weight * res / (weights + pairs[f]))
                state[1, f, xp, a : a + deep] = vector[f] * load + moved
                square = res * res
                squares = square if squares is None else squares + square
            return total + jnp.where(at(free, 0, 0) > 0.5, squares, 0.0)

        def damage(xp, carry):
            at = lambda ref, dx, dy: ref[xp + dx, a + dy : a + dy + deep]
            energy = strain_energy(at, state.at[1], lambda f, v: None, first, last)
            renewed = renew(
                at,
                crack_pad,
                energy,
                at(tough_pad, 0, 0),
                at(crack_pad, 0, 0) > 0.5,
                first,
                last,
            )
            state[1, 3, xp, a : a + deep] = jnp.where(
                jnp.logical_and(row_inside, inside_plane(xp)), renewed, 0.0
            )
            return carry

        def inward(skip, body, carry, most):
            n = nx - 2 * skip
            return lax.fori_loop(HX + skip, HX + nx - skip, body, carry, unroll=part(n, most))

        def outward(far, body, carry, n=5):
            def both(i, carry):
                carry = body(HX - far + i, carry)
                return body(HX + nx + far - n + i, carry)

            return lax.fori_loop(0, n, both, carry, unroll=True)

        own = jnp.zeros((ny, nz), jnp.float32)
        unpack_y()
        inward(1, stiffen, 0, 14)
        unpack_y_clamp()
        total = inward(2, move, jnp.zeros(shape, jnp.float32), 12)
        unpack_y_tough()
        inward(3, damage, 0, 5)
        if sections > 1:
            stiffen1, mover1 = stages(1)
            inward(3, stiffen1, 0, 10)
            own = inward(4, mover1(OY, ny), own, 8)
        unpack_x()
        outward(4, stiffen, 0)
        unpack_clamp()
        total = outward(3, move, total)
        add_up(0, total)
        unpack_tough()
        outward(2, damage, 0)
        if sections > 1:
            outward(2, stiffen1, 0)
            own = outward(0, mover1(OY, ny), own, 4)
        return own

    def send_sums():
        for k, peer in enumerate(peers):
            pltpu.make_async_remote_copy(
                src_ref=r.sums.at[me],
                dst_ref=r.sums.at[me],
                send_sem=r.sum_send.at[k],
                recv_sem=r.sum_recv.at[me],
                device_id=peer,
                device_id_type=MESH,
            ).start()

    def stages(rnd):
        p = rnd % 2
        q = 1 - p
        shape = (wide, nz)
        first, last = lanes(shape, 0), lanes(shape, nz - 1)
        row_inside = inside_rows(shape, 2)
        a = OY - 2

        def stiffen(xp, carry):
            half = 0.5 * (jnp.square(1.0 - state[p, 3, xp, a : a + wide]) + stiff_floor)
            stiff[xp, a : a + wide] = half
            up, down = beside(state[p, 2, xp, a : a + wide], 0.0, first, last)
            div = (
                (state[p, 0, xp + 1, a : a + wide] - state[p, 0, xp - 1, a : a + wide])
                + (state[p, 1, xp, a + 1 : a + 1 + wide] - state[p, 1, xp, a - 1 : a - 1 + wide])
                + (up - down)
            )
            flow[xp, a : a + wide] = jnp.where(
                jnp.logical_and(row_inside, inside_plane(xp)), half * div, 0.0
            )
            return carry

        def mover(b, n):
            shape = (n, nz)
            first, last = lanes(shape, 0), lanes(shape, nz - 1)

            def move(xp, total):
                at = lambda ref, dx, dy: ref[xp + dx, b + dy : b + dy + n]
                pairs, weights, faces, grads = elastic(at, first, last)
                load = at(held, 0, 0)
                pin = at(clamped, 0, 0) + load > 0.5
                squares = None
                for f in range(3):
                    here, spread = laplace(at, state.at[p, f], faces, weights, first, last)
                    res = spread + grads[f]
                    moved = here + relax_weight * res / (weights + pairs[f])
                    state[q, f, xp, b : b + n] = jnp.where(pin, load * vector[f], moved)
                    square = res * res
                    squares = square if squares is None else squares + square
                return total + jnp.where(pin, 0.0, squares)

            return move

        return stiffen, mover

    def sweep(rnd, total):
        p = rnd % 2
        q = 1 - p
        done = rnd == sections - 1
        tough = r.tough_in.at[rnd - 1]

        stiffen, mover = stages(rnd)
        if rnd > 1:
            lax.fori_loop(HX - 2, HX + nx + 2, stiffen, 0, unroll=part(nx + 4, 10))
            total = lax.fori_loop(
                HX, HX + nx, mover(OY, ny), jnp.zeros((ny, nz), jnp.float32), unroll=part(nx, 8)
            )
        add_up(rnd, total)
        if done:
            send_sums()
        none = jnp.zeros((8, nz), jnp.float32)

        def edges(xp, carry):
            mover(OY - 4, 8)(xp, none)
            mover(OY + ny - 3, 8)(xp, none)
            return carry

        lax.fori_loop(HX, HX + nx, edges, 0, unroll=part(nx, 8))
        ends = mover(OY, ny)
        ends(HX - 1, jnp.zeros((ny, nz), jnp.float32))
        ends(HX + nx, jnp.zeros((ny, nz), jnp.float32))
        par = rnd % 2
        mid = pl.ds(OY, ny)
        if not done:
            for f in range(3):
                r.pack_u[0, :, 2 * f : 2 * f + 2] = state[q, f, planes, OY : OY + 2]
                r.pack_u[1, :, 2 * f : 2 * f + 2] = state[q, f, planes, OY + ny - 2 : OY + ny]
            r.pack_u[0, :, 6:7] = state[q, 1, planes, OY + 2 : OY + 3]
            r.pack_u[1, :, 6:7] = state[q, 1, planes, OY + ny - 3 : OY + ny - 2]
            shift = Exchange(r.u_send, r.u_recv.at[par])
            for s in range(2):
                shift.add(
                    x_dev(s),
                    state.at[q, pl.ds(0, 3), pl.ds(HX if s == 0 else HX + nx - 2, 2), mid],
                    r.in_u_x.at[par, 1 - s],
                    r.in_u_x.at[par, s],
                    (1 - s),
                    s,
                )
                shift.add(
                    x_dev(s),
                    state.at[q, 0, HX + 2 if s == 0 else HX + nx - 3, mid],
                    r.in_u_x3.at[par, 1 - s],
                    r.in_u_x3.at[par, s],
                    2 + (1 - s),
                    2 + s,
                )
            for s in range(2):
                shift.add(
                    y_dev(s),
                    r.pack_u.at[s],
                    r.in_u_y.at[par, 1 - s],
                    r.in_u_y.at[par, s],
                    4 + (1 - s),
                    4 + s,
                )
            for sx in range(2):
                for sy in range(2):
                    shift.add(
                        c_dev(sx, sy),
                        r.pack_u.at[sy, pl.ds(0 if sx == 0 else nx - 2, 2)],
                        r.in_u_c.at[par, (1 - sx) * 2 + 1 - sy],
                        r.in_u_c.at[par, sx * 2 + sy],
                        6 + (1 - sx) * 2 + 1 - sy,
                        6 + sx * 2 + sy,
                    )
            shift.start()

        tough_copies[rnd - 1].wait_recv()

        shape = (ny, nz)
        first, last = lanes(shape, 0), lanes(shape, nz - 1)

        def damage(x, carry):
            xp = x + HX
            at = lambda ref, dx, dy: ref[xp + dx, OY + dy : OY + dy + ny]

            def keep(f, here):
                if done:
                    disp_refs[f][x] = here

            energy = strain_energy(at, state.at[q], keep, first, last)
            renewed = renew(
                at, state.at[p, 3], energy, tough[x], crack_ref[x] > 0, first, last
            )
            if done:
                r.dam_ref[x] = renewed
            else:
                state[q, 3, xp, inner] = renewed
            return carry

        lax.fori_loop(0, nx, damage, 0, unroll=part(nx, 8))
        if done:
            return

        r.pack_d[0] = state[q, 3, planes, OY : OY + 2]
        r.pack_d[1] = state[q, 3, planes, OY + ny - 2 : OY + ny]
        crack = Exchange(r.d_send, r.d_recv.at[par])
        for s in range(2):
            crack.add(
                x_dev(s),
                state.at[q, 3, pl.ds(HX if s == 0 else HX + nx - 2, 2), mid],
                r.in_d_x.at[par, 1 - s],
                r.in_d_x.at[par, s],
                1 - s,
                s,
            )
        for s in range(2):
            crack.add(
                y_dev(s),
                r.pack_d.at[s],
                r.in_d_y.at[par, 1 - s],
                r.in_d_y.at[par, s],
                2 + 1 - s,
                2 + s,
            )
        for sx in range(2):
            for sy in range(2):
                crack.add(
                    c_dev(sx, sy),
                    r.pack_d.at[sy, pl.ds(0 if sx == 0 else nx - 1, 1)],
                    r.in_d_c.at[par, (1 - sx) * 2 + 1 - sy],
                    r.in_d_c.at[par, sx * 2 + sy],
                    4 + (1 - sx) * 2 + 1 - sy,
                    4 + sx * 2 + sy,
                )
        crack.start()
        shift.finish()
        third_x = (HX - 3, HX + nx + 2)
        third_y = (slice(OY - 3, OY - 2), slice(OY + ny + 2, OY + ny + 3))
        for s in range(2):

            @pl.when(there["gx"][s])
            def _(s=s):
                state[q, 0:3, x_out(s, 2), inner] = r.in_u_x[par, s]
                state[q, 0, third_x[s], inner] = r.in_u_x3[par, s]

            @pl.when(there["gy"][s])
            def _(s=s):
                for f in range(3):
                    state[q, f, planes, y_out(s, 2)] = r.in_u_y[par, s, :, 2 * f : 2 * f + 2]
                state[q, 1, planes, third_y[s]] = r.in_u_y[par, s, :, 6:7]

        for sx in range(2):
            for sy in range(2):

                @pl.when(c_dev(sx, sy)[0])
                def _(sx=sx, sy=sy):
                    for f in range(3):
                        state[q, f, x_out(sx, 2), y_out(sy, 2)] = r.in_u_c[
                            par, sx * 2 + sy, :, 2 * f : 2 * f + 2
                        ]

        crack.finish()
        for s in range(2):

            @pl.when(there["gx"][s])
            def _(s=s):
                state[q, 3, x_out(s, 2), inner] = r.in_d_x[par, s]

            @pl.when(there["gy"][s])
            def _(s=s):
                state[q, 3, planes, y_out(s, 2)] = r.in_d_y[par, s]

        for sx in range(2):
            for sy in range(2):

                @pl.when(c_dev(sx, sy)[0])
                def _(sx=sx, sy=sy):
                    state[q, 3, x_out(sx, 1), y_out(sy, 2)] = r.in_d_c[par, sx * 2 + sy]

    total = open_sweep()
    if sections == 1:
        send_sums()
    for rnd in range(1, sections):
        sweep(rnd, total)

    cells = 3.0 * nx * ngx * ny * ngy * nz
    beside_y.sent()
    early.sent()
    later.sent()
    last_one.sent()
    for copy in tough_copies:
        copy.wait_send()
    for k, peer in enumerate(peers):
        other = peer["gx"] * ngy + peer["gy"]
        pltpu.make_async_remote_copy(
            src_ref=r.sums.at[me],
            dst_ref=r.sums.at[other],
            send_sem=r.sum_send.at[k],
            recv_sem=r.sum_recv.at[other],
            device_id=peer,
            device_id_type=MESH,
        ).wait()
    total = r.sums[0]
    for k in range(1, group):
        total = total + r.sums[k]
    entries = jnp.sqrt(jnp.sum(total, axis=1, keepdims=True) / cells)
    column = lax.broadcasted_iota(jnp.int32, (1, sections), 1)
    norms = jnp.zeros((1, sections), jnp.float32)
    for rnd in range(sections):
        norms = jnp.where(
            column == lax.rem(sec + rnd, sections), entries[rnd : rnd + 1], norms
        )
    r.norm_ref[...] = norms


def put_out(
    first_ref, second_ref, third_ref, dam_ref, norm_ref, disp_hbm, dam_hbm, norm_out, sems
):
    copies = [
        pltpu.make_async_copy(ref, disp_hbm.at[0, f], sems.at[f])
        for f, ref in enumerate((first_ref, second_ref, third_ref))
    ]
    copies.append(pltpu.make_async_copy(dam_ref, dam_hbm.at[0], sems.at[3]))
    for copy in copies:
        copy.start()
    norm_out[...] = norm_ref[...]
    for copy in copies:
        copy.wait()


def on_device(sizes, load_index, load_table, toughness, clamp_mask, load_mask, crack_mask):
    sections, ngx, ngy = sizes
    nx, ny, nz = clamp_mask.shape
    assert load_index.shape == (1,)
    group = ngx * ngy
    f32 = jnp.float32
    padded = (nx + 2 * HX, ny + 2 * OY, nz)
    vmem = pltpu.VMEM
    dma = pltpu.SemaphoreType.DMA
    later = max(sections - 1, 1)
    more = sections > 2
    scratch = {
        "index_ref": pltpu.SMEM(load_index.shape, jnp.int32),
        "table_ref": pltpu.SMEM(load_table.shape[::-1], f32),
        "tough_ref": vmem((1, nx, ny, nz), f32),
        "clamp_ref": vmem((nx, ny, nz), jnp.int32),
        "load_ref": vmem((nx, ny, nz), jnp.int32),
        "crack_ref": vmem((nx, ny, nz), jnp.int32),
        "local": dma((6,)),
        "state": vmem((2, 4) + padded, f32),
        "stiff": vmem(padded, f32),
        "flow": vmem(padded, f32),
        "held": vmem(padded, f32),
        "clamped": vmem(padded, f32),
        "free": vmem(padded, f32),
        "tough_pad": vmem(padded, f32),
        "crack_pad": vmem(padded, f32),
        "tough_in": vmem((later, nx, ny, nz), f32),
        "pack_l": vmem((2, 5 * nx, nz), jnp.int32),
        "pack_f": vmem((2, 3 * nx, nz), jnp.int32),
        "pack_c": vmem((2, nx, 4, nz), jnp.int32),
        "pack_t": vmem((2, nx, 2, nz), f32),
        "pack_k": vmem((4, 16, nz), jnp.int32),
        "pack_kf": vmem((4, 4, nz), jnp.int32),
        "pack_tk": vmem((4, 1, nz), f32),
        "in_x": vmem((2, 12, ny, nz), jnp.int32),
        "in_tx": vmem((2, 2, ny, nz), f32),
        "in_l": vmem((2, 5 * nx, nz), jnp.int32),
        "in_f": vmem((2, 3 * nx, nz), jnp.int32),
        "in_c": vmem((2, nx, 4, nz), jnp.int32),
        "in_ty": vmem((2, nx, 2, nz), f32),
        "in_k": vmem((4, 16, nz), jnp.int32),
        "in_kf": vmem((4, 4, nz), jnp.int32),
        "in_tk": vmem((4, 1, nz), f32),
        "sums": vmem((group, sections, nz), f32),
        "y_send": dma((8,)),
        "y_recv": dma((8,)),
        "early_send": dma((8,)),
        "early_recv": dma((8,)),
        "later_send": dma((6,)),
        "later_recv": dma((6,)),
        "last_send": dma((6,)),
        "last_recv": dma((6,)),
        "tough_send": dma((later,)),
        "tough_recv": dma((later,)),
        "sum_send": dma((max(group - 1, 1),)),
        "sum_recv": dma((group,)),
    }
    if more:
        scratch |= {
            "pack_u": vmem((2, nx, 8, nz), f32),
            "pack_d": vmem((2, nx, 2, nz), f32),
            "in_u_x": vmem((2, 2, 3, 2, ny, nz), f32),
            "in_u_x3": vmem((2, 2, ny, nz), f32),
            "in_u_y": vmem((2, 2, nx, 8, nz), f32),
            "in_u_c": vmem((2, 4, 2, 8, nz), f32),
            "in_d_x": vmem((2, 2, 2, ny, nz), f32),
            "in_d_y": vmem((2, 2, nx, 2, nz), f32),
            "in_d_c": vmem((2, 4, 1, 2, nz), f32),
            "u_send": dma((10,)),
            "u_recv": dma((2, 10)),
            "d_send": dma((8,)),
            "d_recv": dma((2, 8)),
        }
    ins = ("index_hbm", "table_hbm", "tough_hbm", "clamp_hbm", "load_hbm", "crack_hbm")
    outs = ("first_ref", "second_ref", "third_ref", "dam_ref", "norm_ref")
    names = (*ins, *outs, *scratch)
    block = pl.BlockSpec(memory_space=pltpu.VMEM)
    away = pl.BlockSpec(memory_space=pltpu.HBM)
    results = pl.pallas_call(
        functools.partial(kernel, (sections, ngx, ngy, nx, ny, nz), names),
        out_shape=(
            *[jax.ShapeDtypeStruct((nx, ny, nz), f32)] * 4,
            jax.ShapeDtypeStruct((1, sections), f32),
        ),
        in_specs=[away] * 6,
        out_specs=(block,) * 5,
        scratch_shapes=list(scratch.values()),
        compiler_params=pltpu.CompilerParams(
            collective_id=0, has_side_effects=True, vmem_limit_bytes=56_020_000
        ),
    )(load_index, pltpu.with_memory_space_constraint(load_table.T, pltpu.HBM), toughness, clamp_mask, load_mask, crack_mask)
    return pl.pallas_call(
        put_out,
        out_shape=(
            jax.ShapeDtypeStruct((1, 3, nx, ny, nz), f32),
            jax.ShapeDtypeStruct((1, nx, ny, nz), f32),
            jax.ShapeDtypeStruct((1, sections), f32),
        ),
        in_specs=[block] * 5,
        out_specs=(away, away, block),
        scratch_shapes=[dma((4,))],
        compiler_params=pltpu.CompilerParams(vmem_limit_bytes=1024 * 1024),
    )(*results)


def solution(mesh):
    in_specs = (
        P("section"),
        P(),
        P("section", "gx", "gy", None),
        P("gx", "gy", None),
        P("gx", "gy", None),
        P("gx", "gy", None),
    )
    out_specs = (
        P("section", None, "gx", "gy", None),
        P("section", "gx", "gy", None),
        P("section", None),
    )
    sizes = tuple(mesh.shape[name] for name in ("section", "gx", "gy"))
    return jax.shard_map(
        functools.partial(on_device, sizes),
        mesh=mesh,
        in_specs=in_specs,
        out_specs=out_specs,
        check_vma=False,
    )
```

```python
import functools
import math
import types

import jax
import jax.numpy as jnp
from jax import lax
from jax.experimental import pallas as pl
from jax.experimental.pallas import tpu as pltpu
from jax.sharding import PartitionSpec as P

relax_weight = 0.6
stiff_floor = 0.001
eigen_guard = 1e-08
MESH = pl.DeviceIdType.MESH

HX = 5
OY = 8

ACOS = (
    1.5707963050,
    -0.2145988016,
    0.0889789874,
    -0.0501743046,
    0.0308918810,
    -0.0170881256,
    0.0066700901,
    -0.0012624911,
)


def up8(n):
    return -(-n // 8) * 8


def part(n, most):
    return max(k for k in range(1, most + 1) if n % k == 0)


def root(v):
    return v * lax.rsqrt(jnp.maximum(v, 1.2e-38))


def spectral_energy(xx, yy, zz, xy, xz, yz):
    trace = xx + yy + zz
    mid = trace * (1.0 / 3.0)
    dx = xx - mid
    dy = yy - mid
    dz = zz - mid
    xy2 = xy * xy
    xz2 = xz * xz
    yz2 = yz * yz
    sixth = (dx * dx + dy * dy + dz * dz + 2.0 * (xy2 + xz2 + yz2)) * (1.0 / 6.0)
    twice_radius = 2.0 * root(sixth)
    scale = lax.rsqrt(sixth + eigen_guard)
    det = dx * (dy * dz - yz2) - dz * xy2 - dy * xz2 + 2.0 * (xy * xz * yz)
    ratio = (0.5 * det * scale) * (scale * scale)
    size = jnp.minimum(jnp.abs(ratio), 1.0)
    poly = jnp.full_like(size, ACOS[-1] / 3.0)
    for c in ACOS[-2::-1]:
        poly = poly * size + c / 3.0
    t = root(1.0 - size) * poly
    t2 = t * t
    cos_t = 1.0 + t2 * (-0.5 + t2 * (1.0 / 24.0 + t2 * (-1.0 / 720.0 + t2 * (1.0 / 40320.0))))
    sin_t = t * (1.0 + t2 * (-1.0 / 6.0 + t2 * (1.0 / 120.0 + t2 * (-1.0 / 5040.0))))
    other = 0.5 * cos_t + math.sqrt(0.75) * sin_t
    upper = ratio >= 0.0
    first = jnp.where(upper, cos_t, other)
    last = jnp.where(upper, other, cos_t)
    largest = mid + twice_radius * first
    smallest = mid - twice_radius * last
    between = trace - largest - smallest
    relu = lambda v: jnp.maximum(v, 0.0)
    return (
        0.5 * jnp.square(relu(trace))
        + jnp.square(relu(largest))
        + jnp.square(relu(between))
        + jnp.square(relu(smallest))
    )


def kernel(sizes, names, *refs):
    sections, ngx, ngy, nx, ny, nz = sizes
    r = types.SimpleNamespace(**dict(zip(names, refs)))
    local, state, stiff, flow = r.local, r.state, r.stiff, r.flow
    held, clamped, tough_pad, crack_pad = r.held, r.clamped, r.tough_pad, r.crack_pad
    load_ref, crack_ref, clamp_ref, tough_ref = r.load_ref, r.crack_ref, r.clamp_ref, r.tough_ref
    disp_refs = (r.first_ref, r.second_ref, r.third_ref)
    sec = lax.axis_index("section")
    gx = lax.axis_index("gx")
    gy = lax.axis_index("gy")
    group = ngx * ngy
    me = gx * ngy + gy
    ring = lambda k, n: min(k, n - k)
    offsets = [(i, j) for i in range(ngx) for j in range(ngy) if i or j]
    offsets.sort(key=lambda o: (ring(o[0], ngx) + ring(o[1], ngy), o))
    peers = []
    for i, j in offsets:
        peers.append({"gx": lax.rem(gx + i, ngx), "gy": lax.rem(gy + j, ngy)})

    barrier = pltpu.get_barrier_semaphore()
    for peer in peers:
        pl.semaphore_signal(barrier, inc=1, device_id=peer, device_id_type=MESH)
    for k in range(1, sections):
        pl.semaphore_signal(
            barrier,
            inc=1,
            device_id={"section": lax.rem(sec + k, sections)},
            device_id_type=MESH,
        )

    fetch = [
        pltpu.make_async_copy(src, dst, local.at[n])
        for n, (src, dst) in enumerate(
            (
                (r.load_hbm, load_ref),
                (r.crack_hbm, crack_ref),
                (r.clamp_hbm, clamp_ref),
                (r.tough_hbm, tough_ref),
                (r.index_hbm, r.index_ref),
                (r.table_hbm, r.table_ref),
            )
        )
    ]
    for copy in fetch:
        copy.start()

    there = {
        "gx": (gx > 0, gx < ngx - 1),
        "gy": (gy > 0, gy < ngy - 1),
    }
    step = (-1, 1)

    def x_dev(s):
        return there["gx"][s], {"gx": gx + step[s]}

    def y_dev(s):
        return there["gy"][s], {"gy": gy + step[s]}

    def c_dev(sx, sy):
        return (
            jnp.logical_and(there["gx"][sx], there["gy"][sy]),
            {"gx": gx + step[sx], "gy": gy + step[sy]},
        )

    class Exchange:
        def __init__(self, send, recv):
            self.items = []
            self.send = send
            self.recv = recv

        def add(self, where, src, dst, mine, out_slot, in_slot):
            cond, dev = where
            n = len(self.items)
            copy = pltpu.make_async_remote_copy(
                src_ref=src,
                dst_ref=dst,
                send_sem=self.send.at[n],
                recv_sem=self.recv.at[out_slot],
                device_id=dev,
                device_id_type=MESH,
            )
            back = pltpu.make_async_remote_copy(
                src_ref=src,
                dst_ref=mine,
                send_sem=self.send.at[n],
                recv_sem=self.recv.at[in_slot],
                device_id=dev,
                device_id_type=MESH,
            )
            self.items.append((cond, copy, back))

        def start(self, begin=0, end=None):
            for cond, copy, _ in self.items[begin:end]:
                pl.when(cond)(copy.start)

        def finish(self):
            for cond, copy, back in self.items:

                @pl.when(cond)
                def _():
                    back.wait_recv()
                    copy.wait_send()

        def received(self, begin=0, end=None):
            for cond, _, back in self.items[begin:end]:
                pl.when(cond)(back.wait_recv)

        def sent(self, begin=0, end=None):
            for cond, copy, _ in self.items[begin:end]:
                pl.when(cond)(copy.wait_send)

    rows = ny + 2 * OY

    def clear(xp, carry):
        zero = jnp.zeros((rows, nz), jnp.float32)
        held[xp] = zero
        crack_pad[xp] = zero
        clamped[xp] = zero + 1.0
        tough_pad[xp] = zero + 1.0
        if sections > 2:
            for p in range(2):
                for f in range(4):
                    state[p, f, xp] = zero
        return carry

    lax.fori_loop(0, nx + 2 * HX, clear, 0)

    for copy in fetch[:3]:
        copy.wait()

    for s in range(2):
        side = lambda n, s=s: slice(0, n) if s == 0 else slice(ny - n, ny)
        r.pack_c[s] = crack_ref[:, side(4)]
        for x in range(nx):
            r.pack_l[s, 5 * x : 5 * x + 5] = load_ref[x, side(5)]
            r.pack_f[s, 3 * x : 3 * x + 3] = clamp_ref[x, side(3)]
    corner = (
        (load_ref, held, 1, 4, 0),
        (load_ref, held, 2, 3, 4),
        (load_ref, held, 4, 1, 7),
        (load_ref, held, 3, 2, 8),
        (crack_ref, crack_pad, 1, 3, 10),
        (crack_ref, crack_pad, 2, 2, 13),
        (crack_ref, crack_pad, 3, 1, 15),
        (clamp_ref, clamped, 1, 2, 16),
        (clamp_ref, clamped, 2, 1, 18),
    )
    for sx in range(2):
        for sy in range(2):
            for ref, _, deep, n, at in corner:
                plane = deep - 1 if sx == 0 else nx - deep
                first = 0 if sy == 0 else ny - n
                pack, at = (r.pack_k, at) if at < 16 else (r.pack_kf, at - 16)
                pack[sx * 2 + sy, at : at + n] = ref[plane, first : first + n]

    pl.semaphore_wait(barrier, group - 1 + sections - 1)

    beside_y = Exchange(r.y_send, r.y_recv)
    early = Exchange(r.early_send, r.early_recv)
    later = Exchange(r.later_send, r.later_recv)
    last_one = Exchange(r.last_send, r.last_recv)
    for s in range(2):
        for ex, ref, buf, width, at, slot in (
            (early, load_ref, r.in_x, 5, 0, 0),
            (early, crack_ref, r.in_x, 4, 5, 2),
            (later, clamp_ref, r.in_x, 3, 9, 0),
            (last_one, tough_ref.at[0], r.in_tx, 2, 0, 0),
        ):
            ex.add(
                x_dev(s),
                ref.at[pl.ds(0 if s == 0 else nx - width, width)],
                buf.at[1 - s, pl.ds(at, width)],
                buf.at[s, pl.ds(at, width)],
                slot + 1 - s,
                slot + s,
            )
    for n in range(8):
        s = n % 2
        for pack, buf, slot in (
            (r.pack_c, r.in_c, 0),
            (r.pack_l, r.in_l, 2),
            (r.pack_f, r.in_f, 4),
            (r.pack_t, r.in_ty, 6),
        )[n // 2 : n // 2 + 1]:
            beside_y.add(
                y_dev(s), pack.at[s], buf.at[1 - s], buf.at[s], slot + 1 - s, slot + s
            )
    for sx in range(2):
        for sy in range(2):
            here, away = sx * 2 + sy, (1 - sx) * 2 + 1 - sy
            early.add(
                c_dev(sx, sy), r.pack_k.at[here], r.in_k.at[away], r.in_k.at[here],
                4 + away, 4 + here,
            )
            later.add(
                c_dev(sx, sy), r.pack_kf.at[here], r.in_kf.at[away], r.in_kf.at[here],
                2 + away, 2 + here,
            )
            last_one.add(
                c_dev(sx, sy), r.pack_tk.at[here], r.in_tk.at[away], r.in_tk.at[here],
                2 + away, 2 + here,
            )
    early.start(0, 4)
    beside_y.start(0, 6)
    fetch[3].wait()
    for s in range(2):
        r.pack_t[s] = tough_ref[0, :, 0:2] if s == 0 else tough_ref[0, :, ny - 2 : ny]
    for sx in range(2):
        for sy in range(2):
            row = 0 if sy == 0 else ny - 1
            r.pack_tk[sx * 2 + sy] = tough_ref[0, 0 if sx == 0 else nx - 1, row : row + 1]
    beside_y.start(6)
    early.start(4)
    tough_copies = []
    for k in range(1, sections):
        copy = pltpu.make_async_remote_copy(
            src_ref=tough_ref.at[0],
            dst_ref=r.tough_in.at[k - 1],
            send_sem=r.tough_send.at[k - 1],
            recv_sem=r.tough_recv.at[k - 1],
            device_id={"section": lax.rem(sec + sections - k, sections)},
            device_id_type=MESH,
        )
        copy.start()
        tough_copies.append(copy)

    inner = slice(OY, OY + ny)
    as_float = lambda v: v.astype(jnp.float32)

    def fill(x, carry):
        held[x + HX, inner] = as_float(load_ref[x])
        clamped[x + HX, inner] = as_float(clamp_ref[x])
        crack_pad[x + HX, inner] = as_float(crack_ref[x])
        tough_pad[x + HX, inner] = tough_ref[0, x]
        return carry

    lax.fori_loop(0, nx, fill, 0, unroll=part(nx, 4))

    for copy in fetch[4:]:
        copy.wait()
    case = r.index_ref[0]
    vector = [r.table_ref[f, case] for f in range(3)]

    planes = slice(HX, HX + nx)

    def x_out(s, n):
        return slice(HX - n, HX) if s == 0 else slice(HX + nx, HX + nx + n)

    def y_out(s, n):
        return slice(OY - n, OY) if s == 0 else slice(OY + ny, OY + ny + n)

    def unpack_y():
        beside_y.received(0, 4)
        for s in range(2):

            @pl.when(there["gy"][s])
            def _(s=s):
                crack_pad[planes, y_out(s, 4)] = as_float(r.in_c[s])
                for x in range(nx):
                    held[HX + x, y_out(s, 5)] = as_float(r.in_l[s, 5 * x : 5 * x + 5])

    def unpack_y_clamp():
        beside_y.received(4, 6)
        for s in range(2):

            @pl.when(there["gy"][s])
            def _(s=s):
                for x in range(nx):
                    clamped[HX + x, y_out(s, 3)] = as_float(r.in_f[s, 3 * x : 3 * x + 3])

    def unpack_y_tough():
        beside_y.received(6)
        for s in range(2):

            @pl.when(there["gy"][s])
            def _(s=s):
                tough_pad[planes, y_out(s, 2)] = r.in_ty[s]

    def unpack_x():
        early.received()
        for s in range(2):

            @pl.when(there["gx"][s])
            def _(s=s):
                held[x_out(s, 5), inner] = as_float(r.in_x[s, 0:5])
                crack_pad[x_out(s, 4), inner] = as_float(r.in_x[s, 5:9])

        for sx in range(2):
            for sy in range(2):

                @pl.when(c_dev(sx, sy)[0])
                def _(sx=sx, sy=sy):
                    for _, pad, deep, n, at in corner[:-2]:
                        plane = HX - deep if sx == 0 else HX + nx - 1 + deep
                        pad[plane, y_out(sy, n)] = as_float(r.in_k[sx * 2 + sy, at : at + n])

    def unpack_clamp():
        later.received()
        for s in range(2):

            @pl.when(there["gx"][s])
            def _(s=s):
                clamped[x_out(s, 3), inner] = as_float(r.in_x[s, 9:12])

        for sx in range(2):
            for sy in range(2):

                @pl.when(c_dev(sx, sy)[0])
                def _(sx=sx, sy=sy):
                    for _, pad, deep, n, at in corner[-2:]:
                        plane = HX - deep if sx == 0 else HX + nx - 1 + deep
                        at = at - 16
                        pad[plane, y_out(sy, n)] = as_float(r.in_kf[sx * 2 + sy, at : at + n])

    def unpack_tough():
        last_one.received()
        for s in range(2):

            @pl.when(there["gx"][s])
            def _(s=s):
                tough_pad[x_out(s, 2), inner] = r.in_tx[s]

        for sx in range(2):
            for sy in range(2):

                @pl.when(c_dev(sx, sy)[0])
                def _(sx=sx, sy=sy):
                    plane = HX - 1 if sx == 0 else HX + nx
                    tough_pad[plane, y_out(sy, 1)] = r.in_tk[sx * 2 + sy]

    wide = up8(ny + 4)
    deep = up8(ny + 8)

    def lanes(shape, lane):
        return lax.broadcasted_iota(jnp.int32, shape, 1) == lane

    def beside(v, edge, first, last):
        up = jnp.where(last, edge, pltpu.roll(v, nz - 1, 1))
        down = jnp.where(first, edge, pltpu.roll(v, 1, 1))
        return up, down

    def inside_rows(shape, above):
        row = lax.broadcasted_iota(jnp.int32, shape, 0) + (gy * ny - above)
        return jnp.logical_and(row >= 0, row < ny * ngy)

    def inside_plane(xp):
        plane = xp - HX + gx * nx
        return jnp.logical_and(plane >= 0, plane < nx * ngx)

    edge_stiff = 0.5 * (1.0 + stiff_floor)

    def elastic(at, first, last):
        k = at(stiff, 0, 0)
        sides = (
            (at(stiff, 1, 0), at(stiff, -1, 0)),
            (at(stiff, 0, 1), at(stiff, 0, -1)),
            beside(k, edge_stiff, first, last),
        )
        pairs = [s[0] + s[1] for s in sides]
        weights = pairs[0] + pairs[1] + pairs[2] + 6.0 * k
        faces = [(k + s[0], k + s[1]) for s in sides]
        fz = beside(at(flow, 0, 0), 0.0, first, last)
        grads = (
            at(flow, 1, 0) - at(flow, -1, 0),
            at(flow, 0, 1) - at(flow, 0, -1),
            fz[0] - fz[1],
        )
        return pairs, weights, faces, grads

    def laplace(at, ref, faces, weights, first, last):
        here = at(ref, 0, 0)
        uz = beside(here, 0.0, first, last)
        return here, (
            faces[0][0] * at(ref, 1, 0)
            + faces[0][1] * at(ref, -1, 0)
            + faces[1][0] * at(ref, 0, 1)
            + faces[1][1] * at(ref, 0, -1)
            + faces[2][0] * uz[0]
            + faces[2][1] * uz[1]
            - weights * here
        )

    def strain_energy(at, u, keep, first, last):
        grad = []
        for f in range(3):
            here = at(u.at[f], 0, 0)
            uz = beside(here, 0.0, first, last)
            grad.append(
                (
                    at(u.at[f], 1, 0) - at(u.at[f], -1, 0),
                    at(u.at[f], 0, 1) - at(u.at[f], 0, -1),
                    uz[0] - uz[1],
                )
            )
            keep(f, here)
        return 2.0 * spectral_energy(
            0.5 * grad[0][0],
            0.5 * grad[1][1],
            0.5 * grad[2][2],
            0.25 * (grad[0][1] + grad[1][0]),
            0.25 * (grad[0][2] + grad[2][0]),
            0.25 * (grad[1][2] + grad[2][1]),
        )

    def renew(at, d, energy, g, cracked, first, last):
        dz = beside(at(d, 0, 0), 0.0, first, last)
        around = at(d, 1, 0) + at(d, -1, 0) + at(d, 0, 1) + at(d, 0, -1) + dz[0] + dz[1]
        renewed = (energy + g * around) / (7.0 * g + energy)
        return jnp.where(cracked, 1.0, renewed)

    def add_up(rnd, total):
        r.sums[me, rnd : rnd + 1] = jnp.sum(total, axis=0, keepdims=True)

    def open_stages(above, n):
        shape = (n, nz)
        first, last = lanes(shape, 0), lanes(shape, nz - 1)
        row_inside = inside_rows(shape, above)
        row = lax.broadcasted_iota(jnp.int32, shape, 0)
        a = OY - above

        def stiffen(xp, carry):
            half = 0.5 * (jnp.square(1.0 - crack_pad[xp, a : a + n]) + stiff_floor)
            stiff[xp, a : a + n] = half
            up, down = beside(held[xp, a : a + n], 0.0, first, last)
            div = (
                vector[0] * (held[xp + 1, a : a + n] - held[xp - 1, a : a + n])
                + vector[1] * (held[xp, a + 1 : a + 1 + n] - held[xp, a - 1 : a - 1 + n])
                + vector[2] * (up - down)
            )
            flow[xp, a : a + n] = jnp.where(
                jnp.logical_and(row_inside, inside_plane(xp)), half * div, 0.0
            )
            return carry

        def mover(low, high):
            def move(xp, total):
                at = lambda ref, dx, dy: ref[xp + dx, a + dy : a + dy + n]
                pairs, weights, faces, grads = elastic(at, first, last)
                load, spread = laplace(at, held, faces, weights, first, last)
                pin = at(clamped, 0, 0) + load > 0.5
                squares = None
                for f in range(3):
                    res = vector[f] * spread + grads[f]
                    moved = jnp.where(pin, 0.0, relax_weight * res / (weights + pairs[f]))
                    state[1, f, xp, a : a + n] = vector[f] * load + moved
                    square = res * res
                    squares = square if squares is None else squares + square
                if low >= high:
                    return total
                counted = jnp.logical_and(row >= low + above, row < high + above)
                return total + jnp.where(
                    jnp.logical_and(counted, jnp.logical_not(pin)), squares, 0.0
                )

            return move

        def damage(xp, carry):
            at = lambda ref, dx, dy: ref[xp + dx, a + dy : a + dy + n]
            energy = strain_energy(at, state.at[1], lambda f, v: None, first, last)
            renewed = renew(
                at,
                crack_pad,
                energy,
                at(tough_pad, 0, 0),
                at(crack_pad, 0, 0) > 0.5,
                first,
                last,
            )
            state[1, 3, xp, a : a + n] = jnp.where(
                jnp.logical_and(row_inside, inside_plane(xp)), renewed, 0.0
            )
            return carry

        return stiffen, mover, damage

    def open_sweep():
        def inward(skip, body, carry, most):
            n = nx - 2 * skip
            return lax.fori_loop(HX + skip, HX + nx - skip, body, carry, unroll=part(n, most))

        def outward(far, n, body, carry):
            def both(i, carry):
                carry = body(HX - far + i, carry)
                return body(HX + nx + far - n + i, carry)

            return lax.fori_loop(0, n, both, carry, unroll=True)

        def pair(one, two):
            def body(xp, carry):
                return one(xp, carry[0]), two(xp, carry[1])

            return body

        blank = lambda n: jnp.zeros((n, nz), jnp.float32)
        fold = lambda v: jnp.sum(v, axis=0, keepdims=True)

        stiffen, mover, damage = open_stages(0, ny)
        inward(1, stiffen, 0, 14)
        inside = inward(2, mover(2, ny - 2), blank(ny), 12)
        inward(3, damage, 0, 5)

        early.sent(0, 4)
        later.start()
        last_one.start()

        low = open_stages(4, 8)
        high = open_stages(4 - ny, 8)
        unpack_y()
        inward(1, pair(low[0], high[0]), (0, 0), 14)
        unpack_y_clamp()
        rims = inward(
            2, pair(low[1](0, 2), high[1](ny - 2, ny)), (blank(8), blank(8)), 12
        )
        unpack_y_tough()
        inward(3, pair(low[2], high[2]), (0, 0), 5)
        own = blank(ny)
        if sections > 1:
            stiffen1, mover1 = stages(1)
            inward(3, stiffen1, 0, 10)
            own = inward(4, mover1(OY, ny), own, 8)

        unpack_x()
        stiffen, mover, damage = open_stages(4, deep)
        outward(4, 5, stiffen, 0)
        ends = outward(0, 2, mover(0, ny), blank(deep))
        unpack_clamp()
        outward(3, 3, mover(0, 0), blank(deep))
        r.sums[me, 0:1] = fold(inside) + fold(rims[0] + rims[1]) + fold(ends)
        outward(0, 3, damage, 0)
        unpack_tough()
        outward(2, 2, damage, 0)
        if sections > 1:
            outward(2, 5, stiffen1, 0)
            own = outward(0, 4, mover1(OY, ny), own)
        return own

    def send_sums():
        for k, peer in enumerate(peers):
            pltpu.make_async_remote_copy(
                src_ref=r.sums.at[me],
                dst_ref=r.sums.at[me],
                send_sem=r.sum_send.at[k],
                recv_sem=r.sum_recv.at[me],
                device_id=peer,
                device_id_type=MESH,
            ).start()

    def stages(rnd):
        p = rnd % 2
        q = 1 - p
        shape = (wide, nz)
        first, last = lanes(shape, 0), lanes(shape, nz - 1)
        row_inside = inside_rows(shape, 2)
        a = OY - 2

        def stiffen(xp, carry):
            half = 0.5 * (jnp.square(1.0 - state[p, 3, xp, a : a + wide]) + stiff_floor)
            stiff[xp, a : a + wide] = half
            up, down = beside(state[p, 2, xp, a : a + wide], 0.0, first, last)
            div = (
                (state[p, 0, xp + 1, a : a + wide] - state[p, 0, xp - 1, a : a + wide])
                + (state[p, 1, xp, a + 1 : a + 1 + wide] - state[p, 1, xp, a - 1 : a - 1 + wide])
                + (up - down)
            )
            flow[xp, a : a + wide] = jnp.where(
                jnp.logical_and(row_inside, inside_plane(xp)), half * div, 0.0
            )
            return carry

        def mover(b, n):
            shape = (n, nz)
            first, last = lanes(shape, 0), lanes(shape, nz - 1)

            def move(xp, total):
                at = lambda ref, dx, dy: ref[xp + dx, b + dy : b + dy + n]
                pairs, weights, faces, grads = elastic(at, first, last)
                load = at(held, 0, 0)
                pin = at(clamped, 0, 0) + load > 0.5
                squares = None
                for f in range(3):
                    here, spread = laplace(at, state.at[p, f], faces, weights, first, last)
                    res = spread + grads[f]
                    moved = here + relax_weight * res / (weights + pairs[f])
                    state[q, f, xp, b : b + n] = jnp.where(pin, load * vector[f], moved)
                    square = res * res
                    squares = square if squares is None else squares + square
                return total + jnp.where(pin, 0.0, squares)

            return move

        return stiffen, mover

    def sweep(rnd, total):
        p = rnd % 2
        q = 1 - p
        done = rnd == sections - 1
        tough = r.tough_in.at[rnd - 1]

        stiffen, mover = stages(rnd)
        if rnd > 1:
            lax.fori_loop(HX - 2, HX + nx + 2, stiffen, 0, unroll=part(nx + 4, 10))
            total = lax.fori_loop(
                HX, HX + nx, mover(OY, ny), jnp.zeros((ny, nz), jnp.float32), unroll=part(nx, 8)
            )
        add_up(rnd, total)
        if done:
            send_sums()
        none = jnp.zeros((8, nz), jnp.float32)

        def edges(xp, carry):
            mover(OY - 4, 8)(xp, none)
            mover(OY + ny - 3, 8)(xp, none)
            return carry

        lax.fori_loop(HX, HX + nx, edges, 0, unroll=part(nx, 8))
        ends = mover(OY, ny)
        ends(HX - 1, jnp.zeros((ny, nz), jnp.float32))
        ends(HX + nx, jnp.zeros((ny, nz), jnp.float32))
        par = rnd % 2
        mid = pl.ds(OY, ny)
        if not done:
            for f in range(3):
                r.pack_u[0, :, 2 * f : 2 * f + 2] = state[q, f, planes, OY : OY + 2]
                r.pack_u[1, :, 2 * f : 2 * f + 2] = state[q, f, planes, OY + ny - 2 : OY + ny]
            r.pack_u[0, :, 6:7] = state[q, 1, planes, OY + 2 : OY + 3]
            r.pack_u[1, :, 6:7] = state[q, 1, planes, OY + ny - 3 : OY + ny - 2]
            shift = Exchange(r.u_send, r.u_recv.at[par])
            for s in range(2):
                shift.add(
                    x_dev(s),
                    state.at[q, pl.ds(0, 3), pl.ds(HX if s == 0 else HX + nx - 2, 2), mid],
                    r.in_u_x.at[par, 1 - s],
                    r.in_u_x.at[par, s],
                    (1 - s),
                    s,
                )
                shift.add(
                    x_dev(s),
                    state.at[q, 0, HX + 2 if s == 0 else HX + nx - 3, mid],
                    r.in_u_x3.at[par, 1 - s],
                    r.in_u_x3.at[par, s],
                    2 + (1 - s),
                    2 + s,
                )
            for s in range(2):
                shift.add(
                    y_dev(s),
                    r.pack_u.at[s],
                    r.in_u_y.at[par, 1 - s],
                    r.in_u_y.at[par, s],
                    4 + (1 - s),
                    4 + s,
                )
            for sx in range(2):
                for sy in range(2):
                    shift.add(
                        c_dev(sx, sy),
                        r.pack_u.at[sy, pl.ds(0 if sx == 0 else nx - 2, 2)],
                        r.in_u_c.at[par, (1 - sx) * 2 + 1 - sy],
                        r.in_u_c.at[par, sx * 2 + sy],
                        6 + (1 - sx) * 2 + 1 - sy,
                        6 + sx * 2 + sy,
                    )
            shift.start()

        tough_copies[rnd - 1].wait_recv()

        shape = (ny, nz)
        first, last = lanes(shape, 0), lanes(shape, nz - 1)

        def damage(x, carry):
            xp = x + HX
            at = lambda ref, dx, dy: ref[xp + dx, OY + dy : OY + dy + ny]

            def keep(f, here):
                if done:
                    disp_refs[f][x] = here

            energy = strain_energy(at, state.at[q], keep, first, last)
            renewed = renew(
                at, state.at[p, 3], energy, tough[x], crack_ref[x] > 0, first, last
            )
            if done:
                r.dam_ref[x] = renewed
            else:
                state[q, 3, xp, inner] = renewed
            return carry

        lax.fori_loop(0, nx, damage, 0, unroll=part(nx, 8))
        if done:
            return

        r.pack_d[0] = state[q, 3, planes, OY : OY + 2]
        r.pack_d[1] = state[q, 3, planes, OY + ny - 2 : OY + ny]
        crack = Exchange(r.d_send, r.d_recv.at[par])
        for s in range(2):
            crack.add(
                x_dev(s),
                state.at[q, 3, pl.ds(HX if s == 0 else HX + nx - 2, 2), mid],
                r.in_d_x.at[par, 1 - s],
                r.in_d_x.at[par, s],
                1 - s,
                s,
            )
        for s in range(2):
            crack.add(
                y_dev(s),
                r.pack_d.at[s],
                r.in_d_y.at[par, 1 - s],
                r.in_d_y.at[par, s],
                2 + 1 - s,
                2 + s,
            )
        for sx in range(2):
            for sy in range(2):
                crack.add(
                    c_dev(sx, sy),
                    r.pack_d.at[sy, pl.ds(0 if sx == 0 else nx - 1, 1)],
                    r.in_d_c.at[par, (1 - sx) * 2 + 1 - sy],
                    r.in_d_c.at[par, sx * 2 + sy],
                    4 + (1 - sx) * 2 + 1 - sy,
                    4 + sx * 2 + sy,
                )
        crack.start()
        shift.finish()
        third_x = (HX - 3, HX + nx + 2)
        third_y = (slice(OY - 3, OY - 2), slice(OY + ny + 2, OY + ny + 3))
        for s in range(2):

            @pl.when(there["gx"][s])
            def _(s=s):
                state[q, 0:3, x_out(s, 2), inner] = r.in_u_x[par, s]
                state[q, 0, third_x[s], inner] = r.in_u_x3[par, s]

            @pl.when(there["gy"][s])
            def _(s=s):
                for f in range(3):
                    state[q, f, planes, y_out(s, 2)] = r.in_u_y[par, s, :, 2 * f : 2 * f + 2]
                state[q, 1, planes, third_y[s]] = r.in_u_y[par, s, :, 6:7]

        for sx in range(2):
            for sy in range(2):

                @pl.when(c_dev(sx, sy)[0])
                def _(sx=sx, sy=sy):
                    for f in range(3):
                        state[q, f, x_out(sx, 2), y_out(sy, 2)] = r.in_u_c[
                            par, sx * 2 + sy, :, 2 * f : 2 * f + 2
                        ]

        crack.finish()
        for s in range(2):

            @pl.when(there["gx"][s])
            def _(s=s):
                state[q, 3, x_out(s, 2), inner] = r.in_d_x[par, s]

            @pl.when(there["gy"][s])
            def _(s=s):
                state[q, 3, planes, y_out(s, 2)] = r.in_d_y[par, s]

        for sx in range(2):
            for sy in range(2):

                @pl.when(c_dev(sx, sy)[0])
                def _(sx=sx, sy=sy):
                    state[q, 3, x_out(sx, 1), y_out(sy, 2)] = r.in_d_c[par, sx * 2 + sy]

    total = open_sweep()
    if sections == 1:
        send_sums()
    for rnd in range(1, sections):
        sweep(rnd, total)

    cells = 3.0 * nx * ngx * ny * ngy * nz
    beside_y.sent()
    early.sent(4)
    later.sent()
    last_one.sent()
    for copy in tough_copies:
        copy.wait_send()
    for k, peer in enumerate(peers):
        other = peer["gx"] * ngy + peer["gy"]
        pltpu.make_async_remote_copy(
            src_ref=r.sums.at[me],
            dst_ref=r.sums.at[other],
            send_sem=r.sum_send.at[k],
            recv_sem=r.sum_recv.at[other],
            device_id=peer,
            device_id_type=MESH,
        ).wait()
    total = r.sums[0]
    for k in range(1, group):
        total = total + r.sums[k]
    entries = jnp.sqrt(jnp.sum(total, axis=1, keepdims=True) / cells)
    column = lax.broadcasted_iota(jnp.int32, (1, sections), 1)
    norms = jnp.zeros((1, sections), jnp.float32)
    for rnd in range(sections):
        norms = jnp.where(
            column == lax.rem(sec + rnd, sections), entries[rnd : rnd + 1], norms
        )
    r.norm_ref[...] = norms


def put_out(
    first_ref, second_ref, third_ref, dam_ref, norm_ref, disp_hbm, dam_hbm, norm_out, sems
):
    copies = [
        pltpu.make_async_copy(ref, disp_hbm.at[0, f], sems.at[f])
        for f, ref in enumerate((first_ref, second_ref, third_ref))
    ]
    copies.append(pltpu.make_async_copy(dam_ref, dam_hbm.at[0], sems.at[3]))
    for copy in copies:
        copy.start()
    norm_out[...] = norm_ref[...]
    for copy in copies:
        copy.wait()


def on_device(sizes, load_index, load_table, toughness, clamp_mask, load_mask, crack_mask):
    sections, ngx, ngy = sizes
    nx, ny, nz = clamp_mask.shape
    assert load_index.shape == (1,)
    group = ngx * ngy
    f32 = jnp.float32
    padded = (nx + 2 * HX, ny + 2 * OY, nz)
    vmem = pltpu.VMEM
    dma = pltpu.SemaphoreType.DMA
    later = max(sections - 1, 1)
    more = sections > 2
    scratch = {
        "index_ref": pltpu.SMEM(load_index.shape, jnp.int32),
        "table_ref": pltpu.SMEM(load_table.shape[::-1], f32),
        "tough_ref": vmem((1, nx, ny, nz), f32),
        "clamp_ref": vmem((nx, ny, nz), jnp.int32),
        "load_ref": vmem((nx, ny, nz), jnp.int32),
        "crack_ref": vmem((nx, ny, nz), jnp.int32),
        "local": dma((6,)),
        "state": vmem((2, 4) + padded, f32),
        "stiff": vmem(padded, f32),
        "flow": vmem(padded, f32),
        "held": vmem(padded, f32),
        "clamped": vmem(padded, f32),
        "tough_pad": vmem(padded, f32),
        "crack_pad": vmem(padded, f32),
        "tough_in": vmem((later, nx, ny, nz), f32),
        "pack_l": vmem((2, 5 * nx, nz), jnp.int32),
        "pack_f": vmem((2, 3 * nx, nz), jnp.int32),
        "pack_c": vmem((2, nx, 4, nz), jnp.int32),
        "pack_t": vmem((2, nx, 2, nz), f32),
        "pack_k": vmem((4, 16, nz), jnp.int32),
        "pack_kf": vmem((4, 4, nz), jnp.int32),
        "pack_tk": vmem((4, 1, nz), f32),
        "in_x": vmem((2, 12, ny, nz), jnp.int32),
        "in_tx": vmem((2, 2, ny, nz), f32),
        "in_l": vmem((2, 5 * nx, nz), jnp.int32),
        "in_f": vmem((2, 3 * nx, nz), jnp.int32),
        "in_c": vmem((2, nx, 4, nz), jnp.int32),
        "in_ty": vmem((2, nx, 2, nz), f32),
        "in_k": vmem((4, 16, nz), jnp.int32),
        "in_kf": vmem((4, 4, nz), jnp.int32),
        "in_tk": vmem((4, 1, nz), f32),
        "sums": vmem((group, sections, nz), f32),
        "y_send": dma((8,)),
        "y_recv": dma((8,)),
        "early_send": dma((8,)),
        "early_recv": dma((8,)),
        "later_send": dma((6,)),
        "later_recv": dma((6,)),
        "last_send": dma((6,)),
        "last_recv": dma((6,)),
        "tough_send": dma((later,)),
        "tough_recv": dma((later,)),
        "sum_send": dma((max(group - 1, 1),)),
        "sum_recv": dma((group,)),
    }
    if more:
        scratch |= {
            "pack_u": vmem((2, nx, 8, nz), f32),
            "pack_d": vmem((2, nx, 2, nz), f32),
            "in_u_x": vmem((2, 2, 3, 2, ny, nz), f32),
            "in_u_x3": vmem((2, 2, ny, nz), f32),
            "in_u_y": vmem((2, 2, nx, 8, nz), f32),
            "in_u_c": vmem((2, 4, 2, 8, nz), f32),
            "in_d_x": vmem((2, 2, 2, ny, nz), f32),
            "in_d_y": vmem((2, 2, nx, 2, nz), f32),
            "in_d_c": vmem((2, 4, 1, 2, nz), f32),
            "u_send": dma((10,)),
            "u_recv": dma((2, 10)),
            "d_send": dma((8,)),
            "d_recv": dma((2, 8)),
        }
    ins = ("index_hbm", "table_hbm", "tough_hbm", "clamp_hbm", "load_hbm", "crack_hbm")
    outs = ("first_ref", "second_ref", "third_ref", "dam_ref", "norm_ref")
    names = (*ins, *outs, *scratch)
    block = pl.BlockSpec(memory_space=pltpu.VMEM)
    away = pl.BlockSpec(memory_space=pltpu.HBM)
    results = pl.pallas_call(
        functools.partial(kernel, (sections, ngx, ngy, nx, ny, nz), names),
        out_shape=(
            *[jax.ShapeDtypeStruct((nx, ny, nz), f32)] * 4,
            jax.ShapeDtypeStruct((1, sections), f32),
        ),
        in_specs=[away] * 6,
        out_specs=(block,) * 5,
        scratch_shapes=list(scratch.values()),
        compiler_params=pltpu.CompilerParams(
            collective_id=0, has_side_effects=True, vmem_limit_bytes=56_020_000
        ),
    )(load_index, pltpu.with_memory_space_constraint(load_table.T, pltpu.HBM), toughness, clamp_mask, load_mask, crack_mask)
    return pl.pallas_call(
        put_out,
        out_shape=(
            jax.ShapeDtypeStruct((1, 3, nx, ny, nz), f32),
            jax.ShapeDtypeStruct((1, nx, ny, nz), f32),
            jax.ShapeDtypeStruct((1, sections), f32),
        ),
        in_specs=[block] * 5,
        out_specs=(away, away, block),
        scratch_shapes=[dma((4,))],
        compiler_params=pltpu.CompilerParams(vmem_limit_bytes=1024 * 1024),
    )(*results)


def solution(mesh):
    in_specs = (
        P("section"),
        P(),
        P("section", "gx", "gy", None),
        P("gx", "gy", None),
        P("gx", "gy", None),
        P("gx", "gy", None),
    )
    out_specs = (
        P("section", None, "gx", "gy", None),
        P("section", "gx", "gy", None),
        P("section", None),
    )
    sizes = tuple(mesh.shape[name] for name in ("section", "gx", "gy"))
    return jax.shard_map(
        functools.partial(on_device, sizes),
        mesh=mesh,
        in_specs=in_specs,
        out_specs=out_specs,
        check_vma=False,
    )
```

```python
import functools
import math
import types

import jax
import jax.numpy as jnp
from jax import lax
from jax.experimental import pallas as pl
from jax.experimental.pallas import tpu as pltpu
from jax.sharding import PartitionSpec as P

relax_weight = 0.6
stiff_floor = 0.001
eigen_guard = 1e-08
MESH = pl.DeviceIdType.MESH

HX = 5
OY = 8

ACOS = (
    1.5707963050,
    -0.2145988016,
    0.0889789874,
    -0.0501743046,
    0.0308918810,
    -0.0170881256,
    0.0066700901,
    -0.0012624911,
)


def up8(n):
    return -(-n // 8) * 8


def part(n, most):
    return max(k for k in range(1, most + 1) if n % k == 0)


def root(v):
    return v * lax.rsqrt(jnp.maximum(v, 1.2e-38))


def spectral_energy(xx, yy, zz, xy, xz, yz):
    trace = xx + yy + zz
    mid = trace * (1.0 / 3.0)
    dx = xx - mid
    dy = yy - mid
    dz = zz - mid
    xy2 = xy * xy
    xz2 = xz * xz
    yz2 = yz * yz
    sixth = (dx * dx + dy * dy + dz * dz + 2.0 * (xy2 + xz2 + yz2)) * (1.0 / 6.0)
    twice_radius = 2.0 * root(sixth)
    scale = lax.rsqrt(sixth + eigen_guard)
    det = dx * (dy * dz - yz2) - dz * xy2 - dy * xz2 + 2.0 * (xy * xz * yz)
    ratio = (0.5 * det * scale) * (scale * scale)
    size = jnp.minimum(jnp.abs(ratio), 1.0)
    poly = jnp.full_like(size, ACOS[-1] / 3.0)
    for c in ACOS[-2::-1]:
        poly = poly * size + c / 3.0
    t = root(1.0 - size) * poly
    t2 = t * t
    cos_t = 1.0 + t2 * (-0.5 + t2 * (1.0 / 24.0 + t2 * (-1.0 / 720.0 + t2 * (1.0 / 40320.0))))
    sin_t = t * (1.0 + t2 * (-1.0 / 6.0 + t2 * (1.0 / 120.0 + t2 * (-1.0 / 5040.0))))
    other = 0.5 * cos_t + math.sqrt(0.75) * sin_t
    upper = ratio >= 0.0
    first = jnp.where(upper, cos_t, other)
    last = jnp.where(upper, other, cos_t)
    largest = mid + twice_radius * first
    smallest = mid - twice_radius * last
    between = trace - largest - smallest
    relu = lambda v: jnp.maximum(v, 0.0)
    return (
        0.5 * jnp.square(relu(trace))
        + jnp.square(relu(largest))
        + jnp.square(relu(between))
        + jnp.square(relu(smallest))
    )


def kernel(sizes, names, *refs):
    sections, ngx, ngy, nx, ny, nz = sizes
    r = types.SimpleNamespace(**dict(zip(names, refs)))
    local, state, stiff, flow = r.local, r.state, r.stiff, r.flow
    held, clamped, tough_pad, crack_pad = r.held, r.clamped, r.tough_pad, r.crack_pad
    load_ref, crack_ref, clamp_ref, tough_ref = r.load_ref, r.crack_ref, r.clamp_ref, r.tough_ref
    disp_refs = (r.first_ref, r.second_ref, r.third_ref)
    sec = lax.axis_index("section")
    gx = lax.axis_index("gx")
    gy = lax.axis_index("gy")
    group = ngx * ngy
    me = gx * ngy + gy
    ring = lambda k, n: min(k, n - k)
    offsets = [(i, j) for i in range(ngx) for j in range(ngy) if i or j]
    offsets.sort(key=lambda o: (ring(o[0], ngx) + ring(o[1], ngy), o))
    peers = []
    for i, j in offsets:
        peers.append({"gx": lax.rem(gx + i, ngx), "gy": lax.rem(gy + j, ngy)})

    barrier = pltpu.get_barrier_semaphore()
    for peer in peers:
        pl.semaphore_signal(barrier, inc=1, device_id=peer, device_id_type=MESH)
    for k in range(1, sections):
        pl.semaphore_signal(
            barrier,
            inc=1,
            device_id={"section": lax.rem(sec + k, sections)},
            device_id_type=MESH,
        )

    fetch = [
        pltpu.make_async_copy(src, dst, local.at[n])
        for n, (src, dst) in enumerate(
            (
                (r.load_hbm, load_ref),
                (r.crack_hbm, crack_ref),
                (r.clamp_hbm, clamp_ref),
                (r.tough_hbm, tough_ref),
                (r.index_hbm, r.index_ref),
                (r.table_hbm, r.table_ref),
            )
        )
    ]
    for copy in fetch:
        copy.start()

    there = {
        "gx": (gx > 0, gx < ngx - 1),
        "gy": (gy > 0, gy < ngy - 1),
    }
    step = (-1, 1)

    def x_dev(s):
        return there["gx"][s], {"gx": gx + step[s]}

    def y_dev(s):
        return there["gy"][s], {"gy": gy + step[s]}

    def c_dev(sx, sy):
        return (
            jnp.logical_and(there["gx"][sx], there["gy"][sy]),
            {"gx": gx + step[sx], "gy": gy + step[sy]},
        )

    class Exchange:
        def __init__(self, send, recv):
            self.items = []
            self.send = send
            self.recv = recv

        def add(self, where, src, dst, mine, out_slot, in_slot):
            cond, dev = where
            n = len(self.items)
            copy = pltpu.make_async_remote_copy(
                src_ref=src,
                dst_ref=dst,
                send_sem=self.send.at[n],
                recv_sem=self.recv.at[out_slot],
                device_id=dev,
                device_id_type=MESH,
            )
            back = pltpu.make_async_remote_copy(
                src_ref=src,
                dst_ref=mine,
                send_sem=self.send.at[n],
                recv_sem=self.recv.at[in_slot],
                device_id=dev,
                device_id_type=MESH,
            )
            self.items.append((cond, copy, back))

        def start(self, begin=0, end=None):
            for cond, copy, _ in self.items[begin:end]:
                pl.when(cond)(copy.start)

        def finish(self):
            for cond, copy, back in self.items:

                @pl.when(cond)
                def _():
                    back.wait_recv()
                    copy.wait_send()

        def received(self, begin=0, end=None):
            for cond, _, back in self.items[begin:end]:
                pl.when(cond)(back.wait_recv)

        def sent(self, begin=0, end=None):
            for cond, copy, _ in self.items[begin:end]:
                pl.when(cond)(copy.wait_send)

    rows = ny + 2 * OY

    def clear(xp, carry):
        zero = jnp.zeros((rows, nz), jnp.float32)
        held[xp] = zero
        crack_pad[xp] = zero
        clamped[xp] = zero + 1.0
        tough_pad[xp] = zero + 1.0
        if sections > 2:
            for p in range(2):
                for f in range(4):
                    state[p, f, xp] = zero
        return carry

    lax.fori_loop(0, nx + 2 * HX, clear, 0)

    for copy in fetch[:3]:
        copy.wait()

    for s in range(2):
        side = lambda n, s=s: slice(0, n) if s == 0 else slice(ny - n, ny)
        r.pack_c[s] = crack_ref[:, side(4)]
        for x in range(nx):
            r.pack_l[s, 5 * x : 5 * x + 5] = load_ref[x, side(5)]
            r.pack_f[s, 3 * x : 3 * x + 3] = clamp_ref[x, side(3)]
    near_corner = (
        (load_ref, held, 1, 4, 0),
        (load_ref, held, 2, 3, 4),
        (load_ref, held, 3, 2, 7),
        (crack_ref, crack_pad, 1, 3, 9),
        (crack_ref, crack_pad, 2, 2, 12),
        (clamp_ref, clamped, 1, 2, 14),
    )
    far_corner = (
        (load_ref, held, 4, 1, 0),
        (crack_ref, crack_pad, 3, 1, 1),
        (clamp_ref, clamped, 2, 1, 2),
    )

    def x_from(s, deep):
        return deep - 1 if s == 0 else nx - deep

    def x_at(s, deep):
        return HX - deep if s == 0 else HX + nx - 1 + deep

    for sx in range(2):
        for sy in range(2):
            for pack, corner in ((r.pack_k, near_corner), (r.pack_kf, far_corner)):
                for ref, _, deep, n, at in corner:
                    first = 0 if sy == 0 else ny - n
                    pack[sx * 2 + sy, at : at + n] = ref[x_from(sx, deep), first : first + n]

    pl.semaphore_wait(barrier, group - 1 + sections - 1)

    beside_y = Exchange(r.y_send, r.y_recv)
    part_a = Exchange(r.a_send, r.a_recv)
    part_b = Exchange(r.b_send, r.b_recv)
    part_c = Exchange(r.c_send, r.c_recv)
    for ex, ref, buf, deep, width, at, slot in (
        (part_a, load_ref, r.in_a, 3, 3, 0, 0),
        (part_a, crack_ref, r.in_a, 2, 2, 3, 2),
        (part_a, clamp_ref, r.in_a, 1, 1, 5, 4),
        (part_b, load_ref, r.in_b, 4, 1, 0, 0),
        (part_b, crack_ref, r.in_b, 3, 1, 1, 2),
        (part_b, clamp_ref, r.in_b, 2, 1, 2, 4),
        (part_b, tough_ref.at[0], r.in_tx, 1, 1, 0, 6),
        (part_c, load_ref, r.in_c_x, 5, 1, 0, 0),
        (part_c, crack_ref, r.in_c_x, 4, 1, 1, 2),
        (part_c, clamp_ref, r.in_c_x, 3, 1, 2, 4),
        (part_c, tough_ref.at[0], r.in_tx, 2, 1, 1, 6),
    ):
        for s in range(2):
            first = deep - width if s == 0 else nx - deep
            ex.add(
                x_dev(s),
                ref.at[pl.ds(first, width)],
                buf.at[1 - s, pl.ds(at, width)],
                buf.at[s, pl.ds(at, width)],
                slot + 1 - s,
                slot + s,
            )
    for n in range(8):
        s = n % 2
        for pack, buf, slot in (
            (r.pack_c, r.in_c, 0),
            (r.pack_l, r.in_l, 2),
            (r.pack_f, r.in_f, 4),
            (r.pack_t, r.in_ty, 6),
        )[n // 2 : n // 2 + 1]:
            beside_y.add(
                y_dev(s), pack.at[s], buf.at[1 - s], buf.at[s], slot + 1 - s, slot + s
            )
    for sx in range(2):
        for sy in range(2):
            here, away = sx * 2 + sy, (1 - sx) * 2 + 1 - sy
            for ex, pack, buf, slot in (
                (part_a, r.pack_k, r.in_k, 6),
                (part_b, r.pack_kf, r.in_kf, 8),
                (part_b, r.pack_tk, r.in_tk, 12),
            ):
                ex.add(
                    c_dev(sx, sy), pack.at[here], buf.at[away], buf.at[here],
                    slot + away, slot + here,
                )
    part_a.start(0, 6)
    beside_y.start(0, 6)
    fetch[3].wait()
    for s in range(2):
        r.pack_t[s] = tough_ref[0, :, 0:2] if s == 0 else tough_ref[0, :, ny - 2 : ny]
    for sx in range(2):
        for sy in range(2):
            row = 0 if sy == 0 else ny - 1
            r.pack_tk[sx * 2 + sy] = tough_ref[0, 0 if sx == 0 else nx - 1, row : row + 1]
    beside_y.start(6)
    part_a.start(6)
    part_b.start()
    part_c.start()
    tough_copies = []
    for k in range(1, sections):
        copy = pltpu.make_async_remote_copy(
            src_ref=tough_ref.at[0],
            dst_ref=r.tough_in.at[k - 1],
            send_sem=r.tough_send.at[k - 1],
            recv_sem=r.tough_recv.at[k - 1],
            device_id={"section": lax.rem(sec + sections - k, sections)},
            device_id_type=MESH,
        )
        copy.start()
        tough_copies.append(copy)

    inner = slice(OY, OY + ny)
    as_float = lambda v: v.astype(jnp.float32)

    def fill(x, carry):
        held[x + HX, inner] = as_float(load_ref[x])
        clamped[x + HX, inner] = as_float(clamp_ref[x])
        crack_pad[x + HX, inner] = as_float(crack_ref[x])
        tough_pad[x + HX, inner] = tough_ref[0, x]
        return carry

    lax.fori_loop(0, nx, fill, 0, unroll=part(nx, 4))

    for copy in fetch[4:]:
        copy.wait()
    case = r.index_ref[0]
    vector = [r.table_ref[f, case] for f in range(3)]

    planes = slice(HX, HX + nx)

    def x_out(s, n):
        return slice(HX - n, HX) if s == 0 else slice(HX + nx, HX + nx + n)

    def y_out(s, n):
        return slice(OY - n, OY) if s == 0 else slice(OY + ny, OY + ny + n)

    def unpack_y():
        beside_y.received(0, 4)
        for s in range(2):

            @pl.when(there["gy"][s])
            def _(s=s):
                crack_pad[planes, y_out(s, 4)] = as_float(r.in_c[s])
                for x in range(nx):
                    held[HX + x, y_out(s, 5)] = as_float(r.in_l[s, 5 * x : 5 * x + 5])

    def unpack_y_clamp():
        beside_y.received(4, 6)
        for s in range(2):

            @pl.when(there["gy"][s])
            def _(s=s):
                for x in range(nx):
                    clamped[HX + x, y_out(s, 3)] = as_float(r.in_f[s, 3 * x : 3 * x + 3])

    def unpack_y_tough():
        beside_y.received(6)
        for s in range(2):

            @pl.when(there["gy"][s])
            def _(s=s):
                tough_pad[planes, y_out(s, 2)] = r.in_ty[s]

    def unpack_corners(corner, buf):
        for sx in range(2):
            for sy in range(2):

                @pl.when(c_dev(sx, sy)[0])
                def _(sx=sx, sy=sy):
                    for _, pad, deep, n, at in corner:
                        pad[x_at(sx, deep), y_out(sy, n)] = as_float(
                            buf[sx * 2 + sy, at : at + n]
                        )

    def unpack_a():
        part_a.received()
        for s in range(2):

            @pl.when(there["gx"][s])
            def _(s=s):
                held[x_out(s, 3), inner] = as_float(r.in_a[s, 0:3])
                crack_pad[x_out(s, 2), inner] = as_float(r.in_a[s, 3:5])
                clamped[x_out(s, 1), inner] = as_float(r.in_a[s, 5:6])

        unpack_corners(near_corner, r.in_k)

    def unpack_far(part, buf, less):
        part.received()
        for s in range(2):

            @pl.when(there["gx"][s])
            def _(s=s):
                held[x_at(s, 5 - less), inner] = as_float(buf[s, 0])
                crack_pad[x_at(s, 4 - less), inner] = as_float(buf[s, 1])
                clamped[x_at(s, 3 - less), inner] = as_float(buf[s, 2])
                tough_pad[x_at(s, 2 - less), inner] = r.in_tx[s, 1 - less]

    def unpack_b():
        unpack_far(part_b, r.in_b, 1)
        unpack_corners(far_corner, r.in_kf)
        for sx in range(2):
            for sy in range(2):

                @pl.when(c_dev(sx, sy)[0])
                def _(sx=sx, sy=sy):
                    tough_pad[x_at(sx, 1), y_out(sy, 1)] = r.in_tk[sx * 2 + sy]

    def unpack_c():
        unpack_far(part_c, r.in_c_x, 0)

    wide = up8(ny + 4)
    deep = up8(ny + 8)

    def lanes(shape, lane):
        return lax.broadcasted_iota(jnp.int32, shape, 1) == lane

    def beside(v, edge, first, last):
        up = jnp.where(last, edge, pltpu.roll(v, nz - 1, 1))
        down = jnp.where(first, edge, pltpu.roll(v, 1, 1))
        return up, down

    def inside_rows(shape, above):
        row = lax.broadcasted_iota(jnp.int32, shape, 0) + (gy * ny - above)
        return jnp.logical_and(row >= 0, row < ny * ngy)

    def inside_plane(xp):
        plane = xp - HX + gx * nx
        return jnp.logical_and(plane >= 0, plane < nx * ngx)

    edge_stiff = 0.5 * (1.0 + stiff_floor)

    def elastic(at, first, last):
        k = at(stiff, 0, 0)
        sides = (
            (at(stiff, 1, 0), at(stiff, -1, 0)),
            (at(stiff, 0, 1), at(stiff, 0, -1)),
            beside(k, edge_stiff, first, last),
        )
        pairs = [s[0] + s[1] for s in sides]
        weights = pairs[0] + pairs[1] + pairs[2] + 6.0 * k
        faces = [(k + s[0], k + s[1]) for s in sides]
        fz = beside(at(flow, 0, 0), 0.0, first, last)
        grads = (
            at(flow, 1, 0) - at(flow, -1, 0),
            at(flow, 0, 1) - at(flow, 0, -1),
            fz[0] - fz[1],
        )
        return pairs, weights, faces, grads

    def laplace(at, ref, faces, weights, first, last):
        here = at(ref, 0, 0)
        uz = beside(here, 0.0, first, last)
        return here, (
            faces[0][0] * at(ref, 1, 0)
            + faces[0][1] * at(ref, -1, 0)
            + faces[1][0] * at(ref, 0, 1)
            + faces[1][1] * at(ref, 0, -1)
            + faces[2][0] * uz[0]
            + faces[2][1] * uz[1]
            - weights * here
        )

    def strain_energy(at, u, keep, first, last):
        grad = []
        for f in range(3):
            here = at(u.at[f], 0, 0)
            uz = beside(here, 0.0, first, last)
            grad.append(
                (
                    at(u.at[f], 1, 0) - at(u.at[f], -1, 0),
                    at(u.at[f], 0, 1) - at(u.at[f], 0, -1),
                    uz[0] - uz[1],
                )
            )
            keep(f, here)
        return 2.0 * spectral_energy(
            0.5 * grad[0][0],
            0.5 * grad[1][1],
            0.5 * grad[2][2],
            0.25 * (grad[0][1] + grad[1][0]),
            0.25 * (grad[0][2] + grad[2][0]),
            0.25 * (grad[1][2] + grad[2][1]),
        )

    def renew(at, d, energy, g, cracked, first, last):
        dz = beside(at(d, 0, 0), 0.0, first, last)
        around = at(d, 1, 0) + at(d, -1, 0) + at(d, 0, 1) + at(d, 0, -1) + dz[0] + dz[1]
        renewed = (energy + g * around) / (7.0 * g + energy)
        return jnp.where(cracked, 1.0, renewed)

    def add_up(rnd, total):
        r.sums[me, rnd : rnd + 1] = jnp.sum(total, axis=0, keepdims=True)

    def open_stages(above, n):
        shape = (n, nz)
        first, last = lanes(shape, 0), lanes(shape, nz - 1)
        row_inside = inside_rows(shape, above)
        row = lax.broadcasted_iota(jnp.int32, shape, 0)
        a = OY - above

        def stiffen(xp, carry):
            half = 0.5 * (jnp.square(1.0 - crack_pad[xp, a : a + n]) + stiff_floor)
            stiff[xp, a : a + n] = half
            up, down = beside(held[xp, a : a + n], 0.0, first, last)
            div = (
                vector[0] * (held[xp + 1, a : a + n] - held[xp - 1, a : a + n])
                + vector[1] * (held[xp, a + 1 : a + 1 + n] - held[xp, a - 1 : a - 1 + n])
                + vector[2] * (up - down)
            )
            flow[xp, a : a + n] = jnp.where(
                jnp.logical_and(row_inside, inside_plane(xp)), half * div, 0.0
            )
            return carry

        def mover(low, high):
            def move(xp, total):
                at = lambda ref, dx, dy: ref[xp + dx, a + dy : a + dy + n]
                pairs, weights, faces, grads = elastic(at, first, last)
                load, spread = laplace(at, held, faces, weights, first, last)
                pin = at(clamped, 0, 0) + load > 0.5
                squares = None
                for f in range(3):
                    res = vector[f] * spread + grads[f]
                    moved = jnp.where(pin, 0.0, relax_weight * res / (weights + pairs[f]))
                    state[1, f, xp, a : a + n] = vector[f] * load + moved
                    square = res * res
                    squares = square if squares is None else squares + square
                if low >= high:
                    return total
                counted = jnp.logical_and(row >= low + above, row < high + above)
                return total + jnp.where(
                    jnp.logical_and(counted, jnp.logical_not(pin)), squares, 0.0
                )

            return move

        def damage(xp, carry):
            at = lambda ref, dx, dy: ref[xp + dx, a + dy : a + dy + n]
            energy = strain_energy(at, state.at[1], lambda f, v: None, first, last)
            renewed = renew(
                at,
                crack_pad,
                energy,
                at(tough_pad, 0, 0),
                at(crack_pad, 0, 0) > 0.5,
                first,
                last,
            )
            state[1, 3, xp, a : a + n] = jnp.where(
                jnp.logical_and(row_inside, inside_plane(xp)), renewed, 0.0
            )
            return carry

        return stiffen, mover, damage

    def open_sweep():
        def inward(skip, body, carry, most):
            n = nx - 2 * skip
            return lax.fori_loop(HX + skip, HX + nx - skip, body, carry, unroll=part(n, most))

        def outward(far, n, body, carry):
            def both(i, carry):
                carry = body(HX - far + i, carry)
                return body(HX + nx + far - n + i, carry)

            return lax.fori_loop(0, n, both, carry, unroll=True)

        def pair(one, two):
            def body(xp, carry):
                return one(xp, carry[0]), two(xp, carry[1])

            return body

        blank = lambda n: jnp.zeros((n, nz), jnp.float32)
        fold = lambda v: jnp.sum(v, axis=0, keepdims=True)

        stiffen, mover, damage = open_stages(0, ny)
        inward(1, stiffen, 0, 14)
        inside = inward(2, mover(2, ny - 2), blank(ny), 12)
        inward(3, damage, 0, 5)

        low = open_stages(4, 8)
        high = open_stages(4 - ny, 8)
        unpack_y()
        inward(1, pair(low[0], high[0]), (0, 0), 14)
        unpack_y_clamp()
        rims = inward(
            2, pair(low[1](0, 2), high[1](ny - 2, ny)), (blank(8), blank(8)), 12
        )
        unpack_y_tough()
        inward(3, pair(low[2], high[2]), (0, 0), 5)
        stiffen1, mover1 = stages(1)
        move1 = mover1(OY, ny)
        inward(3, stiffen1, 0, 10)
        own = inward(4, move1, blank(ny), 8)

        stiffen, mover, damage = open_stages(4, deep)
        unpack_a()
        outward(2, 3, stiffen, 0)
        ends = outward(0, 2, mover(0, ny), blank(deep))
        outward(1, 1, mover(0, 0), blank(deep))
        r.sums[me, 0:1] = fold(inside) + fold(rims[0] + rims[1]) + fold(ends)
        outward(0, 3, damage, 0)
        outward(0, 3, stiffen1, 0)
        own = outward(-1, 3, move1, own)

        unpack_b()
        outward(3, 1, stiffen, 0)
        outward(2, 1, mover(0, 0), blank(deep))
        outward(1, 1, damage, 0)
        outward(1, 1, stiffen1, 0)
        own = outward(0, 1, move1, own)

        def finish():
            unpack_c()
            outward(4, 1, stiffen, 0)
            outward(3, 1, mover(0, 0), blank(deep))
            outward(2, 1, damage, 0)
            outward(2, 1, stiffen1, 0)

        return own, finish

    def send_sums():
        for k, peer in enumerate(peers):
            pltpu.make_async_remote_copy(
                src_ref=r.sums.at[me],
                dst_ref=r.sums.at[me],
                send_sem=r.sum_send.at[k],
                recv_sem=r.sum_recv.at[me],
                device_id=peer,
                device_id_type=MESH,
            ).start()

    def stages(rnd):
        p = rnd % 2
        q = 1 - p
        shape = (wide, nz)
        first, last = lanes(shape, 0), lanes(shape, nz - 1)
        row_inside = inside_rows(shape, 2)
        a = OY - 2

        def stiffen(xp, carry):
            half = 0.5 * (jnp.square(1.0 - state[p, 3, xp, a : a + wide]) + stiff_floor)
            stiff[xp, a : a + wide] = half
            up, down = beside(state[p, 2, xp, a : a + wide], 0.0, first, last)
            div = (
                (state[p, 0, xp + 1, a : a + wide] - state[p, 0, xp - 1, a : a + wide])
                + (state[p, 1, xp, a + 1 : a + 1 + wide] - state[p, 1, xp, a - 1 : a - 1 + wide])
                + (up - down)
            )
            flow[xp, a : a + wide] = jnp.where(
                jnp.logical_and(row_inside, inside_plane(xp)), half * div, 0.0
            )
            return carry

        def mover(b, n):
            shape = (n, nz)
            first, last = lanes(shape, 0), lanes(shape, nz - 1)

            def move(xp, total):
                at = lambda ref, dx, dy: ref[xp + dx, b + dy : b + dy + n]
                pairs, weights, faces, grads = elastic(at, first, last)
                load = at(held, 0, 0)
                pin = at(clamped, 0, 0) + load > 0.5
                squares = None
                for f in range(3):
                    here, spread = laplace(at, state.at[p, f], faces, weights, first, last)
                    res = spread + grads[f]
                    moved = here + relax_weight * res / (weights + pairs[f])
                    state[q, f, xp, b : b + n] = jnp.where(pin, load * vector[f], moved)
                    square = res * res
                    squares = square if squares is None else squares + square
                return total + jnp.where(pin, 0.0, squares)

            return move

        return stiffen, mover

    def sweep(rnd, total):
        p = rnd % 2
        q = 1 - p
        done = rnd == sections - 1
        tough = r.tough_in.at[rnd - 1]

        stiffen, mover = stages(rnd)
        if rnd > 1:
            lax.fori_loop(HX - 2, HX + nx + 2, stiffen, 0, unroll=part(nx + 4, 10))
            total = lax.fori_loop(
                HX, HX + nx, mover(OY, ny), jnp.zeros((ny, nz), jnp.float32), unroll=part(nx, 8)
            )
        add_up(rnd, total)
        if done:
            send_sums()
        if rnd == 1:
            finish_open()
        none = jnp.zeros((8, nz), jnp.float32)

        def edges(xp, carry):
            mover(OY - 4, 8)(xp, none)
            mover(OY + ny - 3, 8)(xp, none)
            return carry

        lax.fori_loop(HX, HX + nx, edges, 0, unroll=part(nx, 8))
        ends = mover(OY, ny)
        ends(HX - 1, jnp.zeros((ny, nz), jnp.float32))
        ends(HX + nx, jnp.zeros((ny, nz), jnp.float32))
        par = rnd % 2
        mid = pl.ds(OY, ny)
        if not done:
            for f in range(3):
                r.pack_u[0, :, 2 * f : 2 * f + 2] = state[q, f, planes, OY : OY + 2]
                r.pack_u[1, :, 2 * f : 2 * f + 2] = state[q, f, planes, OY + ny - 2 : OY + ny]
            r.pack_u[0, :, 6:7] = state[q, 1, planes, OY + 2 : OY + 3]
            r.pack_u[1, :, 6:7] = state[q, 1, planes, OY + ny - 3 : OY + ny - 2]
            shift = Exchange(r.u_send, r.u_recv.at[par])
            for s in range(2):
                shift.add(
                    x_dev(s),
                    state.at[q, pl.ds(0, 3), pl.ds(HX if s == 0 else HX + nx - 2, 2), mid],
                    r.in_u_x.at[par, 1 - s],
                    r.in_u_x.at[par, s],
                    (1 - s),
                    s,
                )
                shift.add(
                    x_dev(s),
                    state.at[q, 0, HX + 2 if s == 0 else HX + nx - 3, mid],
                    r.in_u_x3.at[par, 1 - s],
                    r.in_u_x3.at[par, s],
                    2 + (1 - s),
                    2 + s,
                )
            for s in range(2):
                shift.add(
                    y_dev(s),
                    r.pack_u.at[s],
                    r.in_u_y.at[par, 1 - s],
                    r.in_u_y.at[par, s],
                    4 + (1 - s),
                    4 + s,
                )
            for sx in range(2):
                for sy in range(2):
                    shift.add(
                        c_dev(sx, sy),
                        r.pack_u.at[sy, pl.ds(0 if sx == 0 else nx - 2, 2)],
                        r.in_u_c.at[par, (1 - sx) * 2 + 1 - sy],
                        r.in_u_c.at[par, sx * 2 + sy],
                        6 + (1 - sx) * 2 + 1 - sy,
                        6 + sx * 2 + sy,
                    )
            shift.start()

        tough_copies[rnd - 1].wait_recv()

        shape = (ny, nz)
        first, last = lanes(shape, 0), lanes(shape, nz - 1)

        def damage(x, carry):
            xp = x + HX
            at = lambda ref, dx, dy: ref[xp + dx, OY + dy : OY + dy + ny]

            def keep(f, here):
                if done:
                    disp_refs[f][x] = here

            energy = strain_energy(at, state.at[q], keep, first, last)
            renewed = renew(
                at, state.at[p, 3], energy, tough[x], crack_ref[x] > 0, first, last
            )
            if done:
                r.dam_ref[x] = renewed
            else:
                state[q, 3, xp, inner] = renewed
            return carry

        lax.fori_loop(0, nx, damage, 0, unroll=part(nx, 8))
        if done:
            return

        r.pack_d[0] = state[q, 3, planes, OY : OY + 2]
        r.pack_d[1] = state[q, 3, planes, OY + ny - 2 : OY + ny]
        crack = Exchange(r.d_send, r.d_recv.at[par])
        for s in range(2):
            crack.add(
                x_dev(s),
                state.at[q, 3, pl.ds(HX if s == 0 else HX + nx - 2, 2), mid],
                r.in_d_x.at[par, 1 - s],
                r.in_d_x.at[par, s],
                1 - s,
                s,
            )
        for s in range(2):
            crack.add(
                y_dev(s),
                r.pack_d.at[s],
                r.in_d_y.at[par, 1 - s],
                r.in_d_y.at[par, s],
                2 + 1 - s,
                2 + s,
            )
        for sx in range(2):
            for sy in range(2):
                crack.add(
                    c_dev(sx, sy),
                    r.pack_d.at[sy, pl.ds(0 if sx == 0 else nx - 1, 1)],
                    r.in_d_c.at[par, (1 - sx) * 2 + 1 - sy],
                    r.in_d_c.at[par, sx * 2 + sy],
                    4 + (1 - sx) * 2 + 1 - sy,
                    4 + sx * 2 + sy,
                )
        crack.start()
        shift.finish()
        third_x = (HX - 3, HX + nx + 2)
        third_y = (slice(OY - 3, OY - 2), slice(OY + ny + 2, OY + ny + 3))
        for s in range(2):

            @pl.when(there["gx"][s])
            def _(s=s):
                state[q, 0:3, x_out(s, 2), inner] = r.in_u_x[par, s]
                state[q, 0, third_x[s], inner] = r.in_u_x3[par, s]

            @pl.when(there["gy"][s])
            def _(s=s):
                for f in range(3):
                    state[q, f, planes, y_out(s, 2)] = r.in_u_y[par, s, :, 2 * f : 2 * f + 2]
                state[q, 1, planes, third_y[s]] = r.in_u_y[par, s, :, 6:7]

        for sx in range(2):
            for sy in range(2):

                @pl.when(c_dev(sx, sy)[0])
                def _(sx=sx, sy=sy):
                    for f in range(3):
                        state[q, f, x_out(sx, 2), y_out(sy, 2)] = r.in_u_c[
                            par, sx * 2 + sy, :, 2 * f : 2 * f + 2
                        ]

        crack.finish()
        for s in range(2):

            @pl.when(there["gx"][s])
            def _(s=s):
                state[q, 3, x_out(s, 2), inner] = r.in_d_x[par, s]

            @pl.when(there["gy"][s])
            def _(s=s):
                state[q, 3, planes, y_out(s, 2)] = r.in_d_y[par, s]

        for sx in range(2):
            for sy in range(2):

                @pl.when(c_dev(sx, sy)[0])
                def _(sx=sx, sy=sy):
                    state[q, 3, x_out(sx, 1), y_out(sy, 2)] = r.in_d_c[par, sx * 2 + sy]

    total, finish_open = open_sweep()
    for rnd in range(1, sections):
        sweep(rnd, total)

    cells = 3.0 * nx * ngx * ny * ngy * nz
    beside_y.sent()
    part_a.sent()
    part_b.sent()
    part_c.sent()
    for copy in tough_copies:
        copy.wait_send()
    for k, peer in enumerate(peers):
        other = peer["gx"] * ngy + peer["gy"]
        pltpu.make_async_remote_copy(
            src_ref=r.sums.at[me],
            dst_ref=r.sums.at[other],
            send_sem=r.sum_send.at[k],
            recv_sem=r.sum_recv.at[other],
            device_id=peer,
            device_id_type=MESH,
        ).wait()
    total = r.sums[0]
    for k in range(1, group):
        total = total + r.sums[k]
    entries = jnp.sqrt(jnp.sum(total, axis=1, keepdims=True) / cells)
    column = lax.broadcasted_iota(jnp.int32, (1, sections), 1)
    norms = jnp.zeros((1, sections), jnp.float32)
    for rnd in range(sections):
        norms = jnp.where(
            column == lax.rem(sec + rnd, sections), entries[rnd : rnd + 1], norms
        )
    r.norm_ref[...] = norms


def put_out(
    first_ref, second_ref, third_ref, dam_ref, norm_ref, disp_hbm, dam_hbm, norm_out, sems
):
    copies = [
        pltpu.make_async_copy(ref, disp_hbm.at[0, f], sems.at[f])
        for f, ref in enumerate((first_ref, second_ref, third_ref))
    ]
    copies.append(pltpu.make_async_copy(dam_ref, dam_hbm.at[0], sems.at[3]))
    for copy in copies:
        copy.start()
    norm_out[...] = norm_ref[...]
    for copy in copies:
        copy.wait()


def on_device(sizes, load_index, load_table, toughness, clamp_mask, load_mask, crack_mask):
    sections, ngx, ngy = sizes
    nx, ny, nz = clamp_mask.shape
    assert load_index.shape == (1,)
    group = ngx * ngy
    f32 = jnp.float32
    padded = (nx + 2 * HX, ny + 2 * OY, nz)
    vmem = pltpu.VMEM
    dma = pltpu.SemaphoreType.DMA
    later = max(sections - 1, 1)
    more = sections > 2
    scratch = {
        "index_ref": pltpu.SMEM(load_index.shape, jnp.int32),
        "table_ref": pltpu.SMEM(load_table.shape[::-1], f32),
        "tough_ref": vmem((1, nx, ny, nz), f32),
        "clamp_ref": vmem((nx, ny, nz), jnp.int32),
        "load_ref": vmem((nx, ny, nz), jnp.int32),
        "crack_ref": vmem((nx, ny, nz), jnp.int32),
        "local": dma((6,)),
        "state": vmem((2, 4) + padded, f32),
        "stiff": vmem(padded, f32),
        "flow": vmem(padded, f32),
        "held": vmem(padded, f32),
        "clamped": vmem(padded, f32),
        "tough_pad": vmem(padded, f32),
        "crack_pad": vmem(padded, f32),
        "tough_in": vmem((later, nx, ny, nz), f32),
        "pack_l": vmem((2, 5 * nx, nz), jnp.int32),
        "pack_f": vmem((2, 3 * nx, nz), jnp.int32),
        "pack_c": vmem((2, nx, 4, nz), jnp.int32),
        "pack_t": vmem((2, nx, 2, nz), f32),
        "pack_k": vmem((4, 16, nz), jnp.int32),
        "pack_kf": vmem((4, 4, nz), jnp.int32),
        "pack_tk": vmem((4, 1, nz), f32),
        "in_a": vmem((2, 6, ny, nz), jnp.int32),
        "in_b": vmem((2, 3, ny, nz), jnp.int32),
        "in_c_x": vmem((2, 3, ny, nz), jnp.int32),
        "in_tx": vmem((2, 2, ny, nz), f32),
        "in_l": vmem((2, 5 * nx, nz), jnp.int32),
        "in_f": vmem((2, 3 * nx, nz), jnp.int32),
        "in_c": vmem((2, nx, 4, nz), jnp.int32),
        "in_ty": vmem((2, nx, 2, nz), f32),
        "in_k": vmem((4, 16, nz), jnp.int32),
        "in_kf": vmem((4, 4, nz), jnp.int32),
        "in_tk": vmem((4, 1, nz), f32),
        "sums": vmem((group, sections, nz), f32),
        "y_send": dma((8,)),
        "y_recv": dma((8,)),
        "a_send": dma((10,)),
        "a_recv": dma((10,)),
        "b_send": dma((16,)),
        "b_recv": dma((16,)),
        "c_send": dma((8,)),
        "c_recv": dma((8,)),
        "tough_send": dma((later,)),
        "tough_recv": dma((later,)),
        "sum_send": dma((max(group - 1, 1),)),
        "sum_recv": dma((group,)),
    }
    if more:
        scratch |= {
            "pack_u": vmem((2, nx, 8, nz), f32),
            "pack_d": vmem((2, nx, 2, nz), f32),
            "in_u_x": vmem((2, 2, 3, 2, ny, nz), f32),
            "in_u_x3": vmem((2, 2, ny, nz), f32),
            "in_u_y": vmem((2, 2, nx, 8, nz), f32),
            "in_u_c": vmem((2, 4, 2, 8, nz), f32),
            "in_d_x": vmem((2, 2, 2, ny, nz), f32),
            "in_d_y": vmem((2, 2, nx, 2, nz), f32),
            "in_d_c": vmem((2, 4, 1, 2, nz), f32),
            "u_send": dma((10,)),
            "u_recv": dma((2, 10)),
            "d_send": dma((8,)),
            "d_recv": dma((2, 8)),
        }
    ins = ("index_hbm", "table_hbm", "tough_hbm", "clamp_hbm", "load_hbm", "crack_hbm")
    outs = ("first_ref", "second_ref", "third_ref", "dam_ref", "norm_ref")
    names = (*ins, *outs, *scratch)
    block = pl.BlockSpec(memory_space=pltpu.VMEM)
    away = pl.BlockSpec(memory_space=pltpu.HBM)
    results = pl.pallas_call(
        functools.partial(kernel, (sections, ngx, ngy, nx, ny, nz), names),
        out_shape=(
            *[jax.ShapeDtypeStruct((nx, ny, nz), f32)] * 4,
            jax.ShapeDtypeStruct((1, sections), f32),
        ),
        in_specs=[away] * 6,
        out_specs=(block,) * 5,
        scratch_shapes=list(scratch.values()),
        compiler_params=pltpu.CompilerParams(
            collective_id=0, has_side_effects=True, vmem_limit_bytes=56_020_000
        ),
    )(load_index, pltpu.with_memory_space_constraint(load_table.T, pltpu.HBM), toughness, clamp_mask, load_mask, crack_mask)
    return pl.pallas_call(
        put_out,
        out_shape=(
            jax.ShapeDtypeStruct((1, 3, nx, ny, nz), f32),
            jax.ShapeDtypeStruct((1, nx, ny, nz), f32),
            jax.ShapeDtypeStruct((1, sections), f32),
        ),
        in_specs=[block] * 5,
        out_specs=(away, away, block),
        scratch_shapes=[dma((4,))],
        compiler_params=pltpu.CompilerParams(vmem_limit_bytes=1024 * 1024),
    )(*results)


def solution(mesh):
    in_specs = (
        P("section"),
        P(),
        P("section", "gx", "gy", None),
        P("gx", "gy", None),
        P("gx", "gy", None),
        P("gx", "gy", None),
    )
    out_specs = (
        P("section", None, "gx", "gy", None),
        P("section", "gx", "gy", None),
        P("section", None),
    )
    sizes = tuple(mesh.shape[name] for name in ("section", "gx", "gy"))
    return jax.shard_map(
        functools.partial(on_device, sizes),
        mesh=mesh,
        in_specs=in_specs,
        out_specs=out_specs,
        check_vma=False,
    )
```

```python
import functools
import math
import types

import jax
import jax.numpy as jnp
from jax import lax
from jax.experimental import pallas as pl
from jax.experimental.pallas import tpu as pltpu
from jax.sharding import PartitionSpec as P

relax_weight = 0.6
stiff_floor = 0.001
eigen_guard = 1e-08
MESH = pl.DeviceIdType.MESH

HX = 5
OY = 8

ACOS = (
    1.5707963050,
    -0.2145988016,
    0.0889789874,
    -0.0501743046,
    0.0308918810,
    -0.0170881256,
    0.0066700901,
    -0.0012624911,
)


def up8(n):
    return -(-n // 8) * 8


def part(n, most):
    return max(k for k in range(1, most + 1) if n % k == 0)


def root(v):
    return v * lax.rsqrt(jnp.maximum(v, 1.2e-38))


def spectral_energy(xx, yy, zz, xy, xz, yz):
    trace = xx + yy + zz
    mid = trace * (1.0 / 3.0)
    dx = xx - mid
    dy = yy - mid
    dz = zz - mid
    xy2 = xy * xy
    xz2 = xz * xz
    yz2 = yz * yz
    sixth = (dx * dx + dy * dy + dz * dz + 2.0 * (xy2 + xz2 + yz2)) * (1.0 / 6.0)
    twice_radius = 2.0 * root(sixth)
    scale = lax.rsqrt(sixth + eigen_guard)
    det = dx * (dy * dz - yz2) - dz * xy2 - dy * xz2 + 2.0 * (xy * xz * yz)
    ratio = (0.5 * det * scale) * (scale * scale)
    size = jnp.minimum(jnp.abs(ratio), 1.0)
    poly = jnp.full_like(size, ACOS[-1] / 3.0)
    for c in ACOS[-2::-1]:
        poly = poly * size + c / 3.0
    t = root(1.0 - size) * poly
    t2 = t * t
    cos_t = 1.0 + t2 * (-0.5 + t2 * (1.0 / 24.0 + t2 * (-1.0 / 720.0 + t2 * (1.0 / 40320.0))))
    sin_t = t * (1.0 + t2 * (-1.0 / 6.0 + t2 * (1.0 / 120.0 + t2 * (-1.0 / 5040.0))))
    other = 0.5 * cos_t + math.sqrt(0.75) * sin_t
    upper = ratio >= 0.0
    first = jnp.where(upper, cos_t, other)
    last = jnp.where(upper, other, cos_t)
    largest = mid + twice_radius * first
    smallest = mid - twice_radius * last
    between = trace - largest - smallest
    relu = lambda v: jnp.maximum(v, 0.0)
    return (
        0.5 * jnp.square(relu(trace))
        + jnp.square(relu(largest))
        + jnp.square(relu(between))
        + jnp.square(relu(smallest))
    )


def kernel(sizes, names, *refs):
    sections, ngx, ngy, nx, ny, nz = sizes
    r = types.SimpleNamespace(**dict(zip(names, refs)))
    local, state, stiff, flow = r.local, r.state, r.stiff, r.flow
    held, clamped, tough_pad, crack_pad = r.held, r.clamped, r.tough_pad, r.crack_pad
    load_ref, crack_ref, clamp_ref, tough_ref = r.load_ref, r.crack_ref, r.clamp_ref, r.tough_ref
    disp_refs = (r.first_ref, r.second_ref, r.third_ref)
    sec = lax.axis_index("section")
    gx = lax.axis_index("gx")
    gy = lax.axis_index("gy")
    group = ngx * ngy
    me = gx * ngy + gy
    ring = lambda k, n: min(k, n - k)
    offsets = [(i, j) for i in range(ngx) for j in range(ngy) if i or j]
    offsets.sort(key=lambda o: (ring(o[0], ngx) + ring(o[1], ngy), o))
    peers = []
    for i, j in offsets:
        peers.append({"gx": lax.rem(gx + i, ngx), "gy": lax.rem(gy + j, ngy)})

    there = {
        "gx": (gx > 0, gx < ngx - 1),
        "gy": (gy > 0, gy < ngy - 1),
    }
    step = (-1, 1)

    def x_dev(s):
        return there["gx"][s], {"gx": gx + step[s]}

    def y_dev(s):
        return there["gy"][s], {"gy": gy + step[s]}

    def c_dev(sx, sy):
        return (
            jnp.logical_and(there["gx"][sx], there["gy"][sy]),
            {"gx": gx + step[sx], "gy": gy + step[sy]},
        )

    neighbours = [x_dev(s) for s in range(2)] + [y_dev(s) for s in range(2)]
    neighbours += [c_dev(sx, sy) for sx in range(2) for sy in range(2)]
    in_line = lambda name: sum(t.astype(jnp.int32) for t in there[name])
    near_count = (in_line("gx") + 1) * (in_line("gy") + 1) - 1

    def greet(sem):
        for cond, dev in neighbours:

            @pl.when(cond)
            def _(dev=dev):
                pl.semaphore_signal(sem, inc=1, device_id=dev, device_id_type=MESH)

    barrier = pltpu.get_barrier_semaphore()
    greet(barrier)
    for k in range(1, sections):
        pl.semaphore_signal(
            barrier,
            inc=1,
            device_id={"section": lax.rem(sec + k, sections)},
            device_id_type=MESH,
        )

    fetch = [
        pltpu.make_async_copy(src, dst, local.at[n])
        for n, (src, dst) in enumerate(
            (
                (r.load_hbm, load_ref),
                (r.crack_hbm, crack_ref),
                (r.clamp_hbm, clamp_ref),
                (r.tough_hbm, tough_ref),
                (r.index_hbm, r.index_ref),
                (r.table_hbm, r.table_ref),
            )
        )
    ]
    for copy in fetch:
        copy.start()

    class Exchange:
        def __init__(self, send, recv):
            self.items = []
            self.send = send
            self.recv = recv

        def add(self, where, src, dst, mine, out_slot, in_slot):
            cond, dev = where
            n = len(self.items)
            copy = pltpu.make_async_remote_copy(
                src_ref=src,
                dst_ref=dst,
                send_sem=self.send.at[n],
                recv_sem=self.recv.at[out_slot],
                device_id=dev,
                device_id_type=MESH,
            )
            back = pltpu.make_async_remote_copy(
                src_ref=src,
                dst_ref=mine,
                send_sem=self.send.at[n],
                recv_sem=self.recv.at[in_slot],
                device_id=dev,
                device_id_type=MESH,
            )
            self.items.append((cond, copy, back))

        def start(self, begin=0, end=None):
            for cond, copy, _ in self.items[begin:end]:
                pl.when(cond)(copy.start)

        def finish(self):
            for cond, copy, back in self.items:

                @pl.when(cond)
                def _():
                    back.wait_recv()
                    copy.wait_send()

        def received(self, begin=0, end=None):
            for cond, _, back in self.items[begin:end]:
                pl.when(cond)(back.wait_recv)

        def sent(self, begin=0, end=None):
            for cond, copy, _ in self.items[begin:end]:
                pl.when(cond)(copy.wait_send)

    rows = ny + 2 * OY

    def clear(xp, carry):
        zero = jnp.zeros((rows, nz), jnp.float32)
        held[xp] = zero
        crack_pad[xp] = zero
        clamped[xp] = zero + 1.0
        tough_pad[xp] = zero + 1.0
        if sections > 2:
            for p in range(2):
                for f in range(4):
                    state[p, f, xp] = zero
        return carry

    lax.fori_loop(0, nx + 2 * HX, clear, 0)

    for copy in fetch[:3]:
        copy.wait()

    for s in range(2):
        side = lambda n, s=s: slice(0, n) if s == 0 else slice(ny - n, ny)
        r.pack_c[s] = crack_ref[:, side(4)]
        for x in range(nx):
            r.pack_l[s, 5 * x : 5 * x + 5] = load_ref[x, side(5)]
            r.pack_f[s, 3 * x : 3 * x + 3] = clamp_ref[x, side(3)]
    near_corner = (
        (load_ref, held, 1, 4, 0),
        (load_ref, held, 2, 3, 4),
        (load_ref, held, 3, 2, 7),
        (crack_ref, crack_pad, 1, 3, 9),
        (crack_ref, crack_pad, 2, 2, 12),
        (clamp_ref, clamped, 1, 2, 14),
    )
    far_corner = (
        (load_ref, held, 4, 1, 0),
        (crack_ref, crack_pad, 3, 1, 1),
        (clamp_ref, clamped, 2, 1, 2),
    )

    def x_from(s, deep):
        return deep - 1 if s == 0 else nx - deep

    def x_at(s, deep):
        return HX - deep if s == 0 else HX + nx - 1 + deep

    for sx in range(2):
        for sy in range(2):
            for pack, corner in ((r.pack_k, near_corner), (r.pack_kf, far_corner)):
                for ref, _, deep, n, at in corner:
                    first = 0 if sy == 0 else ny - n
                    pack[sx * 2 + sy, at : at + n] = ref[x_from(sx, deep), first : first + n]

    pl.semaphore_wait(barrier, near_count + sections - 1)

    beside_y = Exchange(r.y_send, r.y_recv)
    part_a = Exchange(r.a_send, r.a_recv)
    part_b = Exchange(r.b_send, r.b_recv)
    part_c = Exchange(r.c_send, r.c_recv)
    for ex, ref, buf, deep, width, at, slot in (
        (part_a, load_ref, r.in_a, 3, 3, 0, 0),
        (part_a, crack_ref, r.in_a, 2, 2, 3, 2),
        (part_a, clamp_ref, r.in_a, 1, 1, 5, 4),
        (part_b, load_ref, r.in_b, 4, 1, 0, 0),
        (part_b, crack_ref, r.in_b, 3, 1, 1, 2),
        (part_b, clamp_ref, r.in_b, 2, 1, 2, 4),
        (part_b, tough_ref.at[0], r.in_tx, 1, 1, 0, 6),
        (part_c, load_ref, r.in_c_x, 5, 1, 0, 0),
        (part_c, crack_ref, r.in_c_x, 4, 1, 1, 2),
        (part_c, clamp_ref, r.in_c_x, 3, 1, 2, 4),
        (part_c, tough_ref.at[0], r.in_tx, 2, 1, 1, 6),
    ):
        for s in range(2):
            first = deep - width if s == 0 else nx - deep
            ex.add(
                x_dev(s),
                ref.at[pl.ds(first, width)],
                buf.at[1 - s, pl.ds(at, width)],
                buf.at[s, pl.ds(at, width)],
                slot + 1 - s,
                slot + s,
            )
    for n in range(8):
        s = n % 2
        for pack, buf, slot in (
            (r.pack_c, r.in_c, 0),
            (r.pack_l, r.in_l, 2),
            (r.pack_f, r.in_f, 4),
            (r.pack_t, r.in_ty, 6),
        )[n // 2 : n // 2 + 1]:
            beside_y.add(
                y_dev(s), pack.at[s], buf.at[1 - s], buf.at[s], slot + 1 - s, slot + s
            )
    for sx in range(2):
        for sy in range(2):
            here, away = sx * 2 + sy, (1 - sx) * 2 + 1 - sy
            for ex, pack, buf, slot in (
                (part_a, r.pack_k, r.in_k, 6),
                (part_b, r.pack_kf, r.in_kf, 8),
                (part_b, r.pack_tk, r.in_tk, 12),
            ):
                ex.add(
                    c_dev(sx, sy), pack.at[here], buf.at[away], buf.at[here],
                    slot + away, slot + here,
                )
    beside_y.start(0, 4)
    part_a.start(0, 6)
    beside_y.start(4, 6)
    fetch[3].wait()
    for s in range(2):
        r.pack_t[s] = tough_ref[0, :, 0:2] if s == 0 else tough_ref[0, :, ny - 2 : ny]
    for sx in range(2):
        for sy in range(2):
            row = 0 if sy == 0 else ny - 1
            r.pack_tk[sx * 2 + sy] = tough_ref[0, 0 if sx == 0 else nx - 1, row : row + 1]
    beside_y.start(6)
    part_a.start(6)
    part_b.start()
    part_c.start()
    tough_copies = []
    for k in range(1, sections):
        copy = pltpu.make_async_remote_copy(
            src_ref=tough_ref.at[0],
            dst_ref=r.tough_in.at[k - 1],
            send_sem=r.tough_send.at[k - 1],
            recv_sem=r.tough_recv.at[k - 1],
            device_id={"section": lax.rem(sec + sections - k, sections)},
            device_id_type=MESH,
        )
        copy.start()
        tough_copies.append(copy)

    inner = slice(OY, OY + ny)
    as_float = lambda v: v.astype(jnp.float32)

    def fill(x, carry):
        held[x + HX, inner] = as_float(load_ref[x])
        clamped[x + HX, inner] = as_float(clamp_ref[x])
        crack_pad[x + HX, inner] = as_float(crack_ref[x])
        tough_pad[x + HX, inner] = tough_ref[0, x]
        return carry

    lax.fori_loop(0, nx, fill, 0, unroll=part(nx, 4))

    for copy in fetch[4:]:
        copy.wait()
    case = r.index_ref[0]
    vector = [r.table_ref[f, case] for f in range(3)]

    planes = slice(HX, HX + nx)

    def x_out(s, n):
        return slice(HX - n, HX) if s == 0 else slice(HX + nx, HX + nx + n)

    def y_out(s, n):
        return slice(OY - n, OY) if s == 0 else slice(OY + ny, OY + ny + n)

    def unpack_y():
        beside_y.received(0, 4)
        for s in range(2):

            @pl.when(there["gy"][s])
            def _(s=s):
                crack_pad[planes, y_out(s, 4)] = as_float(r.in_c[s])
                for x in range(nx):
                    held[HX + x, y_out(s, 5)] = as_float(r.in_l[s, 5 * x : 5 * x + 5])

    def unpack_y_clamp():
        beside_y.received(4, 6)
        for s in range(2):

            @pl.when(there["gy"][s])
            def _(s=s):
                for x in range(nx):
                    clamped[HX + x, y_out(s, 3)] = as_float(r.in_f[s, 3 * x : 3 * x + 3])

    def unpack_y_tough():
        beside_y.received(6)
        for s in range(2):

            @pl.when(there["gy"][s])
            def _(s=s):
                tough_pad[planes, y_out(s, 2)] = r.in_ty[s]

    def unpack_corners(corner, buf):
        for sx in range(2):
            for sy in range(2):

                @pl.when(c_dev(sx, sy)[0])
                def _(sx=sx, sy=sy):
                    for _, pad, deep, n, at in corner:
                        pad[x_at(sx, deep), y_out(sy, n)] = as_float(
                            buf[sx * 2 + sy, at : at + n]
                        )

    further = max(ngx, ngy) - 3

    def unpack_a():
        part_a.received()
        if further > 0:
            greet(r.reach.at[0])
        for s in range(2):

            @pl.when(there["gx"][s])
            def _(s=s):
                held[x_out(s, 3), inner] = as_float(r.in_a[s, 0:3])
                crack_pad[x_out(s, 2), inner] = as_float(r.in_a[s, 3:5])
                clamped[x_out(s, 1), inner] = as_float(r.in_a[s, 5:6])

        unpack_corners(near_corner, r.in_k)

    def unpack_far(part, buf, less):
        part.received()
        for s in range(2):

            @pl.when(there["gx"][s])
            def _(s=s):
                held[x_at(s, 5 - less), inner] = as_float(buf[s, 0])
                crack_pad[x_at(s, 4 - less), inner] = as_float(buf[s, 1])
                clamped[x_at(s, 3 - less), inner] = as_float(buf[s, 2])
                tough_pad[x_at(s, 2 - less), inner] = r.in_tx[s, 1 - less]

    def unpack_b():
        unpack_far(part_b, r.in_b, 1)
        unpack_corners(far_corner, r.in_kf)
        for sx in range(2):
            for sy in range(2):

                @pl.when(c_dev(sx, sy)[0])
                def _(sx=sx, sy=sy):
                    tough_pad[x_at(sx, 1), y_out(sy, 1)] = r.in_tk[sx * 2 + sy]

    def unpack_c():
        unpack_far(part_c, r.in_c_x, 0)

    wide = up8(ny + 4)
    deep = up8(ny + 8)

    def lanes(shape, lane):
        return lax.broadcasted_iota(jnp.int32, shape, 1) == lane

    def beside(v, edge, first, last):
        up = jnp.where(last, edge, pltpu.roll(v, nz - 1, 1))
        down = jnp.where(first, edge, pltpu.roll(v, 1, 1))
        return up, down

    def inside_rows(shape, above):
        row = lax.broadcasted_iota(jnp.int32, shape, 0) + (gy * ny - above)
        return jnp.logical_and(row >= 0, row < ny * ngy)

    def inside_plane(xp):
        plane = xp - HX + gx * nx
        return jnp.logical_and(plane >= 0, plane < nx * ngx)

    edge_stiff = 0.5 * (1.0 + stiff_floor)

    def elastic(at, first, last):
        k = at(stiff, 0, 0)
        sides = (
            (at(stiff, 1, 0), at(stiff, -1, 0)),
            (at(stiff, 0, 1), at(stiff, 0, -1)),
            beside(k, edge_stiff, first, last),
        )
        pairs = [s[0] + s[1] for s in sides]
        weights = pairs[0] + pairs[1] + pairs[2] + 6.0 * k
        faces = [(k + s[0], k + s[1]) for s in sides]
        fz = beside(at(flow, 0, 0), 0.0, first, last)
        grads = (
            at(flow, 1, 0) - at(flow, -1, 0),
            at(flow, 0, 1) - at(flow, 0, -1),
            fz[0] - fz[1],
        )
        return pairs, weights, faces, grads

    def laplace(at, ref, faces, weights, first, last):
        here = at(ref, 0, 0)
        uz = beside(here, 0.0, first, last)
        return here, (
            faces[0][0] * at(ref, 1, 0)
            + faces[0][1] * at(ref, -1, 0)
            + faces[1][0] * at(ref, 0, 1)
            + faces[1][1] * at(ref, 0, -1)
            + faces[2][0] * uz[0]
            + faces[2][1] * uz[1]
            - weights * here
        )

    def strain_energy(at, u, keep, first, last):
        grad = []
        for f in range(3):
            here = at(u.at[f], 0, 0)
            uz = beside(here, 0.0, first, last)
            grad.append(
                (
                    at(u.at[f], 1, 0) - at(u.at[f], -1, 0),
                    at(u.at[f], 0, 1) - at(u.at[f], 0, -1),
                    uz[0] - uz[1],
                )
            )
            keep(f, here)
        return 2.0 * spectral_energy(
            0.5 * grad[0][0],
            0.5 * grad[1][1],
            0.5 * grad[2][2],
            0.25 * (grad[0][1] + grad[1][0]),
            0.25 * (grad[0][2] + grad[2][0]),
            0.25 * (grad[1][2] + grad[2][1]),
        )

    def renew(at, d, energy, g, cracked, first, last):
        dz = beside(at(d, 0, 0), 0.0, first, last)
        around = at(d, 1, 0) + at(d, -1, 0) + at(d, 0, 1) + at(d, 0, -1) + dz[0] + dz[1]
        renewed = (energy + g * around) / (7.0 * g + energy)
        return jnp.where(cracked, 1.0, renewed)

    def add_up(rnd, total):
        r.sums[me, rnd : rnd + 1] = jnp.sum(total, axis=0, keepdims=True)

    def open_stages(above, n):
        shape = (n, nz)
        first, last = lanes(shape, 0), lanes(shape, nz - 1)
        row_inside = inside_rows(shape, above)
        row = lax.broadcasted_iota(jnp.int32, shape, 0)
        a = OY - above

        def stiffen(xp, carry):
            half = 0.5 * (jnp.square(1.0 - crack_pad[xp, a : a + n]) + stiff_floor)
            stiff[xp, a : a + n] = half
            up, down = beside(held[xp, a : a + n], 0.0, first, last)
            div = (
                vector[0] * (held[xp + 1, a : a + n] - held[xp - 1, a : a + n])
                + vector[1] * (held[xp, a + 1 : a + 1 + n] - held[xp, a - 1 : a - 1 + n])
                + vector[2] * (up - down)
            )
            flow[xp, a : a + n] = jnp.where(
                jnp.logical_and(row_inside, inside_plane(xp)), half * div, 0.0
            )
            return carry

        def mover(low, high):
            def move(xp, total):
                at = lambda ref, dx, dy: ref[xp + dx, a + dy : a + dy + n]
                pairs, weights, faces, grads = elastic(at, first, last)
                load, spread = laplace(at, held, faces, weights, first, last)
                pin = at(clamped, 0, 0) + load > 0.5
                squares = None
                for f in range(3):
                    res = vector[f] * spread + grads[f]
                    moved = jnp.where(pin, 0.0, relax_weight * res / (weights + pairs[f]))
                    state[1, f, xp, a : a + n] = vector[f] * load + moved
                    square = res * res
                    squares = square if squares is None else squares + square
                if low >= high:
                    return total
                counted = jnp.logical_and(row >= low + above, row < high + above)
                return total + jnp.where(
                    jnp.logical_and(counted, jnp.logical_not(pin)), squares, 0.0
                )

            return move

        def damage(xp, carry):
            at = lambda ref, dx, dy: ref[xp + dx, a + dy : a + dy + n]
            energy = strain_energy(at, state.at[1], lambda f, v: None, first, last)
            renewed = renew(
                at,
                crack_pad,
                energy,
                at(tough_pad, 0, 0),
                at(crack_pad, 0, 0) > 0.5,
                first,
                last,
            )
            state[1, 3, xp, a : a + n] = jnp.where(
                jnp.logical_and(row_inside, inside_plane(xp)), renewed, 0.0
            )
            return carry

        return stiffen, mover, damage

    def open_sweep():
        def inward(skip, body, carry, most):
            n = nx - 2 * skip
            return lax.fori_loop(HX + skip, HX + nx - skip, body, carry, unroll=part(n, most))

        def outward(far, n, body, carry):
            def both(i, carry):
                carry = body(HX - far + i, carry)
                return body(HX + nx + far - n + i, carry)

            return lax.fori_loop(0, n, both, carry, unroll=True)

        def pair(one, two):
            def body(xp, carry):
                return one(xp, carry[0]), two(xp, carry[1])

            return body

        blank = lambda n: jnp.zeros((n, nz), jnp.float32)
        fold = lambda v: jnp.sum(v, axis=0, keepdims=True)

        stiffen, mover, damage = open_stages(0, ny)
        inward(1, stiffen, 0, 14)
        inside = inward(2, mover(2, ny - 2), blank(ny), 12)
        inward(3, damage, 0, 5)

        low = open_stages(4, 8)
        high = open_stages(4 - ny, 8)
        unpack_y()
        inward(1, pair(low[0], high[0]), (0, 0), 14)
        unpack_y_clamp()
        rims = inward(
            2, pair(low[1](0, 2), high[1](ny - 2, ny)), (blank(8), blank(8)), 12
        )
        unpack_y_tough()
        inward(3, pair(low[2], high[2]), (0, 0), 5)
        stiffen1, mover1 = stages(1)
        move1 = mover1(OY, ny)
        inward(3, stiffen1, 0, 10)
        own = inward(4, move1, blank(ny), 8)

        stiffen, mover, damage = open_stages(4, deep)
        unpack_a()
        outward(2, 3, stiffen, 0)
        ends = outward(0, 2, mover(0, ny), blank(deep))
        outward(1, 1, mover(0, 0), blank(deep))
        r.sums[me, 0:1] = fold(inside) + fold(rims[0] + rims[1]) + fold(ends)
        outward(0, 3, damage, 0)
        outward(0, 3, stiffen1, 0)
        own = outward(-1, 3, move1, own)

        unpack_b()
        outward(3, 1, stiffen, 0)
        outward(2, 1, mover(0, 0), blank(deep))
        outward(1, 1, damage, 0)
        outward(1, 1, stiffen1, 0)
        own = outward(0, 1, move1, own)

        def finish():
            unpack_c()
            outward(4, 1, stiffen, 0)
            outward(3, 1, mover(0, 0), blank(deep))
            outward(2, 1, damage, 0)
            outward(2, 1, stiffen1, 0)

        return own, finish

    def send_sums():
        for k in range(further):
            pl.semaphore_wait(r.reach.at[k], near_count)
            if k + 1 < further:
                greet(r.reach.at[k + 1])
        for k, peer in enumerate(peers):
            pltpu.make_async_remote_copy(
                src_ref=r.sums.at[me],
                dst_ref=r.sums.at[me],
                send_sem=r.sum_send.at[k],
                recv_sem=r.sum_recv.at[me],
                device_id=peer,
                device_id_type=MESH,
            ).start()

    def stages(rnd):
        p = rnd % 2
        q = 1 - p
        shape = (wide, nz)
        first, last = lanes(shape, 0), lanes(shape, nz - 1)
        row_inside = inside_rows(shape, 2)
        a = OY - 2

        def stiffen(xp, carry):
            half = 0.5 * (jnp.square(1.0 - state[p, 3, xp, a : a + wide]) + stiff_floor)
            stiff[xp, a : a + wide] = half
            up, down = beside(state[p, 2, xp, a : a + wide], 0.0, first, last)
            div = (
                (state[p, 0, xp + 1, a : a + wide] - state[p, 0, xp - 1, a : a + wide])
                + (state[p, 1, xp, a + 1 : a + 1 + wide] - state[p, 1, xp, a - 1 : a - 1 + wide])
                + (up - down)
            )
            flow[xp, a : a + wide] = jnp.where(
                jnp.logical_and(row_inside, inside_plane(xp)), half * div, 0.0
            )
            return carry

        def mover(b, n):
            shape = (n, nz)
            first, last = lanes(shape, 0), lanes(shape, nz - 1)

            def move(xp, total):
                at = lambda ref, dx, dy: ref[xp + dx, b + dy : b + dy + n]
                pairs, weights, faces, grads = elastic(at, first, last)
                load = at(held, 0, 0)
                pin = at(clamped, 0, 0) + load > 0.5
                squares = None
                for f in range(3):
                    here, spread = laplace(at, state.at[p, f], faces, weights, first, last)
                    res = spread + grads[f]
                    moved = here + relax_weight * res / (weights + pairs[f])
                    state[q, f, xp, b : b + n] = jnp.where(pin, load * vector[f], moved)
                    square = res * res
                    squares = square if squares is None else squares + square
                return total + jnp.where(pin, 0.0, squares)

            return move

        return stiffen, mover

    def sweep(rnd, total):
        p = rnd % 2
        q = 1 - p
        done = rnd == sections - 1
        tough = r.tough_in.at[rnd - 1]

        stiffen, mover = stages(rnd)
        if rnd > 1:
            lax.fori_loop(HX - 2, HX + nx + 2, stiffen, 0, unroll=part(nx + 4, 10))
            total = lax.fori_loop(
                HX, HX + nx, mover(OY, ny), jnp.zeros((ny, nz), jnp.float32), unroll=part(nx, 8)
            )
        add_up(rnd, total)
        if done:
            send_sums()
        if rnd == 1:
            finish_open()
        none = jnp.zeros((8, nz), jnp.float32)

        def edges(xp, carry):
            mover(OY - 4, 8)(xp, none)
            mover(OY + ny - 3, 8)(xp, none)
            return carry

        lax.fori_loop(HX, HX + nx, edges, 0, unroll=part(nx, 8))
        ends = mover(OY, ny)
        ends(HX - 1, jnp.zeros((ny, nz), jnp.float32))
        ends(HX + nx, jnp.zeros((ny, nz), jnp.float32))
        par = rnd % 2
        mid = pl.ds(OY, ny)
        if not done:
            for f in range(3):
                r.pack_u[0, :, 2 * f : 2 * f + 2] = state[q, f, planes, OY : OY + 2]
                r.pack_u[1, :, 2 * f : 2 * f + 2] = state[q, f, planes, OY + ny - 2 : OY + ny]
            r.pack_u[0, :, 6:7] = state[q, 1, planes, OY + 2 : OY + 3]
            r.pack_u[1, :, 6:7] = state[q, 1, planes, OY + ny - 3 : OY + ny - 2]
            shift = Exchange(r.u_send, r.u_recv.at[par])
            for s in range(2):
                shift.add(
                    x_dev(s),
                    state.at[q, pl.ds(0, 3), pl.ds(HX if s == 0 else HX + nx - 2, 2), mid],
                    r.in_u_x.at[par, 1 - s],
                    r.in_u_x.at[par, s],
                    (1 - s),
                    s,
                )
                shift.add(
                    x_dev(s),
                    state.at[q, 0, HX + 2 if s == 0 else HX + nx - 3, mid],
                    r.in_u_x3.at[par, 1 - s],
                    r.in_u_x3.at[par, s],
                    2 + (1 - s),
                    2 + s,
                )
            for s in range(2):
                shift.add(
                    y_dev(s),
                    r.pack_u.at[s],
                    r.in_u_y.at[par, 1 - s],
                    r.in_u_y.at[par, s],
                    4 + (1 - s),
                    4 + s,
                )
            for sx in range(2):
                for sy in range(2):
                    shift.add(
                        c_dev(sx, sy),
                        r.pack_u.at[sy, pl.ds(0 if sx == 0 else nx - 2, 2)],
                        r.in_u_c.at[par, (1 - sx) * 2 + 1 - sy],
                        r.in_u_c.at[par, sx * 2 + sy],
                        6 + (1 - sx) * 2 + 1 - sy,
                        6 + sx * 2 + sy,
                    )
            shift.start()

        tough_copies[rnd - 1].wait_recv()

        shape = (ny, nz)
        first, last = lanes(shape, 0), lanes(shape, nz - 1)

        def damage(x, carry):
            xp = x + HX
            at = lambda ref, dx, dy: ref[xp + dx, OY + dy : OY + dy + ny]

            def keep(f, here):
                if done:
                    disp_refs[f][x] = here

            energy = strain_energy(at, state.at[q], keep, first, last)
            renewed = renew(
                at, state.at[p, 3], energy, tough[x], crack_ref[x] > 0, first, last
            )
            if done:
                r.dam_ref[x] = renewed
            else:
                state[q, 3, xp, inner] = renewed
            return carry

        lax.fori_loop(0, nx, damage, 0, unroll=part(nx, 8))
        if done:
            return

        r.pack_d[0] = state[q, 3, planes, OY : OY + 2]
        r.pack_d[1] = state[q, 3, planes, OY + ny - 2 : OY + ny]
        crack = Exchange(r.d_send, r.d_recv.at[par])
        for s in range(2):
            crack.add(
                x_dev(s),
                state.at[q, 3, pl.ds(HX if s == 0 else HX + nx - 2, 2), mid],
                r.in_d_x.at[par, 1 - s],
                r.in_d_x.at[par, s],
                1 - s,
                s,
            )
        for s in range(2):
            crack.add(
                y_dev(s),
                r.pack_d.at[s],
                r.in_d_y.at[par, 1 - s],
                r.in_d_y.at[par, s],
                2 + 1 - s,
                2 + s,
            )
        for sx in range(2):
            for sy in range(2):
                crack.add(
                    c_dev(sx, sy),
                    r.pack_d.at[sy, pl.ds(0 if sx == 0 else nx - 1, 1)],
                    r.in_d_c.at[par, (1 - sx) * 2 + 1 - sy],
                    r.in_d_c.at[par, sx * 2 + sy],
                    4 + (1 - sx) * 2 + 1 - sy,
                    4 + sx * 2 + sy,
                )
        crack.start()
        shift.finish()
        third_x = (HX - 3, HX + nx + 2)
        third_y = (slice(OY - 3, OY - 2), slice(OY + ny + 2, OY + ny + 3))
        for s in range(2):

            @pl.when(there["gx"][s])
            def _(s=s):
                state[q, 0:3, x_out(s, 2), inner] = r.in_u_x[par, s]
                state[q, 0, third_x[s], inner] = r.in_u_x3[par, s]

            @pl.when(there["gy"][s])
            def _(s=s):
                for f in range(3):
                    state[q, f, planes, y_out(s, 2)] = r.in_u_y[par, s, :, 2 * f : 2 * f + 2]
                state[q, 1, planes, third_y[s]] = r.in_u_y[par, s, :, 6:7]

        for sx in range(2):
            for sy in range(2):

                @pl.when(c_dev(sx, sy)[0])
                def _(sx=sx, sy=sy):
                    for f in range(3):
                        state[q, f, x_out(sx, 2), y_out(sy, 2)] = r.in_u_c[
                            par, sx * 2 + sy, :, 2 * f : 2 * f + 2
                        ]

        crack.finish()
        for s in range(2):

            @pl.when(there["gx"][s])
            def _(s=s):
                state[q, 3, x_out(s, 2), inner] = r.in_d_x[par, s]

            @pl.when(there["gy"][s])
            def _(s=s):
                state[q, 3, planes, y_out(s, 2)] = r.in_d_y[par, s]

        for sx in range(2):
            for sy in range(2):

                @pl.when(c_dev(sx, sy)[0])
                def _(sx=sx, sy=sy):
                    state[q, 3, x_out(sx, 1), y_out(sy, 2)] = r.in_d_c[par, sx * 2 + sy]

    total, finish_open = open_sweep()
    for rnd in range(1, sections):
        sweep(rnd, total)

    cells = 3.0 * nx * ngx * ny * ngy * nz
    beside_y.sent()
    part_a.sent()
    part_b.sent()
    part_c.sent()
    for copy in tough_copies:
        copy.wait_send()
    for k, peer in enumerate(peers):
        other = peer["gx"] * ngy + peer["gy"]
        pltpu.make_async_remote_copy(
            src_ref=r.sums.at[me],
            dst_ref=r.sums.at[other],
            send_sem=r.sum_send.at[k],
            recv_sem=r.sum_recv.at[other],
            device_id=peer,
            device_id_type=MESH,
        ).wait()
    total = r.sums[0]
    for k in range(1, group):
        total = total + r.sums[k]
    entries = jnp.sqrt(jnp.sum(total, axis=1, keepdims=True) / cells)
    column = lax.broadcasted_iota(jnp.int32, (1, sections), 1)
    norms = jnp.zeros((1, sections), jnp.float32)
    for rnd in range(sections):
        norms = jnp.where(
            column == lax.rem(sec + rnd, sections), entries[rnd : rnd + 1], norms
        )
    r.norm_ref[...] = norms


def put_out(
    first_ref, second_ref, third_ref, dam_ref, norm_ref, disp_hbm, dam_hbm, norm_out, sems
):
    copies = [
        pltpu.make_async_copy(ref, disp_hbm.at[0, f], sems.at[f])
        for f, ref in enumerate((first_ref, second_ref, third_ref))
    ]
    copies.append(pltpu.make_async_copy(dam_ref, dam_hbm.at[0], sems.at[3]))
    for copy in copies:
        copy.start()
    norm_out[...] = norm_ref[...]
    for copy in copies:
        copy.wait()


def on_device(sizes, load_index, load_table, toughness, clamp_mask, load_mask, crack_mask):
    sections, ngx, ngy = sizes
    nx, ny, nz = clamp_mask.shape
    assert load_index.shape == (1,)
    group = ngx * ngy
    f32 = jnp.float32
    padded = (nx + 2 * HX, ny + 2 * OY, nz)
    vmem = pltpu.VMEM
    dma = pltpu.SemaphoreType.DMA
    later = max(sections - 1, 1)
    more = sections > 2
    scratch = {
        "index_ref": pltpu.SMEM(load_index.shape, jnp.int32),
        "table_ref": pltpu.SMEM(load_table.shape[::-1], f32),
        "tough_ref": vmem((1, nx, ny, nz), f32),
        "clamp_ref": vmem((nx, ny, nz), jnp.int32),
        "load_ref": vmem((nx, ny, nz), jnp.int32),
        "crack_ref": vmem((nx, ny, nz), jnp.int32),
        "local": dma((6,)),
        "state": vmem((2, 4) + padded, f32),
        "stiff": vmem(padded, f32),
        "flow": vmem(padded, f32),
        "held": vmem(padded, f32),
        "clamped": vmem(padded, f32),
        "tough_pad": vmem(padded, f32),
        "crack_pad": vmem(padded, f32),
        "tough_in": vmem((later, nx, ny, nz), f32),
        "pack_l": vmem((2, 5 * nx, nz), jnp.int32),
        "pack_f": vmem((2, 3 * nx, nz), jnp.int32),
        "pack_c": vmem((2, nx, 4, nz), jnp.int32),
        "pack_t": vmem((2, nx, 2, nz), f32),
        "pack_k": vmem((4, 16, nz), jnp.int32),
        "pack_kf": vmem((4, 4, nz), jnp.int32),
        "pack_tk": vmem((4, 1, nz), f32),
        "in_a": vmem((2, 6, ny, nz), jnp.int32),
        "in_b": vmem((2, 3, ny, nz), jnp.int32),
        "in_c_x": vmem((2, 3, ny, nz), jnp.int32),
        "in_tx": vmem((2, 2, ny, nz), f32),
        "in_l": vmem((2, 5 * nx, nz), jnp.int32),
        "in_f": vmem((2, 3 * nx, nz), jnp.int32),
        "in_c": vmem((2, nx, 4, nz), jnp.int32),
        "in_ty": vmem((2, nx, 2, nz), f32),
        "in_k": vmem((4, 16, nz), jnp.int32),
        "in_kf": vmem((4, 4, nz), jnp.int32),
        "in_tk": vmem((4, 1, nz), f32),
        "sums": vmem((group, sections, nz), f32),
        "y_send": dma((8,)),
        "y_recv": dma((8,)),
        "a_send": dma((10,)),
        "a_recv": dma((10,)),
        "b_send": dma((16,)),
        "b_recv": dma((16,)),
        "c_send": dma((8,)),
        "c_recv": dma((8,)),
        "reach": pltpu.SemaphoreType.REGULAR((max(max(ngx, ngy) - 3, 1),)),
        "tough_send": dma((later,)),
        "tough_recv": dma((later,)),
        "sum_send": dma((max(group - 1, 1),)),
        "sum_recv": dma((group,)),
    }
    if more:
        scratch |= {
            "pack_u": vmem((2, nx, 8, nz), f32),
            "pack_d": vmem((2, nx, 2, nz), f32),
            "in_u_x": vmem((2, 2, 3, 2, ny, nz), f32),
            "in_u_x3": vmem((2, 2, ny, nz), f32),
            "in_u_y": vmem((2, 2, nx, 8, nz), f32),
            "in_u_c": vmem((2, 4, 2, 8, nz), f32),
            "in_d_x": vmem((2, 2, 2, ny, nz), f32),
            "in_d_y": vmem((2, 2, nx, 2, nz), f32),
            "in_d_c": vmem((2, 4, 1, 2, nz), f32),
            "u_send": dma((10,)),
            "u_recv": dma((2, 10)),
            "d_send": dma((8,)),
            "d_recv": dma((2, 8)),
        }
    ins = ("index_hbm", "table_hbm", "tough_hbm", "clamp_hbm", "load_hbm", "crack_hbm")
    outs = ("first_ref", "second_ref", "third_ref", "dam_ref", "norm_ref")
    names = (*ins, *outs, *scratch)
    block = pl.BlockSpec(memory_space=pltpu.VMEM)
    away = pl.BlockSpec(memory_space=pltpu.HBM)
    results = pl.pallas_call(
        functools.partial(kernel, (sections, ngx, ngy, nx, ny, nz), names),
        out_shape=(
            *[jax.ShapeDtypeStruct((nx, ny, nz), f32)] * 4,
            jax.ShapeDtypeStruct((1, sections), f32),
        ),
        in_specs=[away] * 6,
        out_specs=(block,) * 5,
        scratch_shapes=list(scratch.values()),
        compiler_params=pltpu.CompilerParams(
            collective_id=0, has_side_effects=True, vmem_limit_bytes=56_020_000
        ),
    )(load_index, pltpu.with_memory_space_constraint(load_table.T, pltpu.HBM), toughness, clamp_mask, load_mask, crack_mask)
    return pl.pallas_call(
        put_out,
        out_shape=(
            jax.ShapeDtypeStruct((1, 3, nx, ny, nz), f32),
            jax.ShapeDtypeStruct((1, nx, ny, nz), f32),
            jax.ShapeDtypeStruct((1, sections), f32),
        ),
        in_specs=[block] * 5,
        out_specs=(away, away, block),
        scratch_shapes=[dma((4,))],
        compiler_params=pltpu.CompilerParams(vmem_limit_bytes=1024 * 1024),
    )(*results)


def solution(mesh):
    in_specs = (
        P("section"),
        P(),
        P("section", "gx", "gy", None),
        P("gx", "gy", None),
        P("gx", "gy", None),
        P("gx", "gy", None),
    )
    out_specs = (
        P("section", None, "gx", "gy", None),
        P("section", "gx", "gy", None),
        P("section", None),
    )
    sizes = tuple(mesh.shape[name] for name in ("section", "gx", "gy"))
    return jax.shard_map(
        functools.partial(on_device, sizes),
        mesh=mesh,
        in_specs=in_specs,
        out_specs=out_specs,
        check_vma=False,
    )
```

```python
import functools
import math
import types

import jax
import jax.numpy as jnp
from jax import lax
from jax.experimental import pallas as pl
from jax.experimental.pallas import tpu as pltpu
from jax.sharding import PartitionSpec as P

relax_weight = 0.6
stiff_floor = 0.001
eigen_guard = 1e-08
MESH = pl.DeviceIdType.MESH

HX = 5
OY = 8

ACOS = (
    1.5707963050,
    -0.2145988016,
    0.0889789874,
    -0.0501743046,
    0.0308918810,
    -0.0170881256,
    0.0066700901,
    -0.0012624911,
)


def up8(n):
    return -(-n // 8) * 8


def part(n, most):
    return max(k for k in range(1, most + 1) if n % k == 0)


def root(v):
    return v * lax.rsqrt(jnp.maximum(v, 1.2e-38))


def spectral_energy(xx, yy, zz, xy, xz, yz):
    trace = xx + yy + zz
    mid = trace * (1.0 / 3.0)
    dx = xx - mid
    dy = yy - mid
    dz = zz - mid
    xy2 = xy * xy
    xz2 = xz * xz
    yz2 = yz * yz
    sixth = (dx * dx + dy * dy + dz * dz + 2.0 * (xy2 + xz2 + yz2)) * (1.0 / 6.0)
    twice_radius = 2.0 * root(sixth)
    scale = lax.rsqrt(sixth + eigen_guard)
    det = dx * (dy * dz - yz2) - dz * xy2 - dy * xz2 + 2.0 * (xy * xz * yz)
    ratio = (0.5 * det * scale) * (scale * scale)
    size = jnp.minimum(jnp.abs(ratio), 1.0)
    poly = jnp.full_like(size, ACOS[-1] / 3.0)
    for c in ACOS[-2::-1]:
        poly = poly * size + c / 3.0
    t = root(1.0 - size) * poly
    t2 = t * t
    cos_t = 1.0 + t2 * (-0.5 + t2 * (1.0 / 24.0 + t2 * (-1.0 / 720.0 + t2 * (1.0 / 40320.0))))
    sin_t = t * (1.0 + t2 * (-1.0 / 6.0 + t2 * (1.0 / 120.0 + t2 * (-1.0 / 5040.0))))
    other = 0.5 * cos_t + math.sqrt(0.75) * sin_t
    upper = ratio >= 0.0
    first = jnp.where(upper, cos_t, other)
    last = jnp.where(upper, other, cos_t)
    largest = mid + twice_radius * first
    smallest = mid - twice_radius * last
    between = trace - largest - smallest
    relu = lambda v: jnp.maximum(v, 0.0)
    return (
        0.5 * jnp.square(relu(trace))
        + jnp.square(relu(largest))
        + jnp.square(relu(between))
        + jnp.square(relu(smallest))
    )


def kernel(sizes, names, *refs):
    sections, ngx, ngy, nx, ny, nz = sizes
    r = types.SimpleNamespace(**dict(zip(names, refs)))
    local, state, stiff, flow = r.local, r.state, r.stiff, r.flow
    held, clamped, tough_pad, crack_pad = r.held, r.clamped, r.tough_pad, r.crack_pad
    load_ref, crack_ref, clamp_ref, tough_ref = r.load_ref, r.crack_ref, r.clamp_ref, r.tough_ref
    disp_refs = (r.first_ref, r.second_ref, r.third_ref)
    sec = lax.axis_index("section")
    gx = lax.axis_index("gx")
    gy = lax.axis_index("gy")
    group = ngx * ngy
    me = gx * ngy + gy
    ring = lambda k, n: min(k, n - k)
    offsets = [(i, j) for i in range(ngx) for j in range(ngy) if i or j]
    offsets.sort(key=lambda o: (ring(o[0], ngx) + ring(o[1], ngy), o))
    peers = []
    for i, j in offsets:
        peers.append({"gx": lax.rem(gx + i, ngx), "gy": lax.rem(gy + j, ngy)})

    there = {
        "gx": (gx > 0, gx < ngx - 1),
        "gy": (gy > 0, gy < ngy - 1),
    }
    step = (-1, 1)

    def x_dev(s):
        return there["gx"][s], {"gx": gx + step[s]}

    def y_dev(s):
        return there["gy"][s], {"gy": gy + step[s]}

    def c_dev(sx, sy):
        return (
            jnp.logical_and(there["gx"][sx], there["gy"][sy]),
            {"gx": gx + step[sx], "gy": gy + step[sy]},
        )

    neighbours = [x_dev(s) for s in range(2)] + [y_dev(s) for s in range(2)]
    neighbours += [c_dev(sx, sy) for sx in range(2) for sy in range(2)]
    in_line = lambda name: sum(t.astype(jnp.int32) for t in there[name])
    near_count = (in_line("gx") + 1) * (in_line("gy") + 1) - 1

    def greet(sem):
        for cond, dev in neighbours:

            @pl.when(cond)
            def _(dev=dev):
                pl.semaphore_signal(sem, inc=1, device_id=dev, device_id_type=MESH)

    barrier = pltpu.get_barrier_semaphore()
    greet(barrier)
    for k in range(1, sections):
        pl.semaphore_signal(
            barrier,
            inc=1,
            device_id={"section": lax.rem(sec + k, sections)},
            device_id_type=MESH,
        )

    fetch = [
        pltpu.make_async_copy(src, dst, local.at[n])
        for n, (src, dst) in enumerate(
            (
                (r.load_hbm, load_ref),
                (r.crack_hbm, crack_ref),
                (r.clamp_hbm, clamp_ref),
                (r.tough_hbm, tough_ref),
                (r.index_hbm, r.index_ref),
                (r.table_hbm, r.table_ref),
            )
        )
    ]
    for copy in fetch:
        copy.start()

    class Exchange:
        def __init__(self, send, recv):
            self.items = []
            self.send = send
            self.recv = recv

        def add(self, where, src, dst, mine, out_slot, in_slot):
            cond, dev = where
            n = len(self.items)
            copy = pltpu.make_async_remote_copy(
                src_ref=src,
                dst_ref=dst,
                send_sem=self.send.at[n],
                recv_sem=self.recv.at[out_slot],
                device_id=dev,
                device_id_type=MESH,
            )
            back = pltpu.make_async_remote_copy(
                src_ref=src,
                dst_ref=mine,
                send_sem=self.send.at[n],
                recv_sem=self.recv.at[in_slot],
                device_id=dev,
                device_id_type=MESH,
            )
            self.items.append((cond, copy, back))

        def start(self, begin=0, end=None):
            for cond, copy, _ in self.items[begin:end]:
                pl.when(cond)(copy.start)

        def finish(self):
            for cond, copy, back in self.items:

                @pl.when(cond)
                def _():
                    back.wait_recv()
                    copy.wait_send()

        def received(self, begin=0, end=None):
            for cond, _, back in self.items[begin:end]:
                pl.when(cond)(back.wait_recv)

        def sent(self, begin=0, end=None):
            for cond, copy, _ in self.items[begin:end]:
                pl.when(cond)(copy.wait_send)

    rows = ny + 2 * OY

    def clear(xp, carry):
        zero = jnp.zeros((rows, nz), jnp.float32)
        held[xp] = zero
        crack_pad[xp] = zero
        clamped[xp] = zero + 1.0
        tough_pad[xp] = zero + 1.0
        if sections > 2:
            for p in range(2):
                for f in range(4):
                    state[p, f, xp] = zero
        return carry

    lax.fori_loop(0, nx + 2 * HX, clear, 0)

    for copy in fetch[:3]:
        copy.wait()

    for s in range(2):
        side = lambda n, s=s: slice(0, n) if s == 0 else slice(ny - n, ny)
        r.pack_c[s] = crack_ref[:, side(4)]
        for x in range(nx):
            r.pack_l[s, 5 * x : 5 * x + 5] = load_ref[x, side(5)]
            r.pack_f[s, 3 * x : 3 * x + 3] = clamp_ref[x, side(3)]
    near_corner = (
        (load_ref, held, 1, 4, 0),
        (load_ref, held, 2, 3, 4),
        (load_ref, held, 3, 2, 7),
        (crack_ref, crack_pad, 1, 3, 9),
        (crack_ref, crack_pad, 2, 2, 12),
        (clamp_ref, clamped, 1, 2, 14),
    )
    far_corner = (
        (load_ref, held, 4, 1, 0),
        (crack_ref, crack_pad, 3, 1, 1),
        (clamp_ref, clamped, 2, 1, 2),
    )

    def x_from(s, deep):
        return deep - 1 if s == 0 else nx - deep

    def x_at(s, deep):
        return HX - deep if s == 0 else HX + nx - 1 + deep

    for sx in range(2):
        for sy in range(2):
            for pack, corner in ((r.pack_k, near_corner), (r.pack_kf, far_corner)):
                for ref, _, deep, n, at in corner:
                    first = 0 if sy == 0 else ny - n
                    pack[sx * 2 + sy, at : at + n] = ref[x_from(sx, deep), first : first + n]

    pl.semaphore_wait(barrier, near_count + sections - 1)

    beside_y = Exchange(r.y_send, r.y_recv)
    part_a = Exchange(r.a_send, r.a_recv)
    part_b = Exchange(r.b_send, r.b_recv)
    part_c = Exchange(r.c_send, r.c_recv)
    for ex, ref, buf, deep, width, at, slot in (
        (part_a, load_ref, r.in_a, 3, 3, 0, 0),
        (part_a, crack_ref, r.in_a, 2, 2, 3, 2),
        (part_a, clamp_ref, r.in_a, 1, 1, 5, 4),
        (part_b, load_ref, r.in_b, 4, 1, 0, 0),
        (part_b, crack_ref, r.in_b, 3, 1, 1, 2),
        (part_b, clamp_ref, r.in_b, 2, 1, 2, 4),
        (part_b, tough_ref.at[0], r.in_tx, 1, 1, 0, 6),
        (part_c, load_ref, r.in_c_x, 5, 1, 0, 0),
        (part_c, crack_ref, r.in_c_x, 4, 1, 1, 2),
        (part_c, clamp_ref, r.in_c_x, 3, 1, 2, 4),
        (part_c, tough_ref.at[0], r.in_tx, 2, 1, 1, 6),
    ):
        for s in range(2):
            first = deep - width if s == 0 else nx - deep
            ex.add(
                x_dev(s),
                ref.at[pl.ds(first, width)],
                buf.at[1 - s, pl.ds(at, width)],
                buf.at[s, pl.ds(at, width)],
                slot + 1 - s,
                slot + s,
            )
    for n in range(8):
        s = n % 2
        for pack, buf, slot in (
            (r.pack_c, r.in_c, 0),
            (r.pack_l, r.in_l, 2),
            (r.pack_f, r.in_f, 4),
            (r.pack_t, r.in_ty, 6),
        )[n // 2 : n // 2 + 1]:
            beside_y.add(
                y_dev(s), pack.at[s], buf.at[1 - s], buf.at[s], slot + 1 - s, slot + s
            )
    for sx in range(2):
        for sy in range(2):
            here, away = sx * 2 + sy, (1 - sx) * 2 + 1 - sy
            for ex, pack, buf, slot in (
                (part_a, r.pack_k, r.in_k, 6),
                (part_b, r.pack_kf, r.in_kf, 8),
                (part_b, r.pack_tk, r.in_tk, 12),
            ):
                ex.add(
                    c_dev(sx, sy), pack.at[here], buf.at[away], buf.at[here],
                    slot + away, slot + here,
                )
    beside_y.start(0, 4)
    part_a.start(0, 6)
    beside_y.start(4, 6)
    fetch[3].wait()
    for s in range(2):
        r.pack_t[s] = tough_ref[0, :, 0:2] if s == 0 else tough_ref[0, :, ny - 2 : ny]
    for sx in range(2):
        for sy in range(2):
            row = 0 if sy == 0 else ny - 1
            r.pack_tk[sx * 2 + sy] = tough_ref[0, 0 if sx == 0 else nx - 1, row : row + 1]
    beside_y.start(6)
    part_a.start(6)
    part_b.start()
    part_c.start()
    further = max(ngx, ngy) - 2
    if further > 0:
        greet(r.reach.at[0])
    tough_copies = []
    for k in range(1, sections):
        copy = pltpu.make_async_remote_copy(
            src_ref=tough_ref.at[0],
            dst_ref=r.tough_in.at[k - 1],
            send_sem=r.tough_send.at[k - 1],
            recv_sem=r.tough_recv.at[k - 1],
            device_id={"section": lax.rem(sec + sections - k, sections)},
            device_id_type=MESH,
        )
        copy.start()
        tough_copies.append(copy)

    inner = slice(OY, OY + ny)
    as_float = lambda v: v.astype(jnp.float32)

    def fill(x, carry):
        held[x + HX, inner] = as_float(load_ref[x])
        clamped[x + HX, inner] = as_float(clamp_ref[x])
        crack_pad[x + HX, inner] = as_float(crack_ref[x])
        tough_pad[x + HX, inner] = tough_ref[0, x]
        return carry

    lax.fori_loop(0, nx, fill, 0, unroll=part(nx, 4))

    for copy in fetch[4:]:
        copy.wait()
    case = r.index_ref[0]
    vector = [r.table_ref[f, case] for f in range(3)]

    planes = slice(HX, HX + nx)

    def x_out(s, n):
        return slice(HX - n, HX) if s == 0 else slice(HX + nx, HX + nx + n)

    def y_out(s, n):
        return slice(OY - n, OY) if s == 0 else slice(OY + ny, OY + ny + n)

    def from_y(kind, s, put):
        beside_y.received(2 * kind + s, 2 * kind + s + 1)
        pl.when(there["gy"][s])(put)

    def unpack_corners(corner, buf):
        for sx in range(2):
            for sy in range(2):

                @pl.when(c_dev(sx, sy)[0])
                def _(sx=sx, sy=sy):
                    for _, pad, deep, n, at in corner:
                        pad[x_at(sx, deep), y_out(sy, n)] = as_float(
                            buf[sx * 2 + sy, at : at + n]
                        )

    def unpack_a():
        part_a.received()
        for s in range(2):

            @pl.when(there["gx"][s])
            def _(s=s):
                held[x_out(s, 3), inner] = as_float(r.in_a[s, 0:3])
                crack_pad[x_out(s, 2), inner] = as_float(r.in_a[s, 3:5])
                clamped[x_out(s, 1), inner] = as_float(r.in_a[s, 5:6])

        unpack_corners(near_corner, r.in_k)

    def unpack_far(part, buf, less):
        part.received()
        for s in range(2):

            @pl.when(there["gx"][s])
            def _(s=s):
                held[x_at(s, 5 - less), inner] = as_float(buf[s, 0])
                crack_pad[x_at(s, 4 - less), inner] = as_float(buf[s, 1])
                clamped[x_at(s, 3 - less), inner] = as_float(buf[s, 2])
                tough_pad[x_at(s, 2 - less), inner] = r.in_tx[s, 1 - less]

    def unpack_b():
        unpack_far(part_b, r.in_b, 1)
        unpack_corners(far_corner, r.in_kf)
        for sx in range(2):
            for sy in range(2):

                @pl.when(c_dev(sx, sy)[0])
                def _(sx=sx, sy=sy):
                    tough_pad[x_at(sx, 1), y_out(sy, 1)] = r.in_tk[sx * 2 + sy]

    def unpack_c():
        unpack_far(part_c, r.in_c_x, 0)

    wide = up8(ny + 4)
    deep = up8(ny + 8)

    def lanes(shape, lane):
        return lax.broadcasted_iota(jnp.int32, shape, 1) == lane

    def beside(v, edge, first, last):
        up = jnp.where(last, edge, pltpu.roll(v, nz - 1, 1))
        down = jnp.where(first, edge, pltpu.roll(v, 1, 1))
        return up, down

    def inside_rows(shape, above):
        row = lax.broadcasted_iota(jnp.int32, shape, 0) + (gy * ny - above)
        return jnp.logical_and(row >= 0, row < ny * ngy)

    def inside_plane(xp):
        plane = xp - HX + gx * nx
        return jnp.logical_and(plane >= 0, plane < nx * ngx)

    edge_stiff = 0.5 * (1.0 + stiff_floor)

    def elastic(at, first, last):
        k = at(stiff, 0, 0)
        sides = (
            (at(stiff, 1, 0), at(stiff, -1, 0)),
            (at(stiff, 0, 1), at(stiff, 0, -1)),
            beside(k, edge_stiff, first, last),
        )
        pairs = [s[0] + s[1] for s in sides]
        weights = pairs[0] + pairs[1] + pairs[2] + 6.0 * k
        faces = [(k + s[0], k + s[1]) for s in sides]
        fz = beside(at(flow, 0, 0), 0.0, first, last)
        grads = (
            at(flow, 1, 0) - at(flow, -1, 0),
            at(flow, 0, 1) - at(flow, 0, -1),
            fz[0] - fz[1],
        )
        return pairs, weights, faces, grads

    def laplace(at, ref, faces, weights, first, last):
        here = at(ref, 0, 0)
        uz = beside(here, 0.0, first, last)
        return here, (
            faces[0][0] * at(ref, 1, 0)
            + faces[0][1] * at(ref, -1, 0)
            + faces[1][0] * at(ref, 0, 1)
            + faces[1][1] * at(ref, 0, -1)
            + faces[2][0] * uz[0]
            + faces[2][1] * uz[1]
            - weights * here
        )

    def strain_energy(at, u, keep, first, last):
        grad = []
        for f in range(3):
            here = at(u.at[f], 0, 0)
            uz = beside(here, 0.0, first, last)
            grad.append(
                (
                    at(u.at[f], 1, 0) - at(u.at[f], -1, 0),
                    at(u.at[f], 0, 1) - at(u.at[f], 0, -1),
                    uz[0] - uz[1],
                )
            )
            keep(f, here)
        return 2.0 * spectral_energy(
            0.5 * grad[0][0],
            0.5 * grad[1][1],
            0.5 * grad[2][2],
            0.25 * (grad[0][1] + grad[1][0]),
            0.25 * (grad[0][2] + grad[2][0]),
            0.25 * (grad[1][2] + grad[2][1]),
        )

    def renew(at, d, energy, g, cracked, first, last):
        dz = beside(at(d, 0, 0), 0.0, first, last)
        around = at(d, 1, 0) + at(d, -1, 0) + at(d, 0, 1) + at(d, 0, -1) + dz[0] + dz[1]
        renewed = (energy + g * around) / (7.0 * g + energy)
        return jnp.where(cracked, 1.0, renewed)

    def add_up(rnd, total):
        r.sums[me, rnd : rnd + 1] = jnp.sum(total, axis=0, keepdims=True)

    def open_stages(above, n):
        shape = (n, nz)
        first, last = lanes(shape, 0), lanes(shape, nz - 1)
        row_inside = inside_rows(shape, above)
        row = lax.broadcasted_iota(jnp.int32, shape, 0)
        a = OY - above

        def stiffen(xp, carry):
            half = 0.5 * (jnp.square(1.0 - crack_pad[xp, a : a + n]) + stiff_floor)
            stiff[xp, a : a + n] = half
            up, down = beside(held[xp, a : a + n], 0.0, first, last)
            div = (
                vector[0] * (held[xp + 1, a : a + n] - held[xp - 1, a : a + n])
                + vector[1] * (held[xp, a + 1 : a + 1 + n] - held[xp, a - 1 : a - 1 + n])
                + vector[2] * (up - down)
            )
            flow[xp, a : a + n] = jnp.where(
                jnp.logical_and(row_inside, inside_plane(xp)), half * div, 0.0
            )
            return carry

        def mover(low, high):
            def move(xp, total):
                at = lambda ref, dx, dy: ref[xp + dx, a + dy : a + dy + n]
                pairs, weights, faces, grads = elastic(at, first, last)
                load, spread = laplace(at, held, faces, weights, first, last)
                pin = at(clamped, 0, 0) + load > 0.5
                squares = None
                for f in range(3):
                    res = vector[f] * spread + grads[f]
                    moved = jnp.where(pin, 0.0, relax_weight * res / (weights + pairs[f]))
                    state[1, f, xp, a : a + n] = vector[f] * load + moved
                    square = res * res
                    squares = square if squares is None else squares + square
                if low >= high:
                    return total
                counted = jnp.logical_and(row >= low + above, row < high + above)
                return total + jnp.where(
                    jnp.logical_and(counted, jnp.logical_not(pin)), squares, 0.0
                )

            return move

        def damage(xp, carry):
            at = lambda ref, dx, dy: ref[xp + dx, a + dy : a + dy + n]
            energy = strain_energy(at, state.at[1], lambda f, v: None, first, last)
            renewed = renew(
                at,
                crack_pad,
                energy,
                at(tough_pad, 0, 0),
                at(crack_pad, 0, 0) > 0.5,
                first,
                last,
            )
            state[1, 3, xp, a : a + n] = jnp.where(
                jnp.logical_and(row_inside, inside_plane(xp)), renewed, 0.0
            )
            return carry

        return stiffen, mover, damage

    def open_sweep():
        def inward(skip, body, carry, most):
            n = nx - 2 * skip
            return lax.fori_loop(HX + skip, HX + nx - skip, body, carry, unroll=part(n, most))

        def outward(far, n, body, carry):
            def both(i, carry):
                carry = body(HX - far + i, carry)
                return body(HX + nx + far - n + i, carry)

            return lax.fori_loop(0, n, both, carry, unroll=True)

        blank = lambda n: jnp.zeros((n, nz), jnp.float32)
        fold = lambda v: jnp.sum(v, axis=0, keepdims=True)

        stiffen, mover, damage = open_stages(0, ny)
        inward(1, stiffen, 0, 14)
        inside = inward(2, mover(2, ny - 2), blank(ny), 12)
        inward(3, damage, 0, 5)

        if further > 1:
            pl.semaphore_wait(r.reach.at[0], near_count)
            greet(r.reach.at[1])

        def rim(s):
            above = (4, 4 - ny)[s]
            stiffen, mover, damage = open_stages(above, 8)

            def put_crack():
                crack_pad[planes, y_out(s, 4)] = as_float(r.in_c[s])

            def put_load():
                for x in range(nx):
                    held[HX + x, y_out(s, 5)] = as_float(r.in_l[s, 5 * x : 5 * x + 5])

            def put_clamp():
                for x in range(nx):
                    clamped[HX + x, y_out(s, 3)] = as_float(r.in_f[s, 3 * x : 3 * x + 3])

            def put_tough():
                tough_pad[planes, y_out(s, 2)] = r.in_ty[s]

            from_y(0, s, put_crack)
            from_y(1, s, put_load)
            inward(1, stiffen, 0, 14)
            from_y(2, s, put_clamp)
            counted = (0, 2) if s == 0 else (ny - 2, ny)
            r.rims[s] = inward(2, mover(*counted), blank(8), 12)
            from_y(3, s, put_tough)
            inward(3, damage, 0, 10)

        odd = lax.rem(gy, 2) == 1

        @pl.when(odd)
        def _():
            rim(0)
            rim(1)

        @pl.when(jnp.logical_not(odd))
        def _():
            rim(1)
            rim(0)

        stiffen1, mover1 = stages(1)
        move1 = mover1(OY, ny)
        inward(3, stiffen1, 0, 10)
        own = inward(4, move1, blank(ny), 8)

        stiffen, mover, damage = open_stages(4, deep)
        unpack_a()
        outward(2, 3, stiffen, 0)
        ends = outward(0, 2, mover(0, ny), blank(deep))
        outward(1, 1, mover(0, 0), blank(deep))
        r.sums[me, 0:1] = fold(inside) + fold(r.rims[0] + r.rims[1]) + fold(ends)
        outward(0, 3, damage, 0)
        outward(0, 3, stiffen1, 0)
        own = outward(-1, 3, move1, own)

        unpack_b()
        outward(3, 1, stiffen, 0)
        outward(2, 1, mover(0, 0), blank(deep))
        outward(1, 1, damage, 0)
        outward(1, 1, stiffen1, 0)
        own = outward(0, 1, move1, own)

        def finish():
            unpack_c()
            outward(4, 1, stiffen, 0)
            outward(3, 1, mover(0, 0), blank(deep))
            outward(2, 1, damage, 0)
            outward(2, 1, stiffen1, 0)

        return own, finish

    def send_sums():
        for k in range(1 if further > 1 else 0, further):
            pl.semaphore_wait(r.reach.at[k], near_count)
            if k + 1 < further:
                greet(r.reach.at[k + 1])
        for k, peer in enumerate(peers):
            pltpu.make_async_remote_copy(
                src_ref=r.sums.at[me],
                dst_ref=r.sums.at[me],
                send_sem=r.sum_send.at[k],
                recv_sem=r.sum_recv.at[me],
                device_id=peer,
                device_id_type=MESH,
            ).start()

    def stages(rnd):
        p = rnd % 2
        q = 1 - p
        shape = (wide, nz)
        first, last = lanes(shape, 0), lanes(shape, nz - 1)
        row_inside = inside_rows(shape, 2)
        a = OY - 2

        def stiffen(xp, carry):
            half = 0.5 * (jnp.square(1.0 - state[p, 3, xp, a : a + wide]) + stiff_floor)
            stiff[xp, a : a + wide] = half
            up, down = beside(state[p, 2, xp, a : a + wide], 0.0, first, last)
            div = (
                (state[p, 0, xp + 1, a : a + wide] - state[p, 0, xp - 1, a : a + wide])
                + (state[p, 1, xp, a + 1 : a + 1 + wide] - state[p, 1, xp, a - 1 : a - 1 + wide])
                + (up - down)
            )
            flow[xp, a : a + wide] = jnp.where(
                jnp.logical_and(row_inside, inside_plane(xp)), half * div, 0.0
            )
            return carry

        def mover(b, n):
            shape = (n, nz)
            first, last = lanes(shape, 0), lanes(shape, nz - 1)

            def move(xp, total):
                at = lambda ref, dx, dy: ref[xp + dx, b + dy : b + dy + n]
                pairs, weights, faces, grads = elastic(at, first, last)
                load = at(held, 0, 0)
                pin = at(clamped, 0, 0) + load > 0.5
                squares = None
                for f in range(3):
                    here, spread = laplace(at, state.at[p, f], faces, weights, first, last)
                    res = spread + grads[f]
                    moved = here + relax_weight * res / (weights + pairs[f])
                    state[q, f, xp, b : b + n] = jnp.where(pin, load * vector[f], moved)
                    square = res * res
                    squares = square if squares is None else squares + square
                return total + jnp.where(pin, 0.0, squares)

            return move

        return stiffen, mover

    def sweep(rnd, total):
        p = rnd % 2
        q = 1 - p
        done = rnd == sections - 1
        tough = r.tough_in.at[rnd - 1]

        stiffen, mover = stages(rnd)
        if rnd > 1:
            lax.fori_loop(HX - 2, HX + nx + 2, stiffen, 0, unroll=part(nx + 4, 10))
            total = lax.fori_loop(
                HX, HX + nx, mover(OY, ny), jnp.zeros((ny, nz), jnp.float32), unroll=part(nx, 8)
            )
        add_up(rnd, total)
        if done:
            send_sums()
        if rnd == 1:
            finish_open()
        none = jnp.zeros((8, nz), jnp.float32)

        def edges(xp, carry):
            mover(OY - 4, 8)(xp, none)
            mover(OY + ny - 3, 8)(xp, none)
            return carry

        lax.fori_loop(HX, HX + nx, edges, 0, unroll=part(nx, 8))
        ends = mover(OY, ny)
        ends(HX - 1, jnp.zeros((ny, nz), jnp.float32))
        ends(HX + nx, jnp.zeros((ny, nz), jnp.float32))
        par = rnd % 2
        mid = pl.ds(OY, ny)
        if not done:
            for f in range(3):
                r.pack_u[0, :, 2 * f : 2 * f + 2] = state[q, f, planes, OY : OY + 2]
                r.pack_u[1, :, 2 * f : 2 * f + 2] = state[q, f, planes, OY + ny - 2 : OY + ny]
            r.pack_u[0, :, 6:7] = state[q, 1, planes, OY + 2 : OY + 3]
            r.pack_u[1, :, 6:7] = state[q, 1, planes, OY + ny - 3 : OY + ny - 2]
            shift = Exchange(r.u_send, r.u_recv.at[par])
            for s in range(2):
                shift.add(
                    x_dev(s),
                    state.at[q, pl.ds(0, 3), pl.ds(HX if s == 0 else HX + nx - 2, 2), mid],
                    r.in_u_x.at[par, 1 - s],
                    r.in_u_x.at[par, s],
                    (1 - s),
                    s,
                )
                shift.add(
                    x_dev(s),
                    state.at[q, 0, HX + 2 if s == 0 else HX + nx - 3, mid],
                    r.in_u_x3.at[par, 1 - s],
                    r.in_u_x3.at[par, s],
                    2 + (1 - s),
                    2 + s,
                )
            for s in range(2):
                shift.add(
                    y_dev(s),
                    r.pack_u.at[s],
                    r.in_u_y.at[par, 1 - s],
                    r.in_u_y.at[par, s],
                    4 + (1 - s),
                    4 + s,
                )
            for sx in range(2):
                for sy in range(2):
                    shift.add(
                        c_dev(sx, sy),
                        r.pack_u.at[sy, pl.ds(0 if sx == 0 else nx - 2, 2)],
                        r.in_u_c.at[par, (1 - sx) * 2 + 1 - sy],
                        r.in_u_c.at[par, sx * 2 + sy],
                        6 + (1 - sx) * 2 + 1 - sy,
                        6 + sx * 2 + sy,
                    )
            shift.start()

        tough_copies[rnd - 1].wait_recv()

        shape = (ny, nz)
        first, last = lanes(shape, 0), lanes(shape, nz - 1)

        def damage(x, carry):
            xp = x + HX
            at = lambda ref, dx, dy: ref[xp + dx, OY + dy : OY + dy + ny]

            def keep(f, here):
                if done:
                    disp_refs[f][x] = here

            energy = strain_energy(at, state.at[q], keep, first, last)
            renewed = renew(
                at, state.at[p, 3], energy, tough[x], crack_ref[x] > 0, first, last
            )
            if done:
                r.dam_ref[x] = renewed
            else:
                state[q, 3, xp, inner] = renewed
            return carry

        lax.fori_loop(0, nx, damage, 0, unroll=part(nx, 8))
        if done:
            return

        r.pack_d[0] = state[q, 3, planes, OY : OY + 2]
        r.pack_d[1] = state[q, 3, planes, OY + ny - 2 : OY + ny]
        crack = Exchange(r.d_send, r.d_recv.at[par])
        for s in range(2):
            crack.add(
                x_dev(s),
                state.at[q, 3, pl.ds(HX if s == 0 else HX + nx - 2, 2), mid],
                r.in_d_x.at[par, 1 - s],
                r.in_d_x.at[par, s],
                1 - s,
                s,
            )
        for s in range(2):
            crack.add(
                y_dev(s),
                r.pack_d.at[s],
                r.in_d_y.at[par, 1 - s],
                r.in_d_y.at[par, s],
                2 + 1 - s,
                2 + s,
            )
        for sx in range(2):
            for sy in range(2):
                crack.add(
                    c_dev(sx, sy),
                    r.pack_d.at[sy, pl.ds(0 if sx == 0 else nx - 1, 1)],
                    r.in_d_c.at[par, (1 - sx) * 2 + 1 - sy],
                    r.in_d_c.at[par, sx * 2 + sy],
                    4 + (1 - sx) * 2 + 1 - sy,
                    4 + sx * 2 + sy,
                )
        crack.start()
        shift.finish()
        third_x = (HX - 3, HX + nx + 2)
        third_y = (slice(OY - 3, OY - 2), slice(OY + ny + 2, OY + ny + 3))
        for s in range(2):

            @pl.when(there["gx"][s])
            def _(s=s):
                state[q, 0:3, x_out(s, 2), inner] = r.in_u_x[par, s]
                state[q, 0, third_x[s], inner] = r.in_u_x3[par, s]

            @pl.when(there["gy"][s])
            def _(s=s):
                for f in range(3):
                    state[q, f, planes, y_out(s, 2)] = r.in_u_y[par, s, :, 2 * f : 2 * f + 2]
                state[q, 1, planes, third_y[s]] = r.in_u_y[par, s, :, 6:7]

        for sx in range(2):
            for sy in range(2):

                @pl.when(c_dev(sx, sy)[0])
                def _(sx=sx, sy=sy):
                    for f in range(3):
                        state[q, f, x_out(sx, 2), y_out(sy, 2)] = r.in_u_c[
                            par, sx * 2 + sy, :, 2 * f : 2 * f + 2
                        ]

        crack.finish()
        for s in range(2):

            @pl.when(there["gx"][s])
            def _(s=s):
                state[q, 3, x_out(s, 2), inner] = r.in_d_x[par, s]

            @pl.when(there["gy"][s])
            def _(s=s):
                state[q, 3, planes, y_out(s, 2)] = r.in_d_y[par, s]

        for sx in range(2):
            for sy in range(2):

                @pl.when(c_dev(sx, sy)[0])
                def _(sx=sx, sy=sy):
                    state[q, 3, x_out(sx, 1), y_out(sy, 2)] = r.in_d_c[par, sx * 2 + sy]

    total, finish_open = open_sweep()
    for rnd in range(1, sections):
        sweep(rnd, total)

    cells = 3.0 * nx * ngx * ny * ngy * nz
    beside_y.sent()
    part_a.sent()
    part_b.sent()
    part_c.sent()
    for copy in tough_copies:
        copy.wait_send()
    for k, peer in enumerate(peers):
        other = peer["gx"] * ngy + peer["gy"]
        pltpu.make_async_remote_copy(
            src_ref=r.sums.at[me],
            dst_ref=r.sums.at[other],
            send_sem=r.sum_send.at[k],
            recv_sem=r.sum_recv.at[other],
            device_id=peer,
            device_id_type=MESH,
        ).wait()
    total = r.sums[0]
    for k in range(1, group):
        total = total + r.sums[k]
    entries = jnp.sqrt(jnp.sum(total, axis=1, keepdims=True) / cells)
    column = lax.broadcasted_iota(jnp.int32, (1, sections), 1)
    norms = jnp.zeros((1, sections), jnp.float32)
    for rnd in range(sections):
        norms = jnp.where(
            column == lax.rem(sec + rnd, sections), entries[rnd : rnd + 1], norms
        )
    r.norm_ref[...] = norms


def put_out(
    first_ref, second_ref, third_ref, dam_ref, norm_ref, disp_hbm, dam_hbm, norm_out, sems
):
    copies = [
        pltpu.make_async_copy(ref, disp_hbm.at[0, f], sems.at[f])
        for f, ref in enumerate((first_ref, second_ref, third_ref))
    ]
    copies.append(pltpu.make_async_copy(dam_ref, dam_hbm.at[0], sems.at[3]))
    for copy in copies:
        copy.start()
    norm_out[...] = norm_ref[...]
    for copy in copies:
        copy.wait()


def on_device(sizes, load_index, load_table, toughness, clamp_mask, load_mask, crack_mask):
    sections, ngx, ngy = sizes
    nx, ny, nz = clamp_mask.shape
    assert load_index.shape == (1,)
    group = ngx * ngy
    f32 = jnp.float32
    padded = (nx + 2 * HX, ny + 2 * OY, nz)
    vmem = pltpu.VMEM
    dma = pltpu.SemaphoreType.DMA
    later = max(sections - 1, 1)
    more = sections > 2
    scratch = {
        "index_ref": pltpu.SMEM(load_index.shape, jnp.int32),
        "table_ref": pltpu.SMEM(load_table.shape[::-1], f32),
        "tough_ref": vmem((1, nx, ny, nz), f32),
        "clamp_ref": vmem((nx, ny, nz), jnp.int32),
        "load_ref": vmem((nx, ny, nz), jnp.int32),
        "crack_ref": vmem((nx, ny, nz), jnp.int32),
        "local": dma((6,)),
        "state": vmem((2, 4) + padded, f32),
        "stiff": vmem(padded, f32),
        "flow": vmem(padded, f32),
        "held": vmem(padded, f32),
        "clamped": vmem(padded, f32),
        "tough_pad": vmem(padded, f32),
        "crack_pad": vmem(padded, f32),
        "tough_in": vmem((later, nx, ny, nz), f32),
        "pack_l": vmem((2, 5 * nx, nz), jnp.int32),
        "pack_f": vmem((2, 3 * nx, nz), jnp.int32),
        "pack_c": vmem((2, nx, 4, nz), jnp.int32),
        "pack_t": vmem((2, nx, 2, nz), f32),
        "pack_k": vmem((4, 16, nz), jnp.int32),
        "pack_kf": vmem((4, 4, nz), jnp.int32),
        "pack_tk": vmem((4, 1, nz), f32),
        "in_a": vmem((2, 6, ny, nz), jnp.int32),
        "in_b": vmem((2, 3, ny, nz), jnp.int32),
        "in_c_x": vmem((2, 3, ny, nz), jnp.int32),
        "in_tx": vmem((2, 2, ny, nz), f32),
        "in_l": vmem((2, 5 * nx, nz), jnp.int32),
        "in_f": vmem((2, 3 * nx, nz), jnp.int32),
        "in_c": vmem((2, nx, 4, nz), jnp.int32),
        "in_ty": vmem((2, nx, 2, nz), f32),
        "in_k": vmem((4, 16, nz), jnp.int32),
        "in_kf": vmem((4, 4, nz), jnp.int32),
        "in_tk": vmem((4, 1, nz), f32),
        "rims": vmem((2, 8, nz), f32),
        "sums": vmem((group, sections, nz), f32),
        "y_send": dma((8,)),
        "y_recv": dma((8,)),
        "a_send": dma((10,)),
        "a_recv": dma((10,)),
        "b_send": dma((16,)),
        "b_recv": dma((16,)),
        "c_send": dma((8,)),
        "c_recv": dma((8,)),
        "reach": pltpu.SemaphoreType.REGULAR((max(max(ngx, ngy) - 2, 1),)),
        "tough_send": dma((later,)),
        "tough_recv": dma((later,)),
        "sum_send": dma((max(group - 1, 1),)),
        "sum_recv": dma((group,)),
    }
    if more:
        scratch |= {
            "pack_u": vmem((2, nx, 8, nz), f32),
            "pack_d": vmem((2, nx, 2, nz), f32),
            "in_u_x": vmem((2, 2, 3, 2, ny, nz), f32),
            "in_u_x3": vmem((2, 2, ny, nz), f32),
            "in_u_y": vmem((2, 2, nx, 8, nz), f32),
            "in_u_c": vmem((2, 4, 2, 8, nz), f32),
            "in_d_x": vmem((2, 2, 2, ny, nz), f32),
            "in_d_y": vmem((2, 2, nx, 2, nz), f32),
            "in_d_c": vmem((2, 4, 1, 2, nz), f32),
            "u_send": dma((10,)),
            "u_recv": dma((2, 10)),
            "d_send": dma((8,)),
            "d_recv": dma((2, 8)),
        }
    ins = ("index_hbm", "table_hbm", "tough_hbm", "clamp_hbm", "load_hbm", "crack_hbm")
    outs = ("first_ref", "second_ref", "third_ref", "dam_ref", "norm_ref")
    names = (*ins, *outs, *scratch)
    block = pl.BlockSpec(memory_space=pltpu.VMEM)
    away = pl.BlockSpec(memory_space=pltpu.HBM)
    results = pl.pallas_call(
        functools.partial(kernel, (sections, ngx, ngy, nx, ny, nz), names),
        out_shape=(
            *[jax.ShapeDtypeStruct((nx, ny, nz), f32)] * 4,
            jax.ShapeDtypeStruct((1, sections), f32),
        ),
        in_specs=[away] * 6,
        out_specs=(block,) * 5,
        scratch_shapes=list(scratch.values()),
        compiler_params=pltpu.CompilerParams(
            collective_id=0, has_side_effects=True, vmem_limit_bytes=56_020_000
        ),
    )(load_index, pltpu.with_memory_space_constraint(load_table.T, pltpu.HBM), toughness, clamp_mask, load_mask, crack_mask)
    return pl.pallas_call(
        put_out,
        out_shape=(
            jax.ShapeDtypeStruct((1, 3, nx, ny, nz), f32),
            jax.ShapeDtypeStruct((1, nx, ny, nz), f32),
            jax.ShapeDtypeStruct((1, sections), f32),
        ),
        in_specs=[block] * 5,
        out_specs=(away, away, block),
        scratch_shapes=[dma((4,))],
        compiler_params=pltpu.CompilerParams(vmem_limit_bytes=1024 * 1024),
    )(*results)


def solution(mesh):
    in_specs = (
        P("section"),
        P(),
        P("section", "gx", "gy", None),
        P("gx", "gy", None),
        P("gx", "gy", None),
        P("gx", "gy", None),
    )
    out_specs = (
        P("section", None, "gx", "gy", None),
        P("section", "gx", "gy", None),
        P("section", None),
    )
    sizes = tuple(mesh.shape[name] for name in ("section", "gx", "gy"))
    return jax.shard_map(
        functools.partial(on_device, sizes),
        mesh=mesh,
        in_specs=in_specs,
        out_specs=out_specs,
        check_vma=False,
    )
```

```python
import functools
import math
import types

import jax
import jax.numpy as jnp
from jax import lax
from jax.experimental import pallas as pl
from jax.experimental.pallas import tpu as pltpu
from jax.sharding import PartitionSpec as P

relax_weight = 0.6
stiff_floor = 0.001
eigen_guard = 1e-08
MESH = pl.DeviceIdType.MESH

HX = 5
OY = 8

ACOS = (
    1.5707963050,
    -0.2145988016,
    0.0889789874,
    -0.0501743046,
    0.0308918810,
    -0.0170881256,
    0.0066700901,
    -0.0012624911,
)


def up8(n):
    return -(-n // 8) * 8


def part(n, most):
    return max(k for k in range(1, most + 1) if n % k == 0)


def root(v):
    return v * lax.rsqrt(jnp.maximum(v, 1.2e-38))


def spectral_energy(xx, yy, zz, xy, xz, yz):
    trace = xx + yy + zz
    mid = trace * (1.0 / 3.0)
    dx = xx - mid
    dy = yy - mid
    dz = zz - mid
    xy2 = xy * xy
    xz2 = xz * xz
    yz2 = yz * yz
    sixth = (dx * dx + dy * dy + dz * dz + 2.0 * (xy2 + xz2 + yz2)) * (1.0 / 6.0)
    twice_radius = 2.0 * root(sixth)
    scale = lax.rsqrt(sixth + eigen_guard)
    det = dx * (dy * dz - yz2) - dz * xy2 - dy * xz2 + 2.0 * (xy * xz * yz)
    ratio = (0.5 * det * scale) * (scale * scale)
    size = jnp.minimum(jnp.abs(ratio), 1.0)
    poly = jnp.full_like(size, ACOS[-1] / 3.0)
    for c in ACOS[-2::-1]:
        poly = poly * size + c / 3.0
    t = root(1.0 - size) * poly
    t2 = t * t
    cos_t = 1.0 + t2 * (-0.5 + t2 * (1.0 / 24.0 + t2 * (-1.0 / 720.0 + t2 * (1.0 / 40320.0))))
    sin_t = t * (1.0 + t2 * (-1.0 / 6.0 + t2 * (1.0 / 120.0 + t2 * (-1.0 / 5040.0))))
    other = 0.5 * cos_t + math.sqrt(0.75) * sin_t
    upper = ratio >= 0.0
    first = jnp.where(upper, cos_t, other)
    last = jnp.where(upper, other, cos_t)
    largest = mid + twice_radius * first
    smallest = mid - twice_radius * last
    between = trace - largest - smallest
    relu = lambda v: jnp.maximum(v, 0.0)
    return (
        0.5 * jnp.square(relu(trace))
        + jnp.square(relu(largest))
        + jnp.square(relu(between))
        + jnp.square(relu(smallest))
    )


def kernel(sizes, names, *refs):
    sections, ngx, ngy, nx, ny, nz = sizes
    r = types.SimpleNamespace(**dict(zip(names, refs)))
    local, state, stiff, flow = r.local, r.state, r.stiff, r.flow
    held, clamped, tough_pad, crack_pad = r.held, r.clamped, r.tough_pad, r.crack_pad
    load_ref, crack_ref, clamp_ref, tough_ref = r.load_ref, r.crack_ref, r.clamp_ref, r.tough_ref
    disp_refs = (r.first_ref, r.second_ref, r.third_ref)
    sec = lax.axis_index("section")
    gx = lax.axis_index("gx")
    gy = lax.axis_index("gy")
    group = ngx * ngy
    me = gx * ngy + gy
    ring = lambda k, n: min(k, n - k)
    offsets = [(i, j) for i in range(ngx) for j in range(ngy) if i or j]
    offsets.sort(key=lambda o: (ring(o[0], ngx) + ring(o[1], ngy), o))
    peers = []
    for i, j in offsets:
        peers.append({"gx": lax.rem(gx + i, ngx), "gy": lax.rem(gy + j, ngy)})

    there = {
        "gx": (gx > 0, gx < ngx - 1),
        "gy": (gy > 0, gy < ngy - 1),
    }
    step = (-1, 1)

    def x_dev(s):
        return there["gx"][s], {"gx": gx + step[s]}

    def y_dev(s):
        return there["gy"][s], {"gy": gy + step[s]}

    def c_dev(sx, sy):
        return (
            jnp.logical_and(there["gx"][sx], there["gy"][sy]),
            {"gx": gx + step[sx], "gy": gy + step[sy]},
        )

    neighbours = [x_dev(s) for s in range(2)] + [y_dev(s) for s in range(2)]
    neighbours += [c_dev(sx, sy) for sx in range(2) for sy in range(2)]
    in_line = lambda name: sum(t.astype(jnp.int32) for t in there[name])
    near_count = (in_line("gx") + 1) * (in_line("gy") + 1) - 1

    def greet(sem):
        for cond, dev in neighbours:

            @pl.when(cond)
            def _(dev=dev):
                pl.semaphore_signal(sem, inc=1, device_id=dev, device_id_type=MESH)

    barrier = pltpu.get_barrier_semaphore()
    greet(barrier)
    for k in range(1, sections):
        pl.semaphore_signal(
            barrier,
            inc=1,
            device_id={"section": lax.rem(sec + k, sections)},
            device_id_type=MESH,
        )

    fetch = [
        pltpu.make_async_copy(src, dst, local.at[n])
        for n, (src, dst) in enumerate(
            (
                (r.load_hbm, load_ref),
                (r.crack_hbm, crack_ref),
                (r.clamp_hbm, clamp_ref),
                (r.tough_hbm, tough_ref),
                (r.index_hbm, r.index_ref),
                (r.table_hbm, r.table_ref),
            )
        )
    ]
    for copy in fetch:
        copy.start()

    class Exchange:
        def __init__(self, send, recv):
            self.items = []
            self.send = send
            self.recv = recv

        def add(self, where, src, dst, mine, out_slot, in_slot):
            cond, dev = where
            n = len(self.items)
            copy = pltpu.make_async_remote_copy(
                src_ref=src,
                dst_ref=dst,
                send_sem=self.send.at[n],
                recv_sem=self.recv.at[out_slot],
                device_id=dev,
                device_id_type=MESH,
            )
            back = pltpu.make_async_remote_copy(
                src_ref=src,
                dst_ref=mine,
                send_sem=self.send.at[n],
                recv_sem=self.recv.at[in_slot],
                device_id=dev,
                device_id_type=MESH,
            )
            self.items.append((cond, copy, back))

        def start(self, begin=0, end=None):
            for cond, copy, _ in self.items[begin:end]:
                pl.when(cond)(copy.start)

        def finish(self):
            for cond, copy, back in self.items:

                @pl.when(cond)
                def _():
                    back.wait_recv()
                    copy.wait_send()

        def received(self, begin=0, end=None):
            for cond, _, back in self.items[begin:end]:
                pl.when(cond)(back.wait_recv)

        def sent(self, begin=0, end=None):
            for cond, copy, _ in self.items[begin:end]:
                pl.when(cond)(copy.wait_send)

    rows = ny + 2 * OY

    def clear(xp, carry):
        zero = jnp.zeros((rows, nz), jnp.float32)
        held[xp] = zero
        crack_pad[xp] = zero
        clamped[xp] = zero + 1.0
        tough_pad[xp] = zero + 1.0
        for f in range(3):
            state[0, f, xp] = zero
        if sections > 2:
            state[0, 3, xp] = zero
            for f in range(4):
                state[1, f, xp] = zero
        return carry

    lax.fori_loop(0, nx + 2 * HX, clear, 0)

    for copy in fetch[:3]:
        copy.wait()

    for s in range(2):
        side = lambda n, s=s: slice(0, n) if s == 0 else slice(ny - n, ny)
        r.pack_l[s] = load_ref[:, side(4)]
        r.pack_f[s] = clamp_ref[:, side(2)]
        for x in range(nx):
            r.pack_c[s, 3 * x : 3 * x + 3] = crack_ref[x, side(3)]
    corner = (
        (load_ref, held, 1, 3, 0),
        (load_ref, held, 2, 2, 3),
        (load_ref, held, 3, 1, 5),
        (crack_ref, crack_pad, 1, 2, 6),
        (crack_ref, crack_pad, 2, 1, 8),
        (clamp_ref, clamped, 1, 1, 9),
    )

    def x_from(s, deep):
        return deep - 1 if s == 0 else nx - deep

    def x_at(s, deep):
        return HX - deep if s == 0 else HX + nx - 1 + deep

    for sx in range(2):
        for sy in range(2):
            for ref, _, deep, n, at in corner:
                first = 0 if sy == 0 else ny - n
                r.pack_k[sx * 2 + sy, at : at + n] = ref[x_from(sx, deep), first : first + n]

    pl.semaphore_wait(barrier, near_count + sections - 1)

    beside_y = Exchange(r.y_send, r.y_recv)
    part_a = Exchange(r.a_send, r.a_recv)
    part_b = Exchange(r.b_send, r.b_recv)
    for ex, ref, buf, deep, width, at, slot in (
        (part_a, load_ref, r.in_a, 3, 3, 0, 0),
        (part_a, crack_ref, r.in_a, 2, 2, 3, 2),
        (part_a, clamp_ref, r.in_a, 1, 1, 5, 4),
        (part_b, load_ref, r.in_b, 4, 1, 0, 0),
        (part_b, crack_ref, r.in_b, 3, 1, 1, 2),
        (part_b, clamp_ref, r.in_b, 2, 1, 2, 4),
        (part_b, tough_ref.at[0], r.in_tx, 1, 1, 0, 6),
    ):
        for s in range(2):
            first = deep - width if s == 0 else nx - deep
            ex.add(
                x_dev(s),
                ref.at[pl.ds(first, width)],
                buf.at[1 - s, pl.ds(at, width)],
                buf.at[s, pl.ds(at, width)],
                slot + 1 - s,
                slot + s,
            )
    for n in range(8):
        s = n % 2
        for pack, buf, slot in (
            (r.pack_c, r.in_c, 0),
            (r.pack_l, r.in_l, 2),
            (r.pack_f, r.in_f, 4),
            (r.pack_t, r.in_ty, 6),
        )[n // 2 : n // 2 + 1]:
            beside_y.add(
                y_dev(s), pack.at[s], buf.at[1 - s], buf.at[s], slot + 1 - s, slot + s
            )
    for sx in range(2):
        for sy in range(2):
            here, away = sx * 2 + sy, (1 - sx) * 2 + 1 - sy
            part_a.add(
                c_dev(sx, sy), r.pack_k.at[here], r.in_k.at[away], r.in_k.at[here],
                6 + away, 6 + here,
            )
    beside_y.start(0, 4)
    part_a.start(0, 6)
    beside_y.start(4, 6)
    fetch[3].wait()
    for s in range(2):
        r.pack_t[s] = tough_ref[0, :, 0:1] if s == 0 else tough_ref[0, :, ny - 1 : ny]
    beside_y.start(6)
    part_a.start(6)
    part_b.start()
    further = max(ngx, ngy) - 2
    if further > 0:
        greet(r.reach.at[0])
    tough_copies = []
    for k in range(1, sections):
        copy = pltpu.make_async_remote_copy(
            src_ref=tough_ref.at[0],
            dst_ref=r.tough_in.at[k - 1],
            send_sem=r.tough_send.at[k - 1],
            recv_sem=r.tough_recv.at[k - 1],
            device_id={"section": lax.rem(sec + sections - k, sections)},
            device_id_type=MESH,
        )
        copy.start()
        tough_copies.append(copy)

    inner = slice(OY, OY + ny)
    as_float = lambda v: v.astype(jnp.float32)

    def fill(x, carry):
        held[x + HX, inner] = as_float(load_ref[x])
        clamped[x + HX, inner] = as_float(clamp_ref[x])
        crack_pad[x + HX, inner] = as_float(crack_ref[x])
        tough_pad[x + HX, inner] = tough_ref[0, x]
        return carry

    lax.fori_loop(0, nx, fill, 0, unroll=part(nx, 4))

    for copy in fetch[4:]:
        copy.wait()
    case = r.index_ref[0]
    vector = [r.table_ref[f, case] for f in range(3)]

    planes = slice(HX, HX + nx)

    def x_out(s, n):
        return slice(HX - n, HX) if s == 0 else slice(HX + nx, HX + nx + n)

    def y_out(s, n):
        return slice(OY - n, OY) if s == 0 else slice(OY + ny, OY + ny + n)

    def from_y(kind, s, put):
        beside_y.received(2 * kind + s, 2 * kind + s + 1)
        pl.when(there["gy"][s])(put)

    def unpack_a():
        part_a.received()
        for s in range(2):

            @pl.when(there["gx"][s])
            def _(s=s):
                held[x_out(s, 3), inner] = as_float(r.in_a[s, 0:3])
                crack_pad[x_out(s, 2), inner] = as_float(r.in_a[s, 3:5])
                clamped[x_out(s, 1), inner] = as_float(r.in_a[s, 5:6])

        for sx in range(2):
            for sy in range(2):

                @pl.when(c_dev(sx, sy)[0])
                def _(sx=sx, sy=sy):
                    for _, pad, deep, n, at in corner:
                        pad[x_at(sx, deep), y_out(sy, n)] = as_float(
                            r.in_k[sx * 2 + sy, at : at + n]
                        )

    def unpack_b():
        part_b.received()
        for s in range(2):

            @pl.when(there["gx"][s])
            def _(s=s):
                held[x_at(s, 4), inner] = as_float(r.in_b[s, 0])
                crack_pad[x_at(s, 3), inner] = as_float(r.in_b[s, 1])
                clamped[x_at(s, 2), inner] = as_float(r.in_b[s, 2])
                tough_pad[x_at(s, 1), inner] = r.in_tx[s, 0]

    wide = up8(ny + 4)
    deep = up8(ny + 8)

    def lanes(shape, lane):
        return lax.broadcasted_iota(jnp.int32, shape, 1) == lane

    def beside(v, edge, first, last):
        up = jnp.where(last, edge, pltpu.roll(v, nz - 1, 1))
        down = jnp.where(first, edge, pltpu.roll(v, 1, 1))
        return up, down

    def inside_rows(shape, above):
        row = lax.broadcasted_iota(jnp.int32, shape, 0) + (gy * ny - above)
        return jnp.logical_and(row >= 0, row < ny * ngy)

    def inside_plane(xp):
        plane = xp - HX + gx * nx
        return jnp.logical_and(plane >= 0, plane < nx * ngx)

    edge_stiff = 0.5 * (1.0 + stiff_floor)

    def elastic(at, first, last):
        k = at(stiff, 0, 0)
        sides = (
            (at(stiff, 1, 0), at(stiff, -1, 0)),
            (at(stiff, 0, 1), at(stiff, 0, -1)),
            beside(k, edge_stiff, first, last),
        )
        pairs = [s[0] + s[1] for s in sides]
        weights = pairs[0] + pairs[1] + pairs[2] + 6.0 * k
        faces = [(k + s[0], k + s[1]) for s in sides]
        fz = beside(at(flow, 0, 0), 0.0, first, last)
        grads = (
            at(flow, 1, 0) - at(flow, -1, 0),
            at(flow, 0, 1) - at(flow, 0, -1),
            fz[0] - fz[1],
        )
        return pairs, weights, faces, grads

    def laplace(at, ref, faces, weights, first, last):
        here = at(ref, 0, 0)
        uz = beside(here, 0.0, first, last)
        return here, (
            faces[0][0] * at(ref, 1, 0)
            + faces[0][1] * at(ref, -1, 0)
            + faces[1][0] * at(ref, 0, 1)
            + faces[1][1] * at(ref, 0, -1)
            + faces[2][0] * uz[0]
            + faces[2][1] * uz[1]
            - weights * here
        )

    def strain_energy(at, u, keep, first, last):
        grad = []
        for f in range(3):
            here = at(u.at[f], 0, 0)
            uz = beside(here, 0.0, first, last)
            grad.append(
                (
                    at(u.at[f], 1, 0) - at(u.at[f], -1, 0),
                    at(u.at[f], 0, 1) - at(u.at[f], 0, -1),
                    uz[0] - uz[1],
                )
            )
            keep(f, here)
        return 2.0 * spectral_energy(
            0.5 * grad[0][0],
            0.5 * grad[1][1],
            0.5 * grad[2][2],
            0.25 * (grad[0][1] + grad[1][0]),
            0.25 * (grad[0][2] + grad[2][0]),
            0.25 * (grad[1][2] + grad[2][1]),
        )

    def renew(at, d, energy, g, cracked, first, last):
        dz = beside(at(d, 0, 0), 0.0, first, last)
        around = at(d, 1, 0) + at(d, -1, 0) + at(d, 0, 1) + at(d, 0, -1) + dz[0] + dz[1]
        renewed = (energy + g * around) / (7.0 * g + energy)
        return jnp.where(cracked, 1.0, renewed)

    def add_up(rnd, total):
        r.sums[me, rnd : rnd + 1] = jnp.sum(total, axis=0, keepdims=True)

    def open_stages(above, n):
        shape = (n, nz)
        first, last = lanes(shape, 0), lanes(shape, nz - 1)
        row_inside = inside_rows(shape, above)
        row = lax.broadcasted_iota(jnp.int32, shape, 0)
        a = OY - above

        def stiffen(xp, carry):
            half = 0.5 * (jnp.square(1.0 - crack_pad[xp, a : a + n]) + stiff_floor)
            stiff[xp, a : a + n] = half
            up, down = beside(held[xp, a : a + n], 0.0, first, last)
            div = (
                vector[0] * (held[xp + 1, a : a + n] - held[xp - 1, a : a + n])
                + vector[1] * (held[xp, a + 1 : a + 1 + n] - held[xp, a - 1 : a - 1 + n])
                + vector[2] * (up - down)
            )
            flow[xp, a : a + n] = jnp.where(
                jnp.logical_and(row_inside, inside_plane(xp)), half * div, 0.0
            )
            return carry

        def mover(low, high):
            def move(xp, total):
                at = lambda ref, dx, dy: ref[xp + dx, a + dy : a + dy + n]
                pairs, weights, faces, grads = elastic(at, first, last)
                load, spread = laplace(at, held, faces, weights, first, last)
                pin = at(clamped, 0, 0) + load > 0.5
                squares = None
                for f in range(3):
                    res = vector[f] * spread + grads[f]
                    moved = jnp.where(pin, 0.0, relax_weight * res / (weights + pairs[f]))
                    state[1, f, xp, a : a + n] = vector[f] * load + moved
                    square = res * res
                    squares = square if squares is None else squares + square
                if low >= high:
                    return total
                counted = jnp.logical_and(row >= low + above, row < high + above)
                return total + jnp.where(
                    jnp.logical_and(counted, jnp.logical_not(pin)), squares, 0.0
                )

            return move

        def damage(xp, carry):
            at = lambda ref, dx, dy: ref[xp + dx, a + dy : a + dy + n]
            energy = strain_energy(at, state.at[1], lambda f, v: None, first, last)
            renewed = renew(
                at,
                crack_pad,
                energy,
                at(tough_pad, 0, 0),
                at(crack_pad, 0, 0) > 0.5,
                first,
                last,
            )
            state[1, 3, xp, a : a + n] = jnp.where(
                jnp.logical_and(row_inside, inside_plane(xp)), renewed, 0.0
            )
            return carry

        return stiffen, mover, damage

    def open_sweep():
        def inward(skip, body, carry, most):
            n = nx - 2 * skip
            return lax.fori_loop(HX + skip, HX + nx - skip, body, carry, unroll=part(n, most))

        def outward(far, n, body, carry):
            def both(i, carry):
                carry = body(HX - far + i, carry)
                return body(HX + nx + far - n + i, carry)

            return lax.fori_loop(0, n, both, carry, unroll=True)

        blank = lambda n: jnp.zeros((n, nz), jnp.float32)
        fold = lambda v: jnp.sum(v, axis=0, keepdims=True)

        stiffen, mover, damage = open_stages(0, ny)
        inward(1, stiffen, 0, 14)
        inside = inward(2, mover(2, ny - 2), blank(ny), 12)
        inward(3, damage, 0, 5)

        if further > 1:
            pl.semaphore_wait(r.reach.at[0], near_count)
            greet(r.reach.at[1])

        def rim(s):
            above = (4, 4 - ny)[s]
            stiffen, mover, damage = open_stages(above, 8)

            def put_crack():
                for x in range(nx):
                    crack_pad[HX + x, y_out(s, 3)] = as_float(r.in_c[s, 3 * x : 3 * x + 3])

            def put_load():
                held[planes, y_out(s, 4)] = as_float(r.in_l[s])

            def put_clamp():
                clamped[planes, y_out(s, 2)] = as_float(r.in_f[s])

            def put_tough():
                tough_pad[planes, y_out(s, 1)] = r.in_ty[s]

            from_y(0, s, put_crack)
            from_y(1, s, put_load)
            inward(1, stiffen, 0, 14)
            from_y(2, s, put_clamp)
            counted = (0, 2) if s == 0 else (ny - 2, ny)
            r.rims[s] = inward(2, mover(*counted), blank(8), 12)
            from_y(3, s, put_tough)
            inward(3, damage, 0, 10)

        odd = lax.rem(gy, 2) == 1

        @pl.when(odd)
        def _():
            rim(0)
            rim(1)

        @pl.when(jnp.logical_not(odd))
        def _():
            rim(1)
            rim(0)

        stiffen1, mover1 = stages(1)
        move1 = mover1(OY, ny)
        inward(3, stiffen1, 0, 10)
        own = inward(4, move1, blank(ny), 8)

        stiffen, mover, damage = open_stages(4, deep)
        unpack_a()
        outward(2, 3, stiffen, 0)
        ends = outward(0, 2, mover(0, ny), blank(deep))
        outward(1, 1, mover(0, 0), blank(deep))
        r.sums[me, 0:1] = fold(inside) + fold(r.rims[0] + r.rims[1]) + fold(ends)
        outward(0, 3, damage, 0)
        outward(0, 3, stiffen1, 0)
        own = outward(-1, 3, move1, own)

        unpack_b()
        outward(3, 1, stiffen, 0)
        outward(2, 1, mover(0, 0), blank(deep))
        outward(1, 1, damage, 0)
        outward(1, 1, stiffen1, 0)
        own = outward(0, 1, move1, own)

        return own

    def send_sums():
        for k in range(1 if further > 1 else 0, further):
            pl.semaphore_wait(r.reach.at[k], near_count)
            if k + 1 < further:
                greet(r.reach.at[k + 1])
        for k, peer in enumerate(peers):
            pltpu.make_async_remote_copy(
                src_ref=r.sums.at[me],
                dst_ref=r.sums.at[me],
                send_sem=r.sum_send.at[k],
                recv_sem=r.sum_recv.at[me],
                device_id=peer,
                device_id_type=MESH,
            ).start()

    def stages(rnd):
        p = rnd % 2
        q = 1 - p
        shape = (wide, nz)
        first, last = lanes(shape, 0), lanes(shape, nz - 1)
        row_inside = inside_rows(shape, 2)
        a = OY - 2

        def stiffen(xp, carry):
            half = 0.5 * (jnp.square(1.0 - state[p, 3, xp, a : a + wide]) + stiff_floor)
            stiff[xp, a : a + wide] = half
            up, down = beside(state[p, 2, xp, a : a + wide], 0.0, first, last)
            div = (
                (state[p, 0, xp + 1, a : a + wide] - state[p, 0, xp - 1, a : a + wide])
                + (state[p, 1, xp, a + 1 : a + 1 + wide] - state[p, 1, xp, a - 1 : a - 1 + wide])
                + (up - down)
            )
            flow[xp, a : a + wide] = jnp.where(
                jnp.logical_and(row_inside, inside_plane(xp)), half * div, 0.0
            )
            return carry

        def mover(b, n):
            shape = (n, nz)
            first, last = lanes(shape, 0), lanes(shape, nz - 1)

            def move(xp, total):
                at = lambda ref, dx, dy: ref[xp + dx, b + dy : b + dy + n]
                pairs, weights, faces, grads = elastic(at, first, last)
                load = at(held, 0, 0)
                pin = at(clamped, 0, 0) + load > 0.5
                squares = None
                for f in range(3):
                    here, spread = laplace(at, state.at[p, f], faces, weights, first, last)
                    res = spread + grads[f]
                    moved = here + relax_weight * res / (weights + pairs[f])
                    state[q, f, xp, b : b + n] = jnp.where(pin, load * vector[f], moved)
                    square = res * res
                    squares = square if squares is None else squares + square
                return total + jnp.where(pin, 0.0, squares)

            return move

        return stiffen, mover

    def sweep(rnd, total):
        p = rnd % 2
        q = 1 - p
        done = rnd == sections - 1
        tough = r.tough_in.at[rnd - 1]

        stiffen, mover = stages(rnd)
        if rnd > 1:
            lax.fori_loop(HX - 2, HX + nx + 2, stiffen, 0, unroll=part(nx + 4, 10))
            total = lax.fori_loop(
                HX, HX + nx, mover(OY, ny), jnp.zeros((ny, nz), jnp.float32), unroll=part(nx, 8)
            )
        add_up(rnd, total)
        if done:
            send_sums()
        par = rnd % 2
        mid = pl.ds(OY, ny)
        if done:
            rims = Exchange(r.v_send, r.v_recv)
            for s in range(2):
                row = OY if s == 0 else OY + ny - 1
                for f in range(3):
                    r.pack_v[s, f] = state[q, f, planes, row : row + 1]
                rims.add(
                    x_dev(s),
                    state.at[q, pl.ds(0, 3), HX if s == 0 else HX + nx - 1, mid],
                    r.in_vx.at[1 - s],
                    r.in_vx.at[s],
                    1 - s,
                    s,
                )
                rims.add(
                    y_dev(s), r.pack_v.at[s], r.in_vy.at[1 - s], r.in_vy.at[s], 3 - s, 2 + s
                )
            rims.start()
            rims.received()
            for s in range(2):

                @pl.when(there["gx"][s])
                def _(s=s):
                    state[q, 0:3, x_at(s, 1), inner] = r.in_vx[s]

                @pl.when(there["gy"][s])
                def _(s=s):
                    for f in range(3):
                        state[q, f, planes, y_out(s, 1)] = r.in_vy[s, f]
        else:
            for f in range(3):
                r.pack_u[0, :, 2 * f : 2 * f + 2] = state[q, f, planes, OY : OY + 2]
                r.pack_u[1, :, 2 * f : 2 * f + 2] = state[q, f, planes, OY + ny - 2 : OY + ny]
            r.pack_u[0, :, 6:7] = state[q, 1, planes, OY + 2 : OY + 3]
            r.pack_u[1, :, 6:7] = state[q, 1, planes, OY + ny - 3 : OY + ny - 2]
            shift = Exchange(r.u_send, r.u_recv.at[par])
            for s in range(2):
                shift.add(
                    x_dev(s),
                    state.at[q, pl.ds(0, 3), pl.ds(HX if s == 0 else HX + nx - 2, 2), mid],
                    r.in_u_x.at[par, 1 - s],
                    r.in_u_x.at[par, s],
                    (1 - s),
                    s,
                )
                shift.add(
                    x_dev(s),
                    state.at[q, 0, HX + 2 if s == 0 else HX + nx - 3, mid],
                    r.in_u_x3.at[par, 1 - s],
                    r.in_u_x3.at[par, s],
                    2 + (1 - s),
                    2 + s,
                )
            for s in range(2):
                shift.add(
                    y_dev(s),
                    r.pack_u.at[s],
                    r.in_u_y.at[par, 1 - s],
                    r.in_u_y.at[par, s],
                    4 + (1 - s),
                    4 + s,
                )
            for sx in range(2):
                for sy in range(2):
                    shift.add(
                        c_dev(sx, sy),
                        r.pack_u.at[sy, pl.ds(0 if sx == 0 else nx - 2, 2)],
                        r.in_u_c.at[par, (1 - sx) * 2 + 1 - sy],
                        r.in_u_c.at[par, sx * 2 + sy],
                        6 + (1 - sx) * 2 + 1 - sy,
                        6 + sx * 2 + sy,
                    )
            shift.start()
            shift.finish()
            third_x = (HX - 3, HX + nx + 2)
            third_y = (slice(OY - 3, OY - 2), slice(OY + ny + 2, OY + ny + 3))
            for s in range(2):

                @pl.when(there["gx"][s])
                def _(s=s):
                    state[q, 0:3, x_out(s, 2), inner] = r.in_u_x[par, s]
                    state[q, 0, third_x[s], inner] = r.in_u_x3[par, s]

                @pl.when(there["gy"][s])
                def _(s=s):
                    for f in range(3):
                        state[q, f, planes, y_out(s, 2)] = r.in_u_y[par, s, :, 2 * f : 2 * f + 2]
                    state[q, 1, planes, third_y[s]] = r.in_u_y[par, s, :, 6:7]

            for sx in range(2):
                for sy in range(2):

                    @pl.when(c_dev(sx, sy)[0])
                    def _(sx=sx, sy=sy):
                        for f in range(3):
                            state[q, f, x_out(sx, 2), y_out(sy, 2)] = r.in_u_c[
                                par, sx * 2 + sy, :, 2 * f : 2 * f + 2
                            ]

        tough_copies[rnd - 1].wait_recv()

        shape = (ny, nz)
        first, last = lanes(shape, 0), lanes(shape, nz - 1)

        def damage(x, carry):
            xp = x + HX
            at = lambda ref, dx, dy: ref[xp + dx, OY + dy : OY + dy + ny]

            def keep(f, here):
                if done:
                    disp_refs[f][x] = here

            energy = strain_energy(at, state.at[q], keep, first, last)
            renewed = renew(
                at, state.at[p, 3], energy, tough[x], crack_ref[x] > 0, first, last
            )
            if done:
                r.dam_ref[x] = renewed
            else:
                state[q, 3, xp, inner] = renewed
            return carry

        lax.fori_loop(0, nx, damage, 0, unroll=part(nx, 8))
        if done:
            rims.sent()
            return

        r.pack_d[0] = state[q, 3, planes, OY : OY + 2]
        r.pack_d[1] = state[q, 3, planes, OY + ny - 2 : OY + ny]
        crack = Exchange(r.d_send, r.d_recv.at[par])
        for s in range(2):
            crack.add(
                x_dev(s),
                state.at[q, 3, pl.ds(HX if s == 0 else HX + nx - 2, 2), mid],
                r.in_d_x.at[par, 1 - s],
                r.in_d_x.at[par, s],
                1 - s,
                s,
            )
        for s in range(2):
            crack.add(
                y_dev(s),
                r.pack_d.at[s],
                r.in_d_y.at[par, 1 - s],
                r.in_d_y.at[par, s],
                2 + 1 - s,
                2 + s,
            )
        for sx in range(2):
            for sy in range(2):
                crack.add(
                    c_dev(sx, sy),
                    r.pack_d.at[sy, pl.ds(0 if sx == 0 else nx - 1, 1)],
                    r.in_d_c.at[par, (1 - sx) * 2 + 1 - sy],
                    r.in_d_c.at[par, sx * 2 + sy],
                    4 + (1 - sx) * 2 + 1 - sy,
                    4 + sx * 2 + sy,
                )
        crack.start()
        crack.finish()
        for s in range(2):

            @pl.when(there["gx"][s])
            def _(s=s):
                state[q, 3, x_out(s, 2), inner] = r.in_d_x[par, s]

            @pl.when(there["gy"][s])
            def _(s=s):
                state[q, 3, planes, y_out(s, 2)] = r.in_d_y[par, s]

        for sx in range(2):
            for sy in range(2):

                @pl.when(c_dev(sx, sy)[0])
                def _(sx=sx, sy=sy):
                    state[q, 3, x_out(sx, 1), y_out(sy, 2)] = r.in_d_c[par, sx * 2 + sy]

    total = open_sweep()
    for rnd in range(1, sections):
        sweep(rnd, total)

    cells = 3.0 * nx * ngx * ny * ngy * nz
    beside_y.sent()
    part_a.sent()
    part_b.sent()
    for copy in tough_copies:
        copy.wait_send()
    for k, peer in enumerate(peers):
        other = peer["gx"] * ngy + peer["gy"]
        pltpu.make_async_remote_copy(
            src_ref=r.sums.at[me],
            dst_ref=r.sums.at[other],
            send_sem=r.sum_send.at[k],
            recv_sem=r.sum_recv.at[other],
            device_id=peer,
            device_id_type=MESH,
        ).wait()
    total = r.sums[0]
    for k in range(1, group):
        total = total + r.sums[k]
    entries = jnp.sqrt(jnp.sum(total, axis=1, keepdims=True) / cells)
    column = lax.broadcasted_iota(jnp.int32, (1, sections), 1)
    norms = jnp.zeros((1, sections), jnp.float32)
    for rnd in range(sections):
        norms = jnp.where(
            column == lax.rem(sec + rnd, sections), entries[rnd : rnd + 1], norms
        )
    r.norm_ref[...] = norms


def put_out(
    first_ref, second_ref, third_ref, dam_ref, norm_ref, disp_hbm, dam_hbm, norm_out, sems
):
    copies = [
        pltpu.make_async_copy(ref, disp_hbm.at[0, f], sems.at[f])
        for f, ref in enumerate((first_ref, second_ref, third_ref))
    ]
    copies.append(pltpu.make_async_copy(dam_ref, dam_hbm.at[0], sems.at[3]))
    for copy in copies:
        copy.start()
    norm_out[...] = norm_ref[...]
    for copy in copies:
        copy.wait()


def on_device(sizes, load_index, load_table, toughness, clamp_mask, load_mask, crack_mask):
    sections, ngx, ngy = sizes
    nx, ny, nz = clamp_mask.shape
    assert load_index.shape == (1,)
    group = ngx * ngy
    f32 = jnp.float32
    padded = (nx + 2 * HX, ny + 2 * OY, nz)
    vmem = pltpu.VMEM
    dma = pltpu.SemaphoreType.DMA
    later = max(sections - 1, 1)
    more = sections > 2
    scratch = {
        "index_ref": pltpu.SMEM(load_index.shape, jnp.int32),
        "table_ref": pltpu.SMEM(load_table.shape[::-1], f32),
        "tough_ref": vmem((1, nx, ny, nz), f32),
        "clamp_ref": vmem((nx, ny, nz), jnp.int32),
        "load_ref": vmem((nx, ny, nz), jnp.int32),
        "crack_ref": vmem((nx, ny, nz), jnp.int32),
        "local": dma((6,)),
        "state": vmem((2, 4) + padded, f32),
        "stiff": vmem(padded, f32),
        "flow": vmem(padded, f32),
        "held": vmem(padded, f32),
        "clamped": vmem(padded, f32),
        "tough_pad": vmem(padded, f32),
        "crack_pad": vmem(padded, f32),
        "tough_in": vmem((later, nx, ny, nz), f32),
        "pack_l": vmem((2, nx, 4, nz), jnp.int32),
        "pack_f": vmem((2, nx, 2, nz), jnp.int32),
        "pack_c": vmem((2, 3 * nx, nz), jnp.int32),
        "pack_t": vmem((2, nx, 1, nz), f32),
        "pack_k": vmem((4, 16, nz), jnp.int32),
        "in_a": vmem((2, 6, ny, nz), jnp.int32),
        "in_b": vmem((2, 3, ny, nz), jnp.int32),
        "in_tx": vmem((2, 1, ny, nz), f32),
        "in_l": vmem((2, nx, 4, nz), jnp.int32),
        "in_f": vmem((2, nx, 2, nz), jnp.int32),
        "in_c": vmem((2, 3 * nx, nz), jnp.int32),
        "in_ty": vmem((2, nx, 1, nz), f32),
        "in_k": vmem((4, 16, nz), jnp.int32),
        "rims": vmem((2, 8, nz), f32),
        "pack_v": vmem((2, 3, nx, 1, nz), f32),
        "in_vx": vmem((2, 3, ny, nz), f32),
        "in_vy": vmem((2, 3, nx, 1, nz), f32),
        "v_send": dma((4,)),
        "v_recv": dma((4,)),
        "sums": vmem((group, sections, nz), f32),
        "y_send": dma((8,)),
        "y_recv": dma((8,)),
        "a_send": dma((10,)),
        "a_recv": dma((10,)),
        "b_send": dma((8,)),
        "b_recv": dma((8,)),
        "reach": pltpu.SemaphoreType.REGULAR((max(max(ngx, ngy) - 2, 1),)),
        "tough_send": dma((later,)),
        "tough_recv": dma((later,)),
        "sum_send": dma((max(group - 1, 1),)),
        "sum_recv": dma((group,)),
    }
    if more:
        scratch |= {
            "pack_u": vmem((2, nx, 8, nz), f32),
            "pack_d": vmem((2, nx, 2, nz), f32),
            "in_u_x": vmem((2, 2, 3, 2, ny, nz), f32),
            "in_u_x3": vmem((2, 2, ny, nz), f32),
            "in_u_y": vmem((2, 2, nx, 8, nz), f32),
            "in_u_c": vmem((2, 4, 2, 8, nz), f32),
            "in_d_x": vmem((2, 2, 2, ny, nz), f32),
            "in_d_y": vmem((2, 2, nx, 2, nz), f32),
            "in_d_c": vmem((2, 4, 1, 2, nz), f32),
            "u_send": dma((10,)),
            "u_recv": dma((2, 10)),
            "d_send": dma((8,)),
            "d_recv": dma((2, 8)),
        }
    ins = ("index_hbm", "table_hbm", "tough_hbm", "clamp_hbm", "load_hbm", "crack_hbm")
    outs = ("first_ref", "second_ref", "third_ref", "dam_ref", "norm_ref")
    names = (*ins, *outs, *scratch)
    block = pl.BlockSpec(memory_space=pltpu.VMEM)
    away = pl.BlockSpec(memory_space=pltpu.HBM)
    results = pl.pallas_call(
        functools.partial(kernel, (sections, ngx, ngy, nx, ny, nz), names),
        out_shape=(
            *[jax.ShapeDtypeStruct((nx, ny, nz), f32)] * 4,
            jax.ShapeDtypeStruct((1, sections), f32),
        ),
        in_specs=[away] * 6,
        out_specs=(block,) * 5,
        scratch_shapes=list(scratch.values()),
        compiler_params=pltpu.CompilerParams(
            collective_id=0, has_side_effects=True, vmem_limit_bytes=56_020_000
        ),
    )(load_index, pltpu.with_memory_space_constraint(load_table.T, pltpu.HBM), toughness, clamp_mask, load_mask, crack_mask)
    return pl.pallas_call(
        put_out,
        out_shape=(
            jax.ShapeDtypeStruct((1, 3, nx, ny, nz), f32),
            jax.ShapeDtypeStruct((1, nx, ny, nz), f32),
            jax.ShapeDtypeStruct((1, sections), f32),
        ),
        in_specs=[block] * 5,
        out_specs=(away, away, block),
        scratch_shapes=[dma((4,))],
        compiler_params=pltpu.CompilerParams(vmem_limit_bytes=1024 * 1024),
    )(*results)


def solution(mesh):
    in_specs = (
        P("section"),
        P(),
        P("section", "gx", "gy", None),
        P("gx", "gy", None),
        P("gx", "gy", None),
        P("gx", "gy", None),
    )
    out_specs = (
        P("section", None, "gx", "gy", None),
        P("section", "gx", "gy", None),
        P("section", None),
    )
    sizes = tuple(mesh.shape[name] for name in ("section", "gx", "gy"))
    return jax.shard_map(
        functools.partial(on_device, sizes),
        mesh=mesh,
        in_specs=in_specs,
        out_specs=out_specs,
        check_vma=False,
    )
```

```python
import functools
import math
import types

import jax
import jax.numpy as jnp
from jax import lax
from jax.experimental import pallas as pl
from jax.experimental.pallas import tpu as pltpu
from jax.sharding import PartitionSpec as P

relax_weight = 0.6
stiff_floor = 0.001
eigen_guard = 1e-08
MESH = pl.DeviceIdType.MESH

HX = 5
OY = 8

ACOS = (
    1.5707963050,
    -0.2145988016,
    0.0889789874,
    -0.0501743046,
    0.0308918810,
    -0.0170881256,
    0.0066700901,
    -0.0012624911,
)


def up8(n):
    return -(-n // 8) * 8


def part(n, most):
    return max(k for k in range(1, most + 1) if n % k == 0)


def root(v):
    return v * lax.rsqrt(jnp.maximum(v, 1.2e-38))


def spectral_energy(xx, yy, zz, xy, xz, yz):
    trace = xx + yy + zz
    mid = trace * (1.0 / 3.0)
    dx = xx - mid
    dy = yy - mid
    dz = zz - mid
    xy2 = xy * xy
    xz2 = xz * xz
    yz2 = yz * yz
    sixth = (dx * dx + dy * dy + dz * dz + 2.0 * (xy2 + xz2 + yz2)) * (1.0 / 6.0)
    twice_radius = 2.0 * root(sixth)
    scale = lax.rsqrt(sixth + eigen_guard)
    det = dx * (dy * dz - yz2) - dz * xy2 - dy * xz2 + 2.0 * (xy * xz * yz)
    ratio = (0.5 * det * scale) * (scale * scale)
    size = jnp.minimum(jnp.abs(ratio), 1.0)
    poly = jnp.full_like(size, ACOS[-1] / 3.0)
    for c in ACOS[-2::-1]:
        poly = poly * size + c / 3.0
    t = root(1.0 - size) * poly
    t2 = t * t
    cos_t = 1.0 + t2 * (-0.5 + t2 * (1.0 / 24.0 + t2 * (-1.0 / 720.0 + t2 * (1.0 / 40320.0))))
    sin_t = t * (1.0 + t2 * (-1.0 / 6.0 + t2 * (1.0 / 120.0 + t2 * (-1.0 / 5040.0))))
    other = 0.5 * cos_t + math.sqrt(0.75) * sin_t
    upper = ratio >= 0.0
    first = jnp.where(upper, cos_t, other)
    last = jnp.where(upper, other, cos_t)
    largest = mid + twice_radius * first
    smallest = mid - twice_radius * last
    between = trace - largest - smallest
    relu = lambda v: jnp.maximum(v, 0.0)
    return (
        0.5 * jnp.square(relu(trace))
        + jnp.square(relu(largest))
        + jnp.square(relu(between))
        + jnp.square(relu(smallest))
    )


def kernel(sizes, names, *refs):
    sections, ngx, ngy, nx, ny, nz = sizes
    r = types.SimpleNamespace(**dict(zip(names, refs)))
    local, state, stiff, flow = r.local, r.state, r.stiff, r.flow
    held, clamped, tough_pad, crack_pad = r.held, r.clamped, r.tough_pad, r.crack_pad
    load_ref, crack_ref, clamp_ref, tough_ref = r.load_ref, r.crack_ref, r.clamp_ref, r.tough_ref
    disp_refs = (r.first_ref, r.second_ref, r.third_ref)
    sec = lax.axis_index("section")
    gx = lax.axis_index("gx")
    gy = lax.axis_index("gy")
    group = ngx * ngy
    me = gx * ngy + gy
    ring = lambda k, n: min(k, n - k)
    offsets = [(i, j) for i in range(ngx) for j in range(ngy) if i or j]
    offsets.sort(key=lambda o: (ring(o[0], ngx) + ring(o[1], ngy), o))
    peers = []
    for i, j in offsets:
        peers.append({"gx": lax.rem(gx + i, ngx), "gy": lax.rem(gy + j, ngy)})

    there = {
        "gx": (gx > 0, gx < ngx - 1),
        "gy": (gy > 0, gy < ngy - 1),
    }
    step = (-1, 1)

    def x_dev(s):
        return there["gx"][s], {"gx": gx + step[s]}

    def y_dev(s):
        return there["gy"][s], {"gy": gy + step[s]}

    def c_dev(sx, sy):
        return (
            jnp.logical_and(there["gx"][sx], there["gy"][sy]),
            {"gx": gx + step[sx], "gy": gy + step[sy]},
        )

    neighbours = [x_dev(s) for s in range(2)] + [y_dev(s) for s in range(2)]
    neighbours += [c_dev(sx, sy) for sx in range(2) for sy in range(2)]
    in_line = lambda name: sum(t.astype(jnp.int32) for t in there[name])
    near_count = (in_line("gx") + 1) * (in_line("gy") + 1) - 1

    def greet(sem):
        for cond, dev in neighbours:

            @pl.when(cond)
            def _(dev=dev):
                pl.semaphore_signal(sem, inc=1, device_id=dev, device_id_type=MESH)

    barrier = pltpu.get_barrier_semaphore()
    greet(barrier)
    for k in range(1, sections):
        pl.semaphore_signal(
            barrier,
            inc=1,
            device_id={"section": lax.rem(sec + k, sections)},
            device_id_type=MESH,
        )

    fetch = [
        pltpu.make_async_copy(src, dst, local.at[n])
        for n, (src, dst) in enumerate(
            (
                (r.load_hbm, load_ref),
                (r.crack_hbm, crack_ref),
                (r.clamp_hbm, clamp_ref),
                (r.tough_hbm, tough_ref),
                (r.index_hbm, r.index_ref),
                (r.table_hbm, r.table_ref),
            )
        )
    ]
    for copy in fetch:
        copy.start()

    class Exchange:
        def __init__(self, send, recv):
            self.items = []
            self.send = send
            self.recv = recv

        def add(self, where, src, dst, mine, out_slot, in_slot):
            cond, dev = where
            n = len(self.items)
            copy = pltpu.make_async_remote_copy(
                src_ref=src,
                dst_ref=dst,
                send_sem=self.send.at[n],
                recv_sem=self.recv.at[out_slot],
                device_id=dev,
                device_id_type=MESH,
            )
            back = pltpu.make_async_remote_copy(
                src_ref=src,
                dst_ref=mine,
                send_sem=self.send.at[n],
                recv_sem=self.recv.at[in_slot],
                device_id=dev,
                device_id_type=MESH,
            )
            self.items.append((cond, copy, back))

        def start(self, begin=0, end=None):
            for cond, copy, _ in self.items[begin:end]:
                pl.when(cond)(copy.start)

        def finish(self):
            for cond, copy, back in self.items:

                @pl.when(cond)
                def _():
                    back.wait_recv()
                    copy.wait_send()

        def received(self, begin=0, end=None):
            for cond, _, back in self.items[begin:end]:
                pl.when(cond)(back.wait_recv)

        def sent(self, begin=0, end=None):
            for cond, copy, _ in self.items[begin:end]:
                pl.when(cond)(copy.wait_send)

    rows = ny + 2 * OY

    def clear(xp, carry):
        zero = jnp.zeros((rows, nz), jnp.float32)
        held[xp] = zero
        crack_pad[xp] = zero
        clamped[xp] = zero + 1.0
        tough_pad[xp] = zero + 1.0
        for f in range(3):
            state[0, f, xp] = zero
        if sections > 2:
            state[0, 3, xp] = zero
            for f in range(4):
                state[1, f, xp] = zero
        return carry

    lax.fori_loop(0, nx + 2 * HX, clear, 0)

    for copy in fetch[:3]:
        copy.wait()

    for s in range(2):
        side = lambda n, s=s: slice(0, n) if s == 0 else slice(ny - n, ny)
        r.pack_l[s] = load_ref[:, side(4)]
        r.pack_f[s] = clamp_ref[:, side(2)]
        for x in range(nx):
            r.pack_c[s, 3 * x : 3 * x + 3] = crack_ref[x, side(3)]
    corner = (
        (load_ref, held, 1, 3, 0),
        (load_ref, held, 2, 2, 3),
        (load_ref, held, 3, 1, 5),
        (crack_ref, crack_pad, 1, 2, 6),
        (crack_ref, crack_pad, 2, 1, 8),
        (clamp_ref, clamped, 1, 1, 9),
    )

    def x_from(s, deep):
        return deep - 1 if s == 0 else nx - deep

    def x_at(s, deep):
        return HX - deep if s == 0 else HX + nx - 1 + deep

    for sx in range(2):
        for sy in range(2):
            for ref, _, deep, n, at in corner:
                first = 0 if sy == 0 else ny - n
                r.pack_k[sx * 2 + sy, at : at + n] = ref[x_from(sx, deep), first : first + n]

    pl.semaphore_wait(barrier, near_count + sections - 1)

    beside_y = Exchange(r.y_send, r.y_recv)
    part_a = Exchange(r.a_send, r.a_recv)
    part_b = Exchange(r.b_send, r.b_recv)
    for ex, ref, buf, deep, width, at, slot in (
        (part_a, load_ref, r.in_a, 3, 3, 0, 0),
        (part_a, crack_ref, r.in_a, 2, 2, 3, 2),
        (part_a, clamp_ref, r.in_a, 1, 1, 5, 4),
        (part_b, load_ref, r.in_b, 4, 1, 0, 0),
        (part_b, crack_ref, r.in_b, 3, 1, 1, 2),
        (part_b, clamp_ref, r.in_b, 2, 1, 2, 4),
        (part_b, tough_ref.at[0], r.in_tx, 1, 1, 0, 6),
    ):
        for s in range(2):
            first = deep - width if s == 0 else nx - deep
            ex.add(
                x_dev(s),
                ref.at[pl.ds(first, width)],
                buf.at[1 - s, pl.ds(at, width)],
                buf.at[s, pl.ds(at, width)],
                slot + 1 - s,
                slot + s,
            )
    for n in range(8):
        s = n % 2
        for pack, buf, slot in (
            (r.pack_c, r.in_c, 0),
            (r.pack_l, r.in_l, 2),
            (r.pack_f, r.in_f, 4),
            (r.pack_t, r.in_ty, 6),
        )[n // 2 : n // 2 + 1]:
            beside_y.add(
                y_dev(s), pack.at[s], buf.at[1 - s], buf.at[s], slot + 1 - s, slot + s
            )
    for sx in range(2):
        for sy in range(2):
            here, away = sx * 2 + sy, (1 - sx) * 2 + 1 - sy
            part_a.add(
                c_dev(sx, sy), r.pack_k.at[here], r.in_k.at[away], r.in_k.at[here],
                6 + away, 6 + here,
            )
    beside_y.start(0, 4)
    part_a.start(0, 6)
    beside_y.start(4, 6)
    fetch[3].wait()
    for s in range(2):
        r.pack_t[s] = tough_ref[0, :, 0:1] if s == 0 else tough_ref[0, :, ny - 1 : ny]
    beside_y.start(6)
    part_a.start(6)
    part_b.start()
    further = max(ngx, ngy) - 2
    if further > 0:
        greet(r.reach.at[0])
    tough_copies = []
    for k in range(1, sections):
        copy = pltpu.make_async_remote_copy(
            src_ref=tough_ref.at[0],
            dst_ref=r.tough_in.at[k - 1],
            send_sem=r.tough_send.at[k - 1],
            recv_sem=r.tough_recv.at[k - 1],
            device_id={"section": lax.rem(sec + sections - k, sections)},
            device_id_type=MESH,
        )
        copy.start()
        tough_copies.append(copy)

    inner = slice(OY, OY + ny)
    as_float = lambda v: v.astype(jnp.float32)

    def fill(x, carry):
        held[x + HX, inner] = as_float(load_ref[x])
        clamped[x + HX, inner] = as_float(clamp_ref[x])
        crack_pad[x + HX, inner] = as_float(crack_ref[x])
        tough_pad[x + HX, inner] = tough_ref[0, x]
        return carry

    lax.fori_loop(0, nx, fill, 0, unroll=part(nx, 4))

    for copy in fetch[4:]:
        copy.wait()
    case = r.index_ref[0]
    vector = [r.table_ref[f, case] for f in range(3)]

    planes = slice(HX, HX + nx)

    def x_out(s, n):
        return slice(HX - n, HX) if s == 0 else slice(HX + nx, HX + nx + n)

    def y_out(s, n):
        return slice(OY - n, OY) if s == 0 else slice(OY + ny, OY + ny + n)

    def from_y(kind, s, put):
        beside_y.received(2 * kind + s, 2 * kind + s + 1)
        pl.when(there["gy"][s])(put)

    def unpack_a():
        part_a.received()
        for s in range(2):

            @pl.when(there["gx"][s])
            def _(s=s):
                held[x_out(s, 3), inner] = as_float(r.in_a[s, 0:3])
                crack_pad[x_out(s, 2), inner] = as_float(r.in_a[s, 3:5])
                clamped[x_out(s, 1), inner] = as_float(r.in_a[s, 5:6])

        for sx in range(2):
            for sy in range(2):

                @pl.when(c_dev(sx, sy)[0])
                def _(sx=sx, sy=sy):
                    for _, pad, deep, n, at in corner:
                        pad[x_at(sx, deep), y_out(sy, n)] = as_float(
                            r.in_k[sx * 2 + sy, at : at + n]
                        )

    def unpack_b():
        part_b.received()
        for s in range(2):

            @pl.when(there["gx"][s])
            def _(s=s):
                held[x_at(s, 4), inner] = as_float(r.in_b[s, 0])
                crack_pad[x_at(s, 3), inner] = as_float(r.in_b[s, 1])
                clamped[x_at(s, 2), inner] = as_float(r.in_b[s, 2])
                tough_pad[x_at(s, 1), inner] = r.in_tx[s, 0]

    wide = up8(ny + 4)
    deep = up8(ny + 8)

    def lanes(shape, lane):
        return lax.broadcasted_iota(jnp.int32, shape, 1) == lane

    def beside(v, edge, first, last):
        up = jnp.where(last, edge, pltpu.roll(v, nz - 1, 1))
        down = jnp.where(first, edge, pltpu.roll(v, 1, 1))
        return up, down

    def inside_rows(shape, above):
        row = lax.broadcasted_iota(jnp.int32, shape, 0) + (gy * ny - above)
        return jnp.logical_and(row >= 0, row < ny * ngy)

    def inside_plane(xp):
        plane = xp - HX + gx * nx
        return jnp.logical_and(plane >= 0, plane < nx * ngx)

    edge_stiff = 0.5 * (1.0 + stiff_floor)

    def elastic(at, first, last):
        k = at(stiff, 0, 0)
        sides = (
            (at(stiff, 1, 0), at(stiff, -1, 0)),
            (at(stiff, 0, 1), at(stiff, 0, -1)),
            beside(k, edge_stiff, first, last),
        )
        pairs = [s[0] + s[1] for s in sides]
        weights = pairs[0] + pairs[1] + pairs[2] + 6.0 * k
        faces = [(k + s[0], k + s[1]) for s in sides]
        fz = beside(at(flow, 0, 0), 0.0, first, last)
        grads = (
            at(flow, 1, 0) - at(flow, -1, 0),
            at(flow, 0, 1) - at(flow, 0, -1),
            fz[0] - fz[1],
        )
        return pairs, weights, faces, grads

    def laplace(at, ref, faces, weights, first, last):
        here = at(ref, 0, 0)
        uz = beside(here, 0.0, first, last)
        return here, (
            faces[0][0] * at(ref, 1, 0)
            + faces[0][1] * at(ref, -1, 0)
            + faces[1][0] * at(ref, 0, 1)
            + faces[1][1] * at(ref, 0, -1)
            + faces[2][0] * uz[0]
            + faces[2][1] * uz[1]
            - weights * here
        )

    def strain_energy(at, u, keep, first, last):
        grad = []
        for f in range(3):
            here = at(u.at[f], 0, 0)
            uz = beside(here, 0.0, first, last)
            grad.append(
                (
                    at(u.at[f], 1, 0) - at(u.at[f], -1, 0),
                    at(u.at[f], 0, 1) - at(u.at[f], 0, -1),
                    uz[0] - uz[1],
                )
            )
            keep(f, here)
        return 2.0 * spectral_energy(
            0.5 * grad[0][0],
            0.5 * grad[1][1],
            0.5 * grad[2][2],
            0.25 * (grad[0][1] + grad[1][0]),
            0.25 * (grad[0][2] + grad[2][0]),
            0.25 * (grad[1][2] + grad[2][1]),
        )

    def renew(at, d, energy, g, cracked, first, last):
        dz = beside(at(d, 0, 0), 0.0, first, last)
        around = at(d, 1, 0) + at(d, -1, 0) + at(d, 0, 1) + at(d, 0, -1) + dz[0] + dz[1]
        renewed = (energy + g * around) / (7.0 * g + energy)
        return jnp.where(cracked, 1.0, renewed)

    def add_up(rnd, total):
        r.sums[me, rnd : rnd + 1] = jnp.sum(total, axis=0, keepdims=True)

    def open_stages(above, n):
        shape = (n, nz)
        first, last = lanes(shape, 0), lanes(shape, nz - 1)
        row_inside = inside_rows(shape, above)
        row = lax.broadcasted_iota(jnp.int32, shape, 0)
        a = OY - above

        def stiffen(xp, carry):
            half = 0.5 * (jnp.square(1.0 - crack_pad[xp, a : a + n]) + stiff_floor)
            stiff[xp, a : a + n] = half
            up, down = beside(held[xp, a : a + n], 0.0, first, last)
            div = (
                vector[0] * (held[xp + 1, a : a + n] - held[xp - 1, a : a + n])
                + vector[1] * (held[xp, a + 1 : a + 1 + n] - held[xp, a - 1 : a - 1 + n])
                + vector[2] * (up - down)
            )
            flow[xp, a : a + n] = jnp.where(
                jnp.logical_and(row_inside, inside_plane(xp)), half * div, 0.0
            )
            return carry

        def mover(low, high):
            def move(xp, total):
                at = lambda ref, dx, dy: ref[xp + dx, a + dy : a + dy + n]
                pairs, weights, faces, grads = elastic(at, first, last)
                load, spread = laplace(at, held, faces, weights, first, last)
                pin = at(clamped, 0, 0) + load > 0.5
                squares = None
                for f in range(3):
                    res = vector[f] * spread + grads[f]
                    moved = jnp.where(pin, 0.0, relax_weight * res / (weights + pairs[f]))
                    state[1, f, xp, a : a + n] = vector[f] * load + moved
                    square = res * res
                    squares = square if squares is None else squares + square
                if low >= high:
                    return total
                counted = jnp.logical_and(row >= low + above, row < high + above)
                return total + jnp.where(
                    jnp.logical_and(counted, jnp.logical_not(pin)), squares, 0.0
                )

            return move

        def damage(xp, carry):
            at = lambda ref, dx, dy: ref[xp + dx, a + dy : a + dy + n]
            energy = strain_energy(at, state.at[1], lambda f, v: None, first, last)
            renewed = renew(
                at,
                crack_pad,
                energy,
                at(tough_pad, 0, 0),
                at(crack_pad, 0, 0) > 0.5,
                first,
                last,
            )
            state[1, 3, xp, a : a + n] = jnp.where(
                jnp.logical_and(row_inside, inside_plane(xp)), renewed, 0.0
            )
            return carry

        return stiffen, mover, damage

    def open_sweep():
        def inward(skip, body, carry, most):
            n = nx - 2 * skip
            return lax.fori_loop(HX + skip, HX + nx - skip, body, carry, unroll=part(n, most))

        def outward(far, n, body, carry):
            def both(i, carry):
                carry = body(HX - far + i, carry)
                return body(HX + nx + far - n + i, carry)

            return lax.fori_loop(0, n, both, carry, unroll=True)

        blank = lambda n: jnp.zeros((n, nz), jnp.float32)
        fold = lambda v: jnp.sum(v, axis=0, keepdims=True)

        stiffen, mover, damage = open_stages(0, ny)
        inward(1, stiffen, 0, 14)
        inside = inward(2, mover(2, ny - 2), blank(ny), 12)
        inward(3, damage, 0, 5)

        if further > 1:
            pl.semaphore_wait(r.reach.at[0], near_count)
            greet(r.reach.at[1])

        def rim(s):
            above = (4, 4 - ny)[s]
            stiffen, mover, damage = open_stages(above, 8)

            def put_crack():
                for x in range(nx):
                    crack_pad[HX + x, y_out(s, 3)] = as_float(r.in_c[s, 3 * x : 3 * x + 3])

            def put_load():
                held[planes, y_out(s, 4)] = as_float(r.in_l[s])

            def put_clamp():
                clamped[planes, y_out(s, 2)] = as_float(r.in_f[s])

            def put_tough():
                tough_pad[planes, y_out(s, 1)] = r.in_ty[s]

            from_y(0, s, put_crack)
            from_y(1, s, put_load)
            inward(1, stiffen, 0, 14)
            from_y(2, s, put_clamp)
            counted = (0, 2) if s == 0 else (ny - 2, ny)
            r.rims[s] = inward(2, mover(*counted), blank(8), 12)
            from_y(3, s, put_tough)
            inward(3, damage, 0, 10)

        odd = lax.rem(gy, 2) == 1

        @pl.when(odd)
        def _():
            rim(0)
            rim(1)

        @pl.when(jnp.logical_not(odd))
        def _():
            rim(1)
            rim(0)

        stiffen1, mover1 = stages(1)
        move1 = mover1(OY, ny)
        inward(3, stiffen1, 0, 10)
        own = inward(4, move1, blank(ny), 8)

        stiffen, mover, damage = open_stages(4, deep)
        unpack_a()
        outward(2, 3, stiffen, 0)
        ends = outward(0, 2, mover(0, ny), blank(deep))
        outward(1, 1, mover(0, 0), blank(deep))
        r.sums[me, 0:1] = fold(inside) + fold(r.rims[0] + r.rims[1]) + fold(ends)
        outward(0, 3, damage, 0)
        outward(0, 3, stiffen1, 0)
        own = outward(-1, 3, move1, own)

        unpack_b()
        outward(3, 1, stiffen, 0)
        outward(2, 1, mover(0, 0), blank(deep))
        outward(1, 1, damage, 0)
        outward(1, 1, stiffen1, 0)
        own = outward(0, 1, move1, own)

        return own

    def send_sums():
        for k in range(1 if further > 1 else 0, further):
            pl.semaphore_wait(r.reach.at[k], near_count)
            if k + 1 < further:
                greet(r.reach.at[k + 1])
        for k, peer in enumerate(peers):
            pltpu.make_async_remote_copy(
                src_ref=r.sums.at[me],
                dst_ref=r.sums.at[me],
                send_sem=r.sum_send.at[k],
                recv_sem=r.sum_recv.at[me],
                device_id=peer,
                device_id_type=MESH,
            ).start()

    def stages(rnd):
        p = rnd % 2
        q = 1 - p
        shape = (wide, nz)
        first, last = lanes(shape, 0), lanes(shape, nz - 1)
        row_inside = inside_rows(shape, 2)
        a = OY - 2

        def stiffen(xp, carry):
            half = 0.5 * (jnp.square(1.0 - state[p, 3, xp, a : a + wide]) + stiff_floor)
            stiff[xp, a : a + wide] = half
            up, down = beside(state[p, 2, xp, a : a + wide], 0.0, first, last)
            div = (
                (state[p, 0, xp + 1, a : a + wide] - state[p, 0, xp - 1, a : a + wide])
                + (state[p, 1, xp, a + 1 : a + 1 + wide] - state[p, 1, xp, a - 1 : a - 1 + wide])
                + (up - down)
            )
            flow[xp, a : a + wide] = jnp.where(
                jnp.logical_and(row_inside, inside_plane(xp)), half * div, 0.0
            )
            return carry

        def mover(b, n):
            shape = (n, nz)
            first, last = lanes(shape, 0), lanes(shape, nz - 1)

            def move(xp, total):
                at = lambda ref, dx, dy: ref[xp + dx, b + dy : b + dy + n]
                pairs, weights, faces, grads = elastic(at, first, last)
                load = at(held, 0, 0)
                pin = at(clamped, 0, 0) + load > 0.5
                squares = None
                for f in range(3):
                    here, spread = laplace(at, state.at[p, f], faces, weights, first, last)
                    res = spread + grads[f]
                    moved = here + relax_weight * res / (weights + pairs[f])
                    state[q, f, xp, b : b + n] = jnp.where(pin, load * vector[f], moved)
                    square = res * res
                    squares = square if squares is None else squares + square
                return total + jnp.where(pin, 0.0, squares)

            return move

        return stiffen, mover

    def sweep(rnd, total):
        p = rnd % 2
        q = 1 - p
        done = rnd == sections - 1
        tough = r.tough_in.at[rnd - 1]

        stiffen, mover = stages(rnd)
        if rnd > 1:
            lax.fori_loop(HX - 2, HX + nx + 2, stiffen, 0, unroll=part(nx + 4, 10))
            total = lax.fori_loop(
                HX, HX + nx, mover(OY, ny), jnp.zeros((ny, nz), jnp.float32), unroll=part(nx, 8)
            )
        add_up(rnd, total)
        if done:
            send_sums()
        par = rnd % 2
        mid = pl.ds(OY, ny)
        if done:
            rims = Exchange(r.v_send, r.v_recv)
            for s in range(2):
                row = OY if s == 0 else OY + ny - 1
                for f in range(3):
                    r.pack_v[s, f] = state[q, f, planes, row : row + 1]
                rims.add(
                    x_dev(s),
                    state.at[q, pl.ds(0, 3), HX if s == 0 else HX + nx - 1, mid],
                    r.in_vx.at[1 - s],
                    r.in_vx.at[s],
                    1 - s,
                    s,
                )
                rims.add(
                    y_dev(s), r.pack_v.at[s], r.in_vy.at[1 - s], r.in_vy.at[s], 3 - s, 2 + s
                )
            rims.start()
            rims.received()
            for s in range(2):

                @pl.when(there["gx"][s])
                def _(s=s):
                    state[q, 0:3, x_at(s, 1), inner] = r.in_vx[s]

                @pl.when(there["gy"][s])
                def _(s=s):
                    for f in range(3):
                        state[q, f, planes, y_out(s, 1)] = r.in_vy[s, f]
        else:
            for f in range(3):
                r.pack_u[0, :, 2 * f : 2 * f + 2] = state[q, f, planes, OY : OY + 2]
                r.pack_u[1, :, 2 * f : 2 * f + 2] = state[q, f, planes, OY + ny - 2 : OY + ny]
            r.pack_u[0, :, 6:7] = state[q, 1, planes, OY + 2 : OY + 3]
            r.pack_u[1, :, 6:7] = state[q, 1, planes, OY + ny - 3 : OY + ny - 2]
            shift = Exchange(r.u_send, r.u_recv.at[par])
            for s in range(2):
                shift.add(
                    x_dev(s),
                    state.at[q, pl.ds(0, 3), pl.ds(HX if s == 0 else HX + nx - 2, 2), mid],
                    r.in_u_x.at[par, 1 - s],
                    r.in_u_x.at[par, s],
                    (1 - s),
                    s,
                )
                shift.add(
                    x_dev(s),
                    state.at[q, 0, HX + 2 if s == 0 else HX + nx - 3, mid],
                    r.in_u_x3.at[par, 1 - s],
                    r.in_u_x3.at[par, s],
                    2 + (1 - s),
                    2 + s,
                )
            for s in range(2):
                shift.add(
                    y_dev(s),
                    r.pack_u.at[s],
                    r.in_u_y.at[par, 1 - s],
                    r.in_u_y.at[par, s],
                    4 + (1 - s),
                    4 + s,
                )
            for sx in range(2):
                for sy in range(2):
                    shift.add(
                        c_dev(sx, sy),
                        r.pack_u.at[sy, pl.ds(0 if sx == 0 else nx - 2, 2)],
                        r.in_u_c.at[par, (1 - sx) * 2 + 1 - sy],
                        r.in_u_c.at[par, sx * 2 + sy],
                        6 + (1 - sx) * 2 + 1 - sy,
                        6 + sx * 2 + sy,
                    )
            shift.start()
            shift.finish()
            third_x = (HX - 3, HX + nx + 2)
            third_y = (slice(OY - 3, OY - 2), slice(OY + ny + 2, OY + ny + 3))
            for s in range(2):

                @pl.when(there["gx"][s])
                def _(s=s):
                    state[q, 0:3, x_out(s, 2), inner] = r.in_u_x[par, s]
                    state[q, 0, third_x[s], inner] = r.in_u_x3[par, s]

                @pl.when(there["gy"][s])
                def _(s=s):
                    for f in range(3):
                        state[q, f, planes, y_out(s, 2)] = r.in_u_y[par, s, :, 2 * f : 2 * f + 2]
                    state[q, 1, planes, third_y[s]] = r.in_u_y[par, s, :, 6:7]

            for sx in range(2):
                for sy in range(2):

                    @pl.when(c_dev(sx, sy)[0])
                    def _(sx=sx, sy=sy):
                        for f in range(3):
                            state[q, f, x_out(sx, 2), y_out(sy, 2)] = r.in_u_c[
                                par, sx * 2 + sy, :, 2 * f : 2 * f + 2
                            ]

        tough_copies[rnd - 1].wait_recv()

        shape = (ny, nz)
        first, last = lanes(shape, 0), lanes(shape, nz - 1)

        def damage(x, carry):
            xp = x + HX
            at = lambda ref, dx, dy: ref[xp + dx, OY + dy : OY + dy + ny]

            def keep(f, here):
                if done:
                    disp_refs[f][x] = here

            energy = strain_energy(at, state.at[q], keep, first, last)
            renewed = renew(
                at, state.at[p, 3], energy, tough[x], crack_ref[x] > 0, first, last
            )
            if done:
                r.dam_ref[x] = renewed
            else:
                state[q, 3, xp, inner] = renewed
            return carry

        lax.fori_loop(0, nx, damage, 0, unroll=part(nx, 8))
        if done:
            rims.sent()
            return

        r.pack_d[0] = state[q, 3, planes, OY : OY + 2]
        r.pack_d[1] = state[q, 3, planes, OY + ny - 2 : OY + ny]
        crack = Exchange(r.d_send, r.d_recv.at[par])
        for s in range(2):
            crack.add(
                x_dev(s),
                state.at[q, 3, pl.ds(HX if s == 0 else HX + nx - 2, 2), mid],
                r.in_d_x.at[par, 1 - s],
                r.in_d_x.at[par, s],
                1 - s,
                s,
            )
        for s in range(2):
            crack.add(
                y_dev(s),
                r.pack_d.at[s],
                r.in_d_y.at[par, 1 - s],
                r.in_d_y.at[par, s],
                2 + 1 - s,
                2 + s,
            )
        for sx in range(2):
            for sy in range(2):
                crack.add(
                    c_dev(sx, sy),
                    r.pack_d.at[sy, pl.ds(0 if sx == 0 else nx - 1, 1)],
                    r.in_d_c.at[par, (1 - sx) * 2 + 1 - sy],
                    r.in_d_c.at[par, sx * 2 + sy],
                    4 + (1 - sx) * 2 + 1 - sy,
                    4 + sx * 2 + sy,
                )
        crack.start()
        crack.finish()
        for s in range(2):

            @pl.when(there["gx"][s])
            def _(s=s):
                state[q, 3, x_out(s, 2), inner] = r.in_d_x[par, s]

            @pl.when(there["gy"][s])
            def _(s=s):
                state[q, 3, planes, y_out(s, 2)] = r.in_d_y[par, s]

        for sx in range(2):
            for sy in range(2):

                @pl.when(c_dev(sx, sy)[0])
                def _(sx=sx, sy=sy):
                    state[q, 3, x_out(sx, 1), y_out(sy, 2)] = r.in_d_c[par, sx * 2 + sy]

    total = open_sweep()
    for rnd in range(1, sections):
        sweep(rnd, total)

    beside_y.sent()
    part_a.sent()
    part_b.sent()
    for copy in tough_copies:
        copy.wait_send()
    for k, peer in enumerate(peers):
        other = peer["gx"] * ngy + peer["gy"]
        pltpu.make_async_remote_copy(
            src_ref=r.sums.at[me],
            dst_ref=r.sums.at[other],
            send_sem=r.sum_send.at[k],
            recv_sem=r.sum_recv.at[other],
            device_id=peer,
            device_id_type=MESH,
        ).wait()
    total = r.sums[0]
    for k in range(1, group):
        total = total + r.sums[k]
    r.total_ref[...] = total


def put_out(
    sizes,
    first_ref,
    second_ref,
    third_ref,
    dam_ref,
    total_ref,
    disp_hbm,
    dam_hbm,
    norm_hbm,
    norm_ref,
    sems,
):
    sections, ngx, ngy, nx, ny, nz = sizes
    copies = [
        pltpu.make_async_copy(ref, disp_hbm.at[0, f], sems.at[f])
        for f, ref in enumerate((first_ref, second_ref, third_ref))
    ]
    copies.append(pltpu.make_async_copy(dam_ref, dam_hbm.at[0], sems.at[3]))
    for copy in copies:
        copy.start()
    sec = lax.axis_index("section")
    cells = 3.0 * nx * ngx * ny * ngy * nz
    entries = jnp.sqrt(jnp.sum(total_ref[...], axis=1, keepdims=True) / cells)
    column = lax.broadcasted_iota(jnp.int32, (1, sections), 1)
    norms = jnp.zeros((1, sections), jnp.float32)
    for rnd in range(sections):
        norms = jnp.where(
            column == lax.rem(sec + rnd, sections), entries[rnd : rnd + 1], norms
        )
    norm_ref[...] = norms
    last = pltpu.make_async_copy(norm_ref, norm_hbm, sems.at[4])
    last.start()
    for copy in copies:
        copy.wait()
    last.wait()


def on_device(sizes, load_index, load_table, toughness, clamp_mask, load_mask, crack_mask):
    sections, ngx, ngy = sizes
    nx, ny, nz = clamp_mask.shape
    assert load_index.shape == (1,)
    group = ngx * ngy
    f32 = jnp.float32
    padded = (nx + 2 * HX, ny + 2 * OY, nz)
    vmem = pltpu.VMEM
    dma = pltpu.SemaphoreType.DMA
    later = max(sections - 1, 1)
    more = sections > 2
    scratch = {
        "index_ref": pltpu.SMEM(load_index.shape, jnp.int32),
        "table_ref": pltpu.SMEM(load_table.shape[::-1], f32),
        "tough_ref": vmem((1, nx, ny, nz), f32),
        "clamp_ref": vmem((nx, ny, nz), jnp.int32),
        "load_ref": vmem((nx, ny, nz), jnp.int32),
        "crack_ref": vmem((nx, ny, nz), jnp.int32),
        "local": dma((6,)),
        "state": vmem((2, 4) + padded, f32),
        "stiff": vmem(padded, f32),
        "flow": vmem(padded, f32),
        "held": vmem(padded, f32),
        "clamped": vmem(padded, f32),
        "tough_pad": vmem(padded, f32),
        "crack_pad": vmem(padded, f32),
        "tough_in": vmem((later, nx, ny, nz), f32),
        "pack_l": vmem((2, nx, 4, nz), jnp.int32),
        "pack_f": vmem((2, nx, 2, nz), jnp.int32),
        "pack_c": vmem((2, 3 * nx, nz), jnp.int32),
        "pack_t": vmem((2, nx, 1, nz), f32),
        "pack_k": vmem((4, 16, nz), jnp.int32),
        "in_a": vmem((2, 6, ny, nz), jnp.int32),
        "in_b": vmem((2, 3, ny, nz), jnp.int32),
        "in_tx": vmem((2, 1, ny, nz), f32),
        "in_l": vmem((2, nx, 4, nz), jnp.int32),
        "in_f": vmem((2, nx, 2, nz), jnp.int32),
        "in_c": vmem((2, 3 * nx, nz), jnp.int32),
        "in_ty": vmem((2, nx, 1, nz), f32),
        "in_k": vmem((4, 16, nz), jnp.int32),
        "rims": vmem((2, 8, nz), f32),
        "pack_v": vmem((2, 3, nx, 1, nz), f32),
        "in_vx": vmem((2, 3, ny, nz), f32),
        "in_vy": vmem((2, 3, nx, 1, nz), f32),
        "v_send": dma((4,)),
        "v_recv": dma((4,)),
        "sums": vmem((group, sections, nz), f32),
        "y_send": dma((8,)),
        "y_recv": dma((8,)),
        "a_send": dma((10,)),
        "a_recv": dma((10,)),
        "b_send": dma((8,)),
        "b_recv": dma((8,)),
        "reach": pltpu.SemaphoreType.REGULAR((max(max(ngx, ngy) - 2, 1),)),
        "tough_send": dma((later,)),
        "tough_recv": dma((later,)),
        "sum_send": dma((max(group - 1, 1),)),
        "sum_recv": dma((group,)),
    }
    if more:
        scratch |= {
            "pack_u": vmem((2, nx, 8, nz), f32),
            "pack_d": vmem((2, nx, 2, nz), f32),
            "in_u_x": vmem((2, 2, 3, 2, ny, nz), f32),
            "in_u_x3": vmem((2, 2, ny, nz), f32),
            "in_u_y": vmem((2, 2, nx, 8, nz), f32),
            "in_u_c": vmem((2, 4, 2, 8, nz), f32),
            "in_d_x": vmem((2, 2, 2, ny, nz), f32),
            "in_d_y": vmem((2, 2, nx, 2, nz), f32),
            "in_d_c": vmem((2, 4, 1, 2, nz), f32),
            "u_send": dma((10,)),
            "u_recv": dma((2, 10)),
            "d_send": dma((8,)),
            "d_recv": dma((2, 8)),
        }
    ins = ("index_hbm", "table_hbm", "tough_hbm", "clamp_hbm", "load_hbm", "crack_hbm")
    outs = ("first_ref", "second_ref", "third_ref", "dam_ref", "total_ref")
    names = (*ins, *outs, *scratch)
    block = pl.BlockSpec(memory_space=pltpu.VMEM)
    away = pl.BlockSpec(memory_space=pltpu.HBM)
    results = pl.pallas_call(
        functools.partial(kernel, (sections, ngx, ngy, nx, ny, nz), names),
        out_shape=(
            *[jax.ShapeDtypeStruct((nx, ny, nz), f32)] * 4,
            jax.ShapeDtypeStruct((sections, nz), f32),
        ),
        in_specs=[away] * 6,
        out_specs=(block,) * 5,
        scratch_shapes=list(scratch.values()),
        compiler_params=pltpu.CompilerParams(
            collective_id=0, has_side_effects=True, vmem_limit_bytes=56_020_000
        ),
    )(load_index, pltpu.with_memory_space_constraint(load_table.T, pltpu.HBM), toughness, clamp_mask, load_mask, crack_mask)
    return pl.pallas_call(
        functools.partial(put_out, (sections, ngx, ngy, nx, ny, nz)),
        out_shape=(
            jax.ShapeDtypeStruct((1, 3, nx, ny, nz), f32),
            jax.ShapeDtypeStruct((1, nx, ny, nz), f32),
            jax.ShapeDtypeStruct((1, sections), f32),
        ),
        in_specs=[block] * 5,
        out_specs=(away, away, away),
        scratch_shapes=[vmem((1, sections), f32), dma((5,))],
        compiler_params=pltpu.CompilerParams(vmem_limit_bytes=1024 * 1024),
    )(*results)


def solution(mesh):
    in_specs = (
        P("section"),
        P(),
        P("section", "gx", "gy", None),
        P("gx", "gy", None),
        P("gx", "gy", None),
        P("gx", "gy", None),
    )
    out_specs = (
        P("section", None, "gx", "gy", None),
        P("section", "gx", "gy", None),
        P("section", None),
    )
    sizes = tuple(mesh.shape[name] for name in ("section", "gx", "gy"))
    return jax.shard_map(
        functools.partial(on_device, sizes),
        mesh=mesh,
        in_specs=in_specs,
        out_specs=out_specs,
        check_vma=False,
    )
```

```python
import functools
import math
import types

import jax
import jax.numpy as jnp
from jax import lax
from jax.experimental import pallas as pl
from jax.experimental.pallas import tpu as pltpu
from jax.sharding import PartitionSpec as P

relax_weight = 0.6
stiff_floor = 0.001
eigen_guard = 1e-08
MESH = pl.DeviceIdType.MESH

HX = 5
OY = 8

ACOS = (
    1.5707963050,
    -0.2145988016,
    0.0889789874,
    -0.0501743046,
    0.0308918810,
    -0.0170881256,
    0.0066700901,
    -0.0012624911,
)


def up8(n):
    return -(-n // 8) * 8


def part(n, most):
    return max(k for k in range(1, most + 1) if n % k == 0)


def root(v):
    return v * lax.rsqrt(jnp.maximum(v, 1.2e-38))


def spectral_energy(xx, yy, zz, xy, xz, yz):
    trace = xx + yy + zz
    mid = trace * (1.0 / 3.0)
    dx = xx - mid
    dy = yy - mid
    dz = zz - mid
    xy2 = xy * xy
    xz2 = xz * xz
    yz2 = yz * yz
    sixth = (dx * dx + dy * dy + dz * dz + 2.0 * (xy2 + xz2 + yz2)) * (1.0 / 6.0)
    twice_radius = 2.0 * root(sixth)
    scale = lax.rsqrt(sixth + eigen_guard)
    det = dx * (dy * dz - yz2) - dz * xy2 - dy * xz2 + 2.0 * (xy * xz * yz)
    ratio = (0.5 * det * scale) * (scale * scale)
    size = jnp.minimum(jnp.abs(ratio), 1.0)
    poly = jnp.full_like(size, ACOS[-1] / 3.0)
    for c in ACOS[-2::-1]:
        poly = poly * size + c / 3.0
    t = root(1.0 - size) * poly
    t2 = t * t
    cos_t = 1.0 + t2 * (-0.5 + t2 * (1.0 / 24.0 + t2 * (-1.0 / 720.0 + t2 * (1.0 / 40320.0))))
    sin_t = t * (1.0 + t2 * (-1.0 / 6.0 + t2 * (1.0 / 120.0 + t2 * (-1.0 / 5040.0))))
    other = 0.5 * cos_t + math.sqrt(0.75) * sin_t
    upper = ratio >= 0.0
    first = jnp.where(upper, cos_t, other)
    last = jnp.where(upper, other, cos_t)
    largest = mid + twice_radius * first
    smallest = mid - twice_radius * last
    between = trace - largest - smallest
    relu = lambda v: jnp.maximum(v, 0.0)
    return (
        0.5 * jnp.square(relu(trace))
        + jnp.square(relu(largest))
        + jnp.square(relu(between))
        + jnp.square(relu(smallest))
    )


def kernel(sizes, names, *refs):
    sections, ngx, ngy, nx, ny, nz = sizes
    r = types.SimpleNamespace(**dict(zip(names, refs)))
    local, state, stiff, flow = r.local, r.state, r.stiff, r.flow
    held, clamped, tough_pad, crack_pad = r.held, r.clamped, r.tough_pad, r.crack_pad
    load_ref, crack_ref, clamp_ref, tough_ref = r.load_ref, r.crack_ref, r.clamp_ref, r.tough_ref
    disp_refs = (r.first_ref, r.second_ref, r.third_ref)
    sec = lax.axis_index("section")
    gx = lax.axis_index("gx")
    gy = lax.axis_index("gy")
    group = ngx * ngy
    me = gx * ngy + gy
    ring = lambda k, n: min(k, n - k)
    offsets = [(i, j) for i in range(ngx) for j in range(ngy) if i or j]
    offsets.sort(key=lambda o: (ring(o[0], ngx) + ring(o[1], ngy), o))
    peers = []
    for i, j in offsets:
        peers.append({"gx": lax.rem(gx + i, ngx), "gy": lax.rem(gy + j, ngy)})

    there = {
        "gx": (gx > 0, gx < ngx - 1),
        "gy": (gy > 0, gy < ngy - 1),
    }
    step = (-1, 1)

    def x_dev(s):
        return there["gx"][s], {"gx": gx + step[s]}

    def y_dev(s):
        return there["gy"][s], {"gy": gy + step[s]}

    def c_dev(sx, sy):
        return (
            jnp.logical_and(there["gx"][sx], there["gy"][sy]),
            {"gx": gx + step[sx], "gy": gy + step[sy]},
        )

    neighbours = [x_dev(s) for s in range(2)] + [y_dev(s) for s in range(2)]
    neighbours += [c_dev(sx, sy) for sx in range(2) for sy in range(2)]
    in_line = lambda name: sum(t.astype(jnp.int32) for t in there[name])
    near_count = (in_line("gx") + 1) * (in_line("gy") + 1) - 1

    def greet(sem):
        for cond, dev in neighbours:

            @pl.when(cond)
            def _(dev=dev):
                pl.semaphore_signal(sem, inc=1, device_id=dev, device_id_type=MESH)

    barrier = pltpu.get_barrier_semaphore()
    greet(barrier)
    for k in range(1, sections):
        pl.semaphore_signal(
            barrier,
            inc=1,
            device_id={"section": lax.rem(sec + k, sections)},
            device_id_type=MESH,
        )

    fetch = [
        pltpu.make_async_copy(src, dst, local.at[n])
        for n, (src, dst) in enumerate(
            (
                (r.load_hbm, load_ref),
                (r.crack_hbm, crack_ref),
                (r.clamp_hbm, clamp_ref),
                (r.tough_hbm, tough_ref),
                (r.index_hbm, r.index_ref),
                (r.table_hbm, r.table_ref),
            )
        )
    ]
    for copy in fetch:
        copy.start()

    class Exchange:
        def __init__(self, send, recv):
            self.items = []
            self.send = send
            self.recv = recv

        def add(self, where, src, dst, mine, out_slot, in_slot):
            cond, dev = where
            n = len(self.items)
            copy = pltpu.make_async_remote_copy(
                src_ref=src,
                dst_ref=dst,
                send_sem=self.send.at[n],
                recv_sem=self.recv.at[out_slot],
                device_id=dev,
                device_id_type=MESH,
            )
            back = pltpu.make_async_remote_copy(
                src_ref=src,
                dst_ref=mine,
                send_sem=self.send.at[n],
                recv_sem=self.recv.at[in_slot],
                device_id=dev,
                device_id_type=MESH,
            )
            self.items.append((cond, copy, back))

        def start(self, begin=0, end=None):
            for cond, copy, _ in self.items[begin:end]:
                pl.when(cond)(copy.start)

        def finish(self):
            for cond, copy, back in self.items:

                @pl.when(cond)
                def _():
                    back.wait_recv()
                    copy.wait_send()

        def received(self, begin=0, end=None):
            for cond, _, back in self.items[begin:end]:
                pl.when(cond)(back.wait_recv)

        def sent(self, begin=0, end=None):
            for cond, copy, _ in self.items[begin:end]:
                pl.when(cond)(copy.wait_send)

    rows = ny + 2 * OY

    def clear(xp, carry):
        zero = jnp.zeros((rows, nz), jnp.float32)
        held[xp] = zero
        crack_pad[xp] = zero
        clamped[xp] = zero + 1.0
        tough_pad[xp] = zero + 1.0
        for f in range(3):
            state[0, f, xp] = zero
        if sections > 2:
            state[0, 3, xp] = zero
            for f in range(4):
                state[1, f, xp] = zero
        return carry

    lax.fori_loop(0, nx + 2 * HX, clear, 0)

    for copy in fetch[:3]:
        copy.wait()

    for s in range(2):
        side = lambda n, s=s: slice(0, n) if s == 0 else slice(ny - n, ny)
        r.pack_l[s] = load_ref[:, side(4)]
        r.pack_f[s] = clamp_ref[:, side(2)]
        for x in range(nx):
            r.pack_c[s, 3 * x : 3 * x + 3] = crack_ref[x, side(3)]
    corner = (
        (load_ref, held, 1, 3, 0),
        (load_ref, held, 2, 2, 3),
        (load_ref, held, 3, 1, 5),
        (crack_ref, crack_pad, 1, 2, 6),
        (crack_ref, crack_pad, 2, 1, 8),
        (clamp_ref, clamped, 1, 1, 9),
    )

    def x_from(s, deep):
        return deep - 1 if s == 0 else nx - deep

    def x_at(s, deep):
        return HX - deep if s == 0 else HX + nx - 1 + deep

    for sx in range(2):
        for sy in range(2):
            for ref, _, deep, n, at in corner:
                first = 0 if sy == 0 else ny - n
                r.pack_k[sx * 2 + sy, at : at + n] = ref[x_from(sx, deep), first : first + n]

    pl.semaphore_wait(barrier, near_count + sections - 1)

    beside_y = Exchange(r.y_send, r.y_recv)
    part_a = Exchange(r.a_send, r.a_recv)
    part_m = Exchange(r.m_send, r.m_recv)
    part_b = Exchange(r.b_send, r.b_recv)
    for ex, ref, buf, deep, width, at, slot in (
        (part_a, load_ref, r.in_a, 2, 2, 0, 0),
        (part_a, crack_ref, r.in_a, 1, 1, 2, 2),
        (part_m, load_ref, r.in_m, 3, 1, 0, 0),
        (part_m, crack_ref, r.in_m, 2, 1, 1, 2),
        (part_m, clamp_ref, r.in_m, 1, 1, 2, 4),
        (part_b, load_ref, r.in_b, 4, 1, 0, 0),
        (part_b, crack_ref, r.in_b, 3, 1, 1, 2),
        (part_b, clamp_ref, r.in_b, 2, 1, 2, 4),
        (part_b, tough_ref.at[0], r.in_tx, 1, 1, 0, 6),
    ):
        for s in range(2):
            first = deep - width if s == 0 else nx - deep
            ex.add(
                x_dev(s),
                ref.at[pl.ds(first, width)],
                buf.at[1 - s, pl.ds(at, width)],
                buf.at[s, pl.ds(at, width)],
                slot + 1 - s,
                slot + s,
            )
    for n in range(8):
        s = n % 2
        for pack, buf, slot in (
            (r.pack_c, r.in_c, 0),
            (r.pack_l, r.in_l, 2),
            (r.pack_f, r.in_f, 4),
            (r.pack_t, r.in_ty, 6),
        )[n // 2 : n // 2 + 1]:
            beside_y.add(
                y_dev(s), pack.at[s], buf.at[1 - s], buf.at[s], slot + 1 - s, slot + s
            )
    for sx in range(2):
        for sy in range(2):
            here, away = sx * 2 + sy, (1 - sx) * 2 + 1 - sy
            part_a.add(
                c_dev(sx, sy), r.pack_k.at[here], r.in_k.at[away], r.in_k.at[here],
                4 + away, 4 + here,
            )
    beside_y.start(0, 4)
    part_a.start(0, 4)
    beside_y.start(4, 6)
    fetch[3].wait()
    for s in range(2):
        r.pack_t[s] = tough_ref[0, :, 0:1] if s == 0 else tough_ref[0, :, ny - 1 : ny]
    beside_y.start(6)
    part_a.start(4)
    part_m.start()
    part_b.start()
    further = max(ngx, ngy) - 2
    if further > 0:
        greet(r.reach.at[0])
    tough_copies = []
    for k in range(1, sections):
        copy = pltpu.make_async_remote_copy(
            src_ref=tough_ref.at[0],
            dst_ref=r.tough_in.at[k - 1],
            send_sem=r.tough_send.at[k - 1],
            recv_sem=r.tough_recv.at[k - 1],
            device_id={"section": lax.rem(sec + sections - k, sections)},
            device_id_type=MESH,
        )
        copy.start()
        tough_copies.append(copy)

    inner = slice(OY, OY + ny)
    as_float = lambda v: v.astype(jnp.float32)

    def fill(x, carry):
        held[x + HX, inner] = as_float(load_ref[x])
        clamped[x + HX, inner] = as_float(clamp_ref[x])
        crack_pad[x + HX, inner] = as_float(crack_ref[x])
        tough_pad[x + HX, inner] = tough_ref[0, x]
        return carry

    lax.fori_loop(0, nx, fill, 0, unroll=part(nx, 4))

    for copy in fetch[4:]:
        copy.wait()
    case = r.index_ref[0]
    vector = [r.table_ref[f, case] for f in range(3)]

    planes = slice(HX, HX + nx)

    def x_out(s, n):
        return slice(HX - n, HX) if s == 0 else slice(HX + nx, HX + nx + n)

    def y_out(s, n):
        return slice(OY - n, OY) if s == 0 else slice(OY + ny, OY + ny + n)

    def from_y(kind, s, put):
        beside_y.received(2 * kind + s, 2 * kind + s + 1)
        pl.when(there["gy"][s])(put)

    def unpack_a():
        part_a.received()
        for s in range(2):

            @pl.when(there["gx"][s])
            def _(s=s):
                held[x_out(s, 2), inner] = as_float(r.in_a[s, 0:2])
                crack_pad[x_out(s, 1), inner] = as_float(r.in_a[s, 2:3])

        for sx in range(2):
            for sy in range(2):

                @pl.when(c_dev(sx, sy)[0])
                def _(sx=sx, sy=sy):
                    for _, pad, deep, n, at in corner:
                        pad[x_at(sx, deep), y_out(sy, n)] = as_float(
                            r.in_k[sx * 2 + sy, at : at + n]
                        )

    def unpack_m():
        part_m.received()
        for s in range(2):

            @pl.when(there["gx"][s])
            def _(s=s):
                held[x_at(s, 3), inner] = as_float(r.in_m[s, 0])
                crack_pad[x_at(s, 2), inner] = as_float(r.in_m[s, 1])
                clamped[x_at(s, 1), inner] = as_float(r.in_m[s, 2])

    def unpack_b():
        part_b.received()
        for s in range(2):

            @pl.when(there["gx"][s])
            def _(s=s):
                held[x_at(s, 4), inner] = as_float(r.in_b[s, 0])
                crack_pad[x_at(s, 3), inner] = as_float(r.in_b[s, 1])
                clamped[x_at(s, 2), inner] = as_float(r.in_b[s, 2])
                tough_pad[x_at(s, 1), inner] = r.in_tx[s, 0]

    wide = up8(ny + 4)
    deep = up8(ny + 8)

    def lanes(shape, lane):
        return lax.broadcasted_iota(jnp.int32, shape, 1) == lane

    def beside(v, edge, first, last):
        up = jnp.where(last, edge, pltpu.roll(v, nz - 1, 1))
        down = jnp.where(first, edge, pltpu.roll(v, 1, 1))
        return up, down

    def inside_rows(shape, above):
        row = lax.broadcasted_iota(jnp.int32, shape, 0) + (gy * ny - above)
        return jnp.logical_and(row >= 0, row < ny * ngy)

    def inside_plane(xp):
        plane = xp - HX + gx * nx
        return jnp.logical_and(plane >= 0, plane < nx * ngx)

    edge_stiff = 0.5 * (1.0 + stiff_floor)

    def elastic(at, first, last):
        k = at(stiff, 0, 0)
        sides = (
            (at(stiff, 1, 0), at(stiff, -1, 0)),
            (at(stiff, 0, 1), at(stiff, 0, -1)),
            beside(k, edge_stiff, first, last),
        )
        pairs = [s[0] + s[1] for s in sides]
        weights = pairs[0] + pairs[1] + pairs[2] + 6.0 * k
        faces = [(k + s[0], k + s[1]) for s in sides]
        fz = beside(at(flow, 0, 0), 0.0, first, last)
        grads = (
            at(flow, 1, 0) - at(flow, -1, 0),
            at(flow, 0, 1) - at(flow, 0, -1),
            fz[0] - fz[1],
        )
        return pairs, weights, faces, grads

    def laplace(at, ref, faces, weights, first, last):
        here = at(ref, 0, 0)
        uz = beside(here, 0.0, first, last)
        return here, (
            faces[0][0] * at(ref, 1, 0)
            + faces[0][1] * at(ref, -1, 0)
            + faces[1][0] * at(ref, 0, 1)
            + faces[1][1] * at(ref, 0, -1)
            + faces[2][0] * uz[0]
            + faces[2][1] * uz[1]
            - weights * here
        )

    def strain_energy(at, u, keep, first, last):
        grad = []
        for f in range(3):
            here = at(u.at[f], 0, 0)
            uz = beside(here, 0.0, first, last)
            grad.append(
                (
                    at(u.at[f], 1, 0) - at(u.at[f], -1, 0),
                    at(u.at[f], 0, 1) - at(u.at[f], 0, -1),
                    uz[0] - uz[1],
                )
            )
            keep(f, here)
        return 2.0 * spectral_energy(
            0.5 * grad[0][0],
            0.5 * grad[1][1],
            0.5 * grad[2][2],
            0.25 * (grad[0][1] + grad[1][0]),
            0.25 * (grad[0][2] + grad[2][0]),
            0.25 * (grad[1][2] + grad[2][1]),
        )

    def renew(at, d, energy, g, cracked, first, last):
        dz = beside(at(d, 0, 0), 0.0, first, last)
        around = at(d, 1, 0) + at(d, -1, 0) + at(d, 0, 1) + at(d, 0, -1) + dz[0] + dz[1]
        renewed = (energy + g * around) / (7.0 * g + energy)
        return jnp.where(cracked, 1.0, renewed)

    def add_up(rnd, total):
        r.sums[me, rnd : rnd + 1] = jnp.sum(total, axis=0, keepdims=True)

    def open_stages(above, n):
        shape = (n, nz)
        first, last = lanes(shape, 0), lanes(shape, nz - 1)
        row_inside = inside_rows(shape, above)
        row = lax.broadcasted_iota(jnp.int32, shape, 0)
        a = OY - above

        def stiffen(xp, carry):
            half = 0.5 * (jnp.square(1.0 - crack_pad[xp, a : a + n]) + stiff_floor)
            stiff[xp, a : a + n] = half
            up, down = beside(held[xp, a : a + n], 0.0, first, last)
            div = (
                vector[0] * (held[xp + 1, a : a + n] - held[xp - 1, a : a + n])
                + vector[1] * (held[xp, a + 1 : a + 1 + n] - held[xp, a - 1 : a - 1 + n])
                + vector[2] * (up - down)
            )
            flow[xp, a : a + n] = jnp.where(
                jnp.logical_and(row_inside, inside_plane(xp)), half * div, 0.0
            )
            return carry

        def mover(low, high):
            def move(xp, total):
                at = lambda ref, dx, dy: ref[xp + dx, a + dy : a + dy + n]
                pairs, weights, faces, grads = elastic(at, first, last)
                load, spread = laplace(at, held, faces, weights, first, last)
                pin = at(clamped, 0, 0) + load > 0.5
                squares = None
                for f in range(3):
                    res = vector[f] * spread + grads[f]
                    moved = jnp.where(pin, 0.0, relax_weight * res / (weights + pairs[f]))
                    state[1, f, xp, a : a + n] = vector[f] * load + moved
                    square = res * res
                    squares = square if squares is None else squares + square
                if low >= high:
                    return total
                counted = jnp.logical_and(row >= low + above, row < high + above)
                return total + jnp.where(
                    jnp.logical_and(counted, jnp.logical_not(pin)), squares, 0.0
                )

            return move

        def damage(xp, carry):
            at = lambda ref, dx, dy: ref[xp + dx, a + dy : a + dy + n]
            energy = strain_energy(at, state.at[1], lambda f, v: None, first, last)
            renewed = renew(
                at,
                crack_pad,
                energy,
                at(tough_pad, 0, 0),
                at(crack_pad, 0, 0) > 0.5,
                first,
                last,
            )
            state[1, 3, xp, a : a + n] = jnp.where(
                jnp.logical_and(row_inside, inside_plane(xp)), renewed, 0.0
            )
            return carry

        return stiffen, mover, damage

    def open_sweep():
        def inward(skip, body, carry, most):
            n = nx - 2 * skip
            return lax.fori_loop(HX + skip, HX + nx - skip, body, carry, unroll=part(n, most))

        def outward(far, n, body, carry):
            def both(i, carry):
                carry = body(HX - far + i, carry)
                return body(HX + nx + far - n + i, carry)

            return lax.fori_loop(0, n, both, carry, unroll=True)

        blank = lambda n: jnp.zeros((n, nz), jnp.float32)
        fold = lambda v: jnp.sum(v, axis=0, keepdims=True)

        stiffen, mover, damage = open_stages(0, ny)
        inward(1, stiffen, 0, 14)
        inside = inward(2, mover(2, ny - 2), blank(ny), 12)
        inward(3, damage, 0, 5)

        if further > 1:
            pl.semaphore_wait(r.reach.at[0], near_count)
            greet(r.reach.at[1])

        def rim(s):
            above = (4, 4 - ny)[s]
            stiffen, mover, damage = open_stages(above, 8)

            def put_crack():
                for x in range(nx):
                    crack_pad[HX + x, y_out(s, 3)] = as_float(r.in_c[s, 3 * x : 3 * x + 3])

            def put_load():
                held[planes, y_out(s, 4)] = as_float(r.in_l[s])

            def put_clamp():
                clamped[planes, y_out(s, 2)] = as_float(r.in_f[s])

            def put_tough():
                tough_pad[planes, y_out(s, 1)] = r.in_ty[s]

            from_y(0, s, put_crack)
            from_y(1, s, put_load)
            inward(1, stiffen, 0, 14)
            from_y(2, s, put_clamp)
            counted = (0, 2) if s == 0 else (ny - 2, ny)
            r.rims[s] = inward(2, mover(*counted), blank(8), 12)
            from_y(3, s, put_tough)
            inward(3, damage, 0, 10)

        odd = lax.rem(gy, 2) == 1

        @pl.when(odd)
        def _():
            rim(0)
            rim(1)

        @pl.when(jnp.logical_not(odd))
        def _():
            rim(1)
            rim(0)

        stiffen1, mover1 = stages(1)
        move1 = mover1(OY, ny)
        inward(3, stiffen1, 0, 10)
        own = inward(4, move1, blank(ny), 8)

        stiffen, mover, damage = open_stages(4, deep)
        unpack_a()
        outward(1, 2, stiffen, 0)
        ends = outward(0, 2, mover(0, ny), blank(deep))
        r.sums[me, 0:1] = fold(inside) + fold(r.rims[0] + r.rims[1]) + fold(ends)
        outward(-1, 2, damage, 0)
        outward(-1, 2, stiffen1, 0)
        own = outward(-2, 2, move1, own)

        unpack_m()
        outward(2, 1, stiffen, 0)
        outward(1, 1, mover(0, 0), blank(deep))
        outward(0, 1, damage, 0)
        outward(0, 1, stiffen1, 0)
        own = outward(-1, 1, move1, own)

        unpack_b()
        outward(3, 1, stiffen, 0)
        outward(2, 1, mover(0, 0), blank(deep))
        outward(1, 1, damage, 0)
        outward(1, 1, stiffen1, 0)
        own = outward(0, 1, move1, own)

        return own

    def send_sums():
        for k in range(1 if further > 1 else 0, further):
            pl.semaphore_wait(r.reach.at[k], near_count)
            if k + 1 < further:
                greet(r.reach.at[k + 1])
        for k, peer in enumerate(peers):
            pltpu.make_async_remote_copy(
                src_ref=r.sums.at[me],
                dst_ref=r.sums.at[me],
                send_sem=r.sum_send.at[k],
                recv_sem=r.sum_recv.at[me],
                device_id=peer,
                device_id_type=MESH,
            ).start()

    def stages(rnd):
        p = rnd % 2
        q = 1 - p
        shape = (wide, nz)
        first, last = lanes(shape, 0), lanes(shape, nz - 1)
        row_inside = inside_rows(shape, 2)
        a = OY - 2

        def stiffen(xp, carry):
            half = 0.5 * (jnp.square(1.0 - state[p, 3, xp, a : a + wide]) + stiff_floor)
            stiff[xp, a : a + wide] = half
            up, down = beside(state[p, 2, xp, a : a + wide], 0.0, first, last)
            div = (
                (state[p, 0, xp + 1, a : a + wide] - state[p, 0, xp - 1, a : a + wide])
                + (state[p, 1, xp, a + 1 : a + 1 + wide] - state[p, 1, xp, a - 1 : a - 1 + wide])
                + (up - down)
            )
            flow[xp, a : a + wide] = jnp.where(
                jnp.logical_and(row_inside, inside_plane(xp)), half * div, 0.0
            )
            return carry

        def mover(b, n):
            shape = (n, nz)
            first, last = lanes(shape, 0), lanes(shape, nz - 1)

            def move(xp, total):
                at = lambda ref, dx, dy: ref[xp + dx, b + dy : b + dy + n]
                pairs, weights, faces, grads = elastic(at, first, last)
                load = at(held, 0, 0)
                pin = at(clamped, 0, 0) + load > 0.5
                squares = None
                for f in range(3):
                    here, spread = laplace(at, state.at[p, f], faces, weights, first, last)
                    res = spread + grads[f]
                    moved = here + relax_weight * res / (weights + pairs[f])
                    state[q, f, xp, b : b + n] = jnp.where(pin, load * vector[f], moved)
                    square = res * res
                    squares = square if squares is None else squares + square
                return total + jnp.where(pin, 0.0, squares)

            return move

        return stiffen, mover

    def sweep(rnd, total):
        p = rnd % 2
        q = 1 - p
        done = rnd == sections - 1
        tough = r.tough_in.at[rnd - 1]

        stiffen, mover = stages(rnd)
        if rnd > 1:
            lax.fori_loop(HX - 2, HX + nx + 2, stiffen, 0, unroll=part(nx + 4, 10))
            total = lax.fori_loop(
                HX, HX + nx, mover(OY, ny), jnp.zeros((ny, nz), jnp.float32), unroll=part(nx, 8)
            )
        add_up(rnd, total)
        if done:
            send_sums()
        par = rnd % 2
        mid = pl.ds(OY, ny)
        if done:
            rims = Exchange(r.v_send, r.v_recv)
            for s in range(2):
                row = OY if s == 0 else OY + ny - 1
                for f in range(3):
                    r.pack_v[s, f] = state[q, f, planes, row : row + 1]
                rims.add(
                    x_dev(s),
                    state.at[q, pl.ds(0, 3), HX if s == 0 else HX + nx - 1, mid],
                    r.in_vx.at[1 - s],
                    r.in_vx.at[s],
                    1 - s,
                    s,
                )
                rims.add(
                    y_dev(s), r.pack_v.at[s], r.in_vy.at[1 - s], r.in_vy.at[s], 3 - s, 2 + s
                )
            rims.start()
            rims.received()
            for s in range(2):

                @pl.when(there["gx"][s])
                def _(s=s):
                    state[q, 0:3, x_at(s, 1), inner] = r.in_vx[s]

                @pl.when(there["gy"][s])
                def _(s=s):
                    for f in range(3):
                        state[q, f, planes, y_out(s, 1)] = r.in_vy[s, f]
        else:
            for f in range(3):
                r.pack_u[0, :, 2 * f : 2 * f + 2] = state[q, f, planes, OY : OY + 2]
                r.pack_u[1, :, 2 * f : 2 * f + 2] = state[q, f, planes, OY + ny - 2 : OY + ny]
            r.pack_u[0, :, 6:7] = state[q, 1, planes, OY + 2 : OY + 3]
            r.pack_u[1, :, 6:7] = state[q, 1, planes, OY + ny - 3 : OY + ny - 2]
            shift = Exchange(r.u_send, r.u_recv.at[par])
            for s in range(2):
                shift.add(
                    x_dev(s),
                    state.at[q, pl.ds(0, 3), pl.ds(HX if s == 0 else HX + nx - 2, 2), mid],
                    r.in_u_x.at[par, 1 - s],
                    r.in_u_x.at[par, s],
                    (1 - s),
                    s,
                )
                shift.add(
                    x_dev(s),
                    state.at[q, 0, HX + 2 if s == 0 else HX + nx - 3, mid],
                    r.in_u_x3.at[par, 1 - s],
                    r.in_u_x3.at[par, s],
                    2 + (1 - s),
                    2 + s,
                )
            for s in range(2):
                shift.add(
                    y_dev(s),
                    r.pack_u.at[s],
                    r.in_u_y.at[par, 1 - s],
                    r.in_u_y.at[par, s],
                    4 + (1 - s),
                    4 + s,
                )
            for sx in range(2):
                for sy in range(2):
                    shift.add(
                        c_dev(sx, sy),
                        r.pack_u.at[sy, pl.ds(0 if sx == 0 else nx - 2, 2)],
                        r.in_u_c.at[par, (1 - sx) * 2 + 1 - sy],
                        r.in_u_c.at[par, sx * 2 + sy],
                        6 + (1 - sx) * 2 + 1 - sy,
                        6 + sx * 2 + sy,
                    )
            shift.start()
            shift.finish()
            third_x = (HX - 3, HX + nx + 2)
            third_y = (slice(OY - 3, OY - 2), slice(OY + ny + 2, OY + ny + 3))
            for s in range(2):

                @pl.when(there["gx"][s])
                def _(s=s):
                    state[q, 0:3, x_out(s, 2), inner] = r.in_u_x[par, s]
                    state[q, 0, third_x[s], inner] = r.in_u_x3[par, s]

                @pl.when(there["gy"][s])
                def _(s=s):
                    for f in range(3):
                        state[q, f, planes, y_out(s, 2)] = r.in_u_y[par, s, :, 2 * f : 2 * f + 2]
                    state[q, 1, planes, third_y[s]] = r.in_u_y[par, s, :, 6:7]

            for sx in range(2):
                for sy in range(2):

                    @pl.when(c_dev(sx, sy)[0])
                    def _(sx=sx, sy=sy):
                        for f in range(3):
                            state[q, f, x_out(sx, 2), y_out(sy, 2)] = r.in_u_c[
                                par, sx * 2 + sy, :, 2 * f : 2 * f + 2
                            ]

        tough_copies[rnd - 1].wait_recv()

        shape = (ny, nz)
        first, last = lanes(shape, 0), lanes(shape, nz - 1)

        def damage(x, carry):
            xp = x + HX
            at = lambda ref, dx, dy: ref[xp + dx, OY + dy : OY + dy + ny]

            def keep(f, here):
                if done:
                    disp_refs[f][x] = here

            energy = strain_energy(at, state.at[q], keep, first, last)
            renewed = renew(
                at, state.at[p, 3], energy, tough[x], crack_ref[x] > 0, first, last
            )
            if done:
                r.dam_ref[x] = renewed
            else:
                state[q, 3, xp, inner] = renewed
            return carry

        lax.fori_loop(0, nx, damage, 0, unroll=part(nx, 8))
        if done:
            rims.sent()
            return

        r.pack_d[0] = state[q, 3, planes, OY : OY + 2]
        r.pack_d[1] = state[q, 3, planes, OY + ny - 2 : OY + ny]
        crack = Exchange(r.d_send, r.d_recv.at[par])
        for s in range(2):
            crack.add(
                x_dev(s),
                state.at[q, 3, pl.ds(HX if s == 0 else HX + nx - 2, 2), mid],
                r.in_d_x.at[par, 1 - s],
                r.in_d_x.at[par, s],
                1 - s,
                s,
            )
        for s in range(2):
            crack.add(
                y_dev(s),
                r.pack_d.at[s],
                r.in_d_y.at[par, 1 - s],
                r.in_d_y.at[par, s],
                2 + 1 - s,
                2 + s,
            )
        for sx in range(2):
            for sy in range(2):
                crack.add(
                    c_dev(sx, sy),
                    r.pack_d.at[sy, pl.ds(0 if sx == 0 else nx - 1, 1)],
                    r.in_d_c.at[par, (1 - sx) * 2 + 1 - sy],
                    r.in_d_c.at[par, sx * 2 + sy],
                    4 + (1 - sx) * 2 + 1 - sy,
                    4 + sx * 2 + sy,
                )
        crack.start()
        crack.finish()
        for s in range(2):

            @pl.when(there["gx"][s])
            def _(s=s):
                state[q, 3, x_out(s, 2), inner] = r.in_d_x[par, s]

            @pl.when(there["gy"][s])
            def _(s=s):
                state[q, 3, planes, y_out(s, 2)] = r.in_d_y[par, s]

        for sx in range(2):
            for sy in range(2):

                @pl.when(c_dev(sx, sy)[0])
                def _(sx=sx, sy=sy):
                    state[q, 3, x_out(sx, 1), y_out(sy, 2)] = r.in_d_c[par, sx * 2 + sy]

    total = open_sweep()
    for rnd in range(1, sections):
        sweep(rnd, total)

    beside_y.sent()
    part_a.sent()
    part_m.sent()
    part_b.sent()
    for copy in tough_copies:
        copy.wait_send()
    for k, peer in enumerate(peers):
        other = peer["gx"] * ngy + peer["gy"]
        pltpu.make_async_remote_copy(
            src_ref=r.sums.at[me],
            dst_ref=r.sums.at[other],
            send_sem=r.sum_send.at[k],
            recv_sem=r.sum_recv.at[other],
            device_id=peer,
            device_id_type=MESH,
        ).wait()
    total = r.sums[0]
    for k in range(1, group):
        total = total + r.sums[k]
    r.total_ref[...] = total


def put_out(
    sizes,
    first_ref,
    second_ref,
    third_ref,
    dam_ref,
    total_ref,
    disp_hbm,
    dam_hbm,
    norm_hbm,
    norm_ref,
    sems,
):
    sections, ngx, ngy, nx, ny, nz = sizes
    copies = [
        pltpu.make_async_copy(ref, disp_hbm.at[0, f], sems.at[f])
        for f, ref in enumerate((first_ref, second_ref, third_ref))
    ]
    copies.append(pltpu.make_async_copy(dam_ref, dam_hbm.at[0], sems.at[3]))
    for copy in copies:
        copy.start()
    sec = lax.axis_index("section")
    cells = 3.0 * nx * ngx * ny * ngy * nz
    entries = jnp.sqrt(jnp.sum(total_ref[...], axis=1, keepdims=True) / cells)
    column = lax.broadcasted_iota(jnp.int32, (1, sections), 1)
    norms = jnp.zeros((1, sections), jnp.float32)
    for rnd in range(sections):
        norms = jnp.where(
            column == lax.rem(sec + rnd, sections), entries[rnd : rnd + 1], norms
        )
    norm_ref[...] = norms
    last = pltpu.make_async_copy(norm_ref, norm_hbm, sems.at[4])
    last.start()
    for copy in copies:
        copy.wait()
    last.wait()


def on_device(sizes, load_index, load_table, toughness, clamp_mask, load_mask, crack_mask):
    sections, ngx, ngy = sizes
    nx, ny, nz = clamp_mask.shape
    assert load_index.shape == (1,)
    group = ngx * ngy
    f32 = jnp.float32
    padded = (nx + 2 * HX, ny + 2 * OY, nz)
    vmem = pltpu.VMEM
    dma = pltpu.SemaphoreType.DMA
    later = max(sections - 1, 1)
    more = sections > 2
    scratch = {
        "index_ref": pltpu.SMEM(load_index.shape, jnp.int32),
        "table_ref": pltpu.SMEM(load_table.shape[::-1], f32),
        "tough_ref": vmem((1, nx, ny, nz), f32),
        "clamp_ref": vmem((nx, ny, nz), jnp.int32),
        "load_ref": vmem((nx, ny, nz), jnp.int32),
        "crack_ref": vmem((nx, ny, nz), jnp.int32),
        "local": dma((6,)),
        "state": vmem((2, 4) + padded, f32),
        "stiff": vmem(padded, f32),
        "flow": vmem(padded, f32),
        "held": vmem(padded, f32),
        "clamped": vmem(padded, f32),
        "tough_pad": vmem(padded, f32),
        "crack_pad": vmem(padded, f32),
        "tough_in": vmem((later, nx, ny, nz), f32),
        "pack_l": vmem((2, nx, 4, nz), jnp.int32),
        "pack_f": vmem((2, nx, 2, nz), jnp.int32),
        "pack_c": vmem((2, 3 * nx, nz), jnp.int32),
        "pack_t": vmem((2, nx, 1, nz), f32),
        "pack_k": vmem((4, 16, nz), jnp.int32),
        "in_a": vmem((2, 3, ny, nz), jnp.int32),
        "in_m": vmem((2, 3, ny, nz), jnp.int32),
        "in_b": vmem((2, 3, ny, nz), jnp.int32),
        "in_tx": vmem((2, 1, ny, nz), f32),
        "in_l": vmem((2, nx, 4, nz), jnp.int32),
        "in_f": vmem((2, nx, 2, nz), jnp.int32),
        "in_c": vmem((2, 3 * nx, nz), jnp.int32),
        "in_ty": vmem((2, nx, 1, nz), f32),
        "in_k": vmem((4, 16, nz), jnp.int32),
        "rims": vmem((2, 8, nz), f32),
        "pack_v": vmem((2, 3, nx, 1, nz), f32),
        "in_vx": vmem((2, 3, ny, nz), f32),
        "in_vy": vmem((2, 3, nx, 1, nz), f32),
        "v_send": dma((4,)),
        "v_recv": dma((4,)),
        "sums": vmem((group, sections, nz), f32),
        "y_send": dma((8,)),
        "y_recv": dma((8,)),
        "a_send": dma((8,)),
        "a_recv": dma((8,)),
        "m_send": dma((6,)),
        "m_recv": dma((6,)),
        "b_send": dma((8,)),
        "b_recv": dma((8,)),
        "reach": pltpu.SemaphoreType.REGULAR((max(max(ngx, ngy) - 2, 1),)),
        "tough_send": dma((later,)),
        "tough_recv": dma((later,)),
        "sum_send": dma((max(group - 1, 1),)),
        "sum_recv": dma((group,)),
    }
    if more:
        scratch |= {
            "pack_u": vmem((2, nx, 8, nz), f32),
            "pack_d": vmem((2, nx, 2, nz), f32),
            "in_u_x": vmem((2, 2, 3, 2, ny, nz), f32),
            "in_u_x3": vmem((2, 2, ny, nz), f32),
            "in_u_y": vmem((2, 2, nx, 8, nz), f32),
            "in_u_c": vmem((2, 4, 2, 8, nz), f32),
            "in_d_x": vmem((2, 2, 2, ny, nz), f32),
            "in_d_y": vmem((2, 2, nx, 2, nz), f32),
            "in_d_c": vmem((2, 4, 1, 2, nz), f32),
            "u_send": dma((10,)),
            "u_recv": dma((2, 10)),
            "d_send": dma((8,)),
            "d_recv": dma((2, 8)),
        }
    ins = ("index_hbm", "table_hbm", "tough_hbm", "clamp_hbm", "load_hbm", "crack_hbm")
    outs = ("first_ref", "second_ref", "third_ref", "dam_ref", "total_ref")
    names = (*ins, *outs, *scratch)
    block = pl.BlockSpec(memory_space=pltpu.VMEM)
    away = pl.BlockSpec(memory_space=pltpu.HBM)
    results = pl.pallas_call(
        functools.partial(kernel, (sections, ngx, ngy, nx, ny, nz), names),
        out_shape=(
            *[jax.ShapeDtypeStruct((nx, ny, nz), f32)] * 4,
            jax.ShapeDtypeStruct((sections, nz), f32),
        ),
        in_specs=[away] * 6,
        out_specs=(block,) * 5,
        scratch_shapes=list(scratch.values()),
        compiler_params=pltpu.CompilerParams(
            collective_id=0, has_side_effects=True, vmem_limit_bytes=56_020_000
        ),
    )(load_index, pltpu.with_memory_space_constraint(load_table.T, pltpu.HBM), toughness, clamp_mask, load_mask, crack_mask)
    return pl.pallas_call(
        functools.partial(put_out, (sections, ngx, ngy, nx, ny, nz)),
        out_shape=(
            jax.ShapeDtypeStruct((1, 3, nx, ny, nz), f32),
            jax.ShapeDtypeStruct((1, nx, ny, nz), f32),
            jax.ShapeDtypeStruct((1, sections), f32),
        ),
        in_specs=[block] * 5,
        out_specs=(away, away, away),
        scratch_shapes=[vmem((1, sections), f32), dma((5,))],
        compiler_params=pltpu.CompilerParams(vmem_limit_bytes=1024 * 1024),
    )(*results)


def solution(mesh):
    in_specs = (
        P("section"),
        P(),
        P("section", "gx", "gy", None),
        P("gx", "gy", None),
        P("gx", "gy", None),
        P("gx", "gy", None),
    )
    out_specs = (
        P("section", None, "gx", "gy", None),
        P("section", "gx", "gy", None),
        P("section", None),
    )
    sizes = tuple(mesh.shape[name] for name in ("section", "gx", "gy"))
    return jax.shard_map(
        functools.partial(on_device, sizes),
        mesh=mesh,
        in_specs=in_specs,
        out_specs=out_specs,
        check_vma=False,
    )
```

```python
import functools
import math
import types

import jax
import jax.numpy as jnp
from jax import lax
from jax.experimental import pallas as pl
from jax.experimental.pallas import tpu as pltpu
from jax.sharding import PartitionSpec as P

relax_weight = 0.6
stiff_floor = 0.001
eigen_guard = 1e-08
MESH = pl.DeviceIdType.MESH

HX = 5
OY = 8

ACOS = (
    1.5707963050,
    -0.2145988016,
    0.0889789874,
    -0.0501743046,
    0.0308918810,
    -0.0170881256,
    0.0066700901,
    -0.0012624911,
)


def up8(n):
    return -(-n // 8) * 8


def part(n, most):
    return max(k for k in range(1, most + 1) if n % k == 0)


def root(v):
    return v * lax.rsqrt(jnp.maximum(v, 1.2e-38))


def spectral_energy(xx, yy, zz, xy, xz, yz):
    trace = xx + yy + zz
    mid = trace * (1.0 / 3.0)
    dx = xx - mid
    dy = yy - mid
    dz = zz - mid
    xy2 = 0.25 * (xy * xy)
    xz2 = 0.25 * (xz * xz)
    yz2 = 0.25 * (yz * yz)
    sixth = (dx * dx + dy * dy + dz * dz + 2.0 * (xy2 + xz2 + yz2)) * (1.0 / 6.0)
    twice_radius = 2.0 * root(sixth)
    scale = lax.rsqrt(sixth + 4.0 * eigen_guard)
    det = dx * (dy * dz - yz2) - dz * xy2 - dy * xz2 + 0.25 * (xy * xz * yz)
    ratio = (0.5 * det * scale) * (scale * scale)
    size = jnp.minimum(jnp.abs(ratio), 1.0)
    poly = jnp.full_like(size, ACOS[-1] / 3.0)
    for c in ACOS[-2::-1]:
        poly = poly * size + c / 3.0
    t = root(1.0 - size) * poly
    t2 = t * t
    cos_t = 1.0 + t2 * (-0.5 + t2 * (1.0 / 24.0 + t2 * (-1.0 / 720.0 + t2 * (1.0 / 40320.0))))
    sin_t = t * (1.0 + t2 * (-1.0 / 6.0 + t2 * (1.0 / 120.0 + t2 * (-1.0 / 5040.0))))
    other = 0.5 * cos_t + math.sqrt(0.75) * sin_t
    upper = ratio >= 0.0
    first = jnp.where(upper, cos_t, other)
    last = jnp.where(upper, other, cos_t)
    largest = mid + twice_radius * first
    smallest = mid - twice_radius * last
    between = trace - largest - smallest
    relu = lambda v: jnp.maximum(v, 0.0)
    return (
        0.5 * jnp.square(relu(trace))
        + jnp.square(relu(largest))
        + jnp.square(relu(between))
        + jnp.square(relu(smallest))
    )


def kernel(sizes, names, *refs):
    sections, ngx, ngy, nx, ny, nz = sizes
    r = types.SimpleNamespace(**dict(zip(names, refs)))
    local, state, stiff, flow = r.local, r.state, r.stiff, r.flow
    held, clamped, tough_pad, crack_pad = r.held, r.clamped, r.tough_pad, r.crack_pad
    load_ref, crack_ref, clamp_ref, tough_ref = r.load_ref, r.crack_ref, r.clamp_ref, r.tough_ref
    disp_refs = (r.first_ref, r.second_ref, r.third_ref)
    sec = lax.axis_index("section")
    gx = lax.axis_index("gx")
    gy = lax.axis_index("gy")
    group = ngx * ngy
    me = gx * ngy + gy
    ring = lambda k, n: min(k, n - k)
    offsets = [(i, j) for i in range(ngx) for j in range(ngy) if i or j]
    offsets.sort(key=lambda o: (ring(o[0], ngx) + ring(o[1], ngy), o))
    peers = []
    for i, j in offsets:
        peers.append({"gx": lax.rem(gx + i, ngx), "gy": lax.rem(gy + j, ngy)})

    there = {
        "gx": (gx > 0, gx < ngx - 1),
        "gy": (gy > 0, gy < ngy - 1),
    }
    step = (-1, 1)

    def x_dev(s):
        return there["gx"][s], {"gx": gx + step[s]}

    def y_dev(s):
        return there["gy"][s], {"gy": gy + step[s]}

    def c_dev(sx, sy):
        return (
            jnp.logical_and(there["gx"][sx], there["gy"][sy]),
            {"gx": gx + step[sx], "gy": gy + step[sy]},
        )

    neighbours = [x_dev(s) for s in range(2)] + [y_dev(s) for s in range(2)]
    neighbours += [c_dev(sx, sy) for sx in range(2) for sy in range(2)]
    in_line = lambda name: sum(t.astype(jnp.int32) for t in there[name])
    near_count = (in_line("gx") + 1) * (in_line("gy") + 1) - 1

    def greet(sem):
        for cond, dev in neighbours:

            @pl.when(cond)
            def _(dev=dev):
                pl.semaphore_signal(sem, inc=1, device_id=dev, device_id_type=MESH)

    barrier = pltpu.get_barrier_semaphore()
    greet(barrier)
    for k in range(1, sections):
        pl.semaphore_signal(
            barrier,
            inc=1,
            device_id={"section": lax.rem(sec + k, sections)},
            device_id_type=MESH,
        )

    fetch = [
        pltpu.make_async_copy(src, dst, local.at[n])
        for n, (src, dst) in enumerate(
            (
                (r.load_hbm, load_ref),
                (r.crack_hbm, crack_ref),
                (r.clamp_hbm, clamp_ref),
                (r.tough_hbm, tough_ref),
                (r.index_hbm, r.index_ref),
                (r.table_hbm, r.table_ref),
            )
        )
    ]
    for copy in fetch:
        copy.start()

    class Exchange:
        def __init__(self, send, recv):
            self.items = []
            self.send = send
            self.recv = recv

        def add(self, where, src, dst, mine, out_slot, in_slot):
            cond, dev = where
            n = len(self.items)
            copy = pltpu.make_async_remote_copy(
                src_ref=src,
                dst_ref=dst,
                send_sem=self.send.at[n],
                recv_sem=self.recv.at[out_slot],
                device_id=dev,
                device_id_type=MESH,
            )
            back = pltpu.make_async_remote_copy(
                src_ref=src,
                dst_ref=mine,
                send_sem=self.send.at[n],
                recv_sem=self.recv.at[in_slot],
                device_id=dev,
                device_id_type=MESH,
            )
            self.items.append((cond, copy, back))

        def start(self, begin=0, end=None):
            for cond, copy, _ in self.items[begin:end]:
                pl.when(cond)(copy.start)

        def finish(self):
            for cond, copy, back in self.items:

                @pl.when(cond)
                def _():
                    back.wait_recv()
                    copy.wait_send()

        def received(self, begin=0, end=None):
            for cond, _, back in self.items[begin:end]:
                pl.when(cond)(back.wait_recv)

        def sent(self, begin=0, end=None):
            for cond, copy, _ in self.items[begin:end]:
                pl.when(cond)(copy.wait_send)

    rows = ny + 2 * OY

    def clear(xp, carry):
        zero = jnp.zeros((rows, nz), jnp.float32)
        held[xp] = zero
        crack_pad[xp] = zero
        clamped[xp] = zero + 1.0
        tough_pad[xp] = zero + 1.0
        for f in range(3):
            state[0, f, xp] = zero
        if sections > 2:
            state[0, 3, xp] = zero
            for f in range(4):
                state[1, f, xp] = zero
        return carry

    lax.fori_loop(0, nx + 2 * HX, clear, 0)

    for copy in fetch[:3]:
        copy.wait()

    for s in range(2):
        side = lambda n, s=s: slice(0, n) if s == 0 else slice(ny - n, ny)
        r.pack_l[s] = load_ref[:, side(4)]
        r.pack_f[s] = clamp_ref[:, side(2)]
        for x in range(nx):
            r.pack_c[s, 3 * x : 3 * x + 3] = crack_ref[x, side(3)]
    corner = (
        (load_ref, held, 1, 3, 0),
        (load_ref, held, 2, 2, 3),
        (load_ref, held, 3, 1, 5),
        (crack_ref, crack_pad, 1, 2, 6),
        (crack_ref, crack_pad, 2, 1, 8),
        (clamp_ref, clamped, 1, 1, 9),
    )

    def x_from(s, deep):
        return deep - 1 if s == 0 else nx - deep

    def x_at(s, deep):
        return HX - deep if s == 0 else HX + nx - 1 + deep

    for sx in range(2):
        for sy in range(2):
            for ref, _, deep, n, at in corner:
                first = 0 if sy == 0 else ny - n
                r.pack_k[sx * 2 + sy, at : at + n] = ref[x_from(sx, deep), first : first + n]

    pl.semaphore_wait(barrier, near_count + sections - 1)

    beside_y = Exchange(r.y_send, r.y_recv)
    part_a = Exchange(r.a_send, r.a_recv)
    part_m = Exchange(r.m_send, r.m_recv)
    part_b = Exchange(r.b_send, r.b_recv)
    for ex, ref, buf, deep, width, at, slot in (
        (part_a, load_ref, r.in_a, 2, 2, 0, 0),
        (part_a, crack_ref, r.in_a, 1, 1, 2, 2),
        (part_m, load_ref, r.in_m, 3, 1, 0, 0),
        (part_m, crack_ref, r.in_m, 2, 1, 1, 2),
        (part_m, clamp_ref, r.in_m, 1, 1, 2, 4),
        (part_b, load_ref, r.in_b, 4, 1, 0, 0),
        (part_b, crack_ref, r.in_b, 3, 1, 1, 2),
        (part_b, clamp_ref, r.in_b, 2, 1, 2, 4),
        (part_b, tough_ref.at[0], r.in_tx, 1, 1, 0, 6),
    ):
        for s in range(2):
            first = deep - width if s == 0 else nx - deep
            ex.add(
                x_dev(s),
                ref.at[pl.ds(first, width)],
                buf.at[1 - s, pl.ds(at, width)],
                buf.at[s, pl.ds(at, width)],
                slot + 1 - s,
                slot + s,
            )
    for n in range(8):
        s = n % 2
        for pack, buf, slot in (
            (r.pack_c, r.in_c, 0),
            (r.pack_l, r.in_l, 2),
            (r.pack_f, r.in_f, 4),
            (r.pack_t, r.in_ty, 6),
        )[n // 2 : n // 2 + 1]:
            beside_y.add(
                y_dev(s), pack.at[s], buf.at[1 - s], buf.at[s], slot + 1 - s, slot + s
            )
    for sx in range(2):
        for sy in range(2):
            here, away = sx * 2 + sy, (1 - sx) * 2 + 1 - sy
            part_a.add(
                c_dev(sx, sy), r.pack_k.at[here], r.in_k.at[away], r.in_k.at[here],
                4 + away, 4 + here,
            )
    beside_y.start(0, 4)
    part_a.start(0, 4)
    beside_y.start(4, 6)
    fetch[3].wait()
    for s in range(2):
        r.pack_t[s] = tough_ref[0, :, 0:1] if s == 0 else tough_ref[0, :, ny - 1 : ny]
    beside_y.start(6)
    part_a.start(4)
    part_m.start()
    part_b.start()
    further = max(ngx, ngy) - 2
    if further > 0:
        greet(r.reach.at[0])
    tough_copies = []
    for k in range(1, sections):
        copy = pltpu.make_async_remote_copy(
            src_ref=tough_ref.at[0],
            dst_ref=r.tough_in.at[k - 1],
            send_sem=r.tough_send.at[k - 1],
            recv_sem=r.tough_recv.at[k - 1],
            device_id={"section": lax.rem(sec + sections - k, sections)},
            device_id_type=MESH,
        )
        copy.start()
        tough_copies.append(copy)

    inner = slice(OY, OY + ny)
    as_float = lambda v: v.astype(jnp.float32)

    def fill(x, carry):
        held[x + HX, inner] = as_float(load_ref[x])
        clamped[x + HX, inner] = as_float(clamp_ref[x])
        crack_pad[x + HX, inner] = as_float(crack_ref[x])
        tough_pad[x + HX, inner] = tough_ref[0, x]
        return carry

    lax.fori_loop(0, nx, fill, 0, unroll=part(nx, 4))

    for copy in fetch[4:]:
        copy.wait()
    case = r.index_ref[0]
    vector = [r.table_ref[f, case] for f in range(3)]

    planes = slice(HX, HX + nx)

    def x_out(s, n):
        return slice(HX - n, HX) if s == 0 else slice(HX + nx, HX + nx + n)

    def y_out(s, n):
        return slice(OY - n, OY) if s == 0 else slice(OY + ny, OY + ny + n)

    def from_y(kind, s, put):
        beside_y.received(2 * kind + s, 2 * kind + s + 1)
        pl.when(there["gy"][s])(put)

    def unpack_a():
        part_a.received()
        for s in range(2):

            @pl.when(there["gx"][s])
            def _(s=s):
                held[x_out(s, 2), inner] = as_float(r.in_a[s, 0:2])
                crack_pad[x_out(s, 1), inner] = as_float(r.in_a[s, 2:3])

        for sx in range(2):
            for sy in range(2):

                @pl.when(c_dev(sx, sy)[0])
                def _(sx=sx, sy=sy):
                    for _, pad, deep, n, at in corner:
                        pad[x_at(sx, deep), y_out(sy, n)] = as_float(
                            r.in_k[sx * 2 + sy, at : at + n]
                        )

    def unpack_m():
        part_m.received()
        for s in range(2):

            @pl.when(there["gx"][s])
            def _(s=s):
                held[x_at(s, 3), inner] = as_float(r.in_m[s, 0])
                crack_pad[x_at(s, 2), inner] = as_float(r.in_m[s, 1])
                clamped[x_at(s, 1), inner] = as_float(r.in_m[s, 2])

    def unpack_b():
        part_b.received()
        for s in range(2):

            @pl.when(there["gx"][s])
            def _(s=s):
                held[x_at(s, 4), inner] = as_float(r.in_b[s, 0])
                crack_pad[x_at(s, 3), inner] = as_float(r.in_b[s, 1])
                clamped[x_at(s, 2), inner] = as_float(r.in_b[s, 2])
                tough_pad[x_at(s, 1), inner] = r.in_tx[s, 0]

    wide = up8(ny + 4)
    deep = up8(ny + 8)

    def lanes(shape, lane):
        return lax.broadcasted_iota(jnp.int32, shape, 1) == lane

    def beside(v, edge, first, last):
        up = jnp.where(last, edge, pltpu.roll(v, nz - 1, 1))
        down = jnp.where(first, edge, pltpu.roll(v, 1, 1))
        return up, down

    def inside_rows(shape, above):
        row = lax.broadcasted_iota(jnp.int32, shape, 0) + (gy * ny - above)
        return jnp.logical_and(row >= 0, row < ny * ngy)

    def inside_plane(xp):
        plane = xp - HX + gx * nx
        return jnp.logical_and(plane >= 0, plane < nx * ngx)

    edge_stiff = 0.5 * (1.0 + stiff_floor)

    def elastic(at, first, last):
        k = at(stiff, 0, 0)
        sides = (
            (at(stiff, 1, 0), at(stiff, -1, 0)),
            (at(stiff, 0, 1), at(stiff, 0, -1)),
            beside(k, edge_stiff, first, last),
        )
        pairs = [s[0] + s[1] for s in sides]
        weights = pairs[0] + pairs[1] + pairs[2] + 6.0 * k
        faces = [(k + s[0], k + s[1]) for s in sides]
        fz = beside(at(flow, 0, 0), 0.0, first, last)
        grads = (
            at(flow, 1, 0) - at(flow, -1, 0),
            at(flow, 0, 1) - at(flow, 0, -1),
            fz[0] - fz[1],
        )
        return pairs, weights, faces, grads

    def laplace(at, ref, faces, weights, first, last):
        here = at(ref, 0, 0)
        uz = beside(here, 0.0, first, last)
        return here, (
            faces[0][0] * at(ref, 1, 0)
            + faces[0][1] * at(ref, -1, 0)
            + faces[1][0] * at(ref, 0, 1)
            + faces[1][1] * at(ref, 0, -1)
            + faces[2][0] * uz[0]
            + faces[2][1] * uz[1]
            - weights * here
        )

    def strain_energy(at, u, keep, first, last):
        grad = []
        for f in range(3):
            here = at(u.at[f], 0, 0)
            uz = beside(here, 0.0, first, last)
            grad.append(
                (
                    at(u.at[f], 1, 0) - at(u.at[f], -1, 0),
                    at(u.at[f], 0, 1) - at(u.at[f], 0, -1),
                    uz[0] - uz[1],
                )
            )
            keep(f, here)
        return 0.5 * spectral_energy(
            grad[0][0],
            grad[1][1],
            grad[2][2],
            grad[0][1] + grad[1][0],
            grad[0][2] + grad[2][0],
            grad[1][2] + grad[2][1],
        )

    def renew(at, d, energy, g, cracked, first, last):
        dz = beside(at(d, 0, 0), 0.0, first, last)
        around = at(d, 1, 0) + at(d, -1, 0) + at(d, 0, 1) + at(d, 0, -1) + dz[0] + dz[1]
        renewed = (energy + g * around) / (7.0 * g + energy)
        return jnp.where(cracked, 1.0, renewed)

    def add_up(rnd, total):
        r.sums[me, rnd : rnd + 1] = jnp.sum(total, axis=0, keepdims=True)

    def open_stages(above, n):
        shape = (n, nz)
        first, last = lanes(shape, 0), lanes(shape, nz - 1)
        row_inside = inside_rows(shape, above)
        row = lax.broadcasted_iota(jnp.int32, shape, 0)
        a = OY - above

        def stiffen(xp, carry):
            half = 0.5 * (jnp.square(1.0 - crack_pad[xp, a : a + n]) + stiff_floor)
            stiff[xp, a : a + n] = half
            up, down = beside(held[xp, a : a + n], 0.0, first, last)
            div = (
                vector[0] * (held[xp + 1, a : a + n] - held[xp - 1, a : a + n])
                + vector[1] * (held[xp, a + 1 : a + 1 + n] - held[xp, a - 1 : a - 1 + n])
                + vector[2] * (up - down)
            )
            flow[xp, a : a + n] = jnp.where(
                jnp.logical_and(row_inside, inside_plane(xp)), half * div, 0.0
            )
            return carry

        def mover(low, high):
            def move(xp, total):
                at = lambda ref, dx, dy: ref[xp + dx, a + dy : a + dy + n]
                pairs, weights, faces, grads = elastic(at, first, last)
                load, spread = laplace(at, held, faces, weights, first, last)
                pin = at(clamped, 0, 0) + load > 0.5
                squares = None
                for f in range(3):
                    res = vector[f] * spread + grads[f]
                    moved = jnp.where(pin, 0.0, relax_weight * res / (weights + pairs[f]))
                    state[1, f, xp, a : a + n] = vector[f] * load + moved
                    square = res * res
                    squares = square if squares is None else squares + square
                if low >= high:
                    return total
                counted = jnp.logical_and(row >= low + above, row < high + above)
                return total + jnp.where(
                    jnp.logical_and(counted, jnp.logical_not(pin)), squares, 0.0
                )

            return move

        def damage(xp, carry):
            at = lambda ref, dx, dy: ref[xp + dx, a + dy : a + dy + n]
            energy = strain_energy(at, state.at[1], lambda f, v: None, first, last)
            renewed = renew(
                at,
                crack_pad,
                energy,
                at(tough_pad, 0, 0),
                at(crack_pad, 0, 0) > 0.5,
                first,
                last,
            )
            state[1, 3, xp, a : a + n] = jnp.where(
                jnp.logical_and(row_inside, inside_plane(xp)), renewed, 0.0
            )
            return carry

        return stiffen, mover, damage

    def open_sweep():
        def inward(skip, body, carry, most):
            n = nx - 2 * skip
            return lax.fori_loop(HX + skip, HX + nx - skip, body, carry, unroll=part(n, most))

        def outward(far, n, body, carry):
            def both(i, carry):
                carry = body(HX - far + i, carry)
                return body(HX + nx + far - n + i, carry)

            return lax.fori_loop(0, n, both, carry, unroll=True)

        blank = lambda n: jnp.zeros((n, nz), jnp.float32)
        fold = lambda v: jnp.sum(v, axis=0, keepdims=True)

        stiffen, mover, damage = open_stages(0, ny)
        inward(1, stiffen, 0, 14)
        inside = inward(2, mover(2, ny - 2), blank(ny), 12)
        inward(3, damage, 0, 5)

        def rim(s):
            above = (4, 4 - ny)[s]
            stiffen, mover, damage = open_stages(above, 8)

            def put_crack():
                for x in range(nx):
                    crack_pad[HX + x, y_out(s, 3)] = as_float(r.in_c[s, 3 * x : 3 * x + 3])

            def put_load():
                held[planes, y_out(s, 4)] = as_float(r.in_l[s])

            def put_clamp():
                clamped[planes, y_out(s, 2)] = as_float(r.in_f[s])

            def put_tough():
                tough_pad[planes, y_out(s, 1)] = r.in_ty[s]

            from_y(0, s, put_crack)
            from_y(1, s, put_load)
            inward(1, stiffen, 0, 14)
            from_y(2, s, put_clamp)
            counted = (0, 2) if s == 0 else (ny - 2, ny)
            r.rims[s] = inward(2, mover(*counted), blank(8), 12)
            from_y(3, s, put_tough)
            inward(3, damage, 0, 10)

        odd = lax.rem(gy, 2) == 1

        @pl.when(odd)
        def _():
            rim(0)
            rim(1)

        @pl.when(jnp.logical_not(odd))
        def _():
            rim(1)
            rim(0)

        if further > 1:
            pl.semaphore_wait(r.reach.at[0], near_count)
            greet(r.reach.at[1])

        stiffen1, mover1 = stages(1)
        move1 = mover1(OY, ny)
        inward(3, stiffen1, 0, 10)
        own = inward(4, move1, blank(ny), 8)

        stiffen, mover, damage = open_stages(4, deep)
        unpack_a()
        outward(1, 2, stiffen, 0)
        ends = outward(0, 2, mover(0, ny), blank(deep))
        r.sums[me, 0:1] = fold(inside) + fold(r.rims[0] + r.rims[1]) + fold(ends)
        outward(-1, 2, damage, 0)
        outward(-1, 2, stiffen1, 0)
        own = outward(-2, 2, move1, own)

        unpack_m()
        outward(2, 1, stiffen, 0)
        outward(1, 1, mover(0, 0), blank(deep))
        outward(0, 1, damage, 0)
        outward(0, 1, stiffen1, 0)
        own = outward(-1, 1, move1, own)

        unpack_b()
        outward(3, 1, stiffen, 0)
        outward(2, 1, mover(0, 0), blank(deep))
        outward(1, 1, damage, 0)
        outward(1, 1, stiffen1, 0)
        own = outward(0, 1, move1, own)

        return own

    def send_sums():
        for k in range(1 if further > 1 else 0, further):
            pl.semaphore_wait(r.reach.at[k], near_count)
            if k + 1 < further:
                greet(r.reach.at[k + 1])
        for k, peer in enumerate(peers):
            pltpu.make_async_remote_copy(
                src_ref=r.sums.at[me],
                dst_ref=r.sums.at[me],
                send_sem=r.sum_send.at[k],
                recv_sem=r.sum_recv.at[me],
                device_id=peer,
                device_id_type=MESH,
            ).start()

    def stages(rnd):
        p = rnd % 2
        q = 1 - p
        shape = (wide, nz)
        first, last = lanes(shape, 0), lanes(shape, nz - 1)
        row_inside = inside_rows(shape, 2)
        a = OY - 2

        def stiffen(xp, carry):
            half = 0.5 * (jnp.square(1.0 - state[p, 3, xp, a : a + wide]) + stiff_floor)
            stiff[xp, a : a + wide] = half
            up, down = beside(state[p, 2, xp, a : a + wide], 0.0, first, last)
            div = (
                (state[p, 0, xp + 1, a : a + wide] - state[p, 0, xp - 1, a : a + wide])
                + (state[p, 1, xp, a + 1 : a + 1 + wide] - state[p, 1, xp, a - 1 : a - 1 + wide])
                + (up - down)
            )
            flow[xp, a : a + wide] = jnp.where(
                jnp.logical_and(row_inside, inside_plane(xp)), half * div, 0.0
            )
            return carry

        def mover(b, n):
            shape = (n, nz)
            first, last = lanes(shape, 0), lanes(shape, nz - 1)

            def move(xp, total):
                at = lambda ref, dx, dy: ref[xp + dx, b + dy : b + dy + n]
                pairs, weights, faces, grads = elastic(at, first, last)
                load = at(held, 0, 0)
                pin = at(clamped, 0, 0) + load > 0.5
                squares = None
                for f in range(3):
                    here, spread = laplace(at, state.at[p, f], faces, weights, first, last)
                    res = spread + grads[f]
                    moved = here + relax_weight * res / (weights + pairs[f])
                    state[q, f, xp, b : b + n] = jnp.where(pin, load * vector[f], moved)
                    square = res * res
                    squares = square if squares is None else squares + square
                return total + jnp.where(pin, 0.0, squares)

            return move

        return stiffen, mover

    def sweep(rnd, total):
        p = rnd % 2
        q = 1 - p
        done = rnd == sections - 1
        tough = r.tough_in.at[rnd - 1]

        stiffen, mover = stages(rnd)
        if rnd > 1:
            lax.fori_loop(HX - 2, HX + nx + 2, stiffen, 0, unroll=part(nx + 4, 10))
            total = lax.fori_loop(
                HX, HX + nx, mover(OY, ny), jnp.zeros((ny, nz), jnp.float32), unroll=part(nx, 8)
            )
        add_up(rnd, total)
        if done:
            send_sums()
        par = rnd % 2
        mid = pl.ds(OY, ny)
        if done:
            rims = Exchange(r.v_send, r.v_recv)
            for s in range(2):
                row = OY if s == 0 else OY + ny - 1
                for f in range(3):
                    r.pack_v[s, f] = state[q, f, planes, row : row + 1]
                rims.add(
                    x_dev(s),
                    state.at[q, pl.ds(0, 3), HX if s == 0 else HX + nx - 1, mid],
                    r.in_vx.at[1 - s],
                    r.in_vx.at[s],
                    1 - s,
                    s,
                )
                rims.add(
                    y_dev(s), r.pack_v.at[s], r.in_vy.at[1 - s], r.in_vy.at[s], 3 - s, 2 + s
                )
            rims.start()
            rims.received()
            for s in range(2):

                @pl.when(there["gx"][s])
                def _(s=s):
                    state[q, 0:3, x_at(s, 1), inner] = r.in_vx[s]

                @pl.when(there["gy"][s])
                def _(s=s):
                    for f in range(3):
                        state[q, f, planes, y_out(s, 1)] = r.in_vy[s, f]
        else:
            for f in range(3):
                r.pack_u[0, :, 2 * f : 2 * f + 2] = state[q, f, planes, OY : OY + 2]
                r.pack_u[1, :, 2 * f : 2 * f + 2] = state[q, f, planes, OY + ny - 2 : OY + ny]
            r.pack_u[0, :, 6:7] = state[q, 1, planes, OY + 2 : OY + 3]
            r.pack_u[1, :, 6:7] = state[q, 1, planes, OY + ny - 3 : OY + ny - 2]
            shift = Exchange(r.u_send, r.u_recv.at[par])
            for s in range(2):
                shift.add(
                    x_dev(s),
                    state.at[q, pl.ds(0, 3), pl.ds(HX if s == 0 else HX + nx - 2, 2), mid],
                    r.in_u_x.at[par, 1 - s],
                    r.in_u_x.at[par, s],
                    (1 - s),
                    s,
                )
                shift.add(
                    x_dev(s),
                    state.at[q, 0, HX + 2 if s == 0 else HX + nx - 3, mid],
                    r.in_u_x3.at[par, 1 - s],
                    r.in_u_x3.at[par, s],
                    2 + (1 - s),
                    2 + s,
                )
            for s in range(2):
                shift.add(
                    y_dev(s),
                    r.pack_u.at[s],
                    r.in_u_y.at[par, 1 - s],
                    r.in_u_y.at[par, s],
                    4 + (1 - s),
                    4 + s,
                )
            for sx in range(2):
                for sy in range(2):
                    shift.add(
                        c_dev(sx, sy),
                        r.pack_u.at[sy, pl.ds(0 if sx == 0 else nx - 2, 2)],
                        r.in_u_c.at[par, (1 - sx) * 2 + 1 - sy],
                        r.in_u_c.at[par, sx * 2 + sy],
                        6 + (1 - sx) * 2 + 1 - sy,
                        6 + sx * 2 + sy,
                    )
            shift.start()
            shift.finish()
            third_x = (HX - 3, HX + nx + 2)
            third_y = (slice(OY - 3, OY - 2), slice(OY + ny + 2, OY + ny + 3))
            for s in range(2):

                @pl.when(there["gx"][s])
                def _(s=s):
                    state[q, 0:3, x_out(s, 2), inner] = r.in_u_x[par, s]
                    state[q, 0, third_x[s], inner] = r.in_u_x3[par, s]

                @pl.when(there["gy"][s])
                def _(s=s):
                    for f in range(3):
                        state[q, f, planes, y_out(s, 2)] = r.in_u_y[par, s, :, 2 * f : 2 * f + 2]
                    state[q, 1, planes, third_y[s]] = r.in_u_y[par, s, :, 6:7]

            for sx in range(2):
                for sy in range(2):

                    @pl.when(c_dev(sx, sy)[0])
                    def _(sx=sx, sy=sy):
                        for f in range(3):
                            state[q, f, x_out(sx, 2), y_out(sy, 2)] = r.in_u_c[
                                par, sx * 2 + sy, :, 2 * f : 2 * f + 2
                            ]

        tough_copies[rnd - 1].wait_recv()

        shape = (ny, nz)
        first, last = lanes(shape, 0), lanes(shape, nz - 1)

        def damage(x, carry):
            xp = x + HX
            at = lambda ref, dx, dy: ref[xp + dx, OY + dy : OY + dy + ny]

            def keep(f, here):
                if done:
                    disp_refs[f][x] = here

            energy = strain_energy(at, state.at[q], keep, first, last)
            renewed = renew(
                at, state.at[p, 3], energy, tough[x], crack_ref[x] > 0, first, last
            )
            if done:
                r.dam_ref[x] = renewed
            else:
                state[q, 3, xp, inner] = renewed
            return carry

        lax.fori_loop(0, nx, damage, 0, unroll=part(nx, 8))
        if done:
            rims.sent()
            return

        r.pack_d[0] = state[q, 3, planes, OY : OY + 2]
        r.pack_d[1] = state[q, 3, planes, OY + ny - 2 : OY + ny]
        crack = Exchange(r.d_send, r.d_recv.at[par])
        for s in range(2):
            crack.add(
                x_dev(s),
                state.at[q, 3, pl.ds(HX if s == 0 else HX + nx - 2, 2), mid],
                r.in_d_x.at[par, 1 - s],
                r.in_d_x.at[par, s],
                1 - s,
                s,
            )
        for s in range(2):
            crack.add(
                y_dev(s),
                r.pack_d.at[s],
                r.in_d_y.at[par, 1 - s],
                r.in_d_y.at[par, s],
                2 + 1 - s,
                2 + s,
            )
        for sx in range(2):
            for sy in range(2):
                crack.add(
                    c_dev(sx, sy),
                    r.pack_d.at[sy, pl.ds(0 if sx == 0 else nx - 1, 1)],
                    r.in_d_c.at[par, (1 - sx) * 2 + 1 - sy],
                    r.in_d_c.at[par, sx * 2 + sy],
                    4 + (1 - sx) * 2 + 1 - sy,
                    4 + sx * 2 + sy,
                )
        crack.start()
        crack.finish()
        for s in range(2):

            @pl.when(there["gx"][s])
            def _(s=s):
                state[q, 3, x_out(s, 2), inner] = r.in_d_x[par, s]

            @pl.when(there["gy"][s])
            def _(s=s):
                state[q, 3, planes, y_out(s, 2)] = r.in_d_y[par, s]

        for sx in range(2):
            for sy in range(2):

                @pl.when(c_dev(sx, sy)[0])
                def _(sx=sx, sy=sy):
                    state[q, 3, x_out(sx, 1), y_out(sy, 2)] = r.in_d_c[par, sx * 2 + sy]

    total = open_sweep()
    for rnd in range(1, sections):
        sweep(rnd, total)

    beside_y.sent()
    part_a.sent()
    part_m.sent()
    part_b.sent()
    for copy in tough_copies:
        copy.wait_send()
    for k, peer in enumerate(peers):
        other = peer["gx"] * ngy + peer["gy"]
        pltpu.make_async_remote_copy(
            src_ref=r.sums.at[me],
            dst_ref=r.sums.at[other],
            send_sem=r.sum_send.at[k],
            recv_sem=r.sum_recv.at[other],
            device_id=peer,
            device_id_type=MESH,
        ).wait()
    total = r.sums[0]
    for k in range(1, group):
        total = total + r.sums[k]
    r.total_ref[...] = total


def put_out(
    sizes,
    first_ref,
    second_ref,
    third_ref,
    dam_ref,
    total_ref,
    disp_hbm,
    dam_hbm,
    norm_hbm,
    norm_ref,
    sems,
):
    sections, ngx, ngy, nx, ny, nz = sizes
    copies = [
        pltpu.make_async_copy(ref, disp_hbm.at[0, f], sems.at[f])
        for f, ref in enumerate((first_ref, second_ref, third_ref))
    ]
    copies.append(pltpu.make_async_copy(dam_ref, dam_hbm.at[0], sems.at[3]))
    for copy in copies:
        copy.start()
    sec = lax.axis_index("section")
    cells = 3.0 * nx * ngx * ny * ngy * nz
    entries = jnp.sqrt(jnp.sum(total_ref[...], axis=1, keepdims=True) / cells)
    column = lax.broadcasted_iota(jnp.int32, (1, sections), 1)
    norms = jnp.zeros((1, sections), jnp.float32)
    for rnd in range(sections):
        norms = jnp.where(
            column == lax.rem(sec + rnd, sections), entries[rnd : rnd + 1], norms
        )
    norm_ref[...] = norms
    last = pltpu.make_async_copy(norm_ref, norm_hbm, sems.at[4])
    last.start()
    for copy in copies:
        copy.wait()
    last.wait()


def on_device(sizes, load_index, load_table, toughness, clamp_mask, load_mask, crack_mask):
    sections, ngx, ngy = sizes
    nx, ny, nz = clamp_mask.shape
    assert load_index.shape == (1,)
    group = ngx * ngy
    f32 = jnp.float32
    padded = (nx + 2 * HX, ny + 2 * OY, nz)
    vmem = pltpu.VMEM
    dma = pltpu.SemaphoreType.DMA
    later = max(sections - 1, 1)
    more = sections > 2
    scratch = {
        "index_ref": pltpu.SMEM(load_index.shape, jnp.int32),
        "table_ref": pltpu.SMEM(load_table.shape[::-1], f32),
        "tough_ref": vmem((1, nx, ny, nz), f32),
        "clamp_ref": vmem((nx, ny, nz), jnp.int32),
        "load_ref": vmem((nx, ny, nz), jnp.int32),
        "crack_ref": vmem((nx, ny, nz), jnp.int32),
        "local": dma((6,)),
        "state": vmem((2, 4) + padded, f32),
        "stiff": vmem(padded, f32),
        "flow": vmem(padded, f32),
        "held": vmem(padded, f32),
        "clamped": vmem(padded, f32),
        "tough_pad": vmem(padded, f32),
        "crack_pad": vmem(padded, f32),
        "tough_in": vmem((later, nx, ny, nz), f32),
        "pack_l": vmem((2, nx, 4, nz), jnp.int32),
        "pack_f": vmem((2, nx, 2, nz), jnp.int32),
        "pack_c": vmem((2, 3 * nx, nz), jnp.int32),
        "pack_t": vmem((2, nx, 1, nz), f32),
        "pack_k": vmem((4, 16, nz), jnp.int32),
        "in_a": vmem((2, 3, ny, nz), jnp.int32),
        "in_m": vmem((2, 3, ny, nz), jnp.int32),
        "in_b": vmem((2, 3, ny, nz), jnp.int32),
        "in_tx": vmem((2, 1, ny, nz), f32),
        "in_l": vmem((2, nx, 4, nz), jnp.int32),
        "in_f": vmem((2, nx, 2, nz), jnp.int32),
        "in_c": vmem((2, 3 * nx, nz), jnp.int32),
        "in_ty": vmem((2, nx, 1, nz), f32),
        "in_k": vmem((4, 16, nz), jnp.int32),
        "rims": vmem((2, 8, nz), f32),
        "pack_v": vmem((2, 3, nx, 1, nz), f32),
        "in_vx": vmem((2, 3, ny, nz), f32),
        "in_vy": vmem((2, 3, nx, 1, nz), f32),
        "v_send": dma((4,)),
        "v_recv": dma((4,)),
        "sums": vmem((group, sections, nz), f32),
        "y_send": dma((8,)),
        "y_recv": dma((8,)),
        "a_send": dma((8,)),
        "a_recv": dma((8,)),
        "m_send": dma((6,)),
        "m_recv": dma((6,)),
        "b_send": dma((8,)),
        "b_recv": dma((8,)),
        "reach": pltpu.SemaphoreType.REGULAR((max(max(ngx, ngy) - 2, 1),)),
        "tough_send": dma((later,)),
        "tough_recv": dma((later,)),
        "sum_send": dma((max(group - 1, 1),)),
        "sum_recv": dma((group,)),
    }
    if more:
        scratch |= {
            "pack_u": vmem((2, nx, 8, nz), f32),
            "pack_d": vmem((2, nx, 2, nz), f32),
            "in_u_x": vmem((2, 2, 3, 2, ny, nz), f32),
            "in_u_x3": vmem((2, 2, ny, nz), f32),
            "in_u_y": vmem((2, 2, nx, 8, nz), f32),
            "in_u_c": vmem((2, 4, 2, 8, nz), f32),
            "in_d_x": vmem((2, 2, 2, ny, nz), f32),
            "in_d_y": vmem((2, 2, nx, 2, nz), f32),
            "in_d_c": vmem((2, 4, 1, 2, nz), f32),
            "u_send": dma((10,)),
            "u_recv": dma((2, 10)),
            "d_send": dma((8,)),
            "d_recv": dma((2, 8)),
        }
    ins = ("index_hbm", "table_hbm", "tough_hbm", "clamp_hbm", "load_hbm", "crack_hbm")
    outs = ("first_ref", "second_ref", "third_ref", "dam_ref", "total_ref")
    names = (*ins, *outs, *scratch)
    block = pl.BlockSpec(memory_space=pltpu.VMEM)
    away = pl.BlockSpec(memory_space=pltpu.HBM)
    results = pl.pallas_call(
        functools.partial(kernel, (sections, ngx, ngy, nx, ny, nz), names),
        out_shape=(
            *[jax.ShapeDtypeStruct((nx, ny, nz), f32)] * 4,
            jax.ShapeDtypeStruct((sections, nz), f32),
        ),
        in_specs=[away] * 6,
        out_specs=(block,) * 5,
        scratch_shapes=list(scratch.values()),
        compiler_params=pltpu.CompilerParams(
            collective_id=0, has_side_effects=True, vmem_limit_bytes=56_020_000
        ),
    )(load_index, pltpu.with_memory_space_constraint(load_table.T, pltpu.HBM), toughness, clamp_mask, load_mask, crack_mask)
    return pl.pallas_call(
        functools.partial(put_out, (sections, ngx, ngy, nx, ny, nz)),
        out_shape=(
            jax.ShapeDtypeStruct((1, 3, nx, ny, nz), f32),
            jax.ShapeDtypeStruct((1, nx, ny, nz), f32),
            jax.ShapeDtypeStruct((1, sections), f32),
        ),
        in_specs=[block] * 5,
        out_specs=(away, away, away),
        scratch_shapes=[vmem((1, sections), f32), dma((5,))],
        compiler_params=pltpu.CompilerParams(vmem_limit_bytes=1024 * 1024),
    )(*results)


def solution(mesh):
    in_specs = (
        P("section"),
        P(),
        P("section", "gx", "gy", None),
        P("gx", "gy", None),
        P("gx", "gy", None),
        P("gx", "gy", None),
    )
    out_specs = (
        P("section", None, "gx", "gy", None),
        P("section", "gx", "gy", None),
        P("section", None),
    )
    sizes = tuple(mesh.shape[name] for name in ("section", "gx", "gy"))
    return jax.shard_map(
        functools.partial(on_device, sizes),
        mesh=mesh,
        in_specs=in_specs,
        out_specs=out_specs,
        check_vma=False,
    )
```

```python
import functools
import math
import types

import jax
import jax.numpy as jnp
from jax import lax
from jax.experimental import pallas as pl
from jax.experimental.pallas import tpu as pltpu
from jax.sharding import PartitionSpec as P

relax_weight = 0.6
stiff_floor = 0.001
eigen_guard = 1e-08
MESH = pl.DeviceIdType.MESH

HX = 5
OY = 8

ACOS = (
    1.5707963050,
    -0.2145988016,
    0.0889789874,
    -0.0501743046,
    0.0308918810,
    -0.0170881256,
    0.0066700901,
    -0.0012624911,
)


def up8(n):
    return -(-n // 8) * 8


def part(n, most):
    return max(k for k in range(1, most + 1) if n % k == 0)


def root(v):
    return v * lax.rsqrt(jnp.maximum(v, 1.2e-38))


def spectral_energy(xx, yy, zz, xy, xz, yz):
    trace = xx + yy + zz
    mid = trace * (1.0 / 3.0)
    dx = xx - mid
    dy = yy - mid
    dz = zz - mid
    xy2 = xy * xy
    xz2 = xz * xz
    yz2 = yz * yz
    sixth = (dx * dx + dy * dy + dz * dz + 2.0 * (xy2 + xz2 + yz2)) * (1.0 / 6.0)
    twice_radius = 2.0 * root(sixth)
    scale = lax.rsqrt(sixth + eigen_guard)
    det = dx * (dy * dz - yz2) - dz * xy2 - dy * xz2 + 2.0 * (xy * xz * yz)
    ratio = (0.5 * det * scale) * (scale * scale)
    size = jnp.minimum(jnp.abs(ratio), 1.0)
    poly = jnp.full_like(size, ACOS[-1] / 3.0)
    for c in ACOS[-2::-1]:
        poly = poly * size + c / 3.0
    t = root(1.0 - size) * poly
    t2 = t * t
    cos_t = 1.0 + t2 * (-0.5 + t2 * (1.0 / 24.0 + t2 * (-1.0 / 720.0 + t2 * (1.0 / 40320.0))))
    sin_t = t * (1.0 + t2 * (-1.0 / 6.0 + t2 * (1.0 / 120.0 + t2 * (-1.0 / 5040.0))))
    other = 0.5 * cos_t + math.sqrt(0.75) * sin_t
    upper = ratio >= 0.0
    first = jnp.where(upper, cos_t, other)
    last = jnp.where(upper, other, cos_t)
    largest = mid + twice_radius * first
    smallest = mid - twice_radius * last
    between = trace - largest - smallest
    relu = lambda v: jnp.maximum(v, 0.0)
    return (
        0.5 * jnp.square(relu(trace))
        + jnp.square(relu(largest))
        + jnp.square(relu(between))
        + jnp.square(relu(smallest))
    )


def kernel(sizes, names, *refs):
    sections, ngx, ngy, nx, ny, nz = sizes
    r = types.SimpleNamespace(**dict(zip(names, refs)))
    local, state, stiff, flow = r.local, r.state, r.stiff, r.flow
    held, clamped, tough_pad, crack_pad = r.held, r.clamped, r.tough_pad, r.crack_pad
    load_ref, crack_ref, clamp_ref, tough_ref = r.load_ref, r.crack_ref, r.clamp_ref, r.tough_ref
    disp_refs = (r.first_ref, r.second_ref, r.third_ref)
    sec = lax.axis_index("section")
    gx = lax.axis_index("gx")
    gy = lax.axis_index("gy")
    group = ngx * ngy
    me = gx * ngy + gy
    ring = lambda k, n: min(k, n - k)
    offsets = [(i, j) for i in range(ngx) for j in range(ngy) if i or j]
    offsets.sort(key=lambda o: (ring(o[0], ngx) + ring(o[1], ngy), o))
    peers = []
    for i, j in offsets:
        peers.append({"gx": lax.rem(gx + i, ngx), "gy": lax.rem(gy + j, ngy)})

    there = {
        "gx": (gx > 0, gx < ngx - 1),
        "gy": (gy > 0, gy < ngy - 1),
    }
    step = (-1, 1)

    def x_dev(s):
        return there["gx"][s], {"gx": gx + step[s]}

    def y_dev(s):
        return there["gy"][s], {"gy": gy + step[s]}

    def c_dev(sx, sy):
        return (
            jnp.logical_and(there["gx"][sx], there["gy"][sy]),
            {"gx": gx + step[sx], "gy": gy + step[sy]},
        )

    neighbours = [x_dev(s) for s in range(2)] + [y_dev(s) for s in range(2)]
    neighbours += [c_dev(sx, sy) for sx in range(2) for sy in range(2)]
    in_line = lambda name: sum(t.astype(jnp.int32) for t in there[name])
    near_count = (in_line("gx") + 1) * (in_line("gy") + 1) - 1

    def greet(sem):
        for cond, dev in neighbours:

            @pl.when(cond)
            def _(dev=dev):
                pl.semaphore_signal(sem, inc=1, device_id=dev, device_id_type=MESH)

    barrier = pltpu.get_barrier_semaphore()
    for k in range(1, sections):
        pl.semaphore_signal(
            barrier,
            inc=1,
            device_id={"section": lax.rem(sec + k, sections)},
            device_id_type=MESH,
        )
    greet(barrier)

    fetch = [
        pltpu.make_async_copy(src, dst, local.at[n])
        for n, (src, dst) in enumerate(
            (
                (r.load_hbm, load_ref),
                (r.crack_hbm, crack_ref),
                (r.clamp_hbm, clamp_ref),
                (r.tough_hbm, tough_ref),
                (r.index_hbm, r.index_ref),
                (r.table_hbm, r.table_ref),
            )
        )
    ]
    for copy in fetch:
        copy.start()

    class Exchange:
        def __init__(self, send, recv):
            self.items = []
            self.send = send
            self.recv = recv

        def add(self, where, src, dst, mine, out_slot, in_slot):
            cond, dev = where
            n = len(self.items)
            copy = pltpu.make_async_remote_copy(
                src_ref=src,
                dst_ref=dst,
                send_sem=self.send.at[n],
                recv_sem=self.recv.at[out_slot],
                device_id=dev,
                device_id_type=MESH,
            )
            back = pltpu.make_async_remote_copy(
                src_ref=src,
                dst_ref=mine,
                send_sem=self.send.at[n],
                recv_sem=self.recv.at[in_slot],
                device_id=dev,
                device_id_type=MESH,
            )
            self.items.append((cond, copy, back))

        def start(self, begin=0, end=None):
            for cond, copy, _ in self.items[begin:end]:
                pl.when(cond)(copy.start)

        def finish(self):
            for cond, copy, back in self.items:

                @pl.when(cond)
                def _():
                    back.wait_recv()
                    copy.wait_send()

        def received(self, begin=0, end=None):
            for cond, _, back in self.items[begin:end]:
                pl.when(cond)(back.wait_recv)

        def sent(self, begin=0, end=None):
            for cond, copy, _ in self.items[begin:end]:
                pl.when(cond)(copy.wait_send)

    rows = ny + 2 * OY

    def clear(xp, carry):
        zero = jnp.zeros((rows, nz), jnp.float32)
        held[xp] = zero
        crack_pad[xp] = zero
        clamped[xp] = zero + 1.0
        tough_pad[xp] = zero + 1.0
        for f in range(3):
            state[0, f, xp] = zero
        if sections > 2:
            state[0, 3, xp] = zero
            for f in range(4):
                state[1, f, xp] = zero
        return carry

    lax.fori_loop(0, nx + 2 * HX, clear, 0)

    for copy in fetch[:3]:
        copy.wait()

    for s in range(2):
        side = lambda n, s=s: slice(0, n) if s == 0 else slice(ny - n, ny)
        r.pack_l[s] = load_ref[:, side(4)]
        r.pack_f[s] = clamp_ref[:, side(2)]
        for x in range(nx):
            r.pack_c[s, 3 * x : 3 * x + 3] = crack_ref[x, side(3)]
    corner = (
        (load_ref, held, 1, 3, 0),
        (load_ref, held, 2, 2, 3),
        (load_ref, held, 3, 1, 5),
        (crack_ref, crack_pad, 1, 2, 6),
        (crack_ref, crack_pad, 2, 1, 8),
        (clamp_ref, clamped, 1, 1, 9),
    )

    def x_from(s, deep):
        return deep - 1 if s == 0 else nx - deep

    def x_at(s, deep):
        return HX - deep if s == 0 else HX + nx - 1 + deep

    for sx in range(2):
        for sy in range(2):
            for ref, _, deep, n, at in corner:
                first = 0 if sy == 0 else ny - n
                r.pack_k[sx * 2 + sy, at : at + n] = ref[x_from(sx, deep), first : first + n]

    pl.semaphore_wait(barrier, near_count + sections - 1)

    beside_y = Exchange(r.y_send, r.y_recv)
    part_a = Exchange(r.a_send, r.a_recv)
    part_m = Exchange(r.m_send, r.m_recv)
    part_b = Exchange(r.b_send, r.b_recv)
    for ex, ref, buf, deep, width, at, slot in (
        (part_a, load_ref, r.in_a, 2, 2, 0, 0),
        (part_a, crack_ref, r.in_a, 1, 1, 2, 2),
        (part_m, load_ref, r.in_m, 3, 1, 0, 0),
        (part_m, crack_ref, r.in_m, 2, 1, 1, 2),
        (part_m, clamp_ref, r.in_m, 1, 1, 2, 4),
        (part_b, load_ref, r.in_b, 4, 1, 0, 0),
        (part_b, crack_ref, r.in_b, 3, 1, 1, 2),
        (part_b, clamp_ref, r.in_b, 2, 1, 2, 4),
        (part_b, tough_ref.at[0], r.in_tx, 1, 1, 0, 6),
    ):
        for s in range(2):
            first = deep - width if s == 0 else nx - deep
            ex.add(
                x_dev(s),
                ref.at[pl.ds(first, width)],
                buf.at[1 - s, pl.ds(at, width)],
                buf.at[s, pl.ds(at, width)],
                slot + 1 - s,
                slot + s,
            )
    for n in range(8):
        s = n % 2
        for pack, buf, slot in (
            (r.pack_c, r.in_c, 0),
            (r.pack_l, r.in_l, 2),
            (r.pack_f, r.in_f, 4),
            (r.pack_t, r.in_ty, 6),
        )[n // 2 : n // 2 + 1]:
            beside_y.add(
                y_dev(s), pack.at[s], buf.at[1 - s], buf.at[s], slot + 1 - s, slot + s
            )
    for sx in range(2):
        for sy in range(2):
            here, away = sx * 2 + sy, (1 - sx) * 2 + 1 - sy
            part_a.add(
                c_dev(sx, sy), r.pack_k.at[here], r.in_k.at[away], r.in_k.at[here],
                4 + away, 4 + here,
            )
    beside_y.start(0, 4)
    part_a.start(0, 4)
    beside_y.start(4, 6)
    fetch[3].wait()
    for s in range(2):
        r.pack_t[s] = tough_ref[0, :, 0:1] if s == 0 else tough_ref[0, :, ny - 1 : ny]
    beside_y.start(6)
    part_a.start(4)
    part_m.start()
    part_b.start()
    further = max(ngx, ngy) - 2
    if further > 0:
        greet(r.reach.at[0])
    tough_copies = []
    for k in range(1, sections):
        copy = pltpu.make_async_remote_copy(
            src_ref=tough_ref.at[0],
            dst_ref=r.tough_in.at[k - 1],
            send_sem=r.tough_send.at[k - 1],
            recv_sem=r.tough_recv.at[k - 1],
            device_id={"section": lax.rem(sec + sections - k, sections)},
            device_id_type=MESH,
        )
        copy.start()
        tough_copies.append(copy)

    inner = slice(OY, OY + ny)
    as_float = lambda v: v.astype(jnp.float32)

    def fill(x, carry):
        held[x + HX, inner] = as_float(load_ref[x])
        clamped[x + HX, inner] = as_float(clamp_ref[x])
        crack_pad[x + HX, inner] = as_float(crack_ref[x])
        tough_pad[x + HX, inner] = tough_ref[0, x]
        return carry

    lax.fori_loop(0, nx, fill, 0, unroll=part(nx, 4))

    for copy in fetch[4:]:
        copy.wait()
    case = r.index_ref[0]
    vector = [r.table_ref[f, case] for f in range(3)]

    planes = slice(HX, HX + nx)

    def x_out(s, n):
        return slice(HX - n, HX) if s == 0 else slice(HX + nx, HX + nx + n)

    def y_out(s, n):
        return slice(OY - n, OY) if s == 0 else slice(OY + ny, OY + ny + n)

    def from_y(kind, s, put):
        beside_y.received(2 * kind + s, 2 * kind + s + 1)
        pl.when(there["gy"][s])(put)

    def unpack_a():
        part_a.received()
        for s in range(2):

            @pl.when(there["gx"][s])
            def _(s=s):
                held[x_out(s, 2), inner] = as_float(r.in_a[s, 0:2])
                crack_pad[x_out(s, 1), inner] = as_float(r.in_a[s, 2:3])

        for sx in range(2):
            for sy in range(2):

                @pl.when(c_dev(sx, sy)[0])
                def _(sx=sx, sy=sy):
                    for _, pad, deep, n, at in corner:
                        pad[x_at(sx, deep), y_out(sy, n)] = as_float(
                            r.in_k[sx * 2 + sy, at : at + n]
                        )

    def unpack_m():
        part_m.received()
        for s in range(2):

            @pl.when(there["gx"][s])
            def _(s=s):
                held[x_at(s, 3), inner] = as_float(r.in_m[s, 0])
                crack_pad[x_at(s, 2), inner] = as_float(r.in_m[s, 1])
                clamped[x_at(s, 1), inner] = as_float(r.in_m[s, 2])

    def unpack_b():
        part_b.received()
        for s in range(2):

            @pl.when(there["gx"][s])
            def _(s=s):
                held[x_at(s, 4), inner] = as_float(r.in_b[s, 0])
                crack_pad[x_at(s, 3), inner] = as_float(r.in_b[s, 1])
                clamped[x_at(s, 2), inner] = as_float(r.in_b[s, 2])
                tough_pad[x_at(s, 1), inner] = r.in_tx[s, 0]

    wide = up8(ny + 4)
    deep = up8(ny + 8)

    def lanes(shape, lane):
        return lax.broadcasted_iota(jnp.int32, shape, 1) == lane

    def beside(v, edge, first, last):
        up = jnp.where(last, edge, pltpu.roll(v, nz - 1, 1))
        down = jnp.where(first, edge, pltpu.roll(v, 1, 1))
        return up, down

    def inside_rows(shape, above):
        row = lax.broadcasted_iota(jnp.int32, shape, 0) + (gy * ny - above)
        return jnp.logical_and(row >= 0, row < ny * ngy)

    def inside_plane(xp):
        plane = xp - HX + gx * nx
        return jnp.logical_and(plane >= 0, plane < nx * ngx)

    edge_stiff = 0.5 * (1.0 + stiff_floor)

    def elastic(at, first, last):
        k = at(stiff, 0, 0)
        sides = (
            (at(stiff, 1, 0), at(stiff, -1, 0)),
            (at(stiff, 0, 1), at(stiff, 0, -1)),
            beside(k, edge_stiff, first, last),
        )
        pairs = [s[0] + s[1] for s in sides]
        weights = pairs[0] + pairs[1] + pairs[2] + 6.0 * k
        faces = [(k + s[0], k + s[1]) for s in sides]
        fz = beside(at(flow, 0, 0), 0.0, first, last)
        grads = (
            at(flow, 1, 0) - at(flow, -1, 0),
            at(flow, 0, 1) - at(flow, 0, -1),
            fz[0] - fz[1],
        )
        return pairs, weights, faces, grads

    def laplace(at, ref, faces, weights, first, last):
        here = at(ref, 0, 0)
        uz = beside(here, 0.0, first, last)
        return here, (
            faces[0][0] * at(ref, 1, 0)
            + faces[0][1] * at(ref, -1, 0)
            + faces[1][0] * at(ref, 0, 1)
            + faces[1][1] * at(ref, 0, -1)
            + faces[2][0] * uz[0]
            + faces[2][1] * uz[1]
            - weights * here
        )

    def strain_energy(at, u, keep, first, last):
        grad = []
        for f in range(3):
            here = at(u.at[f], 0, 0)
            uz = beside(here, 0.0, first, last)
            grad.append(
                (
                    at(u.at[f], 1, 0) - at(u.at[f], -1, 0),
                    at(u.at[f], 0, 1) - at(u.at[f], 0, -1),
                    uz[0] - uz[1],
                )
            )
            keep(f, here)
        return 2.0 * spectral_energy(
            0.5 * grad[0][0],
            0.5 * grad[1][1],
            0.5 * grad[2][2],
            0.25 * (grad[0][1] + grad[1][0]),
            0.25 * (grad[0][2] + grad[2][0]),
            0.25 * (grad[1][2] + grad[2][1]),
        )

    def renew(at, d, energy, g, cracked, first, last):
        dz = beside(at(d, 0, 0), 0.0, first, last)
        around = at(d, 1, 0) + at(d, -1, 0) + at(d, 0, 1) + at(d, 0, -1) + dz[0] + dz[1]
        renewed = (energy + g * around) / (7.0 * g + energy)
        return jnp.where(cracked, 1.0, renewed)

    def add_up(rnd, total):
        r.sums[me, rnd : rnd + 1] = jnp.sum(total, axis=0, keepdims=True)

    def open_stages(above, n):
        shape = (n, nz)
        first, last = lanes(shape, 0), lanes(shape, nz - 1)
        row_inside = inside_rows(shape, above)
        row = lax.broadcasted_iota(jnp.int32, shape, 0)
        a = OY - above

        def stiffen(xp, carry):
            half = 0.5 * (jnp.square(1.0 - crack_pad[xp, a : a + n]) + stiff_floor)
            stiff[xp, a : a + n] = half
            up, down = beside(held[xp, a : a + n], 0.0, first, last)
            div = (
                vector[0] * (held[xp + 1, a : a + n] - held[xp - 1, a : a + n])
                + vector[1] * (held[xp, a + 1 : a + 1 + n] - held[xp, a - 1 : a - 1 + n])
                + vector[2] * (up - down)
            )
            flow[xp, a : a + n] = jnp.where(
                jnp.logical_and(row_inside, inside_plane(xp)), half * div, 0.0
            )
            return carry

        def mover(low, high):
            def move(xp, total):
                at = lambda ref, dx, dy: ref[xp + dx, a + dy : a + dy + n]
                pairs, weights, faces, grads = elastic(at, first, last)
                load, spread = laplace(at, held, faces, weights, first, last)
                pin = at(clamped, 0, 0) + load > 0.5
                squares = None
                for f in range(3):
                    res = vector[f] * spread + grads[f]
                    moved = jnp.where(pin, 0.0, relax_weight * res / (weights + pairs[f]))
                    state[1, f, xp, a : a + n] = vector[f] * load + moved
                    square = res * res
                    squares = square if squares is None else squares + square
                if low >= high:
                    return total
                counted = jnp.logical_and(row >= low + above, row < high + above)
                return total + jnp.where(
                    jnp.logical_and(counted, jnp.logical_not(pin)), squares, 0.0
                )

            return move

        def damage(xp, carry):
            at = lambda ref, dx, dy: ref[xp + dx, a + dy : a + dy + n]
            energy = strain_energy(at, state.at[1], lambda f, v: None, first, last)
            renewed = renew(
                at,
                crack_pad,
                energy,
                at(tough_pad, 0, 0),
                at(crack_pad, 0, 0) > 0.5,
                first,
                last,
            )
            state[1, 3, xp, a : a + n] = jnp.where(
                jnp.logical_and(row_inside, inside_plane(xp)), renewed, 0.0
            )
            return carry

        return stiffen, mover, damage

    def open_sweep():
        def inward(skip, body, carry, most):
            n = nx - 2 * skip
            return lax.fori_loop(HX + skip, HX + nx - skip, body, carry, unroll=part(n, most))

        def outward(far, n, body, carry):
            def both(i, carry):
                carry = body(HX - far + i, carry)
                return body(HX + nx + far - n + i, carry)

            return lax.fori_loop(0, n, both, carry, unroll=True)

        blank = lambda n: jnp.zeros((n, nz), jnp.float32)
        fold = lambda v: jnp.sum(v, axis=0, keepdims=True)

        stiffen, mover, damage = open_stages(0, ny)
        inward(1, stiffen, 0, 14)
        inside = inward(2, mover(2, ny - 2), blank(ny), 12)
        inward(3, damage, 0, 5)

        if further > 1:
            pl.semaphore_wait(r.reach.at[0], near_count)
            greet(r.reach.at[1])

        def rim(s):
            above = (4, 4 - ny)[s]
            stiffen, mover, damage = open_stages(above, 8)

            def put_crack():
                for x in range(nx):
                    crack_pad[HX + x, y_out(s, 3)] = as_float(r.in_c[s, 3 * x : 3 * x + 3])

            def put_load():
                held[planes, y_out(s, 4)] = as_float(r.in_l[s])

            def put_clamp():
                clamped[planes, y_out(s, 2)] = as_float(r.in_f[s])

            def put_tough():
                tough_pad[planes, y_out(s, 1)] = r.in_ty[s]

            from_y(0, s, put_crack)
            from_y(1, s, put_load)
            inward(1, stiffen, 0, 14)
            from_y(2, s, put_clamp)
            counted = (0, 2) if s == 0 else (ny - 2, ny)
            r.rims[s] = inward(2, mover(*counted), blank(8), 12)
            from_y(3, s, put_tough)
            inward(3, damage, 0, 10)

        odd = lax.rem(gy, 2) == 1

        @pl.when(odd)
        def _():
            rim(0)
            rim(1)

        @pl.when(jnp.logical_not(odd))
        def _():
            rim(1)
            rim(0)

        stiffen1, mover1 = stages(1)
        move1 = mover1(OY, ny)
        inward(3, stiffen1, 0, 10)
        own = inward(4, move1, blank(ny), 8)

        stiffen, mover, damage = open_stages(4, deep)
        unpack_a()
        outward(1, 2, stiffen, 0)
        ends = outward(0, 2, mover(0, ny), blank(deep))
        r.sums[me, 0:1] = fold(inside) + fold(r.rims[0] + r.rims[1]) + fold(ends)
        outward(-1, 2, damage, 0)
        outward(-1, 2, stiffen1, 0)
        own = outward(-2, 2, move1, own)

        unpack_m()
        outward(2, 1, stiffen, 0)
        outward(1, 1, mover(0, 0), blank(deep))
        outward(0, 1, damage, 0)
        outward(0, 1, stiffen1, 0)
        own = outward(-1, 1, move1, own)

        unpack_b()
        outward(3, 1, stiffen, 0)
        outward(2, 1, mover(0, 0), blank(deep))
        outward(1, 1, damage, 0)
        outward(1, 1, stiffen1, 0)
        own = outward(0, 1, move1, own)

        return own

    def send_sums():
        for k in range(1 if further > 1 else 0, further):
            pl.semaphore_wait(r.reach.at[k], near_count)
            if k + 1 < further:
                greet(r.reach.at[k + 1])
        for k, peer in enumerate(peers):
            pltpu.make_async_remote_copy(
                src_ref=r.sums.at[me],
                dst_ref=r.sums.at[me],
                send_sem=r.sum_send.at[k],
                recv_sem=r.sum_recv.at[me],
                device_id=peer,
                device_id_type=MESH,
            ).start()

    def stages(rnd):
        p = rnd % 2
        q = 1 - p
        shape = (wide, nz)
        first, last = lanes(shape, 0), lanes(shape, nz - 1)
        row_inside = inside_rows(shape, 2)
        a = OY - 2

        def stiffen(xp, carry):
            half = 0.5 * (jnp.square(1.0 - state[p, 3, xp, a : a + wide]) + stiff_floor)
            stiff[xp, a : a + wide] = half
            up, down = beside(state[p, 2, xp, a : a + wide], 0.0, first, last)
            div = (
                (state[p, 0, xp + 1, a : a + wide] - state[p, 0, xp - 1, a : a + wide])
                + (state[p, 1, xp, a + 1 : a + 1 + wide] - state[p, 1, xp, a - 1 : a - 1 + wide])
                + (up - down)
            )
            flow[xp, a : a + wide] = jnp.where(
                jnp.logical_and(row_inside, inside_plane(xp)), half * div, 0.0
            )
            return carry

        def mover(b, n):
            shape = (n, nz)
            first, last = lanes(shape, 0), lanes(shape, nz - 1)

            def move(xp, total):
                at = lambda ref, dx, dy: ref[xp + dx, b + dy : b + dy + n]
                pairs, weights, faces, grads = elastic(at, first, last)
                load = at(held, 0, 0)
                pin = at(clamped, 0, 0) + load > 0.5
                squares = None
                for f in range(3):
                    here, spread = laplace(at, state.at[p, f], faces, weights, first, last)
                    res = spread + grads[f]
                    moved = here + relax_weight * res / (weights + pairs[f])
                    state[q, f, xp, b : b + n] = jnp.where(pin, load * vector[f], moved)
                    square = res * res
                    squares = square if squares is None else squares + square
                return total + jnp.where(pin, 0.0, squares)

            return move

        return stiffen, mover

    def sweep(rnd, total):
        p = rnd % 2
        q = 1 - p
        done = rnd == sections - 1
        tough = r.tough_in.at[rnd - 1]

        stiffen, mover = stages(rnd)
        if rnd > 1:
            lax.fori_loop(HX - 2, HX + nx + 2, stiffen, 0, unroll=part(nx + 4, 10))
            total = lax.fori_loop(
                HX, HX + nx, mover(OY, ny), jnp.zeros((ny, nz), jnp.float32), unroll=part(nx, 8)
            )
        add_up(rnd, total)
        if done:
            send_sums()
        par = rnd % 2
        mid = pl.ds(OY, ny)
        if done:
            rims = Exchange(r.v_send, r.v_recv)
            for s in range(2):
                row = OY if s == 0 else OY + ny - 1
                for f in range(3):
                    r.pack_v[s, f] = state[q, f, planes, row : row + 1]
                rims.add(
                    x_dev(s),
                    state.at[q, pl.ds(0, 3), HX if s == 0 else HX + nx - 1, mid],
                    r.in_vx.at[1 - s],
                    r.in_vx.at[s],
                    1 - s,
                    s,
                )
                rims.add(
                    y_dev(s), r.pack_v.at[s], r.in_vy.at[1 - s], r.in_vy.at[s], 3 - s, 2 + s
                )
            rims.start()
            rims.received()
            for s in range(2):

                @pl.when(there["gx"][s])
                def _(s=s):
                    state[q, 0:3, x_at(s, 1), inner] = r.in_vx[s]

                @pl.when(there["gy"][s])
                def _(s=s):
                    for f in range(3):
                        state[q, f, planes, y_out(s, 1)] = r.in_vy[s, f]
        else:
            for f in range(3):
                r.pack_u[0, :, 2 * f : 2 * f + 2] = state[q, f, planes, OY : OY + 2]
                r.pack_u[1, :, 2 * f : 2 * f + 2] = state[q, f, planes, OY + ny - 2 : OY + ny]
            r.pack_u[0, :, 6:7] = state[q, 1, planes, OY + 2 : OY + 3]
            r.pack_u[1, :, 6:7] = state[q, 1, planes, OY + ny - 3 : OY + ny - 2]
            shift = Exchange(r.u_send, r.u_recv.at[par])
            for s in range(2):
                shift.add(
                    x_dev(s),
                    state.at[q, pl.ds(0, 3), pl.ds(HX if s == 0 else HX + nx - 2, 2), mid],
                    r.in_u_x.at[par, 1 - s],
                    r.in_u_x.at[par, s],
                    (1 - s),
                    s,
                )
                shift.add(
                    x_dev(s),
                    state.at[q, 0, HX + 2 if s == 0 else HX + nx - 3, mid],
                    r.in_u_x3.at[par, 1 - s],
                    r.in_u_x3.at[par, s],
                    2 + (1 - s),
                    2 + s,
                )
            for s in range(2):
                shift.add(
                    y_dev(s),
                    r.pack_u.at[s],
                    r.in_u_y.at[par, 1 - s],
                    r.in_u_y.at[par, s],
                    4 + (1 - s),
                    4 + s,
                )
            for sx in range(2):
                for sy in range(2):
                    shift.add(
                        c_dev(sx, sy),
                        r.pack_u.at[sy, pl.ds(0 if sx == 0 else nx - 2, 2)],
                        r.in_u_c.at[par, (1 - sx) * 2 + 1 - sy],
                        r.in_u_c.at[par, sx * 2 + sy],
                        6 + (1 - sx) * 2 + 1 - sy,
                        6 + sx * 2 + sy,
                    )
            shift.start()
            shift.finish()
            third_x = (HX - 3, HX + nx + 2)
            third_y = (slice(OY - 3, OY - 2), slice(OY + ny + 2, OY + ny + 3))
            for s in range(2):

                @pl.when(there["gx"][s])
                def _(s=s):
                    state[q, 0:3, x_out(s, 2), inner] = r.in_u_x[par, s]
                    state[q, 0, third_x[s], inner] = r.in_u_x3[par, s]

                @pl.when(there["gy"][s])
                def _(s=s):
                    for f in range(3):
                        state[q, f, planes, y_out(s, 2)] = r.in_u_y[par, s, :, 2 * f : 2 * f + 2]
                    state[q, 1, planes, third_y[s]] = r.in_u_y[par, s, :, 6:7]

            for sx in range(2):
                for sy in range(2):

                    @pl.when(c_dev(sx, sy)[0])
                    def _(sx=sx, sy=sy):
                        for f in range(3):
                            state[q, f, x_out(sx, 2), y_out(sy, 2)] = r.in_u_c[
                                par, sx * 2 + sy, :, 2 * f : 2 * f + 2
                            ]

        tough_copies[rnd - 1].wait_recv()

        shape = (ny, nz)
        first, last = lanes(shape, 0), lanes(shape, nz - 1)

        def damage(x, carry):
            xp = x + HX
            at = lambda ref, dx, dy: ref[xp + dx, OY + dy : OY + dy + ny]

            def keep(f, here):
                if done:
                    disp_refs[f][x] = here

            energy = strain_energy(at, state.at[q], keep, first, last)
            renewed = renew(
                at, state.at[p, 3], energy, tough[x], crack_ref[x] > 0, first, last
            )
            if done:
                r.dam_ref[x] = renewed
            else:
                state[q, 3, xp, inner] = renewed
            return carry

        lax.fori_loop(0, nx, damage, 0, unroll=part(nx, 8))
        if done:
            rims.sent()
            return

        r.pack_d[0] = state[q, 3, planes, OY : OY + 2]
        r.pack_d[1] = state[q, 3, planes, OY + ny - 2 : OY + ny]
        crack = Exchange(r.d_send, r.d_recv.at[par])
        for s in range(2):
            crack.add(
                x_dev(s),
                state.at[q, 3, pl.ds(HX if s == 0 else HX + nx - 2, 2), mid],
                r.in_d_x.at[par, 1 - s],
                r.in_d_x.at[par, s],
                1 - s,
                s,
            )
        for s in range(2):
            crack.add(
                y_dev(s),
                r.pack_d.at[s],
                r.in_d_y.at[par, 1 - s],
                r.in_d_y.at[par, s],
                2 + 1 - s,
                2 + s,
            )
        for sx in range(2):
            for sy in range(2):
                crack.add(
                    c_dev(sx, sy),
                    r.pack_d.at[sy, pl.ds(0 if sx == 0 else nx - 1, 1)],
                    r.in_d_c.at[par, (1 - sx) * 2 + 1 - sy],
                    r.in_d_c.at[par, sx * 2 + sy],
                    4 + (1 - sx) * 2 + 1 - sy,
                    4 + sx * 2 + sy,
                )
        crack.start()
        crack.finish()
        for s in range(2):

            @pl.when(there["gx"][s])
            def _(s=s):
                state[q, 3, x_out(s, 2), inner] = r.in_d_x[par, s]

            @pl.when(there["gy"][s])
            def _(s=s):
                state[q, 3, planes, y_out(s, 2)] = r.in_d_y[par, s]

        for sx in range(2):
            for sy in range(2):

                @pl.when(c_dev(sx, sy)[0])
                def _(sx=sx, sy=sy):
                    state[q, 3, x_out(sx, 1), y_out(sy, 2)] = r.in_d_c[par, sx * 2 + sy]

    total = open_sweep()
    for rnd in range(1, sections):
        sweep(rnd, total)

    beside_y.sent()
    part_a.sent()
    part_m.sent()
    part_b.sent()
    for copy in tough_copies:
        copy.wait_send()
    for k, peer in enumerate(peers):
        other = peer["gx"] * ngy + peer["gy"]
        pltpu.make_async_remote_copy(
            src_ref=r.sums.at[me],
            dst_ref=r.sums.at[other],
            send_sem=r.sum_send.at[k],
            recv_sem=r.sum_recv.at[other],
            device_id=peer,
            device_id_type=MESH,
        ).wait()
    total = r.sums[0]
    for k in range(1, group):
        total = total + r.sums[k]
    r.total_ref[...] = total


def put_out(
    sizes,
    first_ref,
    second_ref,
    third_ref,
    dam_ref,
    total_ref,
    disp_hbm,
    dam_hbm,
    norm_hbm,
    norm_ref,
    sems,
):
    sections, ngx, ngy, nx, ny, nz = sizes
    copies = [
        pltpu.make_async_copy(ref, disp_hbm.at[0, f], sems.at[f])
        for f, ref in enumerate((first_ref, second_ref, third_ref))
    ]
    copies.append(pltpu.make_async_copy(dam_ref, dam_hbm.at[0], sems.at[3]))
    for copy in copies:
        copy.start()
    sec = lax.axis_index("section")
    cells = 3.0 * nx * ngx * ny * ngy * nz
    entries = jnp.sqrt(jnp.sum(total_ref[...], axis=1, keepdims=True) / cells)
    column = lax.broadcasted_iota(jnp.int32, (1, sections), 1)
    norms = jnp.zeros((1, sections), jnp.float32)
    for rnd in range(sections):
        norms = jnp.where(
            column == lax.rem(sec + rnd, sections), entries[rnd : rnd + 1], norms
        )
    norm_ref[...] = norms
    last = pltpu.make_async_copy(norm_ref, norm_hbm, sems.at[4])
    last.start()
    for copy in copies:
        copy.wait()
    last.wait()


def on_device(sizes, load_index, load_table, toughness, clamp_mask, load_mask, crack_mask):
    sections, ngx, ngy = sizes
    nx, ny, nz = clamp_mask.shape
    assert load_index.shape == (1,)
    group = ngx * ngy
    f32 = jnp.float32
    padded = (nx + 2 * HX, ny + 2 * OY, nz)
    vmem = pltpu.VMEM
    dma = pltpu.SemaphoreType.DMA
    later = max(sections - 1, 1)
    more = sections > 2
    scratch = {
        "index_ref": pltpu.SMEM(load_index.shape, jnp.int32),
        "table_ref": pltpu.SMEM(load_table.shape[::-1], f32),
        "tough_ref": vmem((1, nx, ny, nz), f32),
        "clamp_ref": vmem((nx, ny, nz), jnp.int32),
        "load_ref": vmem((nx, ny, nz), jnp.int32),
        "crack_ref": vmem((nx, ny, nz), jnp.int32),
        "local": dma((6,)),
        "state": vmem((2, 4) + padded, f32),
        "stiff": vmem(padded, f32),
        "flow": vmem(padded, f32),
        "held": vmem(padded, f32),
        "clamped": vmem(padded, f32),
        "tough_pad": vmem(padded, f32),
        "crack_pad": vmem(padded, f32),
        "tough_in": vmem((later, nx, ny, nz), f32),
        "pack_l": vmem((2, nx, 4, nz), jnp.int32),
        "pack_f": vmem((2, nx, 2, nz), jnp.int32),
        "pack_c": vmem((2, 3 * nx, nz), jnp.int32),
        "pack_t": vmem((2, nx, 1, nz), f32),
        "pack_k": vmem((4, 16, nz), jnp.int32),
        "in_a": vmem((2, 3, ny, nz), jnp.int32),
        "in_m": vmem((2, 3, ny, nz), jnp.int32),
        "in_b": vmem((2, 3, ny, nz), jnp.int32),
        "in_tx": vmem((2, 1, ny, nz), f32),
        "in_l": vmem((2, nx, 4, nz), jnp.int32),
        "in_f": vmem((2, nx, 2, nz), jnp.int32),
        "in_c": vmem((2, 3 * nx, nz), jnp.int32),
        "in_ty": vmem((2, nx, 1, nz), f32),
        "in_k": vmem((4, 16, nz), jnp.int32),
        "rims": vmem((2, 8, nz), f32),
        "pack_v": vmem((2, 3, nx, 1, nz), f32),
        "in_vx": vmem((2, 3, ny, nz), f32),
        "in_vy": vmem((2, 3, nx, 1, nz), f32),
        "v_send": dma((4,)),
        "v_recv": dma((4,)),
        "sums": vmem((group, sections, nz), f32),
        "y_send": dma((8,)),
        "y_recv": dma((8,)),
        "a_send": dma((8,)),
        "a_recv": dma((8,)),
        "m_send": dma((6,)),
        "m_recv": dma((6,)),
        "b_send": dma((8,)),
        "b_recv": dma((8,)),
        "reach": pltpu.SemaphoreType.REGULAR((max(max(ngx, ngy) - 2, 1),)),
        "tough_send": dma((later,)),
        "tough_recv": dma((later,)),
        "sum_send": dma((max(group - 1, 1),)),
        "sum_recv": dma((group,)),
    }
    if more:
        scratch |= {
            "pack_u": vmem((2, nx, 8, nz), f32),
            "pack_d": vmem((2, nx, 2, nz), f32),
            "in_u_x": vmem((2, 2, 3, 2, ny, nz), f32),
            "in_u_x3": vmem((2, 2, ny, nz), f32),
            "in_u_y": vmem((2, 2, nx, 8, nz), f32),
            "in_u_c": vmem((2, 4, 2, 8, nz), f32),
            "in_d_x": vmem((2, 2, 2, ny, nz), f32),
            "in_d_y": vmem((2, 2, nx, 2, nz), f32),
            "in_d_c": vmem((2, 4, 1, 2, nz), f32),
            "u_send": dma((10,)),
            "u_recv": dma((2, 10)),
            "d_send": dma((8,)),
            "d_recv": dma((2, 8)),
        }
    ins = ("index_hbm", "table_hbm", "tough_hbm", "clamp_hbm", "load_hbm", "crack_hbm")
    outs = ("first_ref", "second_ref", "third_ref", "dam_ref", "total_ref")
    names = (*ins, *outs, *scratch)
    block = pl.BlockSpec(memory_space=pltpu.VMEM)
    away = pl.BlockSpec(memory_space=pltpu.HBM)
    results = pl.pallas_call(
        functools.partial(kernel, (sections, ngx, ngy, nx, ny, nz), names),
        out_shape=(
            *[jax.ShapeDtypeStruct((nx, ny, nz), f32)] * 4,
            jax.ShapeDtypeStruct((sections, nz), f32),
        ),
        in_specs=[away] * 6,
        out_specs=(block,) * 5,
        scratch_shapes=list(scratch.values()),
        compiler_params=pltpu.CompilerParams(
            collective_id=0, has_side_effects=True, vmem_limit_bytes=56_020_000
        ),
    )(load_index, pltpu.with_memory_space_constraint(load_table.T, pltpu.HBM), toughness, clamp_mask, load_mask, crack_mask)
    return pl.pallas_call(
        functools.partial(put_out, (sections, ngx, ngy, nx, ny, nz)),
        out_shape=(
            jax.ShapeDtypeStruct((1, 3, nx, ny, nz), f32),
            jax.ShapeDtypeStruct((1, nx, ny, nz), f32),
            jax.ShapeDtypeStruct((1, sections), f32),
        ),
        in_specs=[block] * 5,
        out_specs=(away, away, away),
        scratch_shapes=[vmem((1, sections), f32), dma((5,))],
        compiler_params=pltpu.CompilerParams(vmem_limit_bytes=1024 * 1024),
    )(*results)


def solution(mesh):
    in_specs = (
        P("section"),
        P(),
        P("section", "gx", "gy", None),
        P("gx", "gy", None),
        P("gx", "gy", None),
        P("gx", "gy", None),
    )
    out_specs = (
        P("section", None, "gx", "gy", None),
        P("section", "gx", "gy", None),
        P("section", None),
    )
    sizes = tuple(mesh.shape[name] for name in ("section", "gx", "gy"))
    return jax.shard_map(
        functools.partial(on_device, sizes),
        mesh=mesh,
        in_specs=in_specs,
        out_specs=out_specs,
        check_vma=False,
    )
```
